32 devices in a mesh: seg: 8 (over z, x), seq: 4 (over y, core).
Axes of the slice: x: 2, y: 2, z: 4, core: 2. Of those that a mesh axis runs over, the one named last changes fastest.
Arguments:
- tokens: bfloat16 [8, 1024, 2048], P('seg', 'seq'), may hold values from -6 to 6
- norm_gain: bfloat16 [2048], P(('seg', 'seq')), may hold values from 0.5 to 1.5
- in_proj: bfloat16 [2048, 8192], P(('seg', 'seq')), may hold values from -0.125 to 0.125
- conv_weight: bfloat16 [4, 4096], P(None, ('seg', 'seq')), may hold values from -3 to 3
- conv_bias: bfloat16 [4096], P(('seg', 'seq')), may hold values from -3 to 3
- x_proj: bfloat16 [4096, 160], P(('seg', 'seq')), may hold values from -0.09375 to 0.09375
- dt_proj: bfloat16 [128, 4096], P(None, ('seg', 'seq')), may hold values from -0.5 to 0.5
- dt_bias: bfloat16 [4096], P(('seg', 'seq')), may hold values from -16 to 0
- a_log: bfloat16 [16, 4096], P(None, ('seg', 'seq')), may hold values from 0 to 2.765625
- d_skip: bfloat16 [4096], P(('seg', 'seq')), may hold values from 0.5 to 1.5
- out_proj: bfloat16 [4096, 2048], P(('seg', 'seq')), may hold values from -0.375 to 0.375
- init_state: float32 [8, 16, 4096], P('seg'), may hold values from -6 to 6
- init_conv: float32 [8, 3, 4096], P('seg'), may hold values from -6 to 6
- cotangent: bfloat16 [8, 1024, 2048], P('seg', 'seq'), may hold values from -6 to 6
Outputs:
- mixed: bfloat16 [8, 1024, 2048], P('seg', 'seq')
- final_state: float32 [8, 16, 4096], P('seg', None, 'seq')
- final_conv: float32 [8, 3, 4096], P('seg', None, 'seq')
- input_grad: bfloat16 [8, 1024, 2048], P('seg', 'seq')
- init_state_grad: float32 [8, 16, 4096], P('seg', None, 'seq')
- init_conv_grad: float32 [8, 3, 4096], P('seg', None, 'seq')
- gain_grad: float32 [2048], P(('seg', 'seq'))
- in_proj_grad: float32 [2048, 8192], P(('seg', 'seq'))
- conv_weight_grad: float32 [4, 4096], P(None, ('seg', 'seq'))
- conv_bias_grad: float32 [4096], P(('seg', 'seq'))
- x_proj_grad: float32 [4096, 160], P(('seg', 'seq'))
- dt_proj_grad: float32 [128, 4096], P(None, ('seg', 'seq'))
- dt_bias_grad: float32 [4096], P(('seg', 'seq'))
- a_log_grad: float32 [16, 4096], P(None, ('seg', 'seq'))
- d_skip_grad: float32 [4096], P(('seg', 'seq'))
- out_proj_grad: float32 [4096, 2048], P(('seg', 'seq'))
The draws below stay inside these ranges and needn't reach their ends.
All inputs are finite; a program needn't handle non-finite values.
Results may differ from the reference program's by a relative error of at most 0.0095.
Values may be sent and summed in bfloat16 or wider, within the bound.
A program may use at most 320 MiB of HBM per device.

```python
import math
import jax
import jax.numpy as jnp
from jax import lax

D = 2048
DI = 4096
N = 16
R = 128
K = 4
LENGTH = 1024
SEGS = 8


def draw_dt_bias(key, part):
    spread = jax.random.uniform(key, (DI,), jnp.float32, math.log(0.05), math.log(20.0))
    base_rate = jnp.exp(spread) / LENGTH
    return jnp.log(jnp.expm1(base_rate)).astype(jnp.bfloat16)


def steps_of(stream_key, extent, split, low, high):
    def one(position, parts):
        heights = jax.random.uniform(jax.random.fold_in(jax.random.fold_in(stream_key, 6), position), (parts,), jnp.float32, low / len(split), high / len(split))
        return jnp.repeat(jnp.exp(heights), extent[position] // parts).reshape((-1,) + (1,) * (len(extent) - position - 1))

    gain = one(*split[0])
    for cut in split[1:]:
        gain = gain * one(*cut)
    return gain


def normal_values(key, dims, width, most, shards=(), held_as=jnp.bfloat16):
    drawn = jax.random.normal(key, dims, jnp.float32) * width
    if len(shards) > 0:
        drawn = steps_of(key, dims, shards, -0.22, 0.18) * drawn
    return jnp.clip(drawn, min=-most, max=most).astype(held_as)


def setup_inputs(seed: int = 0) -> dict:
    key_list = jax.random.split(jax.random.key(seed), 15)
    tokens = normal_values(key_list[0], (SEGS, LENGTH, D), 1.0, 6.0, ((0, 8), (1, 4)))
    norm_gain = jnp.clip(1.0 + 0.1 * jax.random.normal(key_list[1], (D,), jnp.float32), 0.5, 1.5).astype(jnp.bfloat16)
    in_proj = normal_values(key_list[2], (D, 2 * DI), D ** -0.5, 0.125, ((0, 32),))
    conv_weight = normal_values(key_list[3], (K, DI), K ** -0.5, 3.0, ((1, 32),))
    conv_bias = normal_values(key_list[4], (DI,), 0.5, 3.0, ((0, 32),))
    x_proj = normal_values(key_list[5], (DI, R + 2 * N), DI ** -0.5, 0.09375, ((0, 32),))
    dt_proj = normal_values(key_list[6], (R, DI), R ** -0.5, 0.5, ((1, 32),))
    dt_bias = draw_dt_bias(jax.random.fold_in(key_list[14], 71), 0)
    a_log = jnp.clip(2.765625 * jax.random.uniform(key_list[8], (N, DI), jnp.float32) ** steps_of(key_list[8], (N, DI), ((1, 32),), -0.2, 0.2), 0.0, 2.765625).astype(jnp.bfloat16)
    d_skip = jnp.clip(0.5 + 1.0 * jax.random.uniform(key_list[9], (DI,), jnp.float32) ** steps_of(key_list[9], (DI,), ((0, 32),), -0.2, 0.2), 0.5, 1.5).astype(jnp.bfloat16)
    out_proj = normal_values(key_list[10], (DI, D), (DI // 16) ** -0.5, 0.375, ((0, 32),))
    init_state = normal_values(key_list[11], (SEGS, N, DI), 1.0, 6.0, ((0, 8),), jnp.float32)
    init_conv = normal_values(key_list[12], (SEGS, K - 1, DI), 1.0, 6.0, ((0, 8),), jnp.float32)
    cotangent = normal_values(key_list[13], (SEGS, LENGTH, D), 1.0, 6.0, ((0, 8), (1, 4)))
    return {"tokens": tokens, "norm_gain": norm_gain, "in_proj": in_proj, "conv_weight": conv_weight, "conv_bias": conv_bias, "x_proj": x_proj, "dt_proj": dt_proj, "dt_bias": dt_bias, "a_log": a_log, "d_skip": d_skip, "out_proj": out_proj, "init_state": init_state, "init_conv": init_conv, "cotangent": cotangent}


EPSILON = 1e-05
PRECISE = lax.Precision.HIGHEST

@jax.custom_vjp
def low(v):
    return lax.optimization_barrier(v.astype(jnp.bfloat16)).astype(jnp.float32)

@jax.custom_vjp
def low_back(v):
    return v

def low_keep(v):
    return (low(v), None)

def low_pass(kept, grad):
    return (grad,)

def back_keep(v):
    return (v, None)

def back_low(kept, grad):
    return (low(grad),)
low.defvjp(low_keep, low_pass)
low_back.defvjp(back_keep, back_low)

def matmul(first_op, second_op):
    return jnp.dot(first_op, second_op, precision=PRECISE, preferred_element_type=jnp.float32)

def scan_states(start_state, rate_rows, value_rows, b_rows, c_rows, a_mat):
    length = rate_rows.shape[0]
    block_len = math.gcd(length, 64)

    def scan_token(carry_state, row_items):
        rate_row, value_row, b_row, c_row = row_items
        carry_state = jnp.exp(rate_row[None, :] * a_mat) * carry_state + b_row[:, None] * (rate_row * value_row)[None, :]
        return (carry_state, lax.optimization_barrier(jnp.sum(c_row[:, None] * carry_state, axis=0)))

    def scan_block(carry_state, block_items):
        return lax.scan(scan_token, carry_state, block_items)
    shaped = tuple((v.reshape((length // block_len, block_len) + v.shape[1:]) for v in (rate_rows, value_rows, b_rows, c_rows)))
    final_state, outputs = lax.scan(jax.checkpoint(scan_block), start_state, shaped)
    return (final_state, outputs.reshape(rate_rows.shape))

def layer(weight_set, tokens_seg, state_init, conv_init):
    gain_vec, w_in, w_conv, b_conv, w_x, w_dt, b_dt, log_a, skip_vec, w_out = weight_set
    length = tokens_seg.shape[0]
    rstd_col = lax.rsqrt(lax.optimization_barrier(jnp.mean(tokens_seg * tokens_seg, axis=1, keepdims=True)) + EPSILON)
    normed = low(tokens_seg * rstd_col * gain_vec)
    projected = low_back(matmul(normed, w_in))
    inner_width = w_out.shape[0]
    x_in = projected[:, :inner_width]
    gate_in = projected[:, inner_width:]
    padded = jnp.concatenate([conv_init, x_in], axis=0)
    tap_count = w_conv.shape[0]
    conv_out = b_conv + sum((w_conv[k] * padded[k:k + length] for k in range(tap_count)))
    activated = low(jax.nn.silu(conv_out))
    mixed_x = low_back(matmul(activated, w_x))
    low_rank = w_dt.shape[0]
    state_width = log_a.shape[0]
    dt_low = low(mixed_x[:, :low_rank])
    b_mat = mixed_x[:, low_rank:low_rank + state_width]
    c_mat = mixed_x[:, low_rank + state_width:]
    dt_pre = low_back(matmul(dt_low, w_dt) + b_dt)
    rate_rows = jax.nn.softplus(dt_pre)
    a_mat = -jnp.exp(log_a)
    final_state, scanned = scan_states(state_init, rate_rows, activated, b_mat, c_mat, a_mat)
    y_val = scanned + skip_vec * activated
    gated = low(y_val * jax.nn.silu(gate_in))
    output = matmul(gated, w_out) + tokens_seg
    return (output, final_state, x_in[length - (tap_count - 1):])

def reference(tokens, norm_gain, in_proj, conv_weight, conv_bias, x_proj, dt_proj, dt_bias, a_log, d_skip, out_proj, init_state, init_conv, cotangent):
    weights = tuple((w.astype(jnp.float32) for w in (norm_gain, in_proj, conv_weight, conv_bias, x_proj, dt_proj, dt_bias, a_log, d_skip, out_proj)))

    def one_segment(grad_sums, seg_items):
        tokens_seg, state_init, conv_init, cot_seg = seg_items
        primal, pullback = jax.vjp(layer, weights, tokens_seg.astype(jnp.float32), state_init, conv_init)
        output, final_state, final_conv = primal
        g_weights, g_tokens, g_state, g_conv = pullback((cot_seg.astype(jnp.float32), jnp.zeros_like(final_state), jnp.zeros_like(final_conv)))
        grad_sums = tuple((a + b for a, b in zip(grad_sums, g_weights)))
        return (grad_sums, (output.astype(jnp.bfloat16), final_state, final_conv, g_tokens.astype(jnp.bfloat16), g_state, g_conv))
    zero_sums = tuple((jnp.zeros_like(w) for w in weights))
    grad_sums, per_seg = lax.scan(one_segment, zero_sums, (tokens, init_state, init_conv, cotangent))
    return (per_seg[0], per_seg[1], per_seg[2], per_seg[3], per_seg[4], per_seg[5], grad_sums[0], grad_sums[1], grad_sums[2], grad_sums[3], grad_sums[4], grad_sums[5], grad_sums[6], grad_sums[7], grad_sums[8], grad_sums[9])
```

```python
import functools

import jax
import jax.numpy as jnp
from jax import lax
from jax.experimental import pallas as pl
from jax.experimental.pallas import tpu as pltpu
from jax.sharding import PartitionSpec as P

EPSILON = 1e-05
LOG2E = 1.4426950408889634
LANES = 128
UNROLL = 8
F32 = jnp.float32
BF16 = jnp.bfloat16


def sigmoid(v):
    return 1.0 / (1.0 + jnp.exp(-v))


def softplus(v):
    return jnp.maximum(v, 0.0) + jnp.log1p(jnp.exp(-jnp.abs(v)))


def to_planes(planes_ref, rows):
    count = rows.shape[0]
    for s in range(rows.shape[1] // LANES):
        planes_ref[pl.ds(s * count, count), :] = rows[:, s * LANES : (s + 1) * LANES]


def from_planes(planes_ref, count, planes):
    return jnp.concatenate(
        [planes_ref[pl.ds(s * count, count), :] for s in range(planes)], axis=1
    )


def forward_kernel(
    pre_ref, act_ref, gate_ref, bc_ref, a_ref, skip_ref, init_ref,
    y_ref, gated_ref, check_ref, final_ref,
    state, rate_pl, drive_pl, y_pl,
):
    count = pre_ref.shape[0]
    width, planes, _ = a_ref.shape

    @pl.when(pl.program_id(0) == 0)
    def _():
        state[...] = init_ref[...]

    rate = softplus(pre_ref[...])
    act = act_ref[...].astype(F32)
    to_planes(rate_pl, rate)
    to_planes(drive_pl, rate * act)

    def group(k, carry):
        first = k * UNROLL
        rates = [rate_pl[pl.ds(first + i, planes, stride=count), :] for i in range(UNROLL)]
        drives = [drive_pl[pl.ds(first + i, planes, stride=count), :] for i in range(UNROLL)]
        sums = [None] * UNROLL
        for n in range(width):
            a = a_ref[n]
            h = state[n]
            check_ref[k, n] = h
            for i in range(UNROLL):
                h = jnp.exp2(rates[i] * a) * h + bc_ref[first + i, n] * drives[i]
                term = bc_ref[first + i, width + n] * h
                sums[i] = term if n == 0 else sums[i] + term
            state[n] = h
        for i in range(UNROLL):
            y_pl[pl.ds(first + i, planes, stride=count), :] = sums[i]
        return carry

    lax.fori_loop(0, count // UNROLL, group, 0)
    y_val = from_planes(y_pl, count, planes) + skip_ref[...] * act
    gate = gate_ref[...]
    y_ref[...] = y_val
    gated_ref[...] = (y_val * gate * sigmoid(gate)).astype(BF16)

    @pl.when(pl.program_id(0) == pl.num_programs(0) - 1)
    def _():
        final_ref[...] = state[...]


def backward_kernel(
    pre_ref, act_ref, gy_ref, bc_ref, a_ref, skip_ref, check_ref,
    gdt_ref, gact_ref, gbc_ref, agrad_ref, start_ref, dtb_ref, sgrad_ref,
    carry_s, rate_pl, drive_pl, gy_pl, grate_pl, thr_pl, prod, part,
):
    count = pre_ref.shape[0]
    width, planes, _ = a_ref.shape

    @pl.when(pl.program_id(0) == 0)
    def _():
        carry_s[...] = jnp.zeros_like(carry_s)
        agrad_ref[...] = jnp.zeros_like(agrad_ref)
        dtb_ref[...] = jnp.zeros_like(dtb_ref)
        sgrad_ref[...] = jnp.zeros_like(sgrad_ref)

    pre = pre_ref[...]
    rate = softplus(pre)
    act = act_ref[...].astype(F32)
    gy = gy_ref[...]
    to_planes(rate_pl, rate)
    to_planes(drive_pl, rate * act)
    to_planes(gy_pl, gy)
    groups = count // UNROLL

    def group(j, carry):
        k = groups - 1 - j
        first = k * UNROLL
        rates = [rate_pl[pl.ds(first + i, planes, stride=count), :] for i in range(UNROLL)]
        drives = [drive_pl[pl.ds(first + i, planes, stride=count), :] for i in range(UNROLL)]
        gys = [gy_pl[pl.ds(first + i, planes, stride=count), :] for i in range(UNROLL)]
        g_rate = [None] * UNROLL
        through = [None] * UNROLL
        for n in range(width):
            a = a_ref[n]
            states = [check_ref[k, n]]
            decays = []
            for i in range(UNROLL):
                decays.append(jnp.exp2(rates[i] * a))
                states.append(decays[i] * states[i] + bc_ref[first + i, n] * drives[i])
            lam = carry_s[n]
            acc = agrad_ref[n]
            for i in reversed(range(UNROLL)):
                lam = lam + bc_ref[first + i, width + n] * gys[i]
                b_term = bc_ref[first + i, n] * lam
                prod[pl.ds((i * 2 * width + n) * planes, planes), :] = lam * drives[i]
                prod[pl.ds((i * 2 * width + width + n) * planes, planes), :] = (
                    states[i + 1] * gys[i]
                )
                lam = decays[i] * lam
                weighted = lam * states[i]
                acc = acc + weighted * rates[i]
                a_term = weighted * a
                g_rate[i] = a_term if n == 0 else g_rate[i] + a_term
                through[i] = b_term if n == 0 else through[i] + b_term
            carry_s[n] = lam
            agrad_ref[n] = acc
        for i in range(UNROLL):
            grate_pl[pl.ds(first + i, planes, stride=count), :] = g_rate[i]
            thr_pl[pl.ds(first + i, planes, stride=count), :] = through[i]
            for q in range(2 * width // 8):
                base = (i * 2 * width + q * 8) * planes
                total = prod[pl.ds(base, 8, stride=planes), :]
                for s in range(1, planes):
                    total = total + prod[pl.ds(base + s, 8, stride=planes), :]
                row = pl.multiple_of((first + i) * 2 * width + q * 8, 8)
                part[pl.ds(row, 8), :] = total
        return carry

    lax.fori_loop(0, groups, group, 0)
    g_rate = from_planes(grate_pl, count, planes) * (1.0 / LOG2E)
    through = from_planes(thr_pl, count, planes)
    g_dtpre = ((g_rate + act * through) * sigmoid(pre)).astype(BF16)
    gdt_ref[...] = g_dtpre
    gact_ref[...] = gy * skip_ref[...] + rate * through
    dtb_ref[...] += jnp.sum(g_dtpre.astype(F32), axis=0, keepdims=True)
    sgrad_ref[...] += jnp.sum(gy * act, axis=0, keepdims=True)
    rows = 2 * width
    ones = jnp.ones((LANES, LANES), F32)
    sums = jnp.dot(part[...], ones, preferred_element_type=F32)
    sums = sums.reshape(count, rows, LANES)
    pick = lax.broadcasted_iota(jnp.int32, (1, rows, LANES), 1) == lax.broadcasted_iota(
        jnp.int32, (1, rows, LANES), 2
    )
    gbc_ref[...] = jnp.sum(jnp.where(pick, sums, 0.0), axis=1)

    @pl.when(pl.program_id(0) == pl.num_programs(0) - 1)
    def _():
        start_ref[...] = carry_s[...]


def forward_scan(pre, act, gate, bc, a2, skip, init, block):
    length, features = pre.shape
    width, planes, _ = a2.shape
    steps = length // block
    rows = pl.BlockSpec((block, features), lambda i: (i, 0))
    whole = pl.BlockSpec((width, planes, LANES), lambda i: (0, 0, 0))
    plane = pltpu.VMEM((planes * block, LANES), F32)
    return pl.pallas_call(
        forward_kernel,
        grid=(steps,),
        in_specs=[
            rows, rows, rows,
            pl.BlockSpec((block, 2 * width), lambda i: (i, 0), memory_space=pltpu.SMEM),
            whole,
            pl.BlockSpec((1, features), lambda i: (0, 0)),
            whole,
        ],
        out_specs=[
            rows, rows,
            pl.BlockSpec((block // UNROLL, width, planes, LANES), lambda i: (i, 0, 0, 0)),
            whole,
        ],
        out_shape=[
            jax.ShapeDtypeStruct((length, features), F32),
            jax.ShapeDtypeStruct((length, features), BF16),
            jax.ShapeDtypeStruct((length // UNROLL, width, planes, LANES), F32),
            jax.ShapeDtypeStruct((width, planes, LANES), F32),
        ],
        scratch_shapes=[pltpu.VMEM((width, planes, LANES), F32), plane, plane, plane],
        cost_estimate=pl.CostEstimate(
            flops=8 * length * features * width,
            bytes_accessed=24 * length * features,
            transcendentals=length * features * width,
        ),
        name="scan_forward",
    )(pre, act, gate, bc, a2, skip, init)


def backward_scan(pre, act, gy, bc, a2, skip, checks, block):
    length, features = pre.shape
    width, planes, _ = a2.shape
    steps = length // block
    rows = pl.BlockSpec((block, features), lambda i: (steps - 1 - i, 0))
    whole = pl.BlockSpec((width, planes, LANES), lambda i: (0, 0, 0))
    line = pl.BlockSpec((1, features), lambda i: (0, 0))
    plane = pltpu.VMEM((planes * block, LANES), F32)
    return pl.pallas_call(
        backward_kernel,
        grid=(steps,),
        in_specs=[
            rows, rows, rows,
            pl.BlockSpec(
                (block, 2 * width), lambda i: (steps - 1 - i, 0), memory_space=pltpu.SMEM
            ),
            whole, line,
            pl.BlockSpec(
                (block // UNROLL, width, planes, LANES), lambda i: (steps - 1 - i, 0, 0, 0)
            ),
        ],
        out_specs=[
            rows, rows,
            pl.BlockSpec((block, LANES), lambda i: (steps - 1 - i, 0)),
            whole, whole, line, line,
        ],
        out_shape=[
            jax.ShapeDtypeStruct((length, features), BF16),
            jax.ShapeDtypeStruct((length, features), F32),
            jax.ShapeDtypeStruct((length, LANES), F32),
            jax.ShapeDtypeStruct((width, planes, LANES), F32),
            jax.ShapeDtypeStruct((width, planes, LANES), F32),
            jax.ShapeDtypeStruct((1, features), F32),
            jax.ShapeDtypeStruct((1, features), F32),
        ],
        scratch_shapes=[pltpu.VMEM((width, planes, LANES), F32)]
        + [plane] * 5
        + [
            pltpu.VMEM((UNROLL * 2 * width * planes, LANES), F32),
            pltpu.VMEM((block * 2 * width, LANES), F32),
        ],
        cost_estimate=pl.CostEstimate(
            flops=20 * length * features * width,
            bytes_accessed=28 * length * features,
            transcendentals=length * features * width,
        ),
        name="scan_backward",
    )(pre, act, gy, bc, a2, skip, checks)


def dot_nn(a, b):
    return jnp.dot(a, b, preferred_element_type=F32)


def dot_tn(a, b):
    return lax.dot_general(a, b, (((0,), (0,)), ((), ())), preferred_element_type=F32)


def dot_nt(a, b):
    return lax.dot_general(a, b, (((1,), (1,)), ((), ())), preferred_element_type=F32)


def body(
    tokens, norm_gain, in_proj, conv_weight, conv_bias, x_proj, dt_proj, dt_bias,
    a_log, d_skip, out_proj, init_state, init_conv, cotangent,
):
    segs, seqs = lax.axis_size("seg"), lax.axis_size("seq")
    place = lax.axis_index("seq")
    own_rows, both = in_proj.shape
    part = conv_bias.shape[0]
    feats = segs * part
    taps = conv_weight.shape[0]
    width = a_log.shape[0]
    low_rank = dt_proj.shape[0]
    planes = feats // LANES
    own_len, model = tokens.shape[1:]
    length = own_len * seqs
    block = 64

    def mine(rows):
        shaped = rows.reshape(rows.shape[0], segs, seqs, part)
        return lax.dynamic_index_in_dim(shaped, place, 2, keepdims=False).reshape(
            rows.shape[0], feats
        )

    def to_contiguous(rows):
        count = rows.shape[0]
        shaped = rows.reshape(count, seqs, (segs // seqs) * part)
        got = lax.all_to_all(shaped, "seq", 1, 0, tiled=False)
        return (
            got.reshape(seqs, count, segs // seqs, part)
            .transpose(1, 2, 0, 3)
            .reshape(count, feats)
        )

    gain_col = norm_gain.astype(F32)[:, None]
    own_weight = in_proj.astype(F32)
    scaled = (own_weight * gain_col).astype(BF16)
    scaled = scaled.reshape(own_rows, 2, segs, seqs, part).transpose(3, 1, 0, 2, 4)
    scaled = scaled.reshape(seqs, 2, own_rows, feats)
    swapped = lax.all_to_all(scaled, "seq", 0, 0, tiled=False)
    w_x_half = lax.all_gather(
        swapped[:, 0].reshape(seqs * own_rows, feats), "seg", axis=0, tiled=True
    )
    tok = lax.all_gather(tokens[0], "seq", axis=0, tiled=True)
    small = jnp.concatenate(
        [
            dt_proj, x_proj.T, a_log, conv_weight, conv_bias[None], dt_bias[None], d_skip[None],
        ],
        axis=0,
    )
    small_all = lax.all_gather(small, "seg", axis=0, tiled=False)
    w_g_half = lax.all_gather(
        swapped[:, 1].reshape(seqs * own_rows, feats), "seg", axis=0, tiled=True
    )
    w_out = lax.all_gather(out_proj, "seg", axis=0, tiled=True)
    cot = lax.all_gather(cotangent[0], "seq", axis=0, tiled=True)

    small_all = small_all.transpose(1, 0, 2).reshape(small.shape[0], feats)
    w_dt = small_all[:low_rank]
    w_xt = small_all[low_rank : low_rank + x_proj.shape[1]]
    rest = small_all[low_rank + x_proj.shape[1] :].astype(F32)
    a_mat = -jnp.exp(rest[:width])
    a2 = (a_mat * LOG2E).reshape(width, planes, LANES)
    kernel = rest[width : width + taps]
    b_conv = rest[width + taps][None]
    b_dt = rest[width + taps + 1][None]
    skip = rest[width + taps + 2][None]

    tok_float = tok.astype(F32)
    rstd = lax.rsqrt(jnp.mean(tok_float * tok_float, axis=1, keepdims=True) + EPSILON)
    x_in = rstd * dot_nn(tok, w_x_half)
    history = init_conv.shape[1]
    head = mine(init_conv[0])
    padded = jnp.concatenate([head, x_in], axis=0)
    conv_out = b_conv + sum(kernel[k] * padded[k : k + length] for k in range(taps))
    act = jax.nn.silu(conv_out).astype(BF16)
    mixed_x = lax.psum(dot_nt(act, w_xt), "seq")
    dt_low = mixed_x[:, :low_rank].astype(BF16)
    bc = mixed_x[:, low_rank:]
    pre = dot_nn(dt_low, w_dt) + b_dt
    gate = rstd * dot_nn(tok, w_g_half)
    init = mine(init_state[0]).reshape(width, planes, LANES)
    y_val, gated, checks, final = forward_scan(pre, act, gate, bc, a2, skip, init, block)
    out_part = dot_nn(gated, w_out).astype(BF16)
    mixed_out = lax.psum_scatter(out_part, "seq", scatter_dimension=0, tiled=True)
    mixed_out = (mixed_out.astype(F32) + tokens[0].astype(F32)).astype(BF16)

    g_gated = dot_nt(cot, w_out)
    sig_gate = jax.nn.sigmoid(gate)
    gy = g_gated * gate * sig_gate
    gs_gate = (
        rstd * g_gated * y_val * sig_gate * (1.0 + gate * (1.0 - sig_gate))
    ).astype(BF16)
    out_grad = lax.psum_scatter(
        dot_tn(gated, cot).astype(BF16), "seg", scatter_dimension=0, tiled=True
    )
    gate_grad = lax.psum_scatter(
        dot_tn(tok, gs_gate).astype(BF16), "seg", scatter_dimension=0, tiled=True
    )
    g_dtpre, g_actp, g_bc, a_sum, start, dtb_grad, skip_grad = backward_scan(
        pre, act, gy, bc, a2, skip, checks, block
    )
    g_mixed = jnp.concatenate([dot_nt(g_dtpre, w_dt), g_bc[:, : 2 * width]], axis=1)
    g_mixed = lax.psum(g_mixed, "seq").astype(BF16)
    g_act = g_actp + dot_nn(g_mixed, w_xt)
    sig_conv = jax.nn.sigmoid(conv_out)
    g_conv = g_act * sig_conv * (1.0 + conv_out * (1.0 - sig_conv))
    tail = jnp.concatenate([g_conv, jnp.zeros((history, feats), F32)], axis=0)
    whole = jnp.concatenate([jnp.zeros((history, feats), F32), tail], axis=0)
    g_xin = sum(kernel[k] * tail[history - k : history - k + length] for k in range(taps))
    head_grad = sum(kernel[k] * whole[history - k : 2 * history - k] for k in range(taps))
    gs_x = (rstd * g_xin).astype(BF16)
    x_grad = lax.psum_scatter(
        dot_tn(tok, gs_x).astype(BF16), "seg", scatter_dimension=0, tiled=True
    )
    q_part = (dot_nt(gs_gate, w_g_half) + dot_nt(gs_x, w_x_half)).astype(BF16)
    q_own = lax.psum_scatter(q_part, "seq", scatter_dimension=0, tiled=True).astype(F32)

    cw_grad = jnp.stack([jnp.sum(g_conv * padded[k : k + length], axis=0) for k in range(taps)])
    grads = jnp.concatenate(
        [
            dot_tn(dt_low, g_dtpre),
            dot_tn(g_mixed, act),
            a_sum.reshape(width, feats) * a_mat,
            cw_grad,
            jnp.sum(g_conv, axis=0, keepdims=True),
            dtb_grad,
            skip_grad,
        ],
        axis=0,
    )
    grads = grads.reshape(grads.shape[0], segs, part).transpose(1, 0, 2).astype(BF16)
    grads = lax.psum_scatter(grads, "seg", scatter_dimension=0, tiled=False).astype(F32)

    own = tokens[0].astype(F32)
    own_rstd = lax.rsqrt(jnp.mean(own * own, axis=1, keepdims=True) + EPSILON)
    input_grad = (
        cotangent[0].astype(F32)
        + q_own
        - own * (own_rstd * own_rstd) * jnp.mean(q_own * own, axis=1, keepdims=True)
    ).astype(BF16)

    halves = jnp.stack([x_grad, gate_grad]).reshape(2, seqs, own_rows, feats)
    halves = lax.all_to_all(halves, "seq", 1, 0, tiled=False)
    raw_grad = (
        halves.reshape(seqs, 2, own_rows, segs, part)
        .transpose(2, 1, 3, 0, 4)
        .reshape(own_rows, both)
        .astype(F32)
    )
    in_grad = raw_grad * gain_col
    gain_grad = jnp.sum(raw_grad * own_weight, axis=1)

    ends = to_contiguous(
        jnp.concatenate(
            [
                final.reshape(width, feats),
                x_in[length - history :],
                start.reshape(width, feats),
                head_grad,
            ],
            axis=0,
        )
    )
    at = width + history
    xp_at = low_rank + x_proj.shape[1]
    return (
        mixed_out[None],
        ends[None, :width],
        ends[None, width:at],
        input_grad[None],
        ends[None, at : at + width],
        ends[None, at + width :],
        gain_grad,
        in_grad,
        grads[xp_at + width : xp_at + width + taps],
        grads[xp_at + width + taps],
        grads[low_rank:xp_at].T,
        grads[:low_rank],
        grads[xp_at + width + taps + 1],
        grads[xp_at : xp_at + width],
        grads[xp_at + width + taps + 2],
        out_grad.astype(F32),
    )


def solution(mesh):
    spread = ("seg", "seq")
    placed = (
        P("seg", "seq", None),
        P(spread),
        P(spread, None),
        P(None, spread),
        P(spread),
        P(spread, None),
        P(None, spread),
        P(spread),
        P(None, spread),
        P(spread),
        P(spread, None),
        P("seg", None, None),
        P("seg", None, None),
        P("seg", "seq", None),
    )
    return jax.shard_map(
        body,
        mesh=mesh,
        in_specs=placed,
        out_specs=(
            P("seg", "seq", None),
            P("seg", None, "seq"),
            P("seg", None, "seq"),
            P("seg", "seq", None),
            P("seg", None, "seq"),
            P("seg", None, "seq"),
            P(spread),
            P(spread, None),
            P(None, spread),
            P(spread),
            P(spread, None),
            P(None, spread),
            P(spread),
            P(None, spread),
            P(spread),
            P(spread, None),
        ),
        check_vma=False,
    )
```

```python
import functools

import jax
import jax.numpy as jnp
from jax import lax
from jax.experimental import pallas as pl
from jax.experimental.pallas import tpu as pltpu
from jax.sharding import PartitionSpec as P

EPSILON = 1e-05
LOG2E = 1.4426950408889634
LANES = 128
UNROLL = 8
F32 = jnp.float32
BF16 = jnp.bfloat16


def sigmoid(v):
    return 1.0 / (1.0 + jnp.exp(-v))


def softplus(v):
    return jnp.maximum(v, 0.0) + jnp.log1p(jnp.exp(-jnp.abs(v)))


def to_planes(planes_ref, rows):
    count = rows.shape[0]
    for s in range(rows.shape[1] // LANES):
        planes_ref[pl.ds(s * count, count), :] = rows[:, s * LANES : (s + 1) * LANES]


def from_planes(planes_ref, count, planes):
    return jnp.concatenate(
        [planes_ref[pl.ds(s * count, count), :] for s in range(planes)], axis=1
    )


def forward_kernel(
    pre_ref, act_ref, gate_ref, bc_ref, a_ref, skip_ref, init_ref,
    y_ref, gated_ref, check_ref, final_ref,
    state, rate_pl, drive_pl, y_pl,
):
    count = pre_ref.shape[0]
    width, planes, _ = a_ref.shape

    @pl.when(pl.program_id(0) == 0)
    def _():
        state[...] = init_ref[...]

    rate = softplus(pre_ref[...])
    act = act_ref[...].astype(F32)
    to_planes(rate_pl, rate)
    to_planes(drive_pl, rate * act)

    def group(k, carry):
        first = k * UNROLL
        rates = [rate_pl[pl.ds(first + i, planes, stride=count), :] for i in range(UNROLL)]
        drives = [drive_pl[pl.ds(first + i, planes, stride=count), :] for i in range(UNROLL)]
        sums = [None] * UNROLL
        for n in range(width):
            a = a_ref[n]
            h = state[n]
            check_ref[k, n] = h
            for i in range(UNROLL):
                h = jnp.exp2(rates[i] * a) * h + bc_ref[first + i, n] * drives[i]
                term = bc_ref[first + i, width + n] * h
                sums[i] = term if n == 0 else sums[i] + term
            state[n] = h
        for i in range(UNROLL):
            y_pl[pl.ds(first + i, planes, stride=count), :] = sums[i]
        return carry

    lax.fori_loop(0, count // UNROLL, group, 0)
    y_val = from_planes(y_pl, count, planes) + skip_ref[...] * act
    gate = gate_ref[...]
    y_ref[...] = y_val
    gated_ref[...] = (y_val * gate * sigmoid(gate)).astype(BF16)

    @pl.when(pl.program_id(0) == pl.num_programs(0) - 1)
    def _():
        final_ref[...] = state[...]


def backward_kernel(
    pre_ref, act_ref, gy_ref, bc_ref, a_ref, skip_ref, check_ref,
    gdt_ref, gact_ref, gbc_ref, agrad_ref, start_ref, dtb_ref, sgrad_ref,
    carry_s, rate_pl, drive_pl, gy_pl, grate_pl, thr_pl, prod, part,
):
    count = pre_ref.shape[0]
    width, planes, _ = a_ref.shape

    @pl.when(pl.program_id(0) == 0)
    def _():
        carry_s[...] = jnp.zeros_like(carry_s)
        agrad_ref[...] = jnp.zeros_like(agrad_ref)
        dtb_ref[...] = jnp.zeros_like(dtb_ref)
        sgrad_ref[...] = jnp.zeros_like(sgrad_ref)

    pre = pre_ref[...]
    rate = softplus(pre)
    act = act_ref[...].astype(F32)
    gy = gy_ref[...]
    to_planes(rate_pl, rate)
    to_planes(drive_pl, rate * act)
    to_planes(gy_pl, gy)
    groups = count // UNROLL

    def group(j, carry):
        k = groups - 1 - j
        first = k * UNROLL
        rates = [rate_pl[pl.ds(first + i, planes, stride=count), :] for i in range(UNROLL)]
        drives = [drive_pl[pl.ds(first + i, planes, stride=count), :] for i in range(UNROLL)]
        gys = [gy_pl[pl.ds(first + i, planes, stride=count), :] for i in range(UNROLL)]
        g_rate = [None] * UNROLL
        through = [None] * UNROLL
        for n in range(width):
            a = a_ref[n]
            states = [check_ref[k, n]]
            decays = []
            for i in range(UNROLL):
                decays.append(jnp.exp2(rates[i] * a))
                states.append(decays[i] * states[i] + bc_ref[first + i, n] * drives[i])
            lam = carry_s[n]
            acc = agrad_ref[n]
            for i in reversed(range(UNROLL)):
                lam = lam + bc_ref[first + i, width + n] * gys[i]
                b_term = bc_ref[first + i, n] * lam
                prod[pl.ds((i * 2 * width + n) * planes, planes), :] = lam * drives[i]
                prod[pl.ds((i * 2 * width + width + n) * planes, planes), :] = (
                    states[i + 1] * gys[i]
                )
                lam = decays[i] * lam
                weighted = lam * states[i]
                acc = acc + weighted * rates[i]
                a_term = weighted * a
                g_rate[i] = a_term if n == 0 else g_rate[i] + a_term
                through[i] = b_term if n == 0 else through[i] + b_term
            carry_s[n] = lam
            agrad_ref[n] = acc
        for i in range(UNROLL):
            grate_pl[pl.ds(first + i, planes, stride=count), :] = g_rate[i]
            thr_pl[pl.ds(first + i, planes, stride=count), :] = through[i]
            for q in range(2 * width // 8):
                base = (i * 2 * width + q * 8) * planes
                total = prod[pl.ds(base, 8, stride=planes), :]
                for s in range(1, planes):
                    total = total + prod[pl.ds(base + s, 8, stride=planes), :]
                row = pl.multiple_of((first + i) * 2 * width + q * 8, 8)
                part[pl.ds(row, 8), :] = total
        return carry

    lax.fori_loop(0, groups, group, 0)
    g_rate = from_planes(grate_pl, count, planes) * (1.0 / LOG2E)
    through = from_planes(thr_pl, count, planes)
    g_dtpre = ((g_rate + act * through) * sigmoid(pre)).astype(BF16)
    gdt_ref[...] = g_dtpre
    gact_ref[...] = gy * skip_ref[...] + rate * through
    dtb_ref[...] += jnp.sum(g_dtpre.astype(F32), axis=0, keepdims=True)
    sgrad_ref[...] += jnp.sum(gy * act, axis=0, keepdims=True)
    rows = 2 * width
    ones = jnp.ones((LANES, LANES), F32)
    sums = jnp.dot(part[...], ones, preferred_element_type=F32)
    sums = sums.reshape(count, rows, LANES)
    pick = lax.broadcasted_iota(jnp.int32, (1, rows, LANES), 1) == lax.broadcasted_iota(
        jnp.int32, (1, rows, LANES), 2
    )
    gbc_ref[...] = jnp.sum(jnp.where(pick, sums, 0.0), axis=1)

    @pl.when(pl.program_id(0) == pl.num_programs(0) - 1)
    def _():
        start_ref[...] = carry_s[...]


def forward_scan(pre, act, gate, bc, a2, skip, init, block):
    length, features = pre.shape
    width, planes, _ = a2.shape
    steps = length // block
    rows = pl.BlockSpec((block, features), lambda i: (i, 0))
    whole = pl.BlockSpec((width, planes, LANES), lambda i: (0, 0, 0))
    plane = pltpu.VMEM((planes * block, LANES), F32)
    return pl.pallas_call(
        forward_kernel,
        grid=(steps,),
        in_specs=[
            rows, rows, rows,
            pl.BlockSpec((block, 2 * width), lambda i: (i, 0), memory_space=pltpu.SMEM),
            whole,
            pl.BlockSpec((1, features), lambda i: (0, 0)),
            whole,
        ],
        out_specs=[
            rows, rows,
            pl.BlockSpec((block // UNROLL, width, planes, LANES), lambda i: (i, 0, 0, 0)),
            whole,
        ],
        out_shape=[
            jax.ShapeDtypeStruct((length, features), F32),
            jax.ShapeDtypeStruct((length, features), BF16),
            jax.ShapeDtypeStruct((length // UNROLL, width, planes, LANES), F32),
            jax.ShapeDtypeStruct((width, planes, LANES), F32),
        ],
        scratch_shapes=[pltpu.VMEM((width, planes, LANES), F32), plane, plane, plane],
        cost_estimate=pl.CostEstimate(
            flops=8 * length * features * width,
            bytes_accessed=24 * length * features,
            transcendentals=length * features * width,
        ),
        name="scan_forward",
    )(pre, act, gate, bc, a2, skip, init)


def backward_scan(pre, act, gy, bc, a2, skip, checks, block):
    length, features = pre.shape
    width, planes, _ = a2.shape
    steps = length // block
    rows = pl.BlockSpec((block, features), lambda i: (steps - 1 - i, 0))
    whole = pl.BlockSpec((width, planes, LANES), lambda i: (0, 0, 0))
    line = pl.BlockSpec((1, features), lambda i: (0, 0))
    plane = pltpu.VMEM((planes * block, LANES), F32)
    return pl.pallas_call(
        backward_kernel,
        grid=(steps,),
        in_specs=[
            rows, rows, rows,
            pl.BlockSpec(
                (block, 2 * width), lambda i: (steps - 1 - i, 0), memory_space=pltpu.SMEM
            ),
            whole, line,
            pl.BlockSpec(
                (block // UNROLL, width, planes, LANES), lambda i: (steps - 1 - i, 0, 0, 0)
            ),
        ],
        out_specs=[
            rows, rows,
            pl.BlockSpec((block, LANES), lambda i: (steps - 1 - i, 0)),
            whole, whole, line, line,
        ],
        out_shape=[
            jax.ShapeDtypeStruct((length, features), BF16),
            jax.ShapeDtypeStruct((length, features), F32),
            jax.ShapeDtypeStruct((length, LANES), F32),
            jax.ShapeDtypeStruct((width, planes, LANES), F32),
            jax.ShapeDtypeStruct((width, planes, LANES), F32),
            jax.ShapeDtypeStruct((1, features), F32),
            jax.ShapeDtypeStruct((1, features), F32),
        ],
        scratch_shapes=[pltpu.VMEM((width, planes, LANES), F32)]
        + [plane] * 5
        + [
            pltpu.VMEM((UNROLL * 2 * width * planes, LANES), F32),
            pltpu.VMEM((block * 2 * width, LANES), F32),
        ],
        cost_estimate=pl.CostEstimate(
            flops=20 * length * features * width,
            bytes_accessed=28 * length * features,
            transcendentals=length * features * width,
        ),
        name="scan_backward",
    )(pre, act, gy, bc, a2, skip, checks)


MESH_ID = pl.DeviceIdType.MESH
VMEM_MOST = 60 * 1024 * 1024


class Grid:
    def __init__(self, axis, lines, fast):
        self.axis, self.lines, self.fast = axis, lines, fast
        self.here = lax.axis_index(axis)
        self.line = self.here // fast
        self.lane = self.here - self.line * fast

    def at(self, line, lane):
        return line * self.fast + lane

    def line_peer(self, k):
        return lax.rem(self.line + k, self.lines)

    def lane_peer(self, e):
        return lax.rem(self.lane + e, self.fast)

    def copy(self, src, dst, sent, got, index):
        return pltpu.make_async_remote_copy(
            src_ref=src, dst_ref=dst, send_sem=sent, recv_sem=got,
            device_id={self.axis: index}, device_id_type=MESH_ID,
        )


def meet(groups):
    barrier = pltpu.get_barrier_semaphore()
    total = 0
    for grid in groups:
        size = grid.lines * grid.fast
        for k in range(1, size):
            pl.semaphore_signal(
                barrier, inc=1, device_id={grid.axis: lax.rem(grid.here + k, size)},
                device_id_type=MESH_ID,
            )
        total += size - 1
    pl.semaphore_wait(barrier, total)


class Gather:
    def __init__(self, grid, own, out, sems):
        self.grid, self.own, self.out = grid, own, out
        self.up_s, self.up_r, self.dn_s, self.dn_r, self.x_s, self.x_r = sems

    @staticmethod
    def semaphores(lines, fast):
        hops = pltpu.SemaphoreType.DMA((lines,))
        across = pltpu.SemaphoreType.DMA((lines, fast))
        return [hops, hops, hops, hops, across, across]

    def block(self, line, lane=None):
        grid = self.grid
        return self.out.at[grid.at(line, grid.lane if lane is None else lane)]

    def up(self, k):
        grid = self.grid
        block = self.block(jnp.maximum(grid.line - k, 0))
        return grid.copy(
            self.own if k == 0 else block, block, self.up_s.at[k], self.up_r.at[k],
            grid.at(jnp.minimum(grid.line + 1, grid.lines - 1), grid.lane),
        )

    def down(self, k):
        grid = self.grid
        block = self.block(jnp.minimum(grid.line + k, grid.lines - 1))
        return grid.copy(
            self.own if k == 0 else block, block, self.dn_s.at[k], self.dn_r.at[k],
            grid.at(jnp.maximum(grid.line - 1, 0), grid.lane),
        )

    def sends_up(self, k):
        return jnp.logical_and(self.grid.line + 1 < self.grid.lines, self.grid.line >= k)

    def sends_down(self, k):
        return jnp.logical_and(self.grid.line > 0, self.grid.line + k < self.grid.lines)

    def across(self, line, slot, e, own=False):
        grid = self.grid
        block = self.block(line)
        return grid.copy(
            self.own if own else block, block, self.x_s.at[slot, e], self.x_r.at[slot, e],
            grid.at(grid.line, grid.lane_peer(e)),
        )

    def slots(self):
        return range(self.grid.lines)

    def begin(self):
        grid = self.grid
        for when, copy in ((self.sends_up(0), self.up(0)), (self.sends_down(0), self.down(0))):
            pl.when(when)(copy.start)
        for e in range(1, grid.fast):
            self.across(grid.line, 0, e, own=True).start()

    def step(self, k):
        grid = self.grid

        def arrived(copy, line, slot, forward, onward):
            copy.wait_recv()
            if k < grid.lines - 1:
                pl.when(forward(k))(onward(k).start)
            for e in range(1, grid.fast):
                self.across(line, slot, e).start()

        below, above = grid.line - k, grid.line + k

        @pl.when(below >= 0)
        def _():
            arrived(self.up(k - 1), below, grid.lines - k, self.sends_up, self.up)

        @pl.when(above < grid.lines)
        def _():
            arrived(self.down(k - 1), above, k, self.sends_down, self.down)

    def finish(self):
        grid = self.grid
        for k in range(grid.lines - 1):
            pl.when(self.sends_up(k))(self.up(k).wait_send)
            pl.when(self.sends_down(k))(self.down(k).wait_send)
        for slot in self.slots():
            for e in range(1, grid.fast):
                copy = self.across(grid.line_peer(slot), slot, e, own=slot == 0)
                copy.wait_send()
                copy.wait_recv()


class Scatter:
    def __init__(self, grid, src, scratch):
        self.grid, self.src = grid, src
        (
            self.xbuf, self.own, self.stage, self.zbuf, self.acc,
            self.x_s, self.x_r, self.z_s, self.z_r, self.o_s,
        ) = scratch

    @staticmethod
    def scratch(lines, fast, shape):
        dma = pltpu.SemaphoreType.DMA
        return [
            pltpu.VMEM((lines, fast - 1) + shape, BF16),
            pltpu.VMEM((lines,) + shape, BF16),
            pltpu.VMEM((lines - 1,) + shape, BF16),
            pltpu.VMEM((lines - 1,) + shape, BF16),
            pltpu.VMEM(shape, F32),
            dma((lines, fast)), dma((lines, fast)), dma((lines,)), dma((lines,)), dma((lines,)),
        ]

    def across(self, k, e):
        grid = self.grid
        lane = grid.lane_peer(e)
        return grid.copy(
            self.src.at[grid.at(grid.line_peer(k), lane)], self.xbuf.at[k, e - 1],
            self.x_s.at[k, e], self.x_r.at[k, e], grid.at(grid.line, lane),
        )

    def local(self, k):
        grid = self.grid
        return pltpu.make_async_copy(
            self.src.at[grid.at(grid.line_peer(k), grid.lane)], self.own.at[k], self.o_s.at[k]
        )

    def along(self, k):
        grid = self.grid
        return grid.copy(
            self.stage.at[k - 1], self.zbuf.at[k - 1], self.z_s.at[k], self.z_r.at[k],
            grid.at(grid.line_peer(k), grid.lane),
        )

    def order(self):
        return list(range(self.grid.lines - 1, -1, -1))

    def begin(self):
        for k in self.order():
            for e in range(1, self.grid.fast):
                self.across(k, e).start()
            self.local(k).start()

    def rows(self, step):
        count = self.acc.shape[0]
        size = 16 if count % 16 == 0 else 8
        def run(i, carry):
            step(pl.ds(pl.multiple_of(i * size, size), size))
            return carry
        lax.fori_loop(0, count // size, run, 0)

    def middle(self, k):
        for e in range(1, self.grid.fast):
            self.across(k, e).wait_recv()
        self.local(k).wait()

        def add(at):
            total = self.own[k, at, :].astype(F32)
            for e in range(self.grid.fast - 1):
                total = total + self.xbuf[k, e, at, :].astype(F32)
            if k > 0:
                self.stage[k - 1, at, :] = total.astype(BF16)
            else:
                self.acc[at, :] = total

        self.rows(add)
        if k > 0:
            self.along(k).start()

    def finish(self, out_ref):
        for k in range(1, self.grid.lines):
            self.along(k).wait_recv()

        def add(at):
            total = self.acc[at, :]
            for k in range(self.grid.lines - 1):
                total = total + self.zbuf[k, at, :].astype(F32)
            out_ref[at, :] = total.astype(out_ref.dtype)

        self.rows(add)

    def drain(self):
        for k in self.order():
            for e in range(1, self.grid.fast):
                self.across(k, e).wait_send()
            if k > 0:
                self.along(k).wait_send()


class Exchange:
    def __init__(self, grid, src, dst, sems):
        self.grid, self.src, self.dst = grid, src, dst
        self.sent, self.got = sems
        self.size = grid.lines * grid.fast

    @staticmethod
    def semaphores(size):
        return [pltpu.SemaphoreType.DMA((size,)), pltpu.SemaphoreType.DMA((size,))]

    def one(self, k):
        grid = self.grid
        peer = lax.rem(grid.here + k, self.size)
        return grid.copy(
            self.src(peer), self.dst(grid.here), self.sent.at[k], self.got.at[k], peer
        )

    def begin(self):
        for k in range(1, self.size):
            self.one(k).start()

    def arrived(self):
        for k in range(1, self.size):
            self.one(k).wait_recv()

    def drain(self):
        for k in range(1, self.size):
            self.one(k).wait_send()


ANY = pl.BlockSpec(memory_space=pl.ANY)
INSIDE = pl.BlockSpec(memory_space=pltpu.VMEM)


def comm_params(collective_id):
    return pltpu.CompilerParams(
        collective_id=collective_id, has_side_effects=True, vmem_limit_bytes=VMEM_MOST
    )


def grids(shape):
    lines, fast, seq_lines = shape
    return Grid("seg", lines, fast), Grid("seq", seq_lines, 2)


def gather_kernel(
    shape, scaled, small, tokens,
    w_x, small_all, tok, g_part,
    x_part, tok_in, g_own, local_s, x_sems, small_sems, tok_sems, swap_x, swap_g,
):
    seg, seq = grids(shape)
    load_tok = pltpu.make_async_copy(tokens, tok_in, local_s.at[0])
    load_own = pltpu.make_async_copy(scaled.at[seq.here, 0], x_part.at[seq.here], local_s.at[1])
    load_gate = pltpu.make_async_copy(scaled.at[seq.here, 1], g_own, local_s.at[3])
    load_tok.start()
    load_own.start()
    load_gate.start()
    meet((seg, seq))
    swap_x = Exchange(seq, lambda p: scaled.at[p, 0], lambda m: x_part.at[m], swap_x)
    swap_g = Exchange(seq, lambda p: scaled.at[p, 1], lambda m: g_part.at[m], swap_g)
    swap_x.begin()
    smalls = Gather(seg, small, small_all, small_sems)
    smalls.begin()
    load_tok.wait()
    toks = Gather(seq, tok_in, tok, tok_sems)
    toks.begin()
    store_tok = pltpu.make_async_copy(tok_in, tok.at[seq.here], local_s.at[0])
    store_small = pltpu.make_async_copy(small, small_all.at[seg.here], local_s.at[2])
    store_tok.start()
    store_small.start()
    load_gate.wait()
    store_gate = pltpu.make_async_copy(g_own, g_part.at[seq.here], local_s.at[3])
    store_gate.start()
    load_own.wait()
    swap_x.arrived()
    halves = Gather(seg, x_part, w_x, x_sems)
    halves.begin()
    store_own = pltpu.make_async_copy(x_part, w_x.at[seg.here], local_s.at[1])
    store_own.start()
    swap_g.begin()
    for k in range(1, seq.lines):
        toks.step(k)
    for k in range(1, seg.lines):
        smalls.step(k)
        halves.step(k)
    toks.finish()
    smalls.finish()
    halves.finish()
    swap_g.arrived()
    swap_x.drain()
    swap_g.drain()
    store_tok.wait()
    store_small.wait()
    store_gate.wait()
    store_own.wait()


def gather_start(shape, scaled, small, tokens):
    lines, fast, seq_lines = shape
    segs, seqs = lines * fast, seq_lines * 2
    rows, feats = scaled.shape[2:]
    sems = Gather.semaphores
    flat = [
        pltpu.VMEM((seqs, rows, feats), BF16),
        pltpu.VMEM(tokens.shape, BF16),
        pltpu.VMEM((rows, feats), BF16),
        pltpu.SemaphoreType.DMA((4,)),
        *sems(lines, fast), *sems(lines, fast), *sems(seq_lines, 2),
        *Exchange.semaphores(seqs), *Exchange.semaphores(seqs),
    ]

    def kernel(*refs):
        ins, rest = refs[:7], refs[7:]
        gather_kernel(
            shape, *ins, *rest[:4], rest[4:10], rest[10:16], rest[16:22], rest[22:24], rest[24:26]
        )

    w_x, small_all, tok, g_part = pl.pallas_call(
        kernel,
        in_specs=[ANY, INSIDE, ANY],
        out_specs=[ANY] * 4,
        out_shape=[
            jax.ShapeDtypeStruct((segs, seqs, rows, feats), BF16),
            jax.ShapeDtypeStruct((segs,) + small.shape, BF16),
            jax.ShapeDtypeStruct((seqs,) + tokens.shape, BF16),
            jax.ShapeDtypeStruct((seqs, rows, feats), BF16),
        ],
        scratch_shapes=flat,
        compiler_params=comm_params(1),
        name="gather_start",
    )(scaled, small, tokens)
    return w_x.reshape(-1, feats), small_all, tok.reshape(-1, tokens.shape[1]), g_part


def total_kernel(shape, call, x_ref, out_ref, half, got, mine, others, whole, sems):
    _, seq = grids(shape)
    lane_s, lane_r, line_s, line_r, back_s, back_r = sems
    width = x_ref.shape[1] // 2
    lines = seq.lines
    barrier = pltpu.get_barrier_semaphore()
    other = 1 - seq.lane
    for peer in [seq.at(seq.line, other)] + [
        seq.at(seq.line_peer(k), seq.lane) for k in range(1, lines)
    ]:
        pl.semaphore_signal(barrier, inc=1, device_id={"seq": peer}, device_id_type=MESH_ID)
    pl.semaphore_wait(barrier, lines)
    left = pl.ds(0, width)
    right = pl.ds(width, width)

    @pl.when(seq.lane == 0)
    def _():
        half[...] = x_ref[:, right].astype(BF16)

    @pl.when(seq.lane == 1)
    def _():
        half[...] = x_ref[:, left].astype(BF16)

    swap = seq.copy(half, got, lane_s, lane_r, seq.at(seq.line, other))
    swap.start()
    swap.wait()

    @pl.when(seq.lane == 0)
    def _():
        mine[...] = (x_ref[:, left] + got[...].astype(F32)).astype(BF16)

    @pl.when(seq.lane == 1)
    def _():
        mine[...] = (x_ref[:, right] + got[...].astype(F32)).astype(BF16)

    copies = [
        seq.copy(
            mine, others.at[k - 1], line_s.at[k], line_r.at[k], seq.at(seq.line_peer(k), seq.lane)
        )
        for k in range(1, lines)
    ]
    for copy in copies:
        copy.start()
    for copy in copies:
        copy.wait()
    total = mine[...].astype(F32)
    for k in range(lines - 1):
        total = total + others[k].astype(F32)
    whole[seq.lane] = total.astype(BF16)
    back = seq.copy(
        whole.at[seq.lane], whole.at[seq.lane], back_s, back_r, seq.at(seq.line, other)
    )
    back.start()
    back.wait()
    out_ref[:, left] = whole[0]
    out_ref[:, right] = whole[1]


def total_over_seq(shape, x, collective_id):
    lines = shape[2]
    rows, width = x.shape
    part = pltpu.VMEM((rows, width // 2), BF16)
    dma = pltpu.SemaphoreType.DMA

    def kernel(x_ref, out_ref, half, got, mine, others, whole, *sems):
        total_kernel(shape, collective_id, x_ref, out_ref, half, got, mine, others, whole, sems)

    return pl.pallas_call(
        kernel,
        in_specs=[INSIDE],
        out_specs=INSIDE,
        out_shape=jax.ShapeDtypeStruct(x.shape, BF16),
        scratch_shapes=[
            part, part, part,
            pltpu.VMEM((max(lines - 1, 1), rows, width // 2), BF16),
            pltpu.VMEM((2, rows, width // 2), BF16),
            dma, dma, dma((lines,)), dma((lines,)), dma, dma,
        ],
        compiler_params=comm_params(collective_id),
        name="total_over_seq",
    )(x)


def scatter_end(shape, over_seg, over_seq, ends):
    lines, fast, seq_lines = shape
    seqs = seq_lines * 2
    count = len(over_seg)
    blocks = [a.shape[1:] for a in over_seg]
    own_rows = blocks[1][0] // seqs
    feats = blocks[1][1]
    scratch = []
    spans = []
    for block in blocks:
        part = Scatter.scratch(lines, fast, tuple(block))
        spans.append((len(scratch), len(scratch) + len(part)))
        scratch += part
    part = Scatter.scratch(seq_lines, 2, tuple(over_seq.shape[1:]))
    spans.append((len(scratch), len(scratch) + len(part)))
    scratch += part
    tail = len(scratch)
    scratch += [
        pltpu.VMEM((2, blocks[1][0], feats), BF16),
        *Exchange.semaphores(seqs), *Exchange.semaphores(seqs), *Exchange.semaphores(seqs),
        pltpu.SemaphoreType.DMA((3,)),
    ]

    def kernel(*refs):
        srcs = refs[:count]
        q_src, ends_in = refs[count : count + 2]
        small_out, out_out, halves_out, q_out, ends_out = refs[count + 2 : count + 7]
        sc = refs[count + 7 :]
        seg, seq = grids(shape)
        meet((seg, seq))
        scatters = [Scatter(seg, s, sc[a:b]) for s, (a, b) in zip(srcs, spans)]
        q_sum = Scatter(seq, q_src, sc[spans[-1][0] : spans[-1][1]])
        halves = sc[tail]
        sems = sc[tail + 1 : tail + 7]
        local = sc[tail + 7]
        end_swap = Exchange(
            seq, lambda p: ends_in.at[p], lambda m: ends_out.at[m], sems[:2]
        )
        end_swap.begin()
        q_sum.begin()
        for s in scatters:
            s.begin()

        def swap(half, pair):
            return Exchange(
                seq,
                lambda p: halves.at[half, pl.ds(pl.multiple_of(p * own_rows, own_rows), own_rows)],
                lambda m: halves_out.at[half, m],
                pair,
            )

        swaps = [swap(0, sems[2:4]), swap(1, sems[4:6])]
        small, x_half, g_half, out = scatters
        outs = {0: small_out, 1: halves.at[0], 2: halves.at[1], 3: out_out}
        for k in q_sum.order():
            q_sum.middle(k)
        for i, s in enumerate(scatters):
            for j, k in enumerate(s.order()):
                s.middle(k)
                if i > 0 and j == min(1, lines - 1):
                    scatters[i - 1].finish(outs[i - 1])
                    if i - 1 in (1, 2):
                        swaps[i - 2].begin()
            if i == 0:
                q_sum.finish(q_out)
        out.finish(out_out)
        own = []
        for half in (0, 1):
            own.append(
                pltpu.make_async_copy(
                    halves.at[
                        half, pl.ds(pl.multiple_of(seq.here * own_rows, own_rows), own_rows)
                    ],
                    halves_out.at[half, seq.here],
                    local.at[half],
                )
            )
        own.append(
            pltpu.make_async_copy(ends_in.at[seq.here], ends_out.at[seq.here], local.at[2])
        )
        for copy in own:
            copy.start()
        for s in scatters + [q_sum]:
            s.drain()
        for e in swaps + [end_swap]:
            e.arrived()
            e.drain()
        for copy in own:
            copy.wait()

    return pl.pallas_call(
        kernel,
        in_specs=[ANY] * (count + 1) + [INSIDE],
        out_specs=[INSIDE] * 5,
        out_shape=[
            jax.ShapeDtypeStruct(blocks[0], F32),
            jax.ShapeDtypeStruct(blocks[3], F32),
            jax.ShapeDtypeStruct((2, seqs, own_rows, feats), BF16),
            jax.ShapeDtypeStruct(over_seq.shape[1:], F32),
            jax.ShapeDtypeStruct(ends.shape, F32),
        ],
        scratch_shapes=scratch,
        compiler_params=comm_params(4),
        name="scatter_end",
    )(*over_seg, over_seq, ends)


def dot_nn(a, b):
    return jnp.dot(a, b, preferred_element_type=F32)


def dot_tn(a, b):
    return lax.dot_general(a, b, (((0,), (0,)), ((), ())), preferred_element_type=F32)


def dot_nt(a, b):
    return lax.dot_general(a, b, (((1,), (1,)), ((), ())), preferred_element_type=F32)


def body(
    tokens, norm_gain, in_proj, conv_weight, conv_bias, x_proj, dt_proj, dt_bias,
    a_log, d_skip, out_proj, init_state, init_conv, cotangent,
):
    segs, seqs = lax.axis_size("seg"), lax.axis_size("seq")
    place = lax.axis_index("seq")
    own_rows, both = in_proj.shape
    part = conv_bias.shape[0]
    feats = segs * part
    taps = conv_weight.shape[0]
    width = a_log.shape[0]
    low_rank = dt_proj.shape[0]
    planes = feats // LANES
    own_len, model = tokens.shape[1:]
    length = own_len * seqs
    block = 64
    seq_lines = seqs // 2
    shape = (segs // seq_lines, seq_lines, seq_lines)

    def mine(rows):
        shaped = rows.reshape(rows.shape[0], segs, seqs, part)
        return lax.dynamic_index_in_dim(shaped, place, 2, keepdims=False).reshape(
            rows.shape[0], feats
        )

    gain_col = norm_gain.astype(F32)[:, None]
    own_weight = in_proj.astype(F32)
    scaled = (own_weight * gain_col).astype(BF16)
    scaled = scaled.reshape(own_rows, 2, segs, seqs, part).transpose(3, 1, 0, 2, 4)
    scaled = scaled.reshape(seqs, 2, own_rows, feats)
    small = jnp.concatenate(
        [
            dt_proj, x_proj.T, a_log, conv_weight, conv_bias[None], dt_bias[None], d_skip[None],
        ],
        axis=0,
    )
    small = jnp.pad(small, ((0, -small.shape[0] % 16), (0, 0)))
    w_x_half, small_all, tok, g_part = gather_start(shape, scaled, small, tokens[0])
    w_g_half = lax.all_gather(
        g_part.reshape(seqs * own_rows, feats), "seg", axis=0, tiled=True
    )
    w_out = lax.all_gather(out_proj, "seg", axis=0, tiled=True)
    cot = lax.all_gather(cotangent[0], "seq", axis=0, tiled=True)

    small_all = small_all.transpose(1, 0, 2).reshape(small.shape[0], feats)
    w_dt = small_all[:low_rank]
    w_xt = small_all[low_rank : low_rank + x_proj.shape[1]]
    rest = small_all[low_rank + x_proj.shape[1] :].astype(F32)
    a_mat = -jnp.exp(rest[:width])
    a2 = (a_mat * LOG2E).reshape(width, planes, LANES)
    kernel = rest[width : width + taps]
    b_conv = rest[width + taps][None]
    b_dt = rest[width + taps + 1][None]
    skip = rest[width + taps + 2][None]

    tok_float = tok.astype(F32)
    rstd = lax.rsqrt(jnp.mean(tok_float * tok_float, axis=1, keepdims=True) + EPSILON)
    x_in = rstd * dot_nn(tok, w_x_half)
    history = init_conv.shape[1]
    head = mine(init_conv[0])
    padded = jnp.concatenate([head, x_in], axis=0)
    conv_out = b_conv + sum(kernel[k] * padded[k : k + length] for k in range(taps))
    act = jax.nn.silu(conv_out).astype(BF16)
    mixed_x = total_over_seq(shape, dot_nt(w_xt, act), 2)
    dt_low = mixed_x[:low_rank]
    bc = mixed_x[low_rank:].astype(F32).T
    pre = dot_tn(dt_low, w_dt) + b_dt
    gate = rstd * dot_nn(tok, w_g_half)
    init = mine(init_state[0]).reshape(width, planes, LANES)
    y_val, gated, checks, final = forward_scan(pre, act, gate, bc, a2, skip, init, block)
    out_part = dot_nn(gated, w_out).astype(BF16)
    mixed_out = lax.psum_scatter(out_part, "seq", scatter_dimension=0, tiled=True)
    mixed_out = (mixed_out.astype(F32) + tokens[0].astype(F32)).astype(BF16)

    g_gated = dot_nt(cot, w_out)
    sig_gate = jax.nn.sigmoid(gate)
    gy = g_gated * gate * sig_gate
    gs_gate = (
        rstd * g_gated * y_val * sig_gate * (1.0 + gate * (1.0 - sig_gate))
    ).astype(BF16)
    out_grad = dot_tn(gated, cot).astype(BF16)
    gate_grad = dot_tn(tok, gs_gate).astype(BF16)
    g_dtpre, g_actp, g_bc, a_sum, start, dtb_grad, skip_grad = backward_scan(
        pre, act, gy, bc, a2, skip, checks, block
    )
    g_mixed = jnp.concatenate([dot_nt(w_dt, g_dtpre), g_bc[:, : 2 * width].T], axis=0)
    g_mixed = total_over_seq(shape, g_mixed, 3)
    g_act = g_actp + dot_tn(g_mixed, w_xt)
    sig_conv = jax.nn.sigmoid(conv_out)
    g_conv = g_act * sig_conv * (1.0 + conv_out * (1.0 - sig_conv))
    tail = jnp.concatenate([g_conv, jnp.zeros((history, feats), F32)], axis=0)
    whole = jnp.concatenate([jnp.zeros((history, feats), F32), tail], axis=0)
    g_xin = sum(kernel[k] * tail[history - k : history - k + length] for k in range(taps))
    head_grad = sum(kernel[k] * whole[history - k : 2 * history - k] for k in range(taps))
    gs_x = (rstd * g_xin).astype(BF16)
    x_grad = dot_tn(tok, gs_x).astype(BF16)
    q_part = (dot_nt(gs_gate, w_g_half) + dot_nt(gs_x, w_x_half)).astype(BF16)

    cw_grad = jnp.stack([jnp.sum(g_conv * padded[k : k + length], axis=0) for k in range(taps)])
    grads = jnp.concatenate(
        [
            dot_nn(dt_low, g_dtpre),
            dot_nn(g_mixed, act),
            a_sum.reshape(width, feats) * a_mat,
            cw_grad,
            jnp.sum(g_conv, axis=0, keepdims=True),
            dtb_grad,
            skip_grad,
        ],
        axis=0,
    )
    grads = jnp.pad(grads, ((0, -grads.shape[0] % 16), (0, 0)))
    grads = grads.reshape(grads.shape[0], segs, part).transpose(1, 0, 2).astype(BF16)
    ends = jnp.concatenate(
        [
            final.reshape(width, feats),
            x_in[length - history :],
            start.reshape(width, feats),
            head_grad,
        ],
        axis=0,
    )
    ends = jnp.pad(ends, ((0, -ends.shape[0] % 8), (0, 0)))
    grads, out_grad, halves, q_own, ends = scatter_end(
        shape,
        [
            grads,
            x_grad.reshape(segs, seqs * own_rows, feats),
            gate_grad.reshape(segs, seqs * own_rows, feats),
            out_grad.reshape(segs, part, model),
        ],
        q_part.reshape(seqs, own_len, model),
        ends.reshape(ends.shape[0], seqs, feats // seqs).transpose(1, 0, 2),
    )
    ends = (
        ends.reshape(seqs, ends.shape[1], segs // seqs, part)
        .transpose(1, 2, 0, 3)
        .reshape(ends.shape[1], feats)
    )
    own = tokens[0].astype(F32)
    own_rstd = lax.rsqrt(jnp.mean(own * own, axis=1, keepdims=True) + EPSILON)
    input_grad = (
        cotangent[0].astype(F32)
        + q_own
        - own * (own_rstd * own_rstd) * jnp.mean(q_own * own, axis=1, keepdims=True)
    ).astype(BF16)

    raw_grad = (
        halves.reshape(2, seqs, own_rows, segs, part)
        .transpose(2, 0, 3, 1, 4)
        .reshape(own_rows, both)
        .astype(F32)
    )
    in_grad = raw_grad * gain_col
    gain_grad = jnp.sum(raw_grad * own_weight, axis=1)

    at = width + history
    xp_at = low_rank + x_proj.shape[1]
    return (
        mixed_out[None],
        ends[None, :width],
        ends[None, width:at],
        input_grad[None],
        ends[None, at : at + width],
        ends[None, at + width : at + width + history],
        gain_grad,
        in_grad,
        grads[xp_at + width : xp_at + width + taps],
        grads[xp_at + width + taps],
        grads[low_rank:xp_at].T,
        grads[:low_rank],
        grads[xp_at + width + taps + 1],
        grads[xp_at : xp_at + width],
        grads[xp_at + width + taps + 2],
        out_grad,
    )


def solution(mesh):
    spread = ("seg", "seq")
    placed = (
        P("seg", "seq", None),
        P(spread),
        P(spread, None),
        P(None, spread),
        P(spread),
        P(spread, None),
        P(None, spread),
        P(spread),
        P(None, spread),
        P(spread),
        P(spread, None),
        P("seg", None, None),
        P("seg", None, None),
        P("seg", "seq", None),
    )
    return jax.shard_map(
        body,
        mesh=mesh,
        in_specs=placed,
        out_specs=(
            P("seg", "seq", None),
            P("seg", None, "seq"),
            P("seg", None, "seq"),
            P("seg", "seq", None),
            P("seg", None, "seq"),
            P("seg", None, "seq"),
            P(spread),
            P(spread, None),
            P(None, spread),
            P(spread),
            P(spread, None),
            P(None, spread),
            P(spread),
            P(None, spread),
            P(spread),
            P(spread, None),
        ),
        check_vma=False,
    )
```

```python
import functools

import jax
import jax.numpy as jnp
from jax import lax
from jax.experimental import pallas as pl
from jax.experimental.pallas import tpu as pltpu
from jax.sharding import PartitionSpec as P

EPSILON = 1e-05
LOG2E = 1.4426950408889634
LANES = 128
UNROLL = 8
F32 = jnp.float32
BF16 = jnp.bfloat16


def sigmoid(v):
    return 1.0 / (1.0 + jnp.exp(-v))


def softplus(v):
    return jnp.maximum(v, 0.0) + jnp.log1p(jnp.exp(-jnp.abs(v)))


def to_planes(planes_ref, rows):
    count = rows.shape[0]
    for s in range(rows.shape[1] // LANES):
        planes_ref[pl.ds(s * count, count), :] = rows[:, s * LANES : (s + 1) * LANES]


def from_planes(planes_ref, count, planes):
    return jnp.concatenate(
        [planes_ref[pl.ds(s * count, count), :] for s in range(planes)], axis=1
    )


MESH_ID = pl.DeviceIdType.MESH
VMEM_MOST = 60 * 1024 * 1024


class Grid:
    def __init__(self, axis, lines, fast):
        self.axis, self.lines, self.fast = axis, lines, fast
        self.here = lax.axis_index(axis)
        self.line = self.here // fast
        self.lane = self.here - self.line * fast

    def at(self, line, lane):
        return line * self.fast + lane

    def line_peer(self, k):
        return lax.rem(self.line + k, self.lines)

    def lane_peer(self, e):
        return lax.rem(self.lane + e, self.fast)

    def copy(self, src, dst, sent, got, index):
        return pltpu.make_async_remote_copy(
            src_ref=src, dst_ref=dst, send_sem=sent, recv_sem=got,
            device_id={self.axis: index}, device_id_type=MESH_ID,
        )


def meet(groups):
    barrier = pltpu.get_barrier_semaphore()
    total = 0
    for grid in groups:
        size = grid.lines * grid.fast
        for k in range(1, size):
            pl.semaphore_signal(
                barrier, inc=1, device_id={grid.axis: lax.rem(grid.here + k, size)},
                device_id_type=MESH_ID,
            )
        total += size - 1
    pl.semaphore_wait(barrier, total)


class Gather:
    def __init__(self, grid, own, out, sems):
        self.grid, self.own, self.out = grid, own, out
        self.up_s, self.up_r, self.dn_s, self.dn_r, self.x_s, self.x_r = sems

    @staticmethod
    def semaphores(lines, fast):
        hops = pltpu.SemaphoreType.DMA((lines,))
        across = pltpu.SemaphoreType.DMA((lines, fast))
        return [hops, hops, hops, hops, across, across]

    def block(self, line, lane=None):
        grid = self.grid
        return self.out.at[grid.at(line, grid.lane if lane is None else lane)]

    def up(self, k):
        grid = self.grid
        block = self.block(jnp.maximum(grid.line - k, 0))
        return grid.copy(
            self.own if k == 0 else block, block, self.up_s.at[k], self.up_r.at[k],
            grid.at(jnp.minimum(grid.line + 1, grid.lines - 1), grid.lane),
        )

    def down(self, k):
        grid = self.grid
        block = self.block(jnp.minimum(grid.line + k, grid.lines - 1))
        return grid.copy(
            self.own if k == 0 else block, block, self.dn_s.at[k], self.dn_r.at[k],
            grid.at(jnp.maximum(grid.line - 1, 0), grid.lane),
        )

    def sends_up(self, k):
        return jnp.logical_and(self.grid.line + 1 < self.grid.lines, self.grid.line >= k)

    def sends_down(self, k):
        return jnp.logical_and(self.grid.line > 0, self.grid.line + k < self.grid.lines)

    def across(self, line, slot, e, own=False):
        grid = self.grid
        block = self.block(line)
        return grid.copy(
            self.own if own else block, block, self.x_s.at[slot, e], self.x_r.at[slot, e],
            grid.at(grid.line, grid.lane_peer(e)),
        )

    def slots(self):
        return range(self.grid.lines)

    def begin(self):
        grid = self.grid
        for when, copy in ((self.sends_up(0), self.up(0)), (self.sends_down(0), self.down(0))):
            pl.when(when)(copy.start)
        for e in range(1, grid.fast):
            self.across(grid.line, 0, e, own=True).start()

    def step(self, k):
        grid = self.grid

        def arrived(copy, line, slot, forward, onward):
            copy.wait_recv()
            if k < grid.lines - 1:
                pl.when(forward(k))(onward(k).start)
            for e in range(1, grid.fast):
                self.across(line, slot, e).start()

        below, above = grid.line - k, grid.line + k

        @pl.when(below >= 0)
        def _():
            arrived(self.up(k - 1), below, grid.lines - k, self.sends_up, self.up)

        @pl.when(above < grid.lines)
        def _():
            arrived(self.down(k - 1), above, k, self.sends_down, self.down)

    def finish(self):
        grid = self.grid
        for k in range(grid.lines - 1):
            pl.when(self.sends_up(k))(self.up(k).wait_send)
            pl.when(self.sends_down(k))(self.down(k).wait_send)
        for slot in self.slots():
            for e in range(1, grid.fast):
                copy = self.across(grid.line_peer(slot), slot, e, own=slot == 0)
                copy.wait_send()
                copy.wait_recv()


class Scatter:
    def __init__(self, grid, src, scratch):
        self.grid, self.src = grid, src
        (
            self.xbuf, self.own, self.stage, self.zbuf, self.acc,
            self.x_s, self.x_r, self.z_s, self.z_r, self.o_s,
        ) = scratch

    @staticmethod
    def scratch(lines, fast, shape):
        dma = pltpu.SemaphoreType.DMA
        return [
            pltpu.VMEM((lines, fast - 1) + shape, BF16),
            pltpu.VMEM((lines,) + shape, BF16),
            pltpu.VMEM((lines - 1,) + shape, BF16),
            pltpu.VMEM((lines - 1,) + shape, BF16),
            pltpu.VMEM(shape, F32),
            dma((lines, fast)), dma((lines, fast)), dma((lines,)), dma((lines,)), dma((lines,)),
        ]

    def across(self, k, e):
        grid = self.grid
        lane = grid.lane_peer(e)
        return grid.copy(
            self.src.at[grid.at(grid.line_peer(k), lane)], self.xbuf.at[k, e - 1],
            self.x_s.at[k, e], self.x_r.at[k, e], grid.at(grid.line, lane),
        )

    def local(self, k):
        grid = self.grid
        return pltpu.make_async_copy(
            self.src.at[grid.at(grid.line_peer(k), grid.lane)], self.own.at[k], self.o_s.at[k]
        )

    def along(self, k):
        grid = self.grid
        return grid.copy(
            self.stage.at[k - 1], self.zbuf.at[k - 1], self.z_s.at[k], self.z_r.at[k],
            grid.at(grid.line_peer(k), grid.lane),
        )

    def order(self):
        return list(range(self.grid.lines - 1, -1, -1))

    def begin(self):
        for k in self.order():
            for e in range(1, self.grid.fast):
                self.across(k, e).start()
            self.local(k).start()

    def rows(self, step):
        count = self.acc.shape[0]
        size = 16 if count % 16 == 0 else 8
        def run(i, carry):
            step(pl.ds(pl.multiple_of(i * size, size), size))
            return carry
        lax.fori_loop(0, count // size, run, 0)

    def middle(self, k):
        for e in range(1, self.grid.fast):
            self.across(k, e).wait_recv()
        self.local(k).wait()

        def add(at):
            total = self.own[k, at, :].astype(F32)
            for e in range(self.grid.fast - 1):
                total = total + self.xbuf[k, e, at, :].astype(F32)
            if k > 0:
                self.stage[k - 1, at, :] = total.astype(BF16)
            else:
                self.acc[at, :] = total

        self.rows(add)
        if k > 0:
            self.along(k).start()

    def finish(self, out_ref):
        for k in range(1, self.grid.lines):
            self.along(k).wait_recv()

        def add(at):
            total = self.acc[at, :]
            for k in range(self.grid.lines - 1):
                total = total + self.zbuf[k, at, :].astype(F32)
            out_ref[at, :] = total.astype(out_ref.dtype)

        self.rows(add)

    def drain(self):
        for k in self.order():
            for e in range(1, self.grid.fast):
                self.across(k, e).wait_send()
            if k > 0:
                self.along(k).wait_send()


class Exchange:
    def __init__(self, grid, src, dst, sems):
        self.grid, self.src, self.dst = grid, src, dst
        self.sent, self.got = sems
        self.size = grid.lines * grid.fast

    @staticmethod
    def semaphores(size):
        return [pltpu.SemaphoreType.DMA((size,)), pltpu.SemaphoreType.DMA((size,))]

    def one(self, k):
        grid = self.grid
        peer = lax.rem(grid.here + k, self.size)
        return grid.copy(
            self.src(peer), self.dst(grid.here), self.sent.at[k], self.got.at[k], peer
        )

    def begin(self):
        for k in range(1, self.size):
            self.one(k).start()

    def arrived(self):
        for k in range(1, self.size):
            self.one(k).wait_recv()

    def drain(self):
        for k in range(1, self.size):
            self.one(k).wait_send()


ANY = pl.BlockSpec(memory_space=pl.ANY)
INSIDE = pl.BlockSpec(memory_space=pltpu.VMEM)


def comm_params(collective_id):
    return pltpu.CompilerParams(
        collective_id=collective_id, has_side_effects=True, vmem_limit_bytes=VMEM_MOST
    )


def grids(shape):
    lines, fast, seq_lines = shape
    return Grid("seg", lines, fast), Grid("seq", seq_lines, 2)


def forward_kernel(
    shape, steps,
    pre_ref, act_ref, bc_ref, a_ref, skip_ref, init_ref, weight_ref, cot_ref,
    y_ref, check_ref, final_ref, weights_ref, cots_ref,
    state, rate_pl, drive_pl, y_pl, local_s, *sems,
):
    count = pre_ref.shape[0]
    width, planes, _ = a_ref.shape
    seg, seq = grids(shape)
    weights = Gather(seg, weight_ref, weights_ref, sems[:6])
    cots = Gather(seq, cot_ref, cots_ref, sems[6:])
    keep = [
        pltpu.make_async_copy(weight_ref, weights_ref.at[seg.here], local_s.at[0]),
        pltpu.make_async_copy(cot_ref, cots_ref.at[seq.here], local_s.at[1]),
    ]

    @pl.when(pl.program_id(0) == 0)
    def _():
        meet((seg, seq))
        weights.begin()
        cots.begin()
        for copy in keep:
            copy.start()
        state[...] = init_ref[...]

    rate = softplus(pre_ref[...])
    act = act_ref[...].astype(F32)
    to_planes(rate_pl, rate)
    to_planes(drive_pl, rate * act)

    def group(k, carry):
        first = k * UNROLL
        rates = [rate_pl[pl.ds(first + i, planes, stride=count), :] for i in range(UNROLL)]
        drives = [drive_pl[pl.ds(first + i, planes, stride=count), :] for i in range(UNROLL)]
        sums = [None] * UNROLL
        for n in range(width):
            a = a_ref[n]
            h = state[n]
            check_ref[k, n] = h
            for i in range(UNROLL):
                h = jnp.exp2(rates[i] * a) * h + bc_ref[first + i, n] * drives[i]
                term = bc_ref[first + i, width + n] * h
                sums[i] = term if n == 0 else sums[i] + term
            state[n] = h
        for i in range(UNROLL):
            y_pl[pl.ds(first + i, planes, stride=count), :] = sums[i]
        return carry

    lax.fori_loop(0, count // UNROLL, group, 0)
    y_ref[...] = from_planes(y_pl, count, planes) + skip_ref[...] * act

    for k in range(1, seg.lines):

        @pl.when(pl.program_id(0) == (steps - 1) * k // (seg.lines - 1))
        def _():
            weights.step(k)
            if k < seq.lines:
                cots.step(k)

    @pl.when(pl.program_id(0) == steps - 1)
    def _():
        final_ref[...] = state[...]
        weights.finish()
        cots.finish()
        for copy in keep:
            copy.wait()


def backward_kernel(
    shape, steps,
    pre_ref, act_ref, gy_ref, bc_ref, a_ref, skip_ref, check_ref, first_src, second_src,
    gdt_ref, gact_ref, gbc_ref, agrad_ref, start_ref, dtb_ref, sgrad_ref, first_out, second_out,
    carry_s, rate_pl, drive_pl, gy_pl, grate_pl, thr_pl, prod, part, *scratch,
):
    count = pre_ref.shape[0]
    width, planes, _ = a_ref.shape
    seg, _ = grids(shape)
    half = len(scratch) // 2
    first, second = (
        Scatter(seg, first_src, scratch[:half]), Scatter(seg, second_src, scratch[half:])
    )

    @pl.when(pl.program_id(0) == 0)
    def _():
        meet((seg,))
        first.begin()
        second.begin()
        carry_s[...] = jnp.zeros_like(carry_s)
        agrad_ref[...] = jnp.zeros_like(agrad_ref)
        dtb_ref[...] = jnp.zeros_like(dtb_ref)
        sgrad_ref[...] = jnp.zeros_like(sgrad_ref)

    pre = pre_ref[...]
    rate = softplus(pre)
    act = act_ref[...].astype(F32)
    gy = gy_ref[...]
    to_planes(rate_pl, rate)
    to_planes(drive_pl, rate * act)
    to_planes(gy_pl, gy)
    groups = count // UNROLL

    def group(j, carry):
        k = groups - 1 - j
        first = k * UNROLL
        rates = [rate_pl[pl.ds(first + i, planes, stride=count), :] for i in range(UNROLL)]
        drives = [drive_pl[pl.ds(first + i, planes, stride=count), :] for i in range(UNROLL)]
        gys = [gy_pl[pl.ds(first + i, planes, stride=count), :] for i in range(UNROLL)]
        g_rate = [None] * UNROLL
        through = [None] * UNROLL
        for n in range(width):
            a = a_ref[n]
            states = [check_ref[k, n]]
            decays = []
            for i in range(UNROLL):
                decays.append(jnp.exp2(rates[i] * a))
                states.append(decays[i] * states[i] + bc_ref[first + i, n] * drives[i])
            lam = carry_s[n]
            acc = agrad_ref[n]
            for i in reversed(range(UNROLL)):
                lam = lam + bc_ref[first + i, width + n] * gys[i]
                b_term = bc_ref[first + i, n] * lam
                prod[pl.ds((i * 2 * width + n) * planes, planes), :] = lam * drives[i]
                prod[pl.ds((i * 2 * width + width + n) * planes, planes), :] = (
                    states[i + 1] * gys[i]
                )
                lam = decays[i] * lam
                weighted = lam * states[i]
                acc = acc + weighted * rates[i]
                a_term = weighted * a
                g_rate[i] = a_term if n == 0 else g_rate[i] + a_term
                through[i] = b_term if n == 0 else through[i] + b_term
            carry_s[n] = lam
            agrad_ref[n] = acc
        for i in range(UNROLL):
            grate_pl[pl.ds(first + i, planes, stride=count), :] = g_rate[i]
            thr_pl[pl.ds(first + i, planes, stride=count), :] = through[i]
            for q in range(2 * width // 8):
                base = (i * 2 * width + q * 8) * planes
                total = prod[pl.ds(base, 8, stride=planes), :]
                for s in range(1, planes):
                    total = total + prod[pl.ds(base + s, 8, stride=planes), :]
                row = pl.multiple_of((first + i) * 2 * width + q * 8, 8)
                part[pl.ds(row, 8), :] = total
        return carry

    lax.fori_loop(0, groups, group, 0)
    g_rate = from_planes(grate_pl, count, planes) * (1.0 / LOG2E)
    through = from_planes(thr_pl, count, planes)
    g_dtpre = ((g_rate + act * through) * sigmoid(pre)).astype(BF16)
    gdt_ref[...] = g_dtpre
    gact_ref[...] = gy * skip_ref[...] + rate * through
    dtb_ref[...] += jnp.sum(g_dtpre.astype(F32), axis=0, keepdims=True)
    sgrad_ref[...] += jnp.sum(gy * act, axis=0, keepdims=True)
    rows = 2 * width
    ones = jnp.ones((LANES, LANES), F32)
    sums = jnp.dot(part[...], ones, preferred_element_type=F32)
    sums = sums.reshape(count, rows, LANES)
    pick = lax.broadcasted_iota(jnp.int32, (1, rows, LANES), 1) == lax.broadcasted_iota(
        jnp.int32, (1, rows, LANES), 2
    )
    gbc_ref[...] = jnp.sum(jnp.where(pick, sums, 0.0), axis=1)

    events = [(s, k) for s in (first, second) for k in s.order()]
    for j, (scatter, k) in enumerate(events):

        @pl.when(pl.program_id(0) == min(steps - 1, steps * (j + 1) // len(events)))
        def _():
            scatter.middle(k)

    @pl.when(pl.program_id(0) == steps - 1)
    def _():
        start_ref[...] = carry_s[...]
        first.finish(first_out)
        second.finish(second_out)
        first.drain()
        second.drain()


def forward_scan(shape, pre, act, bc, a2, skip, init, weight, cot, block):
    lines, fast, seq_lines = shape
    length, features = pre.shape
    width, planes, _ = a2.shape
    steps = length // block
    rows = pl.BlockSpec((block, features), lambda i: (i, 0))
    whole = pl.BlockSpec((width, planes, LANES), lambda i: (0, 0, 0))
    plane = pltpu.VMEM((planes * block, LANES), F32)
    return pl.pallas_call(
        functools.partial(forward_kernel, shape, steps),
        grid=(steps,),
        in_specs=[
            rows, rows,
            pl.BlockSpec((block, 2 * width), lambda i: (i, 0), memory_space=pltpu.SMEM),
            whole,
            pl.BlockSpec((1, features), lambda i: (0, 0)),
            whole,
            pl.BlockSpec(weight.shape, lambda i: (0, 0)),
            pl.BlockSpec(cot.shape, lambda i: (0, 0)),
        ],
        out_specs=[
            rows,
            pl.BlockSpec((block // UNROLL, width, planes, LANES), lambda i: (i, 0, 0, 0)),
            whole, ANY, ANY,
        ],
        out_shape=[
            jax.ShapeDtypeStruct((length, features), F32),
            jax.ShapeDtypeStruct((length // UNROLL, width, planes, LANES), F32),
            jax.ShapeDtypeStruct((width, planes, LANES), F32),
            jax.ShapeDtypeStruct((lines * fast,) + weight.shape, BF16),
            jax.ShapeDtypeStruct((seq_lines * 2,) + cot.shape, BF16),
        ],
        scratch_shapes=[
            pltpu.VMEM((width, planes, LANES), F32), plane, plane, plane,
            pltpu.SemaphoreType.DMA((2,)),
            *Gather.semaphores(lines, fast), *Gather.semaphores(seq_lines, 2),
        ],
        compiler_params=comm_params(5),
        cost_estimate=pl.CostEstimate(
            flops=8 * length * features * width,
            bytes_accessed=24 * length * features,
            transcendentals=length * features * width,
        ),
        name="scan_forward",
    )(pre, act, bc, a2, skip, init, weight, cot)


def backward_scan(shape, pre, act, gy, bc, a2, skip, checks, first, second, block):
    length, features = pre.shape
    width, planes, _ = a2.shape
    steps = length // block
    rows = pl.BlockSpec((block, features), lambda i: (steps - 1 - i, 0))
    whole = pl.BlockSpec((width, planes, LANES), lambda i: (0, 0, 0))
    line = pl.BlockSpec((1, features), lambda i: (0, 0))
    plane = pltpu.VMEM((planes * block, LANES), F32)
    return pl.pallas_call(
        functools.partial(backward_kernel, shape, steps),
        grid=(steps,),
        in_specs=[
            rows, rows, rows,
            pl.BlockSpec(
                (block, 2 * width), lambda i: (steps - 1 - i, 0), memory_space=pltpu.SMEM
            ),
            whole, line,
            pl.BlockSpec(
                (block // UNROLL, width, planes, LANES), lambda i: (steps - 1 - i, 0, 0, 0)
            ),
            ANY, ANY,
        ],
        out_specs=[
            rows, rows,
            pl.BlockSpec((block, LANES), lambda i: (steps - 1 - i, 0)),
            whole, whole, line, line,
            pl.BlockSpec(first.shape[1:], lambda i: (0, 0)),
            pl.BlockSpec(second.shape[1:], lambda i: (0, 0)),
        ],
        out_shape=[
            jax.ShapeDtypeStruct((length, features), BF16),
            jax.ShapeDtypeStruct((length, features), F32),
            jax.ShapeDtypeStruct((length, LANES), F32),
            jax.ShapeDtypeStruct((width, planes, LANES), F32),
            jax.ShapeDtypeStruct((width, planes, LANES), F32),
            jax.ShapeDtypeStruct((1, features), F32),
            jax.ShapeDtypeStruct((1, features), F32),
            jax.ShapeDtypeStruct(first.shape[1:], BF16),
            jax.ShapeDtypeStruct(second.shape[1:], F32),
        ],
        scratch_shapes=[pltpu.VMEM((width, planes, LANES), F32)]
        + [plane] * 5
        + [
            pltpu.VMEM((UNROLL * 2 * width * planes, LANES), F32),
            pltpu.VMEM((block * 2 * width, LANES), F32),
            *Scatter.scratch(shape[0], shape[1], tuple(first.shape[1:])),
            *Scatter.scratch(shape[0], shape[1], tuple(second.shape[1:])),
        ],
        compiler_params=comm_params(6),
        cost_estimate=pl.CostEstimate(
            flops=20 * length * features * width,
            bytes_accessed=28 * length * features,
            transcendentals=length * features * width,
        ),
        name="scan_backward",
    )(pre, act, gy, bc, a2, skip, checks, first, second)


def gather_kernel(
    shape, scaled, small, tokens,
    w_x, small_all, tok, g_part,
    x_part, tok_in, g_own, local_s, x_sems, small_sems, tok_sems, swap_x, swap_g,
):
    seg, seq = grids(shape)
    load_tok = pltpu.make_async_copy(tokens, tok_in, local_s.at[0])
    load_own = pltpu.make_async_copy(scaled.at[seq.here, 0], x_part.at[seq.here], local_s.at[1])
    load_gate = pltpu.make_async_copy(scaled.at[seq.here, 1], g_own, local_s.at[3])
    load_tok.start()
    load_own.start()
    load_gate.start()
    meet((seg, seq))
    swap_x = Exchange(seq, lambda p: scaled.at[p, 0], lambda m: x_part.at[m], swap_x)
    swap_g = Exchange(seq, lambda p: scaled.at[p, 1], lambda m: g_part.at[m], swap_g)
    swap_x.begin()
    smalls = Gather(seg, small, small_all, small_sems)
    smalls.begin()
    load_tok.wait()
    toks = Gather(seq, tok_in, tok, tok_sems)
    toks.begin()
    store_tok = pltpu.make_async_copy(tok_in, tok.at[seq.here], local_s.at[0])
    store_small = pltpu.make_async_copy(small, small_all.at[seg.here], local_s.at[2])
    store_tok.start()
    store_small.start()
    load_gate.wait()
    store_gate = pltpu.make_async_copy(g_own, g_part.at[seq.here], local_s.at[3])
    store_gate.start()
    load_own.wait()
    swap_x.arrived()
    halves = Gather(seg, x_part, w_x, x_sems)
    halves.begin()
    store_own = pltpu.make_async_copy(x_part, w_x.at[seg.here], local_s.at[1])
    store_own.start()
    swap_g.begin()
    for k in range(1, seq.lines):
        toks.step(k)
    for k in range(1, seg.lines):
        smalls.step(k)
        halves.step(k)
    toks.finish()
    smalls.finish()
    halves.finish()
    swap_g.arrived()
    swap_x.drain()
    swap_g.drain()
    store_tok.wait()
    store_small.wait()
    store_gate.wait()
    store_own.wait()


def gather_start(shape, scaled, small, tokens):
    lines, fast, seq_lines = shape
    segs, seqs = lines * fast, seq_lines * 2
    rows, feats = scaled.shape[2:]
    sems = Gather.semaphores
    flat = [
        pltpu.VMEM((seqs, rows, feats), BF16),
        pltpu.VMEM(tokens.shape, BF16),
        pltpu.VMEM((rows, feats), BF16),
        pltpu.SemaphoreType.DMA((4,)),
        *sems(lines, fast), *sems(lines, fast), *sems(seq_lines, 2),
        *Exchange.semaphores(seqs), *Exchange.semaphores(seqs),
    ]

    def kernel(*refs):
        ins, rest = refs[:7], refs[7:]
        gather_kernel(
            shape, *ins, *rest[:4], rest[4:10], rest[10:16], rest[16:22], rest[22:24], rest[24:26]
        )

    w_x, small_all, tok, g_part = pl.pallas_call(
        kernel,
        in_specs=[ANY, INSIDE, ANY],
        out_specs=[ANY] * 4,
        out_shape=[
            jax.ShapeDtypeStruct((segs, seqs, rows, feats), BF16),
            jax.ShapeDtypeStruct((segs,) + small.shape, BF16),
            jax.ShapeDtypeStruct((seqs,) + tokens.shape, BF16),
            jax.ShapeDtypeStruct((seqs, rows, feats), BF16),
        ],
        scratch_shapes=flat,
        compiler_params=comm_params(1),
        name="gather_start",
    )(scaled, small, tokens)
    return w_x.reshape(-1, feats), small_all, tok.reshape(-1, tokens.shape[1]), g_part


def total_kernel(shape, call, x_ref, out_ref, half, got, mine, others, whole, sems):
    _, seq = grids(shape)
    lane_s, lane_r, line_s, line_r, back_s, back_r = sems
    width = x_ref.shape[1] // 2
    lines = seq.lines
    barrier = pltpu.get_barrier_semaphore()
    other = 1 - seq.lane
    for peer in [seq.at(seq.line, other)] + [
        seq.at(seq.line_peer(k), seq.lane) for k in range(1, lines)
    ]:
        pl.semaphore_signal(barrier, inc=1, device_id={"seq": peer}, device_id_type=MESH_ID)
    pl.semaphore_wait(barrier, lines)
    left = pl.ds(0, width)
    right = pl.ds(width, width)

    @pl.when(seq.lane == 0)
    def _():
        half[...] = x_ref[:, right].astype(BF16)

    @pl.when(seq.lane == 1)
    def _():
        half[...] = x_ref[:, left].astype(BF16)

    swap = seq.copy(half, got, lane_s, lane_r, seq.at(seq.line, other))
    swap.start()
    swap.wait()

    @pl.when(seq.lane == 0)
    def _():
        mine[...] = (x_ref[:, left] + got[...].astype(F32)).astype(BF16)

    @pl.when(seq.lane == 1)
    def _():
        mine[...] = (x_ref[:, right] + got[...].astype(F32)).astype(BF16)

    copies = [
        seq.copy(
            mine, others.at[k - 1], line_s.at[k], line_r.at[k], seq.at(seq.line_peer(k), seq.lane)
        )
        for k in range(1, lines)
    ]
    for copy in copies:
        copy.start()
    for copy in copies:
        copy.wait()
    total = mine[...].astype(F32)
    for k in range(lines - 1):
        total = total + others[k].astype(F32)
    whole[seq.lane] = total.astype(BF16)
    back = seq.copy(
        whole.at[seq.lane], whole.at[seq.lane], back_s, back_r, seq.at(seq.line, other)
    )
    back.start()
    back.wait()
    out_ref[:, left] = whole[0]
    out_ref[:, right] = whole[1]


def total_over_seq(shape, x, collective_id):
    lines = shape[2]
    rows, width = x.shape
    part = pltpu.VMEM((rows, width // 2), BF16)
    dma = pltpu.SemaphoreType.DMA

    def kernel(x_ref, out_ref, half, got, mine, others, whole, *sems):
        total_kernel(shape, collective_id, x_ref, out_ref, half, got, mine, others, whole, sems)

    return pl.pallas_call(
        kernel,
        in_specs=[INSIDE],
        out_specs=INSIDE,
        out_shape=jax.ShapeDtypeStruct(x.shape, BF16),
        scratch_shapes=[
            part, part, part,
            pltpu.VMEM((max(lines - 1, 1), rows, width // 2), BF16),
            pltpu.VMEM((2, rows, width // 2), BF16),
            dma, dma, dma((lines,)), dma((lines,)), dma, dma,
        ],
        compiler_params=comm_params(collective_id),
        name="total_over_seq",
    )(x)


def scatter_end(shape, over_seg, over_seq, g_half, ends):
    lines, fast, seq_lines = shape
    seqs = seq_lines * 2
    count = len(over_seg)
    blocks = [a.shape[1:] for a in over_seg]
    own_rows = blocks[1][0] // seqs
    feats = blocks[1][1]
    scratch = []
    spans = []
    for block in blocks:
        part = Scatter.scratch(lines, fast, tuple(block))
        spans.append((len(scratch), len(scratch) + len(part)))
        scratch += part
    part = Scatter.scratch(seq_lines, 2, tuple(over_seq.shape[1:]))
    spans.append((len(scratch), len(scratch) + len(part)))
    scratch += part
    tail = len(scratch)
    scratch += [
        pltpu.VMEM((blocks[1][0], feats), BF16),
        *Exchange.semaphores(seqs), *Exchange.semaphores(seqs), *Exchange.semaphores(seqs),
        pltpu.SemaphoreType.DMA((3,)),
    ]

    def kernel(*refs):
        srcs = refs[:count]
        q_src, g_in, ends_in = refs[count : count + 3]
        small_out, halves_out, q_out, ends_out = refs[count + 3 : count + 7]
        sc = refs[count + 7 :]
        seg, seq = grids(shape)
        meet((seg, seq))
        scatters = [Scatter(seg, s, sc[a:b]) for s, (a, b) in zip(srcs, spans)]
        q_sum = Scatter(seq, q_src, sc[spans[-1][0] : spans[-1][1]])
        halves = (sc[tail], g_in)
        sems = sc[tail + 1 : tail + 7]
        local = sc[tail + 7]
        end_swap = Exchange(
            seq, lambda p: ends_in.at[p], lambda m: ends_out.at[m], sems[:2]
        )
        end_swap.begin()
        q_sum.begin()
        for s in scatters:
            s.begin()

        def swap(half, pair):
            return Exchange(
                seq,
                lambda p: halves[half].at[pl.ds(pl.multiple_of(p * own_rows, own_rows), own_rows)],
                lambda m: halves_out.at[half, m],
                pair,
            )

        swaps = [swap(0, sems[2:4]), swap(1, sems[4:6])]
        swaps[1].begin()
        small, x_half = scatters
        for k in small.order():
            small.middle(k)
        for j, k in enumerate(x_half.order()):
            x_half.middle(k)
            if j < seq_lines:
                q_sum.middle(q_sum.order()[j])
        small.finish(small_out)
        q_sum.finish(q_out)
        x_half.finish(halves[0])
        swaps[0].begin()
        own = []
        for half in (0, 1):
            own.append(
                pltpu.make_async_copy(
                    halves[half].at[
                        pl.ds(pl.multiple_of(seq.here * own_rows, own_rows), own_rows)
                    ],
                    halves_out.at[half, seq.here],
                    local.at[half],
                )
            )
        own.append(
            pltpu.make_async_copy(ends_in.at[seq.here], ends_out.at[seq.here], local.at[2])
        )
        for copy in own:
            copy.start()
        for s in scatters + [q_sum]:
            s.drain()
        for e in swaps + [end_swap]:
            e.arrived()
            e.drain()
        for copy in own:
            copy.wait()

    return pl.pallas_call(
        kernel,
        in_specs=[ANY] * (count + 1) + [INSIDE, INSIDE],
        out_specs=[INSIDE] * 4,
        out_shape=[
            jax.ShapeDtypeStruct(blocks[0], F32),
            jax.ShapeDtypeStruct((2, seqs, own_rows, feats), BF16),
            jax.ShapeDtypeStruct(over_seq.shape[1:], F32),
            jax.ShapeDtypeStruct(ends.shape, F32),
        ],
        scratch_shapes=scratch,
        compiler_params=comm_params(4),
        name="scatter_end",
    )(*over_seg, over_seq, g_half, ends)


def dot_nn(a, b):
    return jnp.dot(a, b, preferred_element_type=F32)


def dot_tn(a, b):
    return lax.dot_general(a, b, (((0,), (0,)), ((), ())), preferred_element_type=F32)


def dot_nt(a, b):
    return lax.dot_general(a, b, (((1,), (1,)), ((), ())), preferred_element_type=F32)


def body(
    tokens, norm_gain, in_proj, conv_weight, conv_bias, x_proj, dt_proj, dt_bias,
    a_log, d_skip, out_proj, init_state, init_conv, cotangent,
):
    segs, seqs = lax.axis_size("seg"), lax.axis_size("seq")
    place = lax.axis_index("seq")
    own_rows, both = in_proj.shape
    part = conv_bias.shape[0]
    feats = segs * part
    taps = conv_weight.shape[0]
    width = a_log.shape[0]
    low_rank = dt_proj.shape[0]
    planes = feats // LANES
    own_len, model = tokens.shape[1:]
    length = own_len * seqs
    block = 64
    seq_lines = seqs // 2
    shape = (segs // seq_lines, seq_lines, seq_lines)

    def mine(rows):
        shaped = rows.reshape(rows.shape[0], segs, seqs, part)
        return lax.dynamic_index_in_dim(shaped, place, 2, keepdims=False).reshape(
            rows.shape[0], feats
        )

    gain_col = norm_gain.astype(F32)[:, None]
    own_weight = in_proj.astype(F32)
    scaled = (own_weight * gain_col).astype(BF16)
    scaled = scaled.reshape(own_rows, 2, segs, seqs, part).transpose(3, 1, 0, 2, 4)
    scaled = scaled.reshape(seqs, 2, own_rows, feats)
    small = jnp.concatenate(
        [
            dt_proj, x_proj.T, a_log, conv_weight, conv_bias[None], dt_bias[None], d_skip[None],
        ],
        axis=0,
    )
    small = jnp.pad(small, ((0, -small.shape[0] % 16), (0, 0)))
    w_x_half, small_all, tok, g_part = gather_start(shape, scaled, small, tokens[0])
    w_g_half = lax.all_gather(
        g_part.reshape(seqs * own_rows, feats), "seg", axis=0, tiled=True
    )

    small_all = small_all.transpose(1, 0, 2).reshape(small.shape[0], feats)
    w_dt = small_all[:low_rank]
    w_xt = small_all[low_rank : low_rank + x_proj.shape[1]]
    rest = small_all[low_rank + x_proj.shape[1] :].astype(F32)
    a_mat = -jnp.exp(rest[:width])
    a2 = (a_mat * LOG2E).reshape(width, planes, LANES)
    kernel = rest[width : width + taps]
    b_conv = rest[width + taps][None]
    b_dt = rest[width + taps + 1][None]
    skip = rest[width + taps + 2][None]

    tok_float = tok.astype(F32)
    rstd = lax.rsqrt(jnp.mean(tok_float * tok_float, axis=1, keepdims=True) + EPSILON)
    x_in = rstd * dot_nn(tok, w_x_half)
    history = init_conv.shape[1]
    head = mine(init_conv[0])
    padded = jnp.concatenate([head, x_in], axis=0)
    conv_out = b_conv + sum(kernel[k] * padded[k : k + length] for k in range(taps))
    act = jax.nn.silu(conv_out).astype(BF16)
    mixed_x = total_over_seq(shape, dot_nt(w_xt, act), 2)
    dt_low = mixed_x[:low_rank]
    bc = mixed_x[low_rank:].astype(F32).T
    pre = dot_tn(dt_low, w_dt) + b_dt
    init = mine(init_state[0]).reshape(width, planes, LANES)
    y_val, checks, final, w_out, cot = forward_scan(
        shape, pre, act, bc, a2, skip, init, out_proj, cotangent[0], block
    )
    w_out = w_out.reshape(feats, model)
    cot = cot.reshape(length, model)
    y_val, w_g_half = lax.optimization_barrier((y_val, w_g_half))
    gate = rstd * dot_nn(tok, w_g_half)
    gated = (y_val * jax.nn.silu(gate)).astype(BF16)
    out_part = dot_nn(gated, w_out).astype(BF16)
    mixed_out = lax.psum_scatter(out_part, "seq", scatter_dimension=0, tiled=True)
    mixed_out = (mixed_out.astype(F32) + tokens[0].astype(F32)).astype(BF16)

    g_gated = dot_nt(cot, w_out)
    sig_gate = jax.nn.sigmoid(gate)
    gy = g_gated * gate * sig_gate
    gs_gate = (
        rstd * g_gated * y_val * sig_gate * (1.0 + gate * (1.0 - sig_gate))
    ).astype(BF16)
    out_grad = dot_tn(gated, cot).astype(BF16)
    gate_grad = dot_tn(tok, gs_gate).astype(BF16)
    g_dtpre, g_actp, g_bc, a_sum, start, dtb_grad, skip_grad, g_half, out_grad = backward_scan(
        shape, pre, act, gy, bc, a2, skip, checks,
        gate_grad.reshape(segs, seqs * own_rows, feats),
        out_grad.reshape(segs, part, model),
        block,
    )
    g_mixed = jnp.concatenate([dot_nt(w_dt, g_dtpre), g_bc[:, : 2 * width].T], axis=0)
    g_mixed = total_over_seq(shape, g_mixed, 3)
    g_act = g_actp + dot_tn(g_mixed, w_xt)
    sig_conv = jax.nn.sigmoid(conv_out)
    g_conv = g_act * sig_conv * (1.0 + conv_out * (1.0 - sig_conv))
    tail = jnp.concatenate([g_conv, jnp.zeros((history, feats), F32)], axis=0)
    whole = jnp.concatenate([jnp.zeros((history, feats), F32), tail], axis=0)
    g_xin = sum(kernel[k] * tail[history - k : history - k + length] for k in range(taps))
    head_grad = sum(kernel[k] * whole[history - k : 2 * history - k] for k in range(taps))
    gs_x = (rstd * g_xin).astype(BF16)
    x_grad = dot_tn(tok, gs_x).astype(BF16)
    q_part = (dot_nt(gs_gate, w_g_half) + dot_nt(gs_x, w_x_half)).astype(BF16)

    cw_grad = jnp.stack([jnp.sum(g_conv * padded[k : k + length], axis=0) for k in range(taps)])
    grads = jnp.concatenate(
        [
            dot_nn(dt_low, g_dtpre),
            dot_nn(g_mixed, act),
            a_sum.reshape(width, feats) * a_mat,
            cw_grad,
            jnp.sum(g_conv, axis=0, keepdims=True),
            dtb_grad,
            skip_grad,
        ],
        axis=0,
    )
    grads = jnp.pad(grads, ((0, -grads.shape[0] % 16), (0, 0)))
    grads = grads.reshape(grads.shape[0], segs, part).transpose(1, 0, 2).astype(BF16)
    ends = jnp.concatenate(
        [
            final.reshape(width, feats),
            x_in[length - history :],
            start.reshape(width, feats),
            head_grad,
        ],
        axis=0,
    )
    ends = jnp.pad(ends, ((0, -ends.shape[0] % 8), (0, 0)))
    grads, halves, q_own, ends = scatter_end(
        shape,
        [grads, x_grad.reshape(segs, seqs * own_rows, feats)],
        q_part.reshape(seqs, own_len, model),
        g_half,
        ends.reshape(ends.shape[0], seqs, feats // seqs).transpose(1, 0, 2),
    )
    ends = (
        ends.reshape(seqs, ends.shape[1], segs // seqs, part)
        .transpose(1, 2, 0, 3)
        .reshape(ends.shape[1], feats)
    )
    own = tokens[0].astype(F32)
    own_rstd = lax.rsqrt(jnp.mean(own * own, axis=1, keepdims=True) + EPSILON)
    input_grad = (
        cotangent[0].astype(F32)
        + q_own
        - own * (own_rstd * own_rstd) * jnp.mean(q_own * own, axis=1, keepdims=True)
    ).astype(BF16)

    raw_grad = (
        halves.reshape(2, seqs, own_rows, segs, part)
        .transpose(2, 0, 3, 1, 4)
        .reshape(own_rows, both)
        .astype(F32)
    )
    in_grad = raw_grad * gain_col
    gain_grad = jnp.sum(raw_grad * own_weight, axis=1)

    at = width + history
    xp_at = low_rank + x_proj.shape[1]
    return (
        mixed_out[None],
        ends[None, :width],
        ends[None, width:at],
        input_grad[None],
        ends[None, at : at + width],
        ends[None, at + width : at + width + history],
        gain_grad,
        in_grad,
        grads[xp_at + width : xp_at + width + taps],
        grads[xp_at + width + taps],
        grads[low_rank:xp_at].T,
        grads[:low_rank],
        grads[xp_at + width + taps + 1],
        grads[xp_at : xp_at + width],
        grads[xp_at + width + taps + 2],
        out_grad,
    )


def solution(mesh):
    spread = ("seg", "seq")
    placed = (
        P("seg", "seq", None),
        P(spread),
        P(spread, None),
        P(None, spread),
        P(spread),
        P(spread, None),
        P(None, spread),
        P(spread),
        P(None, spread),
        P(spread),
        P(spread, None),
        P("seg", None, None),
        P("seg", None, None),
        P("seg", "seq", None),
    )
    return jax.shard_map(
        body,
        mesh=mesh,
        in_specs=placed,
        out_specs=(
            P("seg", "seq", None),
            P("seg", None, "seq"),
            P("seg", None, "seq"),
            P("seg", "seq", None),
            P("seg", None, "seq"),
            P("seg", None, "seq"),
            P(spread),
            P(spread, None),
            P(None, spread),
            P(spread),
            P(spread, None),
            P(None, spread),
            P(spread),
            P(None, spread),
            P(spread),
            P(spread, None),
        ),
        check_vma=False,
    )
```

```python
import functools

import jax
import jax.numpy as jnp
from jax import lax
from jax.experimental import pallas as pl
from jax.experimental.pallas import tpu as pltpu
from jax.sharding import PartitionSpec as P

EPSILON = 1e-05
LOG2E = 1.4426950408889634
LANES = 128
UNROLL = 8
F32 = jnp.float32
BF16 = jnp.bfloat16


def dot_nn(a, b):
    return jnp.dot(a, b, preferred_element_type=F32)


def dot_tn(a, b):
    return lax.dot_general(a, b, (((0,), (0,)), ((), ())), preferred_element_type=F32)


def dot_nt(a, b):
    return lax.dot_general(a, b, (((1,), (1,)), ((), ())), preferred_element_type=F32)


def sigmoid(v):
    return 1.0 / (1.0 + jnp.exp(-v))


def softplus(v):
    return jnp.maximum(v, 0.0) + jnp.log1p(jnp.exp(-jnp.abs(v)))


def to_planes(planes_ref, rows):
    count = rows.shape[0]
    for s in range(rows.shape[1] // LANES):
        planes_ref[pl.ds(s * count, count), :] = rows[:, s * LANES : (s + 1) * LANES]


def from_planes(planes_ref, count, planes):
    return jnp.concatenate(
        [planes_ref[pl.ds(s * count, count), :] for s in range(planes)], axis=1
    )


MESH_ID = pl.DeviceIdType.MESH
VMEM_MOST = 63 * 1024 * 1024 + 512 * 1024


class Grid:
    def __init__(self, axis, lines, fast):
        self.axis, self.lines, self.fast = axis, lines, fast
        self.here = lax.axis_index(axis)
        self.line = self.here // fast
        self.lane = self.here - self.line * fast

    def at(self, line, lane):
        return line * self.fast + lane

    def line_peer(self, k):
        return lax.rem(self.line + k, self.lines)

    def lane_peer(self, e):
        return lax.rem(self.lane + e, self.fast)

    def copy(self, src, dst, sent, got, index):
        return pltpu.make_async_remote_copy(
            src_ref=src, dst_ref=dst, send_sem=sent, recv_sem=got,
            device_id={self.axis: index}, device_id_type=MESH_ID,
        )


def meet(groups):
    barrier = pltpu.get_barrier_semaphore()
    total = 0
    for grid in groups:
        size = grid.lines * grid.fast
        for k in range(1, size):
            pl.semaphore_signal(
                barrier, inc=1, device_id={grid.axis: lax.rem(grid.here + k, size)},
                device_id_type=MESH_ID,
            )
        total += size - 1
    pl.semaphore_wait(barrier, total)


class Gather:
    def __init__(self, grid, own, out, sems):
        self.grid, self.own, self.out = grid, own, out
        self.up_s, self.up_r, self.dn_s, self.dn_r, self.x_s, self.x_r = sems

    @staticmethod
    def semaphores(lines, fast):
        hops = pltpu.SemaphoreType.DMA((lines,))
        across = pltpu.SemaphoreType.DMA((lines, fast))
        return [hops, hops, hops, hops, across, across]

    def block(self, line, lane=None):
        grid = self.grid
        return self.out.at[grid.at(line, grid.lane if lane is None else lane)]

    def up(self, k):
        grid = self.grid
        block = self.block(jnp.maximum(grid.line - k, 0))
        return grid.copy(
            self.own if k == 0 else block, block, self.up_s.at[k], self.up_r.at[k],
            grid.at(jnp.minimum(grid.line + 1, grid.lines - 1), grid.lane),
        )

    def down(self, k):
        grid = self.grid
        block = self.block(jnp.minimum(grid.line + k, grid.lines - 1))
        return grid.copy(
            self.own if k == 0 else block, block, self.dn_s.at[k], self.dn_r.at[k],
            grid.at(jnp.maximum(grid.line - 1, 0), grid.lane),
        )

    def sends_up(self, k):
        return jnp.logical_and(self.grid.line + 1 < self.grid.lines, self.grid.line >= k)

    def sends_down(self, k):
        return jnp.logical_and(self.grid.line > 0, self.grid.line + k < self.grid.lines)

    def across(self, line, slot, e, own=False):
        grid = self.grid
        block = self.block(line)
        return grid.copy(
            self.own if own else block, block, self.x_s.at[slot, e], self.x_r.at[slot, e],
            grid.at(grid.line, grid.lane_peer(e)),
        )

    def slots(self):
        return range(self.grid.lines)

    def begin(self):
        grid = self.grid
        for when, copy in ((self.sends_up(0), self.up(0)), (self.sends_down(0), self.down(0))):
            pl.when(when)(copy.start)
        for e in range(1, grid.fast):
            self.across(grid.line, 0, e, own=True).start()

    def step(self, k):
        grid = self.grid

        def arrived(copy, line, slot, forward, onward):
            copy.wait_recv()
            if k < grid.lines - 1:
                pl.when(forward(k))(onward(k).start)
            for e in range(1, grid.fast):
                self.across(line, slot, e).start()

        below, above = grid.line - k, grid.line + k

        @pl.when(below >= 0)
        def _():
            arrived(self.up(k - 1), below, grid.lines - k, self.sends_up, self.up)

        @pl.when(above < grid.lines)
        def _():
            arrived(self.down(k - 1), above, k, self.sends_down, self.down)

    def finish(self):
        grid = self.grid
        for k in range(grid.lines - 1):
            pl.when(self.sends_up(k))(self.up(k).wait_send)
            pl.when(self.sends_down(k))(self.down(k).wait_send)
        for slot in self.slots():
            for e in range(1, grid.fast):
                copy = self.across(grid.line_peer(slot), slot, e, own=slot == 0)
                copy.wait_send()
                copy.wait_recv()


class Scatter:
    def __init__(self, grid, src, scratch, inside=False):
        self.grid, self.src, self.inside = grid, src, inside
        if not inside:
            self.own, self.o_s = scratch[:2]
            scratch = scratch[2:]
        self.xbuf, self.stage, self.zbuf, self.acc = scratch[:4]
        self.x_s, self.x_r, self.z_s, self.z_r = scratch[4:]

    @staticmethod
    def scratch(lines, fast, shape, inside=False):
        dma = pltpu.SemaphoreType.DMA
        shape = tuple(shape)
        loads = [] if inside else [pltpu.VMEM((lines,) + shape, BF16), dma((lines,))]
        return loads + [
            pltpu.VMEM((lines, fast - 1) + shape, BF16),
            pltpu.VMEM((lines - 1,) + shape, BF16),
            pltpu.VMEM((lines - 1,) + shape, BF16),
            pltpu.VMEM(shape, F32),
            dma((lines, fast)), dma((lines, fast)), dma((lines,)), dma((lines,)),
        ]

    def index(self, k, e):
        return self.grid.at(self.grid.line_peer(k), self.grid.lane_peer(e))

    def across(self, k, e):
        grid = self.grid
        return grid.copy(
            self.src.at[self.index(k, e)], self.xbuf.at[k, e - 1],
            self.x_s.at[k, e], self.x_r.at[k, e], grid.at(grid.line, grid.lane_peer(e)),
        )

    def local(self, k):
        return pltpu.make_async_copy(
            self.src.at[self.index(k, 0)], self.own.at[k], self.o_s.at[k]
        )

    def along(self, k):
        grid = self.grid
        return grid.copy(
            self.stage.at[k - 1], self.zbuf.at[k - 1], self.z_s.at[k], self.z_r.at[k],
            grid.at(grid.line_peer(k), grid.lane),
        )

    def order(self):
        return list(range(self.grid.lines - 1, -1, -1))

    def begin(self):
        for k in self.order():
            for e in range(1, self.grid.fast):
                self.across(k, e).start()
            if not self.inside:
                self.local(k).start()

    def rows(self, step):
        count = self.acc.shape[0]
        size = 16 if count % 16 == 0 else 8

        def run(i, carry):
            step(pl.ds(pl.multiple_of(i * size, size), size))
            return carry

        lax.fori_loop(0, count // size, run, 0)

    def middle(self, k):
        for e in range(1, self.grid.fast):
            self.across(k, e).wait_recv()
        if self.inside:
            own = self.src.at[self.index(k, 0)]
        else:
            self.local(k).wait()
            own = self.own.at[k]

        def add(at):
            total = own[at, :].astype(F32)
            for e in range(self.grid.fast - 1):
                total = total + self.xbuf[k, e, at, :].astype(F32)
            if k > 0:
                self.stage[k - 1, at, :] = total.astype(BF16)
            else:
                self.acc[at, :] = total

        self.rows(add)
        if k > 0:
            self.along(k).start()

    def finish(self, write):
        for k in range(1, self.grid.lines):
            self.along(k).wait_recv()

        def add(at):
            total = self.acc[at, :]
            for k in range(self.grid.lines - 1):
                total = total + self.zbuf[k, at, :].astype(F32)
            write(at, total)

        self.rows(add)

    def drain(self):
        for k in self.order():
            for e in range(1, self.grid.fast):
                self.across(k, e).wait_send()
            if k > 0:
                self.along(k).wait_send()


def into(ref):
    def write(at, total):
        ref[at, :] = total.astype(ref.dtype)

    return write


class Exchange:
    def __init__(self, grid, src, dst, sems):
        self.grid, self.src, self.dst = grid, src, dst
        self.sent, self.got = sems
        self.size = grid.lines * grid.fast

    @staticmethod
    def semaphores(size):
        return [pltpu.SemaphoreType.DMA((size,)), pltpu.SemaphoreType.DMA((size,))]

    def one(self, k):
        grid = self.grid
        peer = lax.rem(grid.here + k, self.size)
        return grid.copy(
            self.src(peer), self.dst(grid.here), self.sent.at[k], self.got.at[k], peer
        )

    def begin(self):
        for k in range(1, self.size):
            self.one(k).start()

    def arrived(self):
        for k in range(1, self.size):
            self.one(k).wait_recv()

    def drain(self):
        for k in range(1, self.size):
            self.one(k).wait_send()


ANY = pl.BlockSpec(memory_space=pl.ANY)
INSIDE = pl.BlockSpec(memory_space=pltpu.VMEM)


def comm_params(collective_id):
    return pltpu.CompilerParams(
        collective_id=collective_id, has_side_effects=True, vmem_limit_bytes=VMEM_MOST
    )


def grids(shape):
    lines, fast, seq_lines = shape
    return Grid("seg", lines, fast), Grid("seq", seq_lines, 2)


def sum_over_seq(seq, x_ref, out_ref, half, got, mine, others, whole, *sems):
    lane_s, lane_r, line_s, line_r, back_s, back_r = sems
    width = x_ref.shape[1] // 2
    lines = seq.lines
    other = 1 - seq.lane
    left = pl.ds(0, width)
    right = pl.ds(width, width)

    @pl.when(seq.lane == 0)
    def _():
        half[...] = x_ref[:, right].astype(BF16)

    @pl.when(seq.lane == 1)
    def _():
        half[...] = x_ref[:, left].astype(BF16)

    swap = seq.copy(half, got, lane_s, lane_r, seq.at(seq.line, other))
    swap.start()
    swap.wait()

    @pl.when(seq.lane == 0)
    def _():
        mine[...] = (x_ref[:, left] + got[...].astype(F32)).astype(BF16)

    @pl.when(seq.lane == 1)
    def _():
        mine[...] = (x_ref[:, right] + got[...].astype(F32)).astype(BF16)

    copies = [
        seq.copy(
            mine, others.at[k - 1], line_s.at[k], line_r.at[k], seq.at(seq.line_peer(k), seq.lane)
        )
        for k in range(1, lines)
    ]
    for copy in copies:
        copy.start()
    for copy in copies:
        copy.wait()
    total = mine[...].astype(F32)
    for k in range(lines - 1):
        total = total + others[k].astype(F32)
    whole[seq.lane] = total.astype(BF16)
    back = seq.copy(
        whole.at[seq.lane], whole.at[seq.lane], back_s, back_r, seq.at(seq.line, other)
    )
    back.start()
    back.wait()
    out_ref[:, left] = whole[0]
    out_ref[:, right] = whole[1]


def forward_kernel(
    shape, steps,
    pre_ref, act_ref, bc_ref, a_ref, skip_ref, init_ref, weight_ref, cot_ref,
    y_ref, check_ref, final_ref, weights_ref, cots_ref,
    state, rate_pl, drive_pl, y_pl, local_s, *sems,
):
    count = pre_ref.shape[0]
    width, planes, _ = a_ref.shape
    seg, seq = grids(shape)
    weights = Gather(seg, weight_ref, weights_ref, sems[:6])
    cots = Gather(seq, cot_ref, cots_ref, sems[6:])
    keep = [
        pltpu.make_async_copy(weight_ref, weights_ref.at[seg.here], local_s.at[0]),
        pltpu.make_async_copy(cot_ref, cots_ref.at[seq.here], local_s.at[1]),
    ]

    @pl.when(pl.program_id(0) == 0)
    def _():
        meet((seg, seq))
        weights.begin()
        cots.begin()
        for copy in keep:
            copy.start()
        state[...] = init_ref[...]

    rate = softplus(pre_ref[...])
    act = act_ref[...].astype(F32)
    to_planes(rate_pl, rate)
    to_planes(drive_pl, rate * act)

    def group(k, carry):
        first = k * UNROLL
        rates = [rate_pl[pl.ds(first + i, planes, stride=count), :] for i in range(UNROLL)]
        drives = [drive_pl[pl.ds(first + i, planes, stride=count), :] for i in range(UNROLL)]
        sums = [None] * UNROLL
        for n in range(width):
            a = a_ref[n]
            h = state[n]
            check_ref[k, n] = h
            for i in range(UNROLL):
                h = jnp.exp2(rates[i] * a) * h + bc_ref[first + i, n] * drives[i]
                term = bc_ref[first + i, width + n] * h
                sums[i] = term if n == 0 else sums[i] + term
            state[n] = h
        for i in range(UNROLL):
            y_pl[pl.ds(first + i, planes, stride=count), :] = sums[i]
        return carry

    lax.fori_loop(0, count // UNROLL, group, 0)
    y_ref[...] = from_planes(y_pl, count, planes) + skip_ref[...] * act

    for k in range(1, seg.lines):

        @pl.when(pl.program_id(0) == (steps - 1) * k // (seg.lines - 1))
        def _():
            weights.step(k)
            if k < seq.lines:
                cots.step(k)

    @pl.when(pl.program_id(0) == steps - 1)
    def _():
        final_ref[...] = state[...]
        weights.finish()
        cots.finish()
        for copy in keep:
            copy.wait()


def backward_kernel(
    shape, steps,
    pre_ref, act_ref, gy_ref, bc_ref, a_ref, skip_ref, check_ref, wdt_ref, low_ref, base_ref,
    first_src, second_src, third_src,
    gact_ref, agrad_ref, start_ref, dtb_ref, sgrad_ref, dtp_ref, mix_ref,
    first_out, second_out, third_out,
    carry_s, rate_pl, drive_pl, gy_pl, grate_pl, thr_pl, prod, part, mix_s, *scratch,
):
    count = pre_ref.shape[0]
    width, planes, _ = a_ref.shape
    low_rank = wdt_ref.shape[0]
    seg, seq = grids(shape)
    first, second, third = (
        Scatter(grid, src, scratch[10 * i : 10 * i + 10])
        for i, (grid, src) in enumerate(((seg, first_src), (seg, second_src), (seq, third_src)))
    )
    step = pl.program_id(0)

    @pl.when(step == 0)
    def _():
        meet((seg, seq))
        first.begin()
        third.begin()
        second.begin()
        carry_s[...] = jnp.zeros_like(carry_s)
        agrad_ref[...] = jnp.zeros_like(agrad_ref)
        dtb_ref[...] = jnp.zeros_like(dtb_ref)
        sgrad_ref[...] = jnp.zeros_like(sgrad_ref)
        dtp_ref[...] = jnp.zeros_like(dtp_ref)

    pre = pre_ref[...]
    rate = softplus(pre)
    act = act_ref[...].astype(F32)
    to_planes(rate_pl, rate)
    to_planes(drive_pl, rate * act)
    to_planes(gy_pl, gy_ref[...])
    groups = count // UNROLL

    def group(j, carry):
        k = groups - 1 - j
        at = k * UNROLL
        rates = [rate_pl[pl.ds(at + i, planes, stride=count), :] for i in range(UNROLL)]
        drives = [drive_pl[pl.ds(at + i, planes, stride=count), :] for i in range(UNROLL)]
        gys = [gy_pl[pl.ds(at + i, planes, stride=count), :] for i in range(UNROLL)]
        g_rate = [None] * UNROLL
        through = [None] * UNROLL
        for n in range(width):
            a = a_ref[n]
            states = [check_ref[k, n]]
            decays = []
            for i in range(UNROLL):
                decays.append(jnp.exp2(rates[i] * a))
                states.append(decays[i] * states[i] + bc_ref[at + i, n] * drives[i])
            lam = carry_s[n]
            acc = agrad_ref[n]
            for i in reversed(range(UNROLL)):
                lam = lam + bc_ref[at + i, width + n] * gys[i]
                b_term = bc_ref[at + i, n] * lam
                prod[pl.ds((i * 2 * width + n) * planes, planes), :] = lam * drives[i]
                prod[pl.ds((i * 2 * width + width + n) * planes, planes), :] = (
                    states[i + 1] * gys[i]
                )
                lam = decays[i] * lam
                weighted = lam * states[i]
                acc = acc + weighted * rates[i]
                a_term = weighted * a
                g_rate[i] = a_term if n == 0 else g_rate[i] + a_term
                through[i] = b_term if n == 0 else through[i] + b_term
            carry_s[n] = lam
            agrad_ref[n] = acc
        for i in range(UNROLL):
            grate_pl[pl.ds(at + i, planes, stride=count), :] = g_rate[i]
            thr_pl[pl.ds(at + i, planes, stride=count), :] = through[i]
            for q in range(2 * width // 8):
                base = (i * 2 * width + q * 8) * planes
                total = prod[pl.ds(base, 8, stride=planes), :]
                for s in range(1, planes):
                    total = total + prod[pl.ds(base + s, 8, stride=planes), :]
                row = pl.multiple_of((at + i) * 2 * width + q * 8, 8)
                part[pl.ds(row, 8), :] = total
        return carry

    events = [functools.partial(s.middle, k) for s in (first, second) for k in s.order()]
    ticks = 2 * steps
    plan = [[] for _ in range(ticks)]
    for j, event in enumerate(events):
        plan[min(ticks - 1, ticks * (j + 1) // len(events))].append(event)
    for k in third.order():
        plan[min(ticks - 1, 2)].append(functools.partial(third.middle, k))

    def add_base(at, total):
        third_out[at, :] = (total + base_ref[at, :].astype(F32)).astype(BF16)

    plan[min(ticks - 1, 9)].append(functools.partial(third.finish, add_base))

    def part_of_step(h, carry):
        lax.fori_loop(h * (groups // 2), (h + 1) * (groups // 2), group, 0)
        for tick in range(ticks - 1):
            if plan[tick]:

                @pl.when(step * 2 + h == tick)
                def _():
                    for event in plan[tick]:
                        event()

        return carry

    lax.fori_loop(0, 2, part_of_step, 0)
    g_rate = from_planes(grate_pl, count, planes) * (1.0 / LOG2E)
    through = from_planes(thr_pl, count, planes)
    pre = pre_ref[...]
    rate = softplus(pre)
    act = act_ref[...].astype(F32)
    gy = gy_ref[...]
    g_dtpre = ((g_rate + act * through) * sigmoid(pre)).astype(BF16)
    gact_ref[...] = gy * skip_ref[...] + rate * through
    dtb_ref[...] += jnp.sum(g_dtpre.astype(F32), axis=0, keepdims=True)
    sgrad_ref[...] += jnp.sum(gy * act, axis=0, keepdims=True)
    dtp_ref[...] += dot_nn(low_ref[...], g_dtpre)
    rows = 2 * width
    ones = jnp.ones((LANES, LANES), F32)
    sums = jnp.dot(part[...], ones, preferred_element_type=F32)
    sums = sums.reshape(count, rows, LANES)
    pick = lax.broadcasted_iota(jnp.int32, (1, rows, LANES), 1) == lax.broadcasted_iota(
        jnp.int32, (1, rows, LANES), 2
    )
    g_bc = jnp.sum(jnp.where(pick, sums, 0.0), axis=1)
    tokens_at = pl.ds(pl.multiple_of((steps - 1 - step) * count, count), count)
    mix_s[pl.ds(0, low_rank), tokens_at] = dot_nt(wdt_ref[...], g_dtpre)
    mix_s[pl.ds(low_rank, rows), tokens_at] = g_bc.T[:rows]

    @pl.when(step == steps - 1)
    def _():
        start_ref[...] = carry_s[...]
        sum_over_seq(seq, mix_s, mix_ref, *scratch[30:])
        for event in plan[ticks - 1]:
            event()
        first.finish(into(first_out))
        second.finish(into(second_out))
        for scatter in (first, second, third):
            scatter.drain()


def forward_scan(shape, pre, act, bc, a2, skip, init, weight, cot, block):
    lines, fast, seq_lines = shape
    length, features = pre.shape
    width, planes, _ = a2.shape
    steps = length // block
    rows = pl.BlockSpec((block, features), lambda i: (i, 0))
    whole = pl.BlockSpec((width, planes, LANES), lambda i: (0, 0, 0))
    plane = pltpu.VMEM((planes * block, LANES), F32)
    return pl.pallas_call(
        functools.partial(forward_kernel, shape, steps),
        grid=(steps,),
        in_specs=[
            rows, rows,
            pl.BlockSpec((block, 2 * width), lambda i: (i, 0), memory_space=pltpu.SMEM),
            whole,
            pl.BlockSpec((1, features), lambda i: (0, 0)),
            whole,
            pl.BlockSpec(weight.shape, lambda i: (0, 0)),
            pl.BlockSpec(cot.shape, lambda i: (0, 0)),
        ],
        out_specs=[
            rows,
            pl.BlockSpec((block // UNROLL, width, planes, LANES), lambda i: (i, 0, 0, 0)),
            whole, ANY, ANY,
        ],
        out_shape=[
            jax.ShapeDtypeStruct((length, features), F32),
            jax.ShapeDtypeStruct((length // UNROLL, width, planes, LANES), F32),
            jax.ShapeDtypeStruct((width, planes, LANES), F32),
            jax.ShapeDtypeStruct((lines * fast,) + weight.shape, BF16),
            jax.ShapeDtypeStruct((seq_lines * 2,) + cot.shape, BF16),
        ],
        scratch_shapes=[
            pltpu.VMEM((width, planes, LANES), F32), plane, plane, plane,
            pltpu.SemaphoreType.DMA((2,)),
            *Gather.semaphores(lines, fast), *Gather.semaphores(seq_lines, 2),
        ],
        compiler_params=comm_params(5),
        cost_estimate=pl.CostEstimate(
            flops=8 * length * features * width,
            bytes_accessed=24 * length * features,
            transcendentals=length * features * width,
        ),
        name="scan_forward",
    )(pre, act, bc, a2, skip, init, weight, cot)


def backward_scan(
    shape, pre, act, gy, bc, a2, skip, checks, w_dt, dt_low, base, first, second, third, block
):
    lines, fast, seq_lines = shape
    length, features = pre.shape
    width, planes, _ = a2.shape
    low_rank = w_dt.shape[0]
    steps = length // block
    rows = pl.BlockSpec((block, features), lambda i: (steps - 1 - i, 0))
    whole = pl.BlockSpec((width, planes, LANES), lambda i: (0, 0, 0))

    def all_of(rows, columns):
        return pl.BlockSpec((rows, columns), lambda i: (0, 0))

    line = all_of(1, features)
    plane = pltpu.VMEM((planes * block, LANES), F32)
    mixed = (low_rank + 2 * width, length)
    return pl.pallas_call(
        functools.partial(backward_kernel, shape, steps),
        grid=(steps,),
        in_specs=[
            rows, rows, rows,
            pl.BlockSpec(
                (block, 2 * width), lambda i: (steps - 1 - i, 0), memory_space=pltpu.SMEM
            ),
            whole, line,
            pl.BlockSpec(
                (block // UNROLL, width, planes, LANES), lambda i: (steps - 1 - i, 0, 0, 0)
            ),
            all_of(low_rank, features),
            pl.BlockSpec((low_rank, block), lambda i: (0, steps - 1 - i)),
            all_of(*base.shape),
            ANY, ANY, ANY,
        ],
        out_specs=[
            rows, whole, whole, line, line, all_of(low_rank, features), all_of(*mixed),
            all_of(*first.shape[1:]), all_of(*second.shape[1:]), all_of(*base.shape),
        ],
        out_shape=[
            jax.ShapeDtypeStruct((length, features), F32),
            jax.ShapeDtypeStruct((width, planes, LANES), F32),
            jax.ShapeDtypeStruct((width, planes, LANES), F32),
            jax.ShapeDtypeStruct((1, features), F32),
            jax.ShapeDtypeStruct((1, features), F32),
            jax.ShapeDtypeStruct((low_rank, features), F32),
            jax.ShapeDtypeStruct(mixed, BF16),
            jax.ShapeDtypeStruct(first.shape[1:], BF16),
            jax.ShapeDtypeStruct(second.shape[1:], F32),
            jax.ShapeDtypeStruct(base.shape, BF16),
        ],
        scratch_shapes=[pltpu.VMEM((width, planes, LANES), F32)]
        + [plane] * 5
        + [
            pltpu.VMEM((UNROLL * 2 * width * planes, LANES), F32),
            pltpu.VMEM((block * 2 * width, LANES), F32),
            pltpu.VMEM(mixed, F32),
            *Scatter.scratch(lines, fast, first.shape[1:]),
            *Scatter.scratch(lines, fast, second.shape[1:]),
            *Scatter.scratch(seq_lines, 2, third.shape[1:]),
            *sum_scratch(seq_lines, *mixed),
        ],
        compiler_params=comm_params(6),
        cost_estimate=pl.CostEstimate(
            flops=20 * length * features * width,
            bytes_accessed=28 * length * features,
            transcendentals=length * features * width,
        ),
        name="scan_backward",
    )(pre, act, gy, bc, a2, skip, checks, w_dt, dt_low, base, first, second, third)


def finish_kernel(shape, taps, history, refs, scratch):
    (
        gact, x_in, act, tok, w_x, w_g, gs_gate,
        mix, w_xt, head, kern, b_conv, dtp, a_grad, dtb, sgrad, g_half, own_tok, own_cot,
        final, start,
        small_out, halves_out, input_out, ends_out,
    ) = refs
    (
        gc, xb, actb, tokb, wxb, wgb, gsg, gs_x, xg, q_src, pack, small_src, ends_src, x_half,
        in_s, own_s,
    ) = scratch[:16]
    seg, seq = grids(shape)
    length, feats = act.shape
    at = 16
    sets = []
    for inside, size in ((True, 8), (True, 8), (True, 8)):
        sets.append(scratch[at : at + size])
        at += size
    swaps_s = [scratch[at + 2 * i : at + 2 * i + 2] for i in range(3)]
    small = Scatter(seg, small_src, sets[0], inside=True)
    x_sum = Scatter(seg, xg, sets[1], inside=True)
    q_sum = Scatter(seq, q_src, sets[2], inside=True)
    loads = [
        pltpu.make_async_copy(gact, gc.at[pl.ds(0, length)], in_s.at[0]),
        pltpu.make_async_copy(x_in, xb.at[pl.ds(8, length)], in_s.at[1]),
        pltpu.make_async_copy(tok, tokb, in_s.at[2]),
        pltpu.make_async_copy(act, actb, in_s.at[3]),
        pltpu.make_async_copy(gs_gate, gsg, in_s.at[4]),
        pltpu.make_async_copy(w_g, wgb, in_s.at[5]),
        pltpu.make_async_copy(w_x, wxb, in_s.at[6]),
    ]
    for load in loads:
        load.start()
    meet((seg, seq))
    own_rows = g_half.shape[0] // (seq.lines * seq.fast)

    def swap(half, src, sems):
        return Exchange(
            seq,
            lambda p: src.at[pl.ds(pl.multiple_of(p * own_rows, own_rows), own_rows)],
            lambda m: halves_out.at[half, m],
            sems,
        )

    swap_g = swap(1, g_half, swaps_s[1])
    swap_g.begin()
    xb[pl.ds(0, 8), :] = head[...]
    gc[pl.ds(length, 8), :] = jnp.zeros((8, feats), F32)
    loads[0].wait()
    big = LANES

    def add_mixed(i, carry):
        rows = pl.ds(pl.multiple_of(i * big, big), big)
        gc[rows, :] += dot_tn(mix[:, rows], w_xt[...])
        return carry

    lax.fori_loop(0, length // big, add_mixed, 0)
    loads[1].wait()
    tall = 32
    chunk = min(512, feats)
    sums_at = 8 * (taps + 1)
    pack[...] = jnp.zeros_like(pack)

    def through_conv(i, carry):
        t0 = pl.multiple_of(i * tall, tall)
        for c in range(0, feats, chunk):
            cols = pl.ds(c, chunk)
            wide = xb[pl.ds(t0, tall + 8), cols]
            rows = [wide[8 - history + k : 8 - history + k + tall] for k in range(taps)]
            conv = b_conv[:, cols]
            for k in range(taps):
                conv = conv + kern[pl.ds(k, 1), cols] * rows[k]
            sig = sigmoid(conv)
            g_conv = gc[pl.ds(t0, tall), cols] * sig * (1.0 + conv * (1.0 - sig))
            gc[pl.ds(t0, tall), cols] = g_conv
            for k in range(taps):
                term = g_conv * rows[k]
                pack[pl.ds(8 * k, 8), cols] += sum(
                    term[8 * j : 8 * j + 8] for j in range(tall // 8)
                )
            pack[pl.ds(8 * taps, 8), cols] += sum(
                g_conv[8 * j : 8 * j + 8] for j in range(tall // 8)
            )
        return carry

    lax.fori_loop(0, length // tall, through_conv, 0)
    loads[2].wait()

    def to_input(i, carry):
        t0 = pl.multiple_of(i * tall, tall)
        lines = tokb[pl.ds(t0, tall), :].astype(F32)
        rstd = lax.rsqrt(jnp.mean(lines * lines, axis=1, keepdims=True) + EPSILON)
        for c in range(0, feats, chunk):
            cols = pl.ds(c, chunk)
            wide = gc[pl.ds(t0, tall + 8), cols]
            g_x = kern[pl.ds(0, 1), cols] * wide[history : history + tall]
            for k in range(1, taps):
                g_x = g_x + kern[pl.ds(k, 1), cols] * wide[history - k : history - k + tall]
            gs_x[pl.ds(t0, tall), cols] = (rstd * g_x).astype(BF16)
        return carry

    lax.fori_loop(0, length // tall, to_input, 0)
    loads[3].wait()
    low_rank = dtp.shape[0]
    mixes = mix.shape[0]
    width = a_grad.shape[0]
    part = small_src.shape[2]
    xp = dot_nn(mix[...], actb[...])
    for g in range(small_src.shape[0]):
        cols = slice(g * part, (g + 1) * part)
        small_src[g, pl.ds(0, low_rank), :] = dtp[:, cols].astype(BF16)
        small_src[g, pl.ds(low_rank, mixes), :] = xp[:, cols].astype(BF16)
        base = low_rank + mixes
        small_src[g, pl.ds(base, width), :] = a_grad[:, cols].astype(BF16)
        lines = [
            jnp.sum(pack[pl.ds(8 * k, 8), cols], axis=0, keepdims=True) for k in range(taps + 1)
        ]
        lines += [dtb[:, cols], sgrad[:, cols]]
        lines.append(jnp.zeros((16 - len(lines), part), F32))
        small_src[g, pl.ds(base + width, 16), :] = jnp.concatenate(lines, axis=0).astype(BF16)
    small.begin()

    block_rows = xg.shape[1]

    def partial(index):
        cols = pl.ds(pl.multiple_of(index * block_rows, block_rows), block_rows)
        xg[index] = dot_tn(tokb[:, cols], gs_x[...]).astype(BF16)

    by_block = block_rows % LANES == 0
    if not by_block:
        for index in range(xg.shape[0]):
            cols = slice(index * block_rows, (index + 1) * block_rows)
            xg[index] = dot_tn(tokb[:, cols], gs_x[...]).astype(BF16)

    def leave(j, carry):
        k = seg.lines - 1 - j
        for e in range(1, seg.fast):
            if by_block:
                partial(x_sum.index(k, e))
            x_sum.across(k, e).start()
        return carry

    lax.fori_loop(0, seg.lines, leave, 0)
    def stay(j, carry):
        if by_block:
            partial(x_sum.index(seg.lines - 1 - j, 0))
        return carry

    lax.fori_loop(0, seg.lines, stay, 0)
    ends_in = jnp.concatenate(
        [
            final[...],
            xb[pl.ds(length, 8), :][8 - history :],
            start[...],
            sum_head(gc, kern, history, taps),
            jnp.zeros((ends_src.shape[1] - 2 * (width + history), feats), F32),
        ],
        axis=0,
    )
    piece = ends_src.shape[2]
    for p in range(ends_src.shape[0]):
        ends_src[p] = ends_in[:, p * piece : (p + 1) * piece]
    end_swap = Exchange(seq, lambda p: ends_src.at[p], lambda m: ends_out.at[m], swaps_s[2])
    end_swap.begin()
    loads[4].wait()
    loads[5].wait()
    loads[6].wait()
    own_len = own_tok.shape[0]
    model = own_tok.shape[1]
    wide = 512

    def normed(index):
        rows = pl.ds(pl.multiple_of(index * own_len, own_len), own_len)

        def column(c, carry):
            cols = pl.ds(pl.multiple_of(c * wide, wide), wide)
            q_src[index, :, cols] = (
                dot_nt(gsg[rows, :], wgb[cols, :]) + dot_nt(gs_x[rows, :], wxb[cols, :])
            ).astype(BF16)
            return carry

        lax.fori_loop(0, model // wide, column, 0)

    def leave_q(j, carry):
        k = seq.lines - 1 - j
        normed(q_sum.index(k, 1))
        q_sum.across(k, 1).start()
        return carry

    def stay_q(j, carry):
        normed(q_sum.index(seq.lines - 1 - j, 0))
        return carry

    lax.fori_loop(0, seq.lines, leave_q, 0)
    lax.fori_loop(0, seq.lines, stay_q, 0)
    for k in small.order():
        small.middle(k)
    for j, k in enumerate(x_sum.order()):
        x_sum.middle(k)
        if j == seg.lines - 2:
            for m in q_sum.order():
                q_sum.middle(m)

    def input_grad(at, total):
        own = own_tok[at, :].astype(F32)
        square = 1.0 / (jnp.mean(own * own, axis=1, keepdims=True) + EPSILON)
        input_out[at, :] = (
            own_cot[at, :].astype(F32)
            + total
            - own * (square * jnp.mean(total * own, axis=1, keepdims=True))
        ).astype(BF16)

    q_sum.finish(input_grad)
    small.finish(into(small_out))
    x_sum.finish(into(x_half))
    swap_x = swap(0, x_half, swaps_s[0])
    swap_x.begin()
    own = pl.ds(pl.multiple_of(seq.here * own_rows, own_rows), own_rows)
    keeps = [
        pltpu.make_async_copy(x_half.at[own], halves_out.at[0, seq.here], own_s.at[0]),
        pltpu.make_async_copy(g_half.at[own], halves_out.at[1, seq.here], own_s.at[1]),
        pltpu.make_async_copy(ends_src.at[seq.here], ends_out.at[seq.here], own_s.at[2]),
    ]
    for keep in keeps:
        keep.start()
    for scatter in (small, x_sum, q_sum):
        scatter.drain()
    for exchange in (swap_g, end_swap, swap_x):
        exchange.arrived()
        exchange.drain()
    for keep in keeps:
        keep.wait()


def sum_head(gc, kern, history, taps):
    top = gc[pl.ds(0, 8), :]
    rows = []
    for j in range(history):
        rows.append(
            sum(kern[pl.ds(k, 1), :] * top[j - k : j - k + 1] for k in range(min(j + 1, taps)))
        )
    return jnp.concatenate(rows, axis=0)


def finish_all(shape, taps, history, big, small):
    lines, fast, seq_lines = shape
    segs, seqs = lines * fast, seq_lines * 2
    gact, x_in, act, tok, w_x, w_g, gs_gate = big
    mix, w_xt, head, kern, b_conv, dtp, a_grad, dtb, sgrad, g_half, own_tok, own_cot = small[:12]
    length, feats = act.shape
    own_len, model = own_tok.shape
    width = a_grad.shape[0]
    rows = dtp.shape[0] + mix.shape[0] + width + 16
    block_rows = model // segs
    own_rows = g_half.shape[0] // seqs
    ends = (seqs, 2 * (width + history) + (-2 * (width + history)) % 8, feats // seqs)
    dma = pltpu.SemaphoreType.DMA
    scratch = [
        pltpu.VMEM((length + 8, feats), F32),
        pltpu.VMEM((length + 8, feats), F32),
        pltpu.VMEM((length, feats), BF16),
        pltpu.VMEM((length, model), BF16),
        pltpu.VMEM((model, feats), BF16),
        pltpu.VMEM((model, feats), BF16),
        pltpu.VMEM((length, feats), BF16),
        pltpu.VMEM((length, feats), BF16),
        pltpu.VMEM((segs, block_rows, feats), BF16),
        pltpu.VMEM((seqs, own_len, model), BF16),
        pltpu.VMEM((8 * (taps + 1), feats), F32),
        pltpu.VMEM((segs, rows, feats // segs), BF16),
        pltpu.VMEM(ends, F32),
        pltpu.VMEM((block_rows, feats), BF16),
        dma((7,)), dma((3,)),
        *Scatter.scratch(lines, fast, (rows, feats // segs), inside=True),
        *Scatter.scratch(lines, fast, (block_rows, feats), inside=True),
        *Scatter.scratch(seq_lines, 2, (own_len, model), inside=True),
        *Exchange.semaphores(seqs), *Exchange.semaphores(seqs), *Exchange.semaphores(seqs),
    ]

    def kernel(*refs):
        finish_kernel(shape, taps, history, refs[:25], refs[25:])

    return pl.pallas_call(
        kernel,
        in_specs=[ANY] * 7 + [INSIDE] * 14,
        out_specs=[INSIDE] * 4,
        out_shape=[
            jax.ShapeDtypeStruct((rows, feats // segs), F32),
            jax.ShapeDtypeStruct((2, seqs, own_rows, feats), BF16),
            jax.ShapeDtypeStruct((own_len, model), BF16),
            jax.ShapeDtypeStruct(ends, F32),
        ],
        scratch_shapes=scratch,
        compiler_params=comm_params(4),
        name="finish",
    )(*big, *small)


def gather_kernel(
    shape, scaled, small, tokens,
    w_x, small_all, tok, g_part,
    x_part, tok_in, g_own, local_s, x_sems, small_sems, tok_sems, swap_x, swap_g,
):
    seg, seq = grids(shape)
    load_tok = pltpu.make_async_copy(tokens, tok_in, local_s.at[0])
    load_own = pltpu.make_async_copy(scaled.at[seq.here, 0], x_part.at[seq.here], local_s.at[1])
    load_gate = pltpu.make_async_copy(scaled.at[seq.here, 1], g_own, local_s.at[3])
    load_tok.start()
    load_own.start()
    load_gate.start()
    meet((seg, seq))
    swap_x = Exchange(seq, lambda p: scaled.at[p, 0], lambda m: x_part.at[m], swap_x)
    swap_g = Exchange(seq, lambda p: scaled.at[p, 1], lambda m: g_part.at[m], swap_g)
    swap_x.begin()
    smalls = Gather(seg, small, small_all, small_sems)
    smalls.begin()
    load_tok.wait()
    toks = Gather(seq, tok_in, tok, tok_sems)
    toks.begin()
    store_tok = pltpu.make_async_copy(tok_in, tok.at[seq.here], local_s.at[0])
    store_small = pltpu.make_async_copy(small, small_all.at[seg.here], local_s.at[2])
    store_tok.start()
    store_small.start()
    load_gate.wait()
    store_gate = pltpu.make_async_copy(g_own, g_part.at[seq.here], local_s.at[3])
    store_gate.start()
    load_own.wait()
    swap_x.arrived()
    halves = Gather(seg, x_part, w_x, x_sems)
    halves.begin()
    store_own = pltpu.make_async_copy(x_part, w_x.at[seg.here], local_s.at[1])
    store_own.start()
    swap_g.begin()
    for k in range(1, seq.lines):
        toks.step(k)
    for k in range(1, seg.lines):
        smalls.step(k)
        halves.step(k)
    toks.finish()
    smalls.finish()
    halves.finish()
    swap_g.arrived()
    swap_x.drain()
    swap_g.drain()
    store_tok.wait()
    store_small.wait()
    store_gate.wait()
    store_own.wait()


def gather_start(shape, scaled, small, tokens):
    lines, fast, seq_lines = shape
    segs, seqs = lines * fast, seq_lines * 2
    rows, feats = scaled.shape[2:]
    sems = Gather.semaphores
    flat = [
        pltpu.VMEM((seqs, rows, feats), BF16),
        pltpu.VMEM(tokens.shape, BF16),
        pltpu.VMEM((rows, feats), BF16),
        pltpu.SemaphoreType.DMA((4,)),
        *sems(lines, fast), *sems(lines, fast), *sems(seq_lines, 2),
        *Exchange.semaphores(seqs), *Exchange.semaphores(seqs),
    ]

    def kernel(*refs):
        ins, rest = refs[:7], refs[7:]
        gather_kernel(
            shape, *ins, *rest[:4], rest[4:10], rest[10:16], rest[16:22], rest[22:24], rest[24:26]
        )

    w_x, small_all, tok, g_part = pl.pallas_call(
        kernel,
        in_specs=[ANY, INSIDE, ANY],
        out_specs=[ANY] * 4,
        out_shape=[
            jax.ShapeDtypeStruct((segs, seqs, rows, feats), BF16),
            jax.ShapeDtypeStruct((segs,) + small.shape, BF16),
            jax.ShapeDtypeStruct((seqs,) + tokens.shape, BF16),
            jax.ShapeDtypeStruct((seqs, rows, feats), BF16),
        ],
        scratch_shapes=flat,
        compiler_params=comm_params(1),
        name="gather_start",
    )(scaled, small, tokens)
    return w_x.reshape(-1, feats), small_all, tok.reshape(-1, tokens.shape[1]), g_part


def sum_scratch(seq_lines, rows, width):
    part = pltpu.VMEM((rows, width // 2), BF16)
    dma = pltpu.SemaphoreType.DMA
    return [
        part, part, part,
        pltpu.VMEM((max(seq_lines - 1, 1), rows, width // 2), BF16),
        pltpu.VMEM((2, rows, width // 2), BF16),
        dma, dma, dma((seq_lines,)), dma((seq_lines,)), dma, dma,
    ]


def total_over_seq(shape, x, collective_id):
    def kernel(x_ref, out_ref, *scratch):
        _, seq = grids(shape)
        meet((seq,))
        sum_over_seq(seq, x_ref, out_ref, *scratch)

    return pl.pallas_call(
        kernel,
        in_specs=[INSIDE],
        out_specs=INSIDE,
        out_shape=jax.ShapeDtypeStruct(x.shape, BF16),
        scratch_shapes=sum_scratch(shape[2], *x.shape),
        compiler_params=comm_params(collective_id),
        name="total_over_seq",
    )(x)


def unpack_kernel(
    seqs, taps, history, low_rank, width,
    small, halves, ends, mixed, input_grad, out_grad, weight, gain,
    mixed_o, final_o, final_c, input_o, start_o, start_c, gain_o, in_o, cw_o, cb_o, xp_o, dtp_o,
    dtb_o, a_o, skip_o, out_o,
):
    mixed_o[0] = mixed[...]
    input_o[0] = input_grad[...]
    out_o[...] = out_grad[...]
    part = small.shape[1]
    columns = xp_o.shape[1]
    dtp_o[...] = small[pl.ds(0, low_rank), :]
    turned = small[pl.ds(low_rank, low_rank), :].T
    xp_o[:, pl.ds(0, low_rank)] = turned
    xp_o[:, pl.ds(low_rank, columns - low_rank)] = small[
        pl.ds(2 * low_rank, columns - low_rank), :
    ].T
    at = low_rank + columns
    a_o[...] = small[pl.ds(at, width), :]
    lines = small[pl.ds(at + width, 16), :]
    cw_o[...] = lines[:taps]
    cb_o[...] = lines[taps]
    dtb_o[...] = lines[taps + 1]
    skip_o[...] = lines[taps + 2]
    each = final_o.shape[2] // part // seqs
    for s in range(seqs):
        rows = ends[s]
        for g in range(each):
            got = rows[:, g * part : (g + 1) * part]
            cols = pl.ds((g * seqs + s) * part, part)
            final_o[0, :, cols] = got[:width]
            final_c[0, :, cols] = got[width : width + history]
            start_o[0, :, cols] = got[width + history : 2 * width + history]
            start_c[0, :, cols] = got[2 * width + history : 2 * (width + history)]
    scale = gain[...]
    total = jnp.zeros((in_o.shape[0], part), F32)
    groups = halves.shape[3] // part
    for half in range(2):
        for s in range(seqs):
            for g in range(groups):
                raw = halves[half, s, :, g * part : (g + 1) * part].astype(F32)
                cols = pl.ds(((half * groups + g) * seqs + s) * part, part)
                in_o[:, cols] = raw * scale
                total = total + raw * weight[:, cols].astype(F32)
    gain_o[...] = jnp.sum(total.T, axis=0)


def unpack(taps, history, low_rank, width, small, halves, ends, mixed, input_grad, out_grad,
           weight, gain):
    seqs, own_rows, feats = halves.shape[1:]
    part = small.shape[1]
    model = mixed.shape[1]
    kept = ends.shape[2] * seqs
    f32 = lambda *dims: jax.ShapeDtypeStruct(dims, F32)
    return pl.pallas_call(
        functools.partial(unpack_kernel, seqs, taps, history, low_rank, width),
        in_specs=[INSIDE] * 8,
        out_specs=[INSIDE] * 16,
        out_shape=[
            jax.ShapeDtypeStruct((1,) + mixed.shape, BF16),
            f32(1, width, kept), f32(1, history, kept),
            jax.ShapeDtypeStruct((1,) + input_grad.shape, BF16),
            f32(1, width, kept), f32(1, history, kept),
            f32(own_rows), f32(*weight.shape),
            f32(taps, part), f32(part), f32(part, low_rank + 2 * width), f32(low_rank, part),
            f32(part), f32(width, part), f32(part), f32(part, model),
        ],
        name="unpack",
    )(small, halves, ends, mixed, input_grad, out_grad, weight, gain)


def body(
    tokens, norm_gain, in_proj, conv_weight, conv_bias, x_proj, dt_proj, dt_bias,
    a_log, d_skip, out_proj, init_state, init_conv, cotangent,
):
    segs, seqs = lax.axis_size("seg"), lax.axis_size("seq")
    place = lax.axis_index("seq")
    own_rows, both = in_proj.shape
    part = conv_bias.shape[0]
    feats = segs * part
    taps = conv_weight.shape[0]
    width = a_log.shape[0]
    low_rank = dt_proj.shape[0]
    planes = feats // LANES
    own_len, model = tokens.shape[1:]
    length = own_len * seqs
    block = 64
    seq_lines = seqs // 2
    shape = (segs // seq_lines, seq_lines, seq_lines)

    def mine(rows):
        shaped = rows.reshape(rows.shape[0], segs, seqs, part)
        return lax.dynamic_index_in_dim(shaped, place, 2, keepdims=False).reshape(
            rows.shape[0], feats
        )

    gain_col = norm_gain.astype(F32)[:, None]
    own_weight = in_proj.astype(F32)
    scaled = (own_weight * gain_col).astype(BF16)
    scaled = scaled.reshape(own_rows, 2, segs, seqs, part).transpose(3, 1, 0, 2, 4)
    scaled = scaled.reshape(seqs, 2, own_rows, feats)
    small = jnp.concatenate(
        [
            dt_proj, x_proj.T, a_log, conv_weight, conv_bias[None], dt_bias[None], d_skip[None],
        ],
        axis=0,
    )
    small = jnp.pad(small, ((0, -small.shape[0] % 16), (0, 0)))
    w_x_half, small_all, tok, g_part = gather_start(shape, scaled, small, tokens[0])
    w_g_half = lax.all_gather(
        g_part.reshape(seqs * own_rows, feats), "seg", axis=0, tiled=True
    )

    small_all = small_all.transpose(1, 0, 2).reshape(small.shape[0], feats)
    w_dt = small_all[:low_rank]
    w_xt = small_all[low_rank : low_rank + x_proj.shape[1]]
    rest = small_all[low_rank + x_proj.shape[1] :].astype(F32)
    a_mat = -jnp.exp(rest[:width])
    a2 = (a_mat * LOG2E).reshape(width, planes, LANES)
    kernel = rest[width : width + taps]
    b_conv = rest[width + taps][None]
    b_dt = rest[width + taps + 1][None]
    skip = rest[width + taps + 2][None]

    tok_float = tok.astype(F32)
    rstd = lax.rsqrt(jnp.mean(tok_float * tok_float, axis=1, keepdims=True) + EPSILON)
    x_in = rstd * dot_nn(tok, w_x_half)
    history = init_conv.shape[1]
    head = mine(init_conv[0])
    padded = jnp.concatenate([head, x_in], axis=0)
    conv_out = b_conv + sum(kernel[k] * padded[k : k + length] for k in range(taps))
    act = jax.nn.silu(conv_out).astype(BF16)
    mixed_x = total_over_seq(shape, dot_nt(w_xt, act), 2)
    dt_low = mixed_x[:low_rank]
    bc = mixed_x[low_rank:].astype(F32).T
    pre = dot_tn(dt_low, w_dt) + b_dt
    init = mine(init_state[0]).reshape(width, planes, LANES)
    y_val, checks, final, w_out, cot = forward_scan(
        shape, pre, act, bc, a2, skip, init, out_proj, cotangent[0], block
    )
    w_out = w_out.reshape(feats, model)
    cot = cot.reshape(length, model)
    y_val, w_g_half = lax.optimization_barrier((y_val, w_g_half))
    gate = rstd * dot_nn(tok, w_g_half)
    gated = (y_val * jax.nn.silu(gate)).astype(BF16)
    out_part = dot_nn(gated, w_out).astype(BF16)

    g_gated = dot_nt(cot, w_out)
    sig_gate = jax.nn.sigmoid(gate)
    gy = g_gated * gate * sig_gate
    gs_gate = (
        rstd * g_gated * y_val * sig_gate * (1.0 + gate * (1.0 - sig_gate))
    ).astype(BF16)
    out_grad = dot_tn(gated, cot).astype(BF16)
    gate_grad = dot_tn(tok, gs_gate).astype(BF16)
    g_actp, a_sum, start, dtb_grad, skip_grad, dtp_grad, g_mixed, g_half, out_grad, mixed_out = (
        backward_scan(
            shape, pre, act, gy, bc, a2, skip, checks, w_dt, dt_low, tokens[0],
            gate_grad.reshape(segs, seqs * own_rows, feats),
            out_grad.reshape(segs, part, model),
            out_part.reshape(seqs, own_len, model),
            2 * block,
        )
    )
    grads, halves, input_grad, ends = finish_all(
        shape, taps, history,
        (g_actp, x_in, act, tok, w_x_half, w_g_half, gs_gate),
        (
            g_mixed, w_xt,
            jnp.pad(head, ((8 - history, 0), (0, 0))),
            jnp.pad(kernel, ((0, -taps % 8), (0, 0))),
            b_conv, dtp_grad, a_sum.reshape(width, feats) * a_mat, dtb_grad, skip_grad, g_half,
            tokens[0], cotangent[0],
            final.reshape(width, feats), start.reshape(width, feats),
        ),
    )
    if part % LANES == 0:
        return unpack(
            taps, history, low_rank, width, grads, halves, ends, mixed_out, input_grad, out_grad,
            in_proj, gain_col,
        )
    ends = (
        ends.reshape(seqs, ends.shape[1], segs // seqs, part)
        .transpose(1, 2, 0, 3)
        .reshape(ends.shape[1], feats)
    )
    raw_grad = (
        halves.reshape(2, seqs, own_rows, segs, part)
        .transpose(2, 0, 3, 1, 4)
        .reshape(own_rows, both)
        .astype(F32)
    )
    in_grad = raw_grad * gain_col
    gain_grad = jnp.sum(raw_grad * own_weight, axis=1)

    at = width + history
    xp_at = low_rank + x_proj.shape[1]
    return (
        mixed_out[None],
        ends[None, :width],
        ends[None, width:at],
        input_grad[None],
        ends[None, at : at + width],
        ends[None, at + width : at + width + history],
        gain_grad,
        in_grad,
        grads[xp_at + width : xp_at + width + taps],
        grads[xp_at + width + taps],
        grads[low_rank:xp_at].T,
        grads[:low_rank],
        grads[xp_at + width + taps + 1],
        grads[xp_at : xp_at + width],
        grads[xp_at + width + taps + 2],
        out_grad,
    )


def solution(mesh):
    spread = ("seg", "seq")
    placed = (
        P("seg", "seq", None),
        P(spread),
        P(spread, None),
        P(None, spread),
        P(spread),
        P(spread, None),
        P(None, spread),
        P(spread),
        P(None, spread),
        P(spread),
        P(spread, None),
        P("seg", None, None),
        P("seg", None, None),
        P("seg", "seq", None),
    )
    return jax.shard_map(
        body,
        mesh=mesh,
        in_specs=placed,
        out_specs=(
            P("seg", "seq", None),
            P("seg", None, "seq"),
            P("seg", None, "seq"),
            P("seg", "seq", None),
            P("seg", None, "seq"),
            P("seg", None, "seq"),
            P(spread),
            P(spread, None),
            P(None, spread),
            P(spread),
            P(spread, None),
            P(None, spread),
            P(spread),
            P(None, spread),
            P(spread),
            P(spread, None),
        ),
        check_vma=False,
    )
```

```python
import functools

import jax
import jax.numpy as jnp
from jax import lax
from jax.experimental import pallas as pl
from jax.experimental.pallas import tpu as pltpu
from jax.sharding import PartitionSpec as P

EPSILON = 1e-05
LOG2E = 1.4426950408889634
LANES = 128
UNROLL = 8
F32 = jnp.float32
BF16 = jnp.bfloat16


def dot_nn(a, b):
    return jnp.dot(a, b, preferred_element_type=F32)


def dot_tn(a, b):
    return lax.dot_general(a, b, (((0,), (0,)), ((), ())), preferred_element_type=F32)


def dot_nt(a, b):
    return lax.dot_general(a, b, (((1,), (1,)), ((), ())), preferred_element_type=F32)


def sigmoid(v):
    return 1.0 / (1.0 + jnp.exp(-v))


def softplus(v):
    return jnp.maximum(v, 0.0) + jnp.log1p(jnp.exp(-jnp.abs(v)))


def to_planes(planes_ref, rows):
    count = rows.shape[0]
    for s in range(rows.shape[1] // LANES):
        planes_ref[pl.ds(s * count, count), :] = rows[:, s * LANES : (s + 1) * LANES]


def from_planes(planes_ref, count, planes):
    return jnp.concatenate(
        [planes_ref[pl.ds(s * count, count), :] for s in range(planes)], axis=1
    )


MESH_ID = pl.DeviceIdType.MESH
VMEM_MOST = 63 * 1024 * 1024 + 512 * 1024


class Grid:
    def __init__(self, axis, lines, fast):
        self.axis, self.lines, self.fast = axis, lines, fast
        self.here = lax.axis_index(axis)
        self.line = self.here // fast
        self.lane = self.here - self.line * fast

    def at(self, line, lane):
        return line * self.fast + lane

    def line_peer(self, k):
        return lax.rem(self.line + k, self.lines)

    def lane_peer(self, e):
        return lax.rem(self.lane + e, self.fast)

    def copy(self, src, dst, sent, got, index):
        return pltpu.make_async_remote_copy(
            src_ref=src, dst_ref=dst, send_sem=sent, recv_sem=got,
            device_id={self.axis: index}, device_id_type=MESH_ID,
        )


def meet(groups):
    barrier = pltpu.get_barrier_semaphore()
    total = 0
    for grid in groups:
        size = grid.lines * grid.fast
        for k in range(1, size):
            pl.semaphore_signal(
                barrier, inc=1, device_id={grid.axis: lax.rem(grid.here + k, size)},
                device_id_type=MESH_ID,
            )
        total += size - 1
    pl.semaphore_wait(barrier, total)


class Gather:
    def __init__(self, grid, own, out, sems, piece=None):
        self.grid, self.own, self.out, self.piece = grid, own, out, piece
        self.up_s, self.up_r, self.dn_s, self.dn_r, self.x_s, self.x_r = sems

    @staticmethod
    def semaphores(lines, fast):
        hops = pltpu.SemaphoreType.DMA((lines,))
        across = pltpu.SemaphoreType.DMA((lines, fast))
        return [hops, hops, hops, hops, across, across]

    def block(self, line, lane=None):
        grid = self.grid
        index = grid.at(line, grid.lane if lane is None else lane)
        return self.out.at[index] if self.piece is None else self.out.at[index, self.piece]

    def up(self, k):
        grid = self.grid
        block = self.block(jnp.maximum(grid.line - k, 0))
        return grid.copy(
            self.own if k == 0 else block, block, self.up_s.at[k], self.up_r.at[k],
            grid.at(jnp.minimum(grid.line + 1, grid.lines - 1), grid.lane),
        )

    def down(self, k):
        grid = self.grid
        block = self.block(jnp.minimum(grid.line + k, grid.lines - 1))
        return grid.copy(
            self.own if k == 0 else block, block, self.dn_s.at[k], self.dn_r.at[k],
            grid.at(jnp.maximum(grid.line - 1, 0), grid.lane),
        )

    def sends_up(self, k):
        return jnp.logical_and(self.grid.line + 1 < self.grid.lines, self.grid.line >= k)

    def sends_down(self, k):
        return jnp.logical_and(self.grid.line > 0, self.grid.line + k < self.grid.lines)

    def across(self, line, slot, e, own=False):
        grid = self.grid
        block = self.block(line)
        return grid.copy(
            self.own if own else block, block, self.x_s.at[slot, e], self.x_r.at[slot, e],
            grid.at(grid.line, grid.lane_peer(e)),
        )

    def slots(self):
        return range(self.grid.lines)

    def begin(self):
        grid = self.grid
        for when, copy in ((self.sends_up(0), self.up(0)), (self.sends_down(0), self.down(0))):
            pl.when(when)(copy.start)
        for e in range(1, grid.fast):
            self.across(grid.line, 0, e, own=True).start()

    def step(self, k):
        grid = self.grid

        def arrived(copy, line, slot, forward, onward):
            copy.wait_recv()
            if k < grid.lines - 1:
                pl.when(forward(k))(onward(k).start)
            for e in range(1, grid.fast):
                self.across(line, slot, e).start()

        below, above = grid.line - k, grid.line + k

        @pl.when(below >= 0)
        def _():
            arrived(self.up(k - 1), below, grid.lines - k, self.sends_up, self.up)

        @pl.when(above < grid.lines)
        def _():
            arrived(self.down(k - 1), above, k, self.sends_down, self.down)

    def finish(self):
        grid = self.grid
        for k in range(grid.lines - 1):
            pl.when(self.sends_up(k))(self.up(k).wait_send)
            pl.when(self.sends_down(k))(self.down(k).wait_send)
        for slot in self.slots():
            for e in range(1, grid.fast):
                copy = self.across(grid.line_peer(slot), slot, e, own=slot == 0)
                copy.wait_send()
                copy.wait_recv()


class Scatter:
    def __init__(self, grid, src, scratch, inside=False):
        self.grid, self.src, self.inside = grid, src, inside
        if not inside:
            self.own, self.o_s = scratch[:2]
            scratch = scratch[2:]
        self.xbuf, self.stage, self.zbuf, self.acc = scratch[:4]
        self.x_s, self.x_r, self.z_s, self.z_r = scratch[4:]

    @staticmethod
    def scratch(lines, fast, shape, inside=False):
        dma = pltpu.SemaphoreType.DMA
        shape = tuple(shape)
        loads = [] if inside else [pltpu.VMEM((lines,) + shape, BF16), dma((lines,))]
        return loads + [
            pltpu.VMEM((lines, fast - 1) + shape, BF16),
            pltpu.VMEM((lines - 1,) + shape, BF16),
            pltpu.VMEM((lines - 1,) + shape, BF16),
            pltpu.VMEM(shape, F32),
            dma((lines, fast)), dma((lines, fast)), dma((lines,)), dma((lines,)),
        ]

    def index(self, k, e):
        return self.grid.at(self.grid.line_peer(k), self.grid.lane_peer(e))

    def across(self, k, e):
        grid = self.grid
        return grid.copy(
            self.src.at[self.index(k, e)], self.xbuf.at[k, e - 1],
            self.x_s.at[k, e], self.x_r.at[k, e], grid.at(grid.line, grid.lane_peer(e)),
        )

    def local(self, k):
        return pltpu.make_async_copy(
            self.src.at[self.index(k, 0)], self.own.at[k], self.o_s.at[k]
        )

    def along(self, k):
        grid = self.grid
        return grid.copy(
            self.stage.at[k - 1], self.zbuf.at[k - 1], self.z_s.at[k], self.z_r.at[k],
            grid.at(grid.line_peer(k), grid.lane),
        )

    def order(self):
        return list(range(self.grid.lines - 1, -1, -1))

    def begin(self):
        for k in self.order():
            for e in range(1, self.grid.fast):
                self.across(k, e).start()
            if not self.inside:
                self.local(k).start()

    def rows(self, step):
        count = self.acc.shape[0]
        size = 16 if count % 16 == 0 else 8

        def run(i, carry):
            step(pl.ds(pl.multiple_of(i * size, size), size))
            return carry

        lax.fori_loop(0, count // size, run, 0)

    def middle(self, k):
        for e in range(1, self.grid.fast):
            self.across(k, e).wait_recv()
        if self.inside:
            own = self.src.at[self.index(k, 0)]
        else:
            self.local(k).wait()
            own = self.own.at[k]

        def add(at):
            total = own[at, :].astype(F32)
            for e in range(self.grid.fast - 1):
                total = total + self.xbuf[k, e, at, :].astype(F32)
            if k > 0:
                self.stage[k - 1, at, :] = total.astype(BF16)
            else:
                self.acc[at, :] = total

        self.rows(add)
        if k > 0:
            self.along(k).start()

    def finish(self, write):
        for k in range(1, self.grid.lines):
            self.along(k).wait_recv()

        def add(at):
            total = self.acc[at, :]
            for k in range(self.grid.lines - 1):
                total = total + self.zbuf[k, at, :].astype(F32)
            write(at, total)

        self.rows(add)

    def drain(self):
        for k in self.order():
            for e in range(1, self.grid.fast):
                self.across(k, e).wait_send()
            if k > 0:
                self.along(k).wait_send()


def into(ref):
    def write(at, total):
        ref[at, :] = total.astype(ref.dtype)

    return write


class Exchange:
    def __init__(self, grid, src, dst, sems):
        self.grid, self.src, self.dst = grid, src, dst
        self.sent, self.got = sems
        self.size = grid.lines * grid.fast

    @staticmethod
    def semaphores(size):
        return [pltpu.SemaphoreType.DMA((size,)), pltpu.SemaphoreType.DMA((size,))]

    def one(self, k):
        grid = self.grid
        peer = lax.rem(grid.here + k, self.size)
        return grid.copy(
            self.src(peer), self.dst(grid.here), self.sent.at[k], self.got.at[k], peer
        )

    def begin(self):
        for k in range(1, self.size):
            self.one(k).start()

    def arrived(self):
        for k in range(1, self.size):
            self.one(k).wait_recv()

    def drain(self):
        for k in range(1, self.size):
            self.one(k).wait_send()


ANY = pl.BlockSpec(memory_space=pl.ANY)
INSIDE = pl.BlockSpec(memory_space=pltpu.VMEM)


def comm_params(collective_id):
    return pltpu.CompilerParams(
        collective_id=collective_id, has_side_effects=True, vmem_limit_bytes=VMEM_MOST
    )


def grids(shape):
    lines, fast, seq_lines = shape
    return Grid("seg", lines, fast), Grid("seq", seq_lines, 2)


def sum_over_seq(seq, x_ref, out_ref, half, got, mine, others, whole, *sems):
    lane_s, lane_r, line_s, line_r, back_s, back_r = sems
    width = x_ref.shape[1] // 2
    lines = seq.lines
    other = 1 - seq.lane
    left = pl.ds(0, width)
    right = pl.ds(width, width)

    @pl.when(seq.lane == 0)
    def _():
        half[...] = x_ref[:, right].astype(BF16)

    @pl.when(seq.lane == 1)
    def _():
        half[...] = x_ref[:, left].astype(BF16)

    swap = seq.copy(half, got, lane_s, lane_r, seq.at(seq.line, other))
    swap.start()
    swap.wait()

    @pl.when(seq.lane == 0)
    def _():
        mine[...] = (x_ref[:, left] + got[...].astype(F32)).astype(BF16)

    @pl.when(seq.lane == 1)
    def _():
        mine[...] = (x_ref[:, right] + got[...].astype(F32)).astype(BF16)

    copies = [
        seq.copy(
            mine, others.at[k - 1], line_s.at[k], line_r.at[k], seq.at(seq.line_peer(k), seq.lane)
        )
        for k in range(1, lines)
    ]
    for copy in copies:
        copy.start()
    for copy in copies:
        copy.wait()
    total = mine[...].astype(F32)
    for k in range(lines - 1):
        total = total + others[k].astype(F32)
    whole[seq.lane] = total.astype(BF16)
    back = seq.copy(
        whole.at[seq.lane], whole.at[seq.lane], back_s, back_r, seq.at(seq.line, other)
    )
    back.start()
    back.wait()
    out_ref[:, left] = whole[0]
    out_ref[:, right] = whole[1]


def forward_kernel(
    shape, steps,
    low_ref, wdt_ref, bias_ref, act_ref, bc_ref, a_ref, skip_ref, init_ref, weight_ref, cot_ref,
    tok_ref, gate_one, gate_src,
    y_ref, pre_ref, check_ref, final_ref, gate_ref, gated_ref, weights_ref, cots_ref, gate_two,
    state, rate_pl, drive_pl, y_pl, w_one, w_two, local_s, *sems,
):
    count = pre_ref.shape[0]
    width, planes, _ = a_ref.shape
    seg, seq = grids(shape)
    gates = Gather(seg, gate_src.at[:, 1], gate_two, sems[:6])
    weights = Gather(seg, weight_ref, weights_ref, sems[6:12])
    cots = Gather(seq, cot_ref, cots_ref, sems[12:])
    step = pl.program_id(0)
    keeps = [
        pltpu.make_async_copy(weight_ref, weights_ref.at[seg.here], local_s.at[0]),
        pltpu.make_async_copy(cot_ref, cots_ref.at[seq.here], local_s.at[1]),
        pltpu.make_async_copy(gate_src.at[:, 1], gate_two.at[seg.here], local_s.at[2]),
    ]
    load_one = pltpu.make_async_copy(gate_one, w_one, local_s.at[3])

    @pl.when(step == 0)
    def _():
        meet((seg, seq))
        gates.begin()
        weights.begin()
        cots.begin()
        for keep in keeps:
            keep.start()
        load_one.start()
        state[...] = init_ref[...]

    pre = dot_tn(low_ref[...], wdt_ref[...]) + bias_ref[...]
    pre_ref[...] = pre
    rate = softplus(pre)
    act = act_ref[...].astype(F32)
    to_planes(rate_pl, rate)
    to_planes(drive_pl, rate * act)
    groups = count // UNROLL

    def group(k, carry):
        at = k * UNROLL
        rates = [rate_pl[pl.ds(at + i, planes, stride=count), :] for i in range(UNROLL)]
        drives = [drive_pl[pl.ds(at + i, planes, stride=count), :] for i in range(UNROLL)]
        sums = [None] * UNROLL
        for n in range(width):
            a = a_ref[n]
            h = state[n]
            check_ref[k, n] = h
            for i in range(UNROLL):
                h = jnp.exp2(rates[i] * a) * h + bc_ref[at + i, n] * drives[i]
                term = bc_ref[at + i, width + n] * h
                sums[i] = term if n == 0 else sums[i] + term
            state[n] = h
        for i in range(UNROLL):
            y_pl[pl.ds(at + i, planes, stride=count), :] = sums[i]
        return carry

    ticks = 2 * steps
    plan = [[] for _ in range(ticks)]
    late = []
    for k in range(1, seg.lines):
        for gather, share in ((gates, 4 * k), (weights, 9 * k)):
            tick = ticks * share // 16
            (plan[tick - 1] if tick < ticks else late).append(functools.partial(gather.step, k))
        if k < seq.lines:
            plan[ticks - 1].append(functools.partial(cots.step, k))

    def part_of_step(h, carry):
        lax.fori_loop(h * (groups // 2), (h + 1) * (groups // 2), group, 0)
        for tick in range(ticks):
            if plan[tick]:

                @pl.when(step * 2 + h == tick)
                def _():
                    for event in plan[tick]:
                        event()

        return carry

    lax.fori_loop(0, 2, part_of_step, 0)
    y_ref[pl.ds(pl.multiple_of(step * count, count), count), :] = (
        from_planes(y_pl, count, planes) + skip_ref[...] * act_ref[...].astype(F32)
    )

    @pl.when(step == steps - 1)
    def _():
        final_ref[...] = state[...]
        for event in late[:-1]:
            event()
        gates.finish()
        keeps[2].wait()
        load_one.wait()
        load_two = pltpu.make_async_copy(gate_two, w_two, local_s.at[3])
        load_two.start()
        load_two.wait()
        model = tok_ref.shape[1]
        half = w_one.shape[3]
        block = 256

        def gating(i, carry):
            rows = pl.ds(pl.multiple_of(i * block, block), block)
            lines = tok_ref[rows, :].astype(F32)
            rstd = lax.rsqrt(jnp.mean(lines * lines, axis=1, keepdims=True) + EPSILON)
            for j, w in enumerate((w_one, w_two)):
                cols = pl.ds(j * half, half)
                gate = rstd * dot_nn(tok_ref[rows, :], w[...].reshape(model, half))
                gate_ref[rows, cols] = gate
                gated_ref[rows, cols] = (y_ref[rows, cols] * gate * sigmoid(gate)).astype(BF16)
            return carry

        blocks = y_ref.shape[0] // block
        lax.fori_loop(0, blocks // 2, gating, 0)
        late[-1]()
        lax.fori_loop(blocks // 2, blocks, gating, 0)
        weights.finish()
        cots.finish()
        for keep in keeps[:2]:
            keep.wait()


def backward_kernel(
    shape, steps,
    pre_ref, act_ref, gy_ref, bc_ref, a_ref, skip_ref, check_ref, wdt_ref, low_ref, base_ref,
    first_src, second_src, third_src,
    gact_ref, agrad_ref, start_ref, dtb_ref, sgrad_ref, dtp_ref, mix_ref,
    first_out, second_out, third_out,
    carry_s, rate_pl, drive_pl, gy_pl, grate_pl, thr_pl, prod, part, mix_s, *scratch,
):
    count = pre_ref.shape[0]
    width, planes, _ = a_ref.shape
    low_rank = wdt_ref.shape[0]
    seg, seq = grids(shape)
    first, second, third = (
        Scatter(grid, src, scratch[10 * i : 10 * i + 10])
        for i, (grid, src) in enumerate(((seg, first_src), (seg, second_src), (seq, third_src)))
    )
    step = pl.program_id(0)

    @pl.when(step == 0)
    def _():
        meet((seg, seq))
        first.begin()
        third.begin()
        second.begin()
        carry_s[...] = jnp.zeros_like(carry_s)
        agrad_ref[...] = jnp.zeros_like(agrad_ref)
        dtb_ref[...] = jnp.zeros_like(dtb_ref)
        sgrad_ref[...] = jnp.zeros_like(sgrad_ref)
        dtp_ref[...] = jnp.zeros_like(dtp_ref)

    pre = pre_ref[...]
    rate = softplus(pre)
    act = act_ref[...].astype(F32)
    to_planes(rate_pl, rate)
    to_planes(drive_pl, rate * act)
    to_planes(gy_pl, gy_ref[...])
    groups = count // UNROLL

    def group(j, carry):
        k = groups - 1 - j
        at = k * UNROLL
        rates = [rate_pl[pl.ds(at + i, planes, stride=count), :] for i in range(UNROLL)]
        drives = [drive_pl[pl.ds(at + i, planes, stride=count), :] for i in range(UNROLL)]
        gys = [gy_pl[pl.ds(at + i, planes, stride=count), :] for i in range(UNROLL)]
        g_rate = [None] * UNROLL
        through = [None] * UNROLL
        for n in range(width):
            a = a_ref[n]
            states = [check_ref[k, n]]
            decays = []
            for i in range(UNROLL):
                decays.append(jnp.exp2(rates[i] * a))
                states.append(decays[i] * states[i] + bc_ref[at + i, n] * drives[i])
            lam = carry_s[n]
            acc = agrad_ref[n]
            for i in reversed(range(UNROLL)):
                lam = lam + bc_ref[at + i, width + n] * gys[i]
                b_term = bc_ref[at + i, n] * lam
                prod[pl.ds((i * 2 * width + n) * planes, planes), :] = lam * drives[i]
                prod[pl.ds((i * 2 * width + width + n) * planes, planes), :] = (
                    states[i + 1] * gys[i]
                )
                lam = decays[i] * lam
                weighted = lam * states[i]
                acc = acc + weighted * rates[i]
                a_term = weighted * a
                g_rate[i] = a_term if n == 0 else g_rate[i] + a_term
                through[i] = b_term if n == 0 else through[i] + b_term
            carry_s[n] = lam
            agrad_ref[n] = acc
        for i in range(UNROLL):
            grate_pl[pl.ds(at + i, planes, stride=count), :] = g_rate[i]
            thr_pl[pl.ds(at + i, planes, stride=count), :] = through[i]
            for q in range(2 * width // 8):
                base = (i * 2 * width + q * 8) * planes
                total = prod[pl.ds(base, 8, stride=planes), :]
                for s in range(1, planes):
                    total = total + prod[pl.ds(base + s, 8, stride=planes), :]
                row = pl.multiple_of((at + i) * 2 * width + q * 8, 8)
                part[pl.ds(row, 8), :] = total
        return carry

    events = [functools.partial(s.middle, k) for s in (first, second) for k in s.order()]
    ticks = 2 * steps
    plan = [[] for _ in range(ticks)]
    for j, event in enumerate(events):
        plan[min(ticks - 1, ticks * (j + 1) // len(events))].append(event)
    for k in third.order():
        plan[min(ticks - 1, 2)].append(functools.partial(third.middle, k))

    def add_base(at, total):
        third_out[at, :] = (total + base_ref[at, :].astype(F32)).astype(BF16)

    plan[min(ticks - 1, 9)].append(functools.partial(third.finish, add_base))

    def part_of_step(h, carry):
        lax.fori_loop(h * (groups // 2), (h + 1) * (groups // 2), group, 0)
        for tick in range(ticks - 1):
            if plan[tick]:

                @pl.when(step * 2 + h == tick)
                def _():
                    for event in plan[tick]:
                        event()

        return carry

    lax.fori_loop(0, 2, part_of_step, 0)
    g_rate = from_planes(grate_pl, count, planes) * (1.0 / LOG2E)
    through = from_planes(thr_pl, count, planes)
    pre = pre_ref[...]
    rate = softplus(pre)
    act = act_ref[...].astype(F32)
    gy = gy_ref[...]
    g_dtpre = ((g_rate + act * through) * sigmoid(pre)).astype(BF16)
    gact_ref[...] = gy * skip_ref[...] + rate * through
    dtb_ref[...] += jnp.sum(g_dtpre.astype(F32), axis=0, keepdims=True)
    sgrad_ref[...] += jnp.sum(gy * act, axis=0, keepdims=True)
    dtp_ref[...] += dot_nn(low_ref[...], g_dtpre)
    rows = 2 * width
    ones = jnp.ones((LANES, LANES), F32)
    sums = jnp.dot(part[...], ones, preferred_element_type=F32)
    sums = sums.reshape(count, rows, LANES)
    pick = lax.broadcasted_iota(jnp.int32, (1, rows, LANES), 1) == lax.broadcasted_iota(
        jnp.int32, (1, rows, LANES), 2
    )
    g_bc = jnp.sum(jnp.where(pick, sums, 0.0), axis=1)
    tokens_at = pl.ds(pl.multiple_of((steps - 1 - step) * count, count), count)
    mix_s[pl.ds(0, low_rank), tokens_at] = dot_nt(wdt_ref[...], g_dtpre)
    mix_s[pl.ds(low_rank, rows), tokens_at] = g_bc.T[:rows]

    @pl.when(step == steps - 1)
    def _():
        start_ref[...] = carry_s[...]
        sum_over_seq(seq, mix_s, mix_ref, *scratch[30:])
        for event in plan[ticks - 1]:
            event()
        first.finish(into(first_out))
        second.finish(into(second_out))
        for scatter in (first, second, third):
            scatter.drain()


def forward_scan(
    shape, low, w_dt, bias, act, bc, a2, skip, init, weight, cot, tok, gate_one, gate_part, block
):
    lines, fast, seq_lines = shape
    length, features = act.shape
    width, planes, _ = a2.shape
    low_rank = w_dt.shape[0]
    steps = length // block
    rows = pl.BlockSpec((block, features), lambda i: (i, 0))
    one = pl.Buffered(1)

    def whole(*dims):
        return pl.BlockSpec(dims, lambda i: (0,) * len(dims), pipeline_mode=one)

    plane = pltpu.VMEM((planes * block, LANES), F32)
    return pl.pallas_call(
        functools.partial(forward_kernel, shape, steps),
        grid=(steps,),
        in_specs=[
            pl.BlockSpec((low_rank, block), lambda i: (0, i)),
            whole(low_rank, features), whole(1, features), rows,
            pl.BlockSpec((block, 2 * width), lambda i: (i, 0), memory_space=pltpu.SMEM),
            whole(width, planes, LANES), whole(1, features), whole(width, planes, LANES),
            whole(*weight.shape), whole(*cot.shape), whole(*tok.shape), ANY, ANY,
        ],
        out_specs=[
            whole(length, features), rows,
            pl.BlockSpec((block // UNROLL, width, planes, LANES), lambda i: (i, 0, 0, 0)),
            whole(width, planes, LANES), whole(length, features), whole(length, features),
            ANY, ANY, ANY,
        ],
        out_shape=[
            jax.ShapeDtypeStruct((length, features), F32),
            jax.ShapeDtypeStruct((length, features), F32),
            jax.ShapeDtypeStruct((length // UNROLL, width, planes, LANES), F32),
            jax.ShapeDtypeStruct((width, planes, LANES), F32),
            jax.ShapeDtypeStruct((length, features), F32),
            jax.ShapeDtypeStruct((length, features), BF16),
            jax.ShapeDtypeStruct((lines * fast,) + weight.shape, BF16),
            jax.ShapeDtypeStruct((seq_lines * 2,) + cot.shape, BF16),
            jax.ShapeDtypeStruct(gate_one.shape, BF16),
        ],
        scratch_shapes=[
            pltpu.VMEM((width, planes, LANES), F32), plane, plane, plane,
            pltpu.VMEM(gate_one.shape, BF16), pltpu.VMEM(gate_one.shape, BF16),
            pltpu.SemaphoreType.DMA((4,)),
            *Gather.semaphores(lines, fast), *Gather.semaphores(lines, fast),
            *Gather.semaphores(seq_lines, 2),
        ],
        compiler_params=comm_params(5),
        cost_estimate=pl.CostEstimate(
            flops=8 * length * features * width,
            bytes_accessed=24 * length * features,
            transcendentals=length * features * width,
        ),
        name="scan_forward",
    )(low, w_dt, bias, act, bc, a2, skip, init, weight, cot, tok, gate_one, gate_part)


def backward_scan(
    shape, pre, act, gy, bc, a2, skip, checks, w_dt, dt_low, base, first, second, third, block
):
    lines, fast, seq_lines = shape
    length, features = pre.shape
    width, planes, _ = a2.shape
    low_rank = w_dt.shape[0]
    steps = length // block
    rows = pl.BlockSpec((block, features), lambda i: (steps - 1 - i, 0))
    whole = pl.BlockSpec((width, planes, LANES), lambda i: (0, 0, 0))

    def all_of(rows, columns):
        return pl.BlockSpec((rows, columns), lambda i: (0, 0))

    line = all_of(1, features)
    plane = pltpu.VMEM((planes * block, LANES), F32)
    mixed = (low_rank + 2 * width, length)
    return pl.pallas_call(
        functools.partial(backward_kernel, shape, steps),
        grid=(steps,),
        in_specs=[
            rows, rows, rows,
            pl.BlockSpec(
                (block, 2 * width), lambda i: (steps - 1 - i, 0), memory_space=pltpu.SMEM
            ),
            whole, line,
            pl.BlockSpec(
                (block // UNROLL, width, planes, LANES), lambda i: (steps - 1 - i, 0, 0, 0)
            ),
            all_of(low_rank, features),
            pl.BlockSpec((low_rank, block), lambda i: (0, steps - 1 - i)),
            all_of(*base.shape),
            ANY, ANY, ANY,
        ],
        out_specs=[
            rows, whole, whole, line, line, all_of(low_rank, features), all_of(*mixed),
            all_of(*first.shape[1:]), all_of(*second.shape[1:]), all_of(*base.shape),
        ],
        out_shape=[
            jax.ShapeDtypeStruct((length, features), F32),
            jax.ShapeDtypeStruct((width, planes, LANES), F32),
            jax.ShapeDtypeStruct((width, planes, LANES), F32),
            jax.ShapeDtypeStruct((1, features), F32),
            jax.ShapeDtypeStruct((1, features), F32),
            jax.ShapeDtypeStruct((low_rank, features), F32),
            jax.ShapeDtypeStruct(mixed, BF16),
            jax.ShapeDtypeStruct(first.shape[1:], BF16),
            jax.ShapeDtypeStruct(second.shape[1:], F32),
            jax.ShapeDtypeStruct(base.shape, BF16),
        ],
        scratch_shapes=[pltpu.VMEM((width, planes, LANES), F32)]
        + [plane] * 5
        + [
            pltpu.VMEM((UNROLL * 2 * width * planes, LANES), F32),
            pltpu.VMEM((block * 2 * width, LANES), F32),
            pltpu.VMEM(mixed, F32),
            *Scatter.scratch(lines, fast, first.shape[1:]),
            *Scatter.scratch(lines, fast, second.shape[1:]),
            *Scatter.scratch(seq_lines, 2, third.shape[1:]),
            *sum_scratch(seq_lines, *mixed),
        ],
        compiler_params=comm_params(6),
        cost_estimate=pl.CostEstimate(
            flops=20 * length * features * width,
            bytes_accessed=28 * length * features,
            transcendentals=length * features * width,
        ),
        name="scan_backward",
    )(pre, act, gy, bc, a2, skip, checks, w_dt, dt_low, base, first, second, third)


def finish_kernel(shape, taps, history, refs, scratch):
    (
        gact, x_in, act, tok, w_x, w_g, w_h, gs_gate,
        mix, w_xt, head, kern, b_conv, dtp, a_grad, dtb, sgrad, g_half, own_tok, own_cot,
        final, start,
        small_out, halves_out, input_out, ends_out,
    ) = refs
    (
        gc, xb, actb, tokb, wxb, wgb, gsg, gs_x, xg, q_src, pack, small_src, ends_src, x_half,
        in_s, own_s,
    ) = scratch[:16]
    seg, seq = grids(shape)
    length, feats = act.shape
    at = 16
    sets = []
    for inside, size in ((True, 8), (True, 8), (True, 8)):
        sets.append(scratch[at : at + size])
        at += size
    swaps_s = [scratch[at + 2 * i : at + 2 * i + 2] for i in range(3)]
    small = Scatter(seg, small_src, sets[0], inside=True)
    x_sum = Scatter(seg, xg, sets[1], inside=True)
    q_sum = Scatter(seq, q_src, sets[2], inside=True)
    loads = [
        pltpu.make_async_copy(gact, gc.at[pl.ds(0, length)], in_s.at[0]),
        pltpu.make_async_copy(x_in, xb.at[pl.ds(8, length)], in_s.at[1]),
        pltpu.make_async_copy(tok, tokb, in_s.at[2]),
        pltpu.make_async_copy(act, actb, in_s.at[3]),
        pltpu.make_async_copy(gs_gate, gsg, in_s.at[4]),
        pltpu.make_async_copy(w_g, wgb.at[0], in_s.at[5]),
        pltpu.make_async_copy(w_h, wgb.at[1], in_s.at[6]),
        pltpu.make_async_copy(w_x, wxb, in_s.at[7]),
    ]
    for load in loads:
        load.start()
    meet((seg, seq))
    own_rows = g_half.shape[0] // (seq.lines * seq.fast)

    def swap(half, src, sems):
        return Exchange(
            seq,
            lambda p: src.at[pl.ds(pl.multiple_of(p * own_rows, own_rows), own_rows)],
            lambda m: halves_out.at[half, m],
            sems,
        )

    swap_g = swap(1, g_half, swaps_s[1])
    swap_g.begin()
    xb[pl.ds(0, 8), :] = head[...]
    gc[pl.ds(length, 8), :] = jnp.zeros((8, feats), F32)
    loads[0].wait()
    big = LANES

    def add_mixed(i, carry):
        rows = pl.ds(pl.multiple_of(i * big, big), big)
        gc[rows, :] += dot_tn(mix[:, rows], w_xt[...])
        return carry

    lax.fori_loop(0, length // big, add_mixed, 0)
    loads[1].wait()
    tall = 32
    chunk = min(512, feats)
    sums_at = 8 * (taps + 1)
    pack[...] = jnp.zeros_like(pack)

    def through_conv(i, carry):
        t0 = pl.multiple_of(i * tall, tall)
        for c in range(0, feats, chunk):
            cols = pl.ds(c, chunk)
            wide = xb[pl.ds(t0, tall + 8), cols]
            rows = [wide[8 - history + k : 8 - history + k + tall] for k in range(taps)]
            conv = b_conv[:, cols]
            for k in range(taps):
                conv = conv + kern[pl.ds(k, 1), cols] * rows[k]
            sig = sigmoid(conv)
            g_conv = gc[pl.ds(t0, tall), cols] * sig * (1.0 + conv * (1.0 - sig))
            gc[pl.ds(t0, tall), cols] = g_conv
            for k in range(taps):
                term = g_conv * rows[k]
                pack[pl.ds(8 * k, 8), cols] += sum(
                    term[8 * j : 8 * j + 8] for j in range(tall // 8)
                )
            pack[pl.ds(8 * taps, 8), cols] += sum(
                g_conv[8 * j : 8 * j + 8] for j in range(tall // 8)
            )
        return carry

    lax.fori_loop(0, length // tall, through_conv, 0)
    loads[2].wait()

    def to_input(i, carry):
        t0 = pl.multiple_of(i * tall, tall)
        lines = tokb[pl.ds(t0, tall), :].astype(F32)
        rstd = lax.rsqrt(jnp.mean(lines * lines, axis=1, keepdims=True) + EPSILON)
        for c in range(0, feats, chunk):
            cols = pl.ds(c, chunk)
            wide = gc[pl.ds(t0, tall + 8), cols]
            g_x = kern[pl.ds(0, 1), cols] * wide[history : history + tall]
            for k in range(1, taps):
                g_x = g_x + kern[pl.ds(k, 1), cols] * wide[history - k : history - k + tall]
            gs_x[pl.ds(t0, tall), cols] = (rstd * g_x).astype(BF16)
        return carry

    lax.fori_loop(0, length // tall, to_input, 0)
    loads[3].wait()
    low_rank = dtp.shape[0]
    mixes = mix.shape[0]
    width = a_grad.shape[0]
    part = small_src.shape[2]
    xp = dot_nn(mix[...], actb[...])
    for g in range(small_src.shape[0]):
        cols = slice(g * part, (g + 1) * part)
        small_src[g, pl.ds(0, low_rank), :] = dtp[:, cols].astype(BF16)
        small_src[g, pl.ds(low_rank, mixes), :] = xp[:, cols].astype(BF16)
        base = low_rank + mixes
        small_src[g, pl.ds(base, width), :] = a_grad[:, cols].astype(BF16)
        lines = [
            jnp.sum(pack[pl.ds(8 * k, 8), cols], axis=0, keepdims=True) for k in range(taps + 1)
        ]
        lines += [dtb[:, cols], sgrad[:, cols]]
        lines.append(jnp.zeros((16 - len(lines), part), F32))
        small_src[g, pl.ds(base + width, 16), :] = jnp.concatenate(lines, axis=0).astype(BF16)
    small.begin()

    block_rows = xg.shape[1]

    def partial(index):
        cols = pl.ds(pl.multiple_of(index * block_rows, block_rows), block_rows)
        xg[index] = dot_tn(tokb[:, cols], gs_x[...]).astype(BF16)

    by_block = block_rows % LANES == 0
    if not by_block:
        for index in range(xg.shape[0]):
            cols = slice(index * block_rows, (index + 1) * block_rows)
            xg[index] = dot_tn(tokb[:, cols], gs_x[...]).astype(BF16)

    def leave(j, carry):
        k = seg.lines - 1 - j
        for e in range(1, seg.fast):
            if by_block:
                partial(x_sum.index(k, e))
            x_sum.across(k, e).start()
        return carry

    lax.fori_loop(0, seg.lines, leave, 0)
    def stay(j, carry):
        if by_block:
            partial(x_sum.index(seg.lines - 1 - j, 0))
        return carry

    lax.fori_loop(0, seg.lines, stay, 0)
    ends_in = jnp.concatenate(
        [
            final[...],
            xb[pl.ds(length, 8), :][8 - history :],
            start[...],
            sum_head(gc, kern, history, taps),
            jnp.zeros((ends_src.shape[1] - 2 * (width + history), feats), F32),
        ],
        axis=0,
    )
    piece = ends_src.shape[2]
    for p in range(ends_src.shape[0]):
        ends_src[p] = ends_in[:, p * piece : (p + 1) * piece]
    end_swap = Exchange(seq, lambda p: ends_src.at[p], lambda m: ends_out.at[m], swaps_s[2])
    end_swap.begin()
    loads[4].wait()
    loads[5].wait()
    loads[6].wait()
    loads[7].wait()
    own_len = own_tok.shape[0]
    model = own_tok.shape[1]
    wide = 512
    half = feats // 2

    def normed(index):
        rows = pl.ds(pl.multiple_of(index * own_len, own_len), own_len)

        def column(c, carry):
            cols = pl.ds(pl.multiple_of(c * wide, wide), wide)
            q_src[index, :, cols] = (
                dot_nt(gsg[rows, pl.ds(0, half)], wgb[0, cols, :])
                + dot_nt(gsg[rows, pl.ds(half, half)], wgb[1, cols, :])
                + dot_nt(gs_x[rows, :], wxb[cols, :])
            ).astype(BF16)
            return carry

        lax.fori_loop(0, model // wide, column, 0)

    def leave_q(j, carry):
        k = seq.lines - 1 - j
        normed(q_sum.index(k, 1))
        q_sum.across(k, 1).start()
        return carry

    def stay_q(j, carry):
        normed(q_sum.index(seq.lines - 1 - j, 0))
        return carry

    lax.fori_loop(0, seq.lines, leave_q, 0)
    lax.fori_loop(0, seq.lines, stay_q, 0)
    for k in small.order():
        small.middle(k)
    for j, k in enumerate(x_sum.order()):
        x_sum.middle(k)
        if j == seg.lines - 2:
            for m in q_sum.order():
                q_sum.middle(m)

    def input_grad(at, total):
        own = own_tok[at, :].astype(F32)
        square = 1.0 / (jnp.mean(own * own, axis=1, keepdims=True) + EPSILON)
        input_out[at, :] = (
            own_cot[at, :].astype(F32)
            + total
            - own * (square * jnp.mean(total * own, axis=1, keepdims=True))
        ).astype(BF16)

    q_sum.finish(input_grad)
    small.finish(into(small_out))
    x_sum.finish(into(x_half))
    swap_x = swap(0, x_half, swaps_s[0])
    swap_x.begin()
    own = pl.ds(pl.multiple_of(seq.here * own_rows, own_rows), own_rows)
    keeps = [
        pltpu.make_async_copy(x_half.at[own], halves_out.at[0, seq.here], own_s.at[0]),
        pltpu.make_async_copy(g_half.at[own], halves_out.at[1, seq.here], own_s.at[1]),
        pltpu.make_async_copy(ends_src.at[seq.here], ends_out.at[seq.here], own_s.at[2]),
    ]
    for keep in keeps:
        keep.start()
    for scatter in (small, x_sum, q_sum):
        scatter.drain()
    for exchange in (swap_g, end_swap, swap_x):
        exchange.arrived()
        exchange.drain()
    for keep in keeps:
        keep.wait()


def sum_head(gc, kern, history, taps):
    top = gc[pl.ds(0, 8), :]
    rows = []
    for j in range(history):
        rows.append(
            sum(kern[pl.ds(k, 1), :] * top[j - k : j - k + 1] for k in range(min(j + 1, taps)))
        )
    return jnp.concatenate(rows, axis=0)


def finish_all(shape, taps, history, big, small):
    lines, fast, seq_lines = shape
    segs, seqs = lines * fast, seq_lines * 2
    gact, x_in, act, tok, w_x, w_g, w_h, gs_gate = big
    mix, w_xt, head, kern, b_conv, dtp, a_grad, dtb, sgrad, g_half, own_tok, own_cot = small[:12]
    length, feats = act.shape
    own_len, model = own_tok.shape
    width = a_grad.shape[0]
    rows = dtp.shape[0] + mix.shape[0] + width + 16
    block_rows = model // segs
    own_rows = g_half.shape[0] // seqs
    ends = (seqs, 2 * (width + history) + (-2 * (width + history)) % 8, feats // seqs)
    dma = pltpu.SemaphoreType.DMA
    scratch = [
        pltpu.VMEM((length + 8, feats), F32),
        pltpu.VMEM((length + 8, feats), F32),
        pltpu.VMEM((length, feats), BF16),
        pltpu.VMEM((length, model), BF16),
        pltpu.VMEM((model, feats), BF16),
        pltpu.VMEM((2, model, feats // 2), BF16),
        pltpu.VMEM((length, feats), BF16),
        pltpu.VMEM((length, feats), BF16),
        pltpu.VMEM((segs, block_rows, feats), BF16),
        pltpu.VMEM((seqs, own_len, model), BF16),
        pltpu.VMEM((8 * (taps + 1), feats), F32),
        pltpu.VMEM((segs, rows, feats // segs), BF16),
        pltpu.VMEM(ends, F32),
        pltpu.VMEM((block_rows, feats), BF16),
        dma((8,)), dma((3,)),
        *Scatter.scratch(lines, fast, (rows, feats // segs), inside=True),
        *Scatter.scratch(lines, fast, (block_rows, feats), inside=True),
        *Scatter.scratch(seq_lines, 2, (own_len, model), inside=True),
        *Exchange.semaphores(seqs), *Exchange.semaphores(seqs), *Exchange.semaphores(seqs),
    ]

    def kernel(*refs):
        finish_kernel(shape, taps, history, refs[:26], refs[26:])

    return pl.pallas_call(
        kernel,
        in_specs=[ANY] * 8 + [INSIDE] * 14,
        out_specs=[INSIDE] * 4,
        out_shape=[
            jax.ShapeDtypeStruct((rows, feats // segs), F32),
            jax.ShapeDtypeStruct((2, seqs, own_rows, feats), BF16),
            jax.ShapeDtypeStruct((own_len, model), BF16),
            jax.ShapeDtypeStruct(ends, F32),
        ],
        scratch_shapes=scratch,
        compiler_params=comm_params(4),
        name="finish",
    )(*big, *small)


def gather_kernel(
    shape, scaled_x, scaled_g, small, tokens, w_x, small_all, tok, g_part, x_part, tok_in, g_own,
    local_s, small_sems, tok_sems, swap_x, swap_g, x_sems,
):
    seg, seq = grids(shape)
    size = seq.lines * seq.fast
    load_tok = pltpu.make_async_copy(tokens, tok_in, local_s.at[0])
    load_own = pltpu.make_async_copy(scaled_x.at[seq.here], x_part.at[seq.here], local_s.at[1])
    load_gate = pltpu.make_async_copy(scaled_g.at[seq.here], g_own, local_s.at[3])
    load_tok.start()
    load_own.start()
    load_gate.start()
    meet((seg, seq))
    swap_x = Exchange(seq, lambda p: scaled_x.at[p], lambda m: x_part.at[m], swap_x)
    swap_g = Exchange(seq, lambda p: scaled_g.at[p], lambda m: g_part.at[m], swap_g)
    swap_x.begin()
    pieces = []
    for k in range(size):
        place = lax.rem(seq.here - k + size, size)
        pieces.append(Gather(seg, x_part.at[place], w_x, x_sems[6 * k : 6 * k + 6], place))
    smalls = Gather(seg, small, small_all, small_sems)
    load_own.wait()
    pieces[0].begin()
    smalls.begin()
    load_tok.wait()
    toks = Gather(seq, tok_in, tok, tok_sems)
    for k in range(1, size):
        swap_x.one(k).wait_recv()
        pieces[k].begin()
    toks.begin()
    swap_g.begin()
    load_gate.wait()
    keeps = [
        pltpu.make_async_copy(tok_in, tok.at[seq.here], local_s.at[0]),
        pltpu.make_async_copy(x_part, w_x.at[seg.here], local_s.at[1]),
        pltpu.make_async_copy(small, small_all.at[seg.here], local_s.at[2]),
        pltpu.make_async_copy(g_own, g_part.at[seq.here], local_s.at[3]),
    ]
    for keep in keeps:
        keep.start()
    for k in range(1, max(seg.lines, seq.lines)):
        if k < seg.lines:
            pieces[0].step(k)
            smalls.step(k)
            for piece in pieces[1:]:
                piece.step(k)
        if k < seq.lines:
            toks.step(k)
    toks.finish()
    smalls.finish()
    for piece in pieces:
        piece.finish()
    swap_g.arrived()
    swap_x.drain()
    swap_g.drain()
    for keep in keeps:
        keep.wait()


def gather_start(shape, scaled_x, scaled_g, small, tokens):
    lines, fast, seq_lines = shape
    segs, seqs = lines * fast, seq_lines * 2
    rows, feats = scaled_x.shape[1:]
    sems = Gather.semaphores

    def kernel(*refs):
        ins, rest = refs[:11], refs[11:]
        gather_kernel(
            shape, *ins, rest[0], rest[1:7], rest[7:13], rest[13:15], rest[15:17], rest[17:]
        )

    w_x, small_all, tok, g_part = pl.pallas_call(
        kernel,
        in_specs=[ANY, ANY, INSIDE, ANY],
        out_specs=[ANY] * 4,
        out_shape=[
            jax.ShapeDtypeStruct((segs, seqs, rows, feats), BF16),
            jax.ShapeDtypeStruct((segs,) + small.shape, BF16),
            jax.ShapeDtypeStruct((seqs,) + tokens.shape, BF16),
            jax.ShapeDtypeStruct((seqs,) + scaled_g.shape[1:], BF16),
        ],
        scratch_shapes=[
            pltpu.VMEM((seqs, rows, feats), BF16),
            pltpu.VMEM(tokens.shape, BF16),
            pltpu.VMEM(scaled_g.shape[1:], BF16),
            pltpu.SemaphoreType.DMA((4,)),
            *sems(lines, fast), *sems(seq_lines, 2),
            *Exchange.semaphores(seqs), *Exchange.semaphores(seqs),
            *(sems(lines, fast) * seqs),
        ],
        compiler_params=comm_params(1),
        name="gather_start",
    )(scaled_x, scaled_g, small, tokens)
    return w_x.reshape(-1, feats), small_all, tok.reshape(-1, tokens.shape[1]), g_part


def front_kernel(
    shape, steps, taps, history, width,
    tok_ref, wx_ref, small_ref, head_ref, gate_src,
    x_ref, act_ref, rstd_ref, wdt_ref, wxt_ref, par_ref, a2_ref, low_ref, bc_ref, gate_out,
    xb, mix_s, mix, local_s, *scratch,
):
    seg, seq = grids(shape)
    step = pl.program_id(0)
    gates = Gather(seg, gate_src.at[:, 0], gate_out, scratch[:6])
    count = tok_ref.shape[0]
    low_rank = wdt_ref.shape[0]
    mixes = wxt_ref.shape[0]
    feats = wx_ref.shape[1]
    part = small_ref.shape[2]

    @pl.when(step == 0)
    def _():
        meet((seg, seq))
        gates.begin()
        xb[pl.ds(0, 8), :] = head_ref[...]
        for g in range(small_ref.shape[0]):
            cols = slice(g * part, (g + 1) * part)
            wdt_ref[:, cols] = small_ref[g, pl.ds(0, low_rank), :]
            wxt_ref[:, cols] = small_ref[g, pl.ds(low_rank, mixes), :]
            rest = small_ref[g, pl.ds(low_rank + mixes, width + 16), :].astype(F32)
            par_ref[:, cols] = rest
        a_mat = -jnp.exp(par_ref[pl.ds(0, width), :])
        par_ref[pl.ds(0, width), :] = a_mat
        for s in range(feats // LANES):
            a2_ref[:, s, :] = a_mat[:, s * LANES : (s + 1) * LANES] * LOG2E

    kern = par_ref[pl.ds(width, 8), :]
    rows = tok_ref[...].astype(F32)
    rstd = lax.rsqrt(jnp.mean(rows * rows, axis=1, keepdims=True) + EPSILON)
    rstd_ref[...] = jnp.broadcast_to(rstd, rstd_ref.shape)
    x_in = rstd * dot_nn(tok_ref[...], wx_ref[...])
    x_ref[...] = x_in
    xb[pl.ds(8, count), :] = x_in
    tall = 32
    chunk = min(512, feats)

    def through_conv(i, carry):
        t0 = pl.multiple_of(i * tall, tall)
        for c in range(0, feats, chunk):
            cols = slice(c, c + chunk)
            wide = xb[pl.ds(t0, tall + 8), pl.ds(c, chunk)]
            conv = kern[taps : taps + 1, cols]
            for k in range(taps):
                conv = conv + kern[k : k + 1, cols] * wide[8 - history + k : 8 - history + k + tall]
            act_ref[pl.ds(t0, tall), pl.ds(c, chunk)] = (conv * sigmoid(conv)).astype(BF16)
        return carry

    lax.fori_loop(0, count // tall, through_conv, 0)
    xb[pl.ds(0, 8), :] = xb[pl.ds(count, 8), :]
    mix_s[:, pl.ds(pl.multiple_of(step * count, count), count)] = dot_nt(wxt_ref[...], act_ref[...])
    for k in range(1, seg.lines - 1):

        @pl.when(step == min(steps - 1, 2 * k - 1))
        def _():
            gates.step(k)

    @pl.when(step == steps - 1)
    def _():
        sum_over_seq(seq, mix_s, mix, *scratch[6:])
        low_ref[...] = mix[pl.ds(0, low_rank), :]
        bc_ref[...] = mix[pl.ds(low_rank, 2 * width), :].astype(F32).T
        gates.step(seg.lines - 1)
        keep = pltpu.make_async_copy(gate_src.at[:, 0], gate_out.at[seg.here], local_s)
        keep.start()
        gates.finish()
        keep.wait()


def front(shape, taps, history, width, tok, w_x, small_all, head, gate_part, block):
    lines, fast, seq_lines = shape
    segs, seqs = lines * fast, seq_lines * 2
    length, model = tok.shape
    feats = w_x.shape[1]
    low_rank = LANES
    mixes = low_rank + 2 * width
    steps = length // block

    def whole(*dims):
        return pl.BlockSpec(dims, lambda i: (0,) * len(dims))

    def rows(columns):
        return pl.BlockSpec((block, columns), lambda i: (i, 0))

    one = pl.Buffered(1)
    return pl.pallas_call(
        functools.partial(front_kernel, shape, steps, taps, history, width),
        grid=(steps,),
        in_specs=[
            rows(model),
            pl.BlockSpec((model, feats), lambda i: (0, 0), pipeline_mode=one),
            whole(*small_all.shape), whole(*head.shape), ANY,
        ],
        out_specs=[
            rows(feats), rows(feats), rows(LANES), whole(low_rank, feats), whole(mixes, feats),
            whole(width + 16, feats), whole(width, feats // LANES, LANES),
            whole(low_rank, length), whole(length, 2 * width), ANY,
        ],
        out_shape=[
            jax.ShapeDtypeStruct((length, feats), F32),
            jax.ShapeDtypeStruct((length, feats), BF16),
            jax.ShapeDtypeStruct((length, LANES), F32),
            jax.ShapeDtypeStruct((low_rank, feats), BF16),
            jax.ShapeDtypeStruct((mixes, feats), BF16),
            jax.ShapeDtypeStruct((width + 16, feats), F32),
            jax.ShapeDtypeStruct((width, feats // LANES, LANES), F32),
            jax.ShapeDtypeStruct((low_rank, length), BF16),
            jax.ShapeDtypeStruct((length, 2 * width), F32),
            jax.ShapeDtypeStruct((segs, seqs) + gate_part.shape[2:], BF16),
        ],
        scratch_shapes=[
            pltpu.VMEM((block + 8, feats), F32),
            pltpu.VMEM((mixes, length), F32),
            pltpu.VMEM((mixes, length), BF16),
            pltpu.SemaphoreType.DMA,
            *Gather.semaphores(lines, fast),
            *sum_scratch(seq_lines, mixes, length),
        ],
        compiler_params=comm_params(2),
        name="front",
    )(tok, w_x, small_all, head, gate_part)


def sum_scratch(seq_lines, rows, width):
    part = pltpu.VMEM((rows, width // 2), BF16)
    dma = pltpu.SemaphoreType.DMA
    return [
        part, part, part,
        pltpu.VMEM((max(seq_lines - 1, 1), rows, width // 2), BF16),
        pltpu.VMEM((2, rows, width // 2), BF16),
        dma, dma, dma((seq_lines,)), dma((seq_lines,)), dma, dma,
    ]


def unpack_kernel(
    seqs, taps, history, low_rank, width,
    small, halves, ends, mixed, input_grad, out_grad, weight, gain,
    mixed_o, final_o, final_c, input_o, start_o, start_c, gain_o, in_o, cw_o, cb_o, xp_o, dtp_o,
    dtb_o, a_o, skip_o, out_o,
):
    mixed_o[0] = mixed[...]
    input_o[0] = input_grad[...]
    out_o[...] = out_grad[...]
    part = small.shape[1]
    columns = xp_o.shape[1]
    dtp_o[...] = small[pl.ds(0, low_rank), :]
    turned = small[pl.ds(low_rank, low_rank), :].T
    xp_o[:, pl.ds(0, low_rank)] = turned
    xp_o[:, pl.ds(low_rank, columns - low_rank)] = small[
        pl.ds(2 * low_rank, columns - low_rank), :
    ].T
    at = low_rank + columns
    a_o[...] = small[pl.ds(at, width), :]
    lines = small[pl.ds(at + width, 16), :]
    cw_o[...] = lines[:taps]
    cb_o[...] = lines[taps]
    dtb_o[...] = lines[taps + 1]
    skip_o[...] = lines[taps + 2]
    each = final_o.shape[2] // part // seqs
    for s in range(seqs):
        rows = ends[s]
        for g in range(each):
            got = rows[:, g * part : (g + 1) * part]
            cols = pl.ds((g * seqs + s) * part, part)
            final_o[0, :, cols] = got[:width]
            final_c[0, :, cols] = got[width : width + history]
            start_o[0, :, cols] = got[width + history : 2 * width + history]
            start_c[0, :, cols] = got[2 * width + history : 2 * (width + history)]
    scale = gain[...]
    total = jnp.zeros((in_o.shape[0], part), F32)
    groups = halves.shape[3] // part
    for half in range(2):
        for s in range(seqs):
            for g in range(groups):
                raw = halves[half, s, :, g * part : (g + 1) * part].astype(F32)
                cols = pl.ds(((half * groups + g) * seqs + s) * part, part)
                in_o[:, cols] = raw * scale
                total = total + raw * weight[:, cols].astype(F32)
    gain_o[...] = jnp.sum(total.T, axis=0)


def unpack(taps, history, low_rank, width, small, halves, ends, mixed, input_grad, out_grad,
           weight, gain):
    seqs, own_rows, feats = halves.shape[1:]
    part = small.shape[1]
    model = mixed.shape[1]
    kept = ends.shape[2] * seqs
    f32 = lambda *dims: jax.ShapeDtypeStruct(dims, F32)
    return pl.pallas_call(
        functools.partial(unpack_kernel, seqs, taps, history, low_rank, width),
        in_specs=[INSIDE] * 8,
        out_specs=[INSIDE] * 16,
        out_shape=[
            jax.ShapeDtypeStruct((1,) + mixed.shape, BF16),
            f32(1, width, kept), f32(1, history, kept),
            jax.ShapeDtypeStruct((1,) + input_grad.shape, BF16),
            f32(1, width, kept), f32(1, history, kept),
            f32(own_rows), f32(*weight.shape),
            f32(taps, part), f32(part), f32(part, low_rank + 2 * width), f32(low_rank, part),
            f32(part), f32(width, part), f32(part), f32(part, model),
        ],
        name="unpack",
    )(small, halves, ends, mixed, input_grad, out_grad, weight, gain)


def body(
    tokens, norm_gain, in_proj, conv_weight, conv_bias, x_proj, dt_proj, dt_bias,
    a_log, d_skip, out_proj, init_state, init_conv, cotangent,
):
    segs, seqs = lax.axis_size("seg"), lax.axis_size("seq")
    place = lax.axis_index("seq")
    own_rows, both = in_proj.shape
    part = conv_bias.shape[0]
    feats = segs * part
    taps = conv_weight.shape[0]
    width = a_log.shape[0]
    low_rank = dt_proj.shape[0]
    planes = feats // LANES
    own_len, model = tokens.shape[1:]
    length = own_len * seqs
    block = 64
    seq_lines = seqs // 2
    shape = (segs // seq_lines, seq_lines, seq_lines)

    def mine(rows):
        shaped = rows.reshape(rows.shape[0], segs, seqs, part)
        return lax.dynamic_index_in_dim(shaped, place, 2, keepdims=False).reshape(
            rows.shape[0], feats
        )

    gain_col = norm_gain.astype(F32)[:, None]
    own_weight = in_proj.astype(F32)
    scaled = (own_weight * gain_col).astype(BF16)
    scaled = scaled.reshape(own_rows, 2, segs, seqs, part)
    scaled_x = scaled[:, 0].transpose(2, 0, 1, 3).reshape(seqs, own_rows, feats)
    scaled_g = scaled[:, 1].reshape(own_rows, 2, segs // 2, seqs, part).transpose(3, 1, 0, 2, 4)
    scaled_g = scaled_g.reshape(seqs, 2, own_rows, feats // 2)
    small = jnp.concatenate(
        [
            dt_proj, x_proj.T, a_log, conv_weight, conv_bias[None], dt_bias[None], d_skip[None],
        ],
        axis=0,
    )
    small = jnp.pad(small, ((0, -small.shape[0] % 16), (0, 0)))
    w_x_half, small_all, tok, g_part = gather_start(shape, scaled_x, scaled_g, small, tokens[0])
    history = init_conv.shape[1]
    head = jnp.pad(mine(init_conv[0]), ((8 - history, 0), (0, 0)))
    x_in, act, rstd, w_dt, w_xt, params, a2, dt_low, bc, w_g_one = front(
        shape, taps, history, width, tok, w_x_half, small_all, head, g_part, 4 * block
    )
    rstd = rstd[:, :1]
    init = mine(init_state[0]).reshape(width, planes, LANES)
    a_mat = params[:width]
    kernel = params[width : width + 8]
    b_conv, b_dt, skip = (params[width + taps + i][None] for i in range(3))
    y_val, pre, checks, final, gate, gated, w_out, cot, w_g_two = forward_scan(
        shape, dt_low, w_dt, b_dt, act, bc, a2, skip, init, out_proj, cotangent[0], tok,
        w_g_one, g_part, 2 * block,
    )
    w_out = w_out.reshape(feats, model)
    cot = cot.reshape(length, model)
    w_g_one = w_g_one.reshape(model, feats // 2)
    w_g_two = w_g_two.reshape(model, feats // 2)
    out_part = dot_nn(gated, w_out).astype(BF16)

    g_gated = dot_nt(cot, w_out)
    sig_gate = jax.nn.sigmoid(gate)
    gy = g_gated * gate * sig_gate
    gs_gate = (
        rstd * g_gated * y_val * sig_gate * (1.0 + gate * (1.0 - sig_gate))
    ).astype(BF16)
    out_grad = dot_tn(gated, cot).astype(BF16)
    gate_grad = dot_tn(tok, gs_gate).astype(BF16)
    g_actp, a_sum, start, dtb_grad, skip_grad, dtp_grad, g_mixed, g_half, out_grad, mixed_out = (
        backward_scan(
            shape, pre, act, gy, bc, a2, skip, checks, w_dt, dt_low, tokens[0],
            gate_grad.reshape(segs, seqs * own_rows, feats),
            out_grad.reshape(segs, part, model),
            out_part.reshape(seqs, own_len, model),
            2 * block,
        )
    )
    grads, halves, input_grad, ends = finish_all(
        shape, taps, history,
        (g_actp, x_in, act, tok, w_x_half, w_g_one, w_g_two, gs_gate),
        (
            g_mixed, w_xt, head, kernel, b_conv, dtp_grad, a_sum.reshape(width, feats) * a_mat, dtb_grad, skip_grad, g_half,
            tokens[0], cotangent[0],
            final.reshape(width, feats), start.reshape(width, feats),
        ),
    )
    if part % LANES == 0:
        return unpack(
            taps, history, low_rank, width, grads, halves, ends, mixed_out, input_grad, out_grad,
            in_proj, gain_col,
        )
    ends = (
        ends.reshape(seqs, ends.shape[1], segs // seqs, part)
        .transpose(1, 2, 0, 3)
        .reshape(ends.shape[1], feats)
    )
    raw_grad = (
        halves.reshape(2, seqs, own_rows, segs, part)
        .transpose(2, 0, 3, 1, 4)
        .reshape(own_rows, both)
        .astype(F32)
    )
    in_grad = raw_grad * gain_col
    gain_grad = jnp.sum(raw_grad * own_weight, axis=1)

    at = width + history
    xp_at = low_rank + x_proj.shape[1]
    return (
        mixed_out[None],
        ends[None, :width],
        ends[None, width:at],
        input_grad[None],
        ends[None, at : at + width],
        ends[None, at + width : at + width + history],
        gain_grad,
        in_grad,
        grads[xp_at + width : xp_at + width + taps],
        grads[xp_at + width + taps],
        grads[low_rank:xp_at].T,
        grads[:low_rank],
        grads[xp_at + width + taps + 1],
        grads[xp_at : xp_at + width],
        grads[xp_at + width + taps + 2],
        out_grad,
    )


def solution(mesh):
    spread = ("seg", "seq")
    placed = (
        P("seg", "seq", None),
        P(spread),
        P(spread, None),
        P(None, spread),
        P(spread),
        P(spread, None),
        P(None, spread),
        P(spread),
        P(None, spread),
        P(spread),
        P(spread, None),
        P("seg", None, None),
        P("seg", None, None),
        P("seg", "seq", None),
    )
    return jax.shard_map(
        body,
        mesh=mesh,
        in_specs=placed,
        out_specs=(
            P("seg", "seq", None),
            P("seg", None, "seq"),
            P("seg", None, "seq"),
            P("seg", "seq", None),
            P("seg", None, "seq"),
            P("seg", None, "seq"),
            P(spread),
            P(spread, None),
            P(None, spread),
            P(spread),
            P(spread, None),
            P(None, spread),
            P(spread),
            P(None, spread),
            P(spread),
            P(spread, None),
        ),
        check_vma=False,
    )
```

```python
import functools

import jax
import jax.numpy as jnp
from jax import lax
from jax.experimental import pallas as pl
from jax.experimental.pallas import tpu as pltpu
from jax.sharding import PartitionSpec as P

EPSILON = 1e-05
LOG2E = 1.4426950408889634
LANES = 128
UNROLL = 8
F32 = jnp.float32
BF16 = jnp.bfloat16


def dot_nn(a, b):
    return jnp.dot(a, b, preferred_element_type=F32)


def dot_tn(a, b):
    return lax.dot_general(a, b, (((0,), (0,)), ((), ())), preferred_element_type=F32)


def dot_nt(a, b):
    return lax.dot_general(a, b, (((1,), (1,)), ((), ())), preferred_element_type=F32)


def sigmoid(v):
    return 1.0 / (1.0 + jnp.exp(-v))


def softplus(v):
    return jnp.maximum(v, 0.0) + jnp.log1p(jnp.exp(-jnp.abs(v)))


def to_planes(planes_ref, rows):
    groups = planes_ref.shape[0]
    for s in range(rows.shape[1] // LANES):
        tile = rows[:, s * LANES : (s + 1) * LANES].reshape(groups, UNROLL, LANES)
        planes_ref[:, pl.ds(s * UNROLL, UNROLL), :] = tile


def from_planes(planes_ref):
    groups, rows, _ = planes_ref.shape
    return jnp.concatenate(
        [
            planes_ref[:, pl.ds(s * UNROLL, UNROLL), :].reshape(groups * UNROLL, LANES)
            for s in range(rows // UNROLL)
        ],
        axis=1,
    )


def token_of(planes, i):
    return pl.ds(i, planes, stride=UNROLL)


MESH_ID = pl.DeviceIdType.MESH
VMEM_MOST = 67_043_328


class Grid:
    def __init__(self, axis, lines, fast):
        self.axis, self.lines, self.fast = axis, lines, fast
        self.here = lax.axis_index(axis)
        self.line = self.here // fast
        self.lane = self.here - self.line * fast

    def at(self, line, lane):
        return line * self.fast + lane

    def line_peer(self, k):
        return lax.rem(self.line + k, self.lines)

    def lane_peer(self, e):
        return lax.rem(self.lane + e, self.fast)

    def copy(self, src, dst, sent, got, index):
        return pltpu.make_async_remote_copy(
            src_ref=src, dst_ref=dst, send_sem=sent, recv_sem=got,
            device_id={self.axis: index}, device_id_type=MESH_ID,
        )


def meet(groups):
    barrier = pltpu.get_barrier_semaphore()
    total = 0
    for grid in groups:
        size = grid.lines * grid.fast
        for k in range(1, size):
            pl.semaphore_signal(
                barrier, inc=1, device_id={grid.axis: lax.rem(grid.here + k, size)},
                device_id_type=MESH_ID,
            )
        total += size - 1
    pl.semaphore_wait(barrier, total)


class Gather:
    def __init__(self, grid, own, out, sems, piece=None):
        self.grid, self.own, self.out, self.piece = grid, own, out, piece
        self.up_s, self.up_r, self.dn_s, self.dn_r, self.x_s, self.x_r = sems

    @staticmethod
    def semaphores(lines, fast):
        hops = pltpu.SemaphoreType.DMA((lines,))
        across = pltpu.SemaphoreType.DMA((lines, fast))
        return [hops, hops, hops, hops, across, across]

    def block(self, line, lane=None):
        grid = self.grid
        index = grid.at(line, grid.lane if lane is None else lane)
        return self.out.at[index] if self.piece is None else self.out.at[index, self.piece]

    def up(self, k):
        grid = self.grid
        block = self.block(jnp.maximum(grid.line - k, 0))
        return grid.copy(
            self.own if k == 0 else block, block, self.up_s.at[k], self.up_r.at[k],
            grid.at(jnp.minimum(grid.line + 1, grid.lines - 1), grid.lane),
        )

    def down(self, k):
        grid = self.grid
        block = self.block(jnp.minimum(grid.line + k, grid.lines - 1))
        return grid.copy(
            self.own if k == 0 else block, block, self.dn_s.at[k], self.dn_r.at[k],
            grid.at(jnp.maximum(grid.line - 1, 0), grid.lane),
        )

    def sends_up(self, k):
        return jnp.logical_and(self.grid.line + 1 < self.grid.lines, self.grid.line >= k)

    def sends_down(self, k):
        return jnp.logical_and(self.grid.line > 0, self.grid.line + k < self.grid.lines)

    def across(self, line, slot, e, own=False):
        grid = self.grid
        block = self.block(line)
        return grid.copy(
            self.own if own else block, block, self.x_s.at[slot, e], self.x_r.at[slot, e],
            grid.at(grid.line, grid.lane_peer(e)),
        )

    def slots(self):
        return range(self.grid.lines)

    def begin(self):
        grid = self.grid
        for when, copy in ((self.sends_up(0), self.up(0)), (self.sends_down(0), self.down(0))):
            pl.when(when)(copy.start)
        for e in range(1, grid.fast):
            self.across(grid.line, 0, e, own=True).start()

    def step(self, k):
        grid = self.grid

        def arrived(copy, line, slot, forward, onward):
            copy.wait_recv()
            if k < grid.lines - 1:
                pl.when(forward(k))(onward(k).start)
            for e in range(1, grid.fast):
                self.across(line, slot, e).start()

        below, above = grid.line - k, grid.line + k

        @pl.when(below >= 0)
        def _():
            arrived(self.up(k - 1), below, grid.lines - k, self.sends_up, self.up)

        @pl.when(above < grid.lines)
        def _():
            arrived(self.down(k - 1), above, k, self.sends_down, self.down)

    def finish(self):
        grid = self.grid
        for k in range(grid.lines - 1):
            pl.when(self.sends_up(k))(self.up(k).wait_send)
            pl.when(self.sends_down(k))(self.down(k).wait_send)
        for slot in self.slots():
            for e in range(1, grid.fast):
                copy = self.across(grid.line_peer(slot), slot, e, own=slot == 0)
                copy.wait_send()
                copy.wait_recv()


class Scatter:
    def __init__(self, grid, src, scratch, inside=False):
        self.grid, self.src, self.inside = grid, src, inside
        if not inside:
            self.own, self.o_s = scratch[:2]
            scratch = scratch[2:]
        self.xbuf, self.stage, self.zbuf, self.acc = scratch[:4]
        self.x_s, self.x_r, self.z_s, self.z_r = scratch[4:]
        self.last = grid.lines - 1

    @staticmethod
    def scratch(lines, fast, shape, inside=False):
        dma = pltpu.SemaphoreType.DMA
        shape = tuple(shape)
        loads = [] if inside else [pltpu.VMEM((lines,) + shape, BF16), dma((lines,))]
        return loads + [
            pltpu.VMEM((lines, fast - 1) + shape, BF16),
            pltpu.VMEM((lines - 1,) + shape, BF16),
            pltpu.VMEM((lines + 1,) + shape, BF16),
            pltpu.VMEM(shape, F32),
            dma((lines, fast)), dma((lines, fast)), dma((lines,)), dma((lines + 1,)),
        ]

    def dest(self, j):
        line, last = self.grid.line, self.last
        above, below = last - line, line
        low = jnp.where(j < above, last - j, j - above)
        high = jnp.where(j < below, j, last - (j - below))
        other = jnp.where(2 * line <= last, low, high)
        return jnp.where(j == last, line, other)

    def index(self, j, e):
        return self.grid.at(self.dest(j), self.grid.lane_peer(e))

    def across(self, j, e):
        grid = self.grid
        return grid.copy(
            self.src.at[self.index(j, e)], self.xbuf.at[j, e - 1],
            self.x_s.at[j, e], self.x_r.at[j, e], grid.at(grid.line, grid.lane_peer(e)),
        )

    def local(self, j):
        return pltpu.make_async_copy(
            self.src.at[self.index(j, 0)], self.own.at[j], self.o_s.at[j]
        )

    def along(self, j):
        grid = self.grid
        dest = self.dest(j)
        up = dest > grid.line
        to = jnp.clip(jnp.where(up, grid.line + 1, grid.line - 1), 0, self.last)
        slot = jnp.where(jnp.logical_and(jnp.logical_not(up), dest == to), grid.lines, dest)
        return grid.copy(
            self.stage.at[j], self.zbuf.at[slot], self.z_s.at[j], self.z_r.at[slot],
            grid.at(to, grid.lane),
        )

    def arrival(self, slot):
        grid = self.grid
        return grid.copy(
            self.stage.at[0], self.zbuf.at[slot], self.z_s.at[0], self.z_r.at[slot],
            grid.at(lax.rem(grid.line + 1, grid.lines), grid.lane),
        )

    def order(self):
        return list(range(self.grid.lines))

    def begin(self):
        for j in self.order():
            for e in range(1, self.grid.fast):
                self.across(j, e).start()
            if not self.inside:
                self.local(j).start()

    def rows(self, step):
        count = self.acc.shape[0]
        size = 16 if count % 16 == 0 else 8

        def run(i, carry):
            step(pl.ds(pl.multiple_of(i * size, size), size))
            return carry

        lax.fori_loop(0, count // size, run, 0)

    def middle(self, j):
        grid = self.grid
        for e in range(1, grid.fast):
            self.across(j, e).wait_recv()
        if self.inside:
            own = self.src.at[self.index(j, 0)]
        else:
            self.local(j).wait()
            own = self.own.at[j]

        def partial(at):
            total = own[at, :].astype(F32)
            for e in range(grid.fast - 1):
                total = total + self.xbuf[j, e, at, :].astype(F32)
            return total

        if j == self.last:

            def keep(at):
                self.acc[at, :] = partial(at)

            self.rows(keep)
            return
        dest = self.dest(j)
        carried = jnp.where(dest > grid.line, grid.line > 0, grid.line < self.last)

        @pl.when(carried)
        def _():
            self.arrival(dest).wait_recv()

            def add(at):
                total = partial(at) + self.zbuf[dest, at, :].astype(F32)
                self.stage[j, at, :] = total.astype(BF16)

            self.rows(add)

        @pl.when(jnp.logical_not(carried))
        def _():
            def add(at):
                self.stage[j, at, :] = partial(at).astype(BF16)

            self.rows(add)

        self.along(j).start()

    def finish(self, write):
        line, last = self.grid.line, self.last
        from_below, from_above = line > 0, line < last

        @pl.when(from_below)
        def _():
            self.arrival(line).wait_recv()

        @pl.when(from_above)
        def _():
            self.arrival(self.grid.lines).wait_recv()

        def total(at, below, above):
            result = self.acc[at, :]
            if below:
                result = result + self.zbuf[line, at, :].astype(F32)
            if above:
                result = result + self.zbuf[last + 1, at, :].astype(F32)
            write(at, result)

        for when, below, above in (
            (jnp.logical_and(from_below, from_above), True, True),
            (jnp.logical_not(from_below), False, True),
            (jnp.logical_not(from_above), True, False),
        ):

            @pl.when(when)
            def _():
                self.rows(lambda at: total(at, below, above))

    def drain(self):
        for j in self.order():
            for e in range(1, self.grid.fast):
                self.across(j, e).wait_send()
            if j < self.last:
                self.along(j).wait_send()


def into(ref):
    def write(at, total):
        ref[at, :] = total.astype(ref.dtype)

    return write


class Exchange:
    def __init__(self, grid, src, dst, sems):
        self.grid, self.src, self.dst = grid, src, dst
        self.sent, self.got = sems
        self.size = grid.lines * grid.fast

    @staticmethod
    def semaphores(size):
        return [pltpu.SemaphoreType.DMA((size,)), pltpu.SemaphoreType.DMA((size,))]

    def one(self, k):
        grid = self.grid
        peer = lax.rem(grid.here + k, self.size)
        return grid.copy(
            self.src(peer), self.dst(grid.here), self.sent.at[k], self.got.at[k], peer
        )

    def begin(self):
        for k in range(1, self.size):
            self.one(k).start()

    def arrived(self):
        for k in range(1, self.size):
            self.one(k).wait_recv()

    def drain(self):
        for k in range(1, self.size):
            self.one(k).wait_send()


ANY = pl.BlockSpec(memory_space=pl.ANY)
INSIDE = pl.BlockSpec(memory_space=pltpu.VMEM)


def comm_params(collective_id):
    return pltpu.CompilerParams(
        collective_id=collective_id, has_side_effects=True, vmem_limit_bytes=VMEM_MOST
    )


def grids(shape):
    lines, fast, seq_lines = shape
    return Grid("seg", lines, fast), Grid("seq", seq_lines, 2)


def sum_over_seq(seq, x_ref, out_ref, half, got, mine, others, whole, *sems):
    lane_s, lane_r, line_s, line_r, back_s, back_r = sems
    width = x_ref.shape[1] // 2
    lines = seq.lines
    other = 1 - seq.lane
    left = pl.ds(0, width)
    right = pl.ds(width, width)

    @pl.when(seq.lane == 0)
    def _():
        half[...] = x_ref[:, right].astype(BF16)

    @pl.when(seq.lane == 1)
    def _():
        half[...] = x_ref[:, left].astype(BF16)

    swap = seq.copy(half, got, lane_s, lane_r, seq.at(seq.line, other))
    swap.start()
    swap.wait()

    @pl.when(seq.lane == 0)
    def _():
        mine[...] = (x_ref[:, left] + got[...].astype(F32)).astype(BF16)

    @pl.when(seq.lane == 1)
    def _():
        mine[...] = (x_ref[:, right] + got[...].astype(F32)).astype(BF16)

    copies = [
        seq.copy(
            mine, others.at[k - 1], line_s.at[k], line_r.at[k], seq.at(seq.line_peer(k), seq.lane)
        )
        for k in range(1, lines)
    ]
    for copy in copies:
        copy.start()
    for copy in copies:
        copy.wait()
    total = mine[...].astype(F32)
    for k in range(lines - 1):
        total = total + others[k].astype(F32)
    whole[seq.lane] = total.astype(BF16)
    back = seq.copy(
        whole.at[seq.lane], whole.at[seq.lane], back_s, back_r, seq.at(seq.line, other)
    )
    back.start()
    back.wait()
    out_ref[:, left] = whole[0]
    out_ref[:, right] = whole[1]


def forward_kernel(
    shape, steps,
    low_ref, wdt_ref, bias_ref, act_ref, bc_ref, a_ref, skip_ref, init_ref, weight_ref, cot_ref,
    tok_ref, gate_one, gate_src,
    y_ref, pre_ref, check_ref, final_ref, gate_ref, gated_ref, weights_ref, cots_ref, gate_two,
    state, rate_pl, drive_pl, y_pl, w_one, w_two, local_s, *sems,
):
    count = pre_ref.shape[0]
    width, planes, _ = a_ref.shape
    seg, seq = grids(shape)
    gates = Gather(seg, gate_src.at[:, 1], gate_two, sems[:6])
    weights = Gather(seg, weight_ref, weights_ref, sems[6:12])
    cots = Gather(seq, cot_ref, cots_ref, sems[12:])
    step = pl.program_id(0)
    keeps = [
        pltpu.make_async_copy(weight_ref, weights_ref.at[seg.here], local_s.at[0]),
        pltpu.make_async_copy(cot_ref, cots_ref.at[seq.here], local_s.at[1]),
        pltpu.make_async_copy(gate_src.at[:, 1], gate_two.at[seg.here], local_s.at[2]),
    ]
    load_one = pltpu.make_async_copy(gate_one, w_one, local_s.at[3])

    @pl.when(step == 0)
    def _():
        meet((seg, seq))
        gates.begin()
        weights.begin()
        cots.begin()
        for keep in keeps:
            keep.start()
        load_one.start()
        state[...] = init_ref[...]

    pre = dot_tn(low_ref[...], wdt_ref[...]) + bias_ref[...]
    pre_ref[...] = pre
    rate = softplus(pre)
    act = act_ref[...].astype(F32)
    to_planes(rate_pl, rate)
    to_planes(drive_pl, rate * act)
    groups = count // UNROLL

    def group(k, carry):
        at = k * UNROLL
        rates = [rate_pl[k, token_of(planes, i), :] for i in range(UNROLL)]
        drives = [drive_pl[k, token_of(planes, i), :] for i in range(UNROLL)]
        sums = [None] * UNROLL
        for n in range(width):
            a = a_ref[n]
            h = state[n]
            check_ref[k, n] = h
            for i in range(UNROLL):
                h = jnp.exp2(rates[i] * a) * h + bc_ref[at + i, n] * drives[i]
                term = bc_ref[at + i, width + n] * h
                sums[i] = term if n == 0 else sums[i] + term
            state[n] = h
        for i in range(UNROLL):
            y_pl[k, token_of(planes, i), :] = sums[i]
        return carry

    ticks = 2 * steps
    plan = [[] for _ in range(ticks)]
    late = []
    for k in range(1, seg.lines):
        for gather, share in ((gates, 4 * k), (weights, 9 * k)):
            tick = ticks * share // 16
            (plan[tick - 1] if tick < ticks else late).append(functools.partial(gather.step, k))
        if k < seq.lines:
            plan[ticks - 1].append(functools.partial(cots.step, k))

    def part_of_step(h, carry):
        lax.fori_loop(h * (groups // 2), (h + 1) * (groups // 2), group, 0)
        for tick in range(ticks):
            if plan[tick]:

                @pl.when(step * 2 + h == tick)
                def _():
                    for event in plan[tick]:
                        event()

        return carry

    lax.fori_loop(0, 2, part_of_step, 0)
    y_ref[pl.ds(pl.multiple_of(step * count, count), count), :] = (
        from_planes(y_pl) + skip_ref[...] * act_ref[...].astype(F32)
    )

    @pl.when(step == steps - 1)
    def _():
        final_ref[...] = state[...]
        for event in late[:-1]:
            event()
        gates.finish()
        keeps[2].wait()
        load_one.wait()
        load_two = pltpu.make_async_copy(gate_two, w_two, local_s.at[3])
        load_two.start()
        load_two.wait()
        model = tok_ref.shape[1]
        half = w_one.shape[3]
        block = 256

        def gating(i, carry):
            rows = pl.ds(pl.multiple_of(i * block, block), block)
            lines = tok_ref[rows, :].astype(F32)
            rstd = lax.rsqrt(jnp.mean(lines * lines, axis=1, keepdims=True) + EPSILON)
            for j, w in enumerate((w_one, w_two)):
                cols = pl.ds(j * half, half)
                gate = rstd * dot_nn(tok_ref[rows, :], w[...].reshape(model, half))
                gate_ref[rows, cols] = gate
                gated_ref[rows, cols] = (y_ref[rows, cols] * gate * sigmoid(gate)).astype(BF16)
            return carry

        blocks = y_ref.shape[0] // block
        lax.fori_loop(0, blocks // 2, gating, 0)
        late[-1]()
        lax.fori_loop(blocks // 2, blocks, gating, 0)
        weights.finish()
        cots.finish()
        for keep in keeps[:2]:
            keep.wait()


def backward_kernel(
    shape, steps,
    pre_ref, act_ref, gy_ref, bc_ref, a_ref, skip_ref, check_ref, wdt_ref, low_ref, base_ref,
    first_src, second_src, gated_src, weight_src,
    gact_ref, agrad_ref, start_ref, dtb_ref, sgrad_ref, dtp_ref, mix_ref,
    first_out, second_out, third_out,
    carry_s, rate_pl, drive_pl, gy_pl, grate_pl, thr_pl, prod, part, mix_s,
    gated_in, weight_in, third_src, load_s, *scratch,
):
    count = pre_ref.shape[0]
    width, planes, _ = a_ref.shape
    low_rank = wdt_ref.shape[0]
    seg, seq = grids(shape)
    first = Scatter(seg, first_src, scratch[:10])
    second = Scatter(seg, second_src, scratch[10:20])
    third = Scatter(seq, third_src, scratch[20:28], inside=True)
    loads = [
        pltpu.make_async_copy(gated_src, gated_in, load_s.at[0]),
        pltpu.make_async_copy(weight_src, weight_in, load_s.at[1]),
    ]
    step = pl.program_id(0)

    @pl.when(step == 0)
    def _():
        meet((seg, seq))
        first.begin()
        second.begin()
        for load in loads:
            load.start()
        carry_s[...] = jnp.zeros_like(carry_s)
        agrad_ref[...] = jnp.zeros_like(agrad_ref)
        dtb_ref[...] = jnp.zeros_like(dtb_ref)
        sgrad_ref[...] = jnp.zeros_like(sgrad_ref)
        dtp_ref[...] = jnp.zeros_like(dtp_ref)

    pre = pre_ref[...]
    rate = softplus(pre)
    act = act_ref[...].astype(F32)
    to_planes(rate_pl, rate)
    to_planes(drive_pl, rate * act)
    to_planes(gy_pl, gy_ref[...])
    groups = count // UNROLL

    def group(j, carry):
        k = groups - 1 - j
        at = k * UNROLL
        rates = [rate_pl[k, token_of(planes, i), :] for i in range(UNROLL)]
        drives = [drive_pl[k, token_of(planes, i), :] for i in range(UNROLL)]
        gys = [gy_pl[k, token_of(planes, i), :] for i in range(UNROLL)]
        g_rate = [None] * UNROLL
        through = [None] * UNROLL
        for n in range(width):
            a = a_ref[n]
            states = [check_ref[k, n]]
            decays = []
            for i in range(UNROLL):
                decays.append(jnp.exp2(rates[i] * a))
                states.append(decays[i] * states[i] + bc_ref[at + i, n] * drives[i])
            lam = carry_s[n]
            acc = agrad_ref[n]
            for i in reversed(range(UNROLL)):
                lam = lam + bc_ref[at + i, width + n] * gys[i]
                b_term = bc_ref[at + i, n] * lam
                region = (i * 2 * width + n) // 8
                prod[region, token_of(planes, n % 8), :] = lam * drives[i]
                prod[region + width // 8, token_of(planes, n % 8), :] = states[i + 1] * gys[i]
                lam = decays[i] * lam
                weighted = lam * states[i]
                acc = acc + weighted * rates[i]
                a_term = weighted * a
                g_rate[i] = a_term if n == 0 else g_rate[i] + a_term
                through[i] = b_term if n == 0 else through[i] + b_term
            carry_s[n] = lam
            agrad_ref[n] = acc
        for i in range(UNROLL):
            grate_pl[k, token_of(planes, i), :] = g_rate[i]
            thr_pl[k, token_of(planes, i), :] = through[i]
            for q in range(2 * width // 8):
                region = i * 2 * width // 8 + q
                total = prod[region, pl.ds(0, 8), :]
                for s in range(1, planes):
                    total = total + prod[region, pl.ds(s * 8, 8), :]
                row = pl.multiple_of((at + i) * 2 * width + q * 8, 8)
                part[pl.ds(row, 8), :] = total
        return carry

    events = [functools.partial(s.middle, k) for s in (first, second) for k in s.order()]
    ticks = 2 * steps
    plan = [[] for _ in range(ticks)]
    for j, event in enumerate(events):
        plan[min(ticks - 1, ticks * (j + 1) // len(events))].append(event)

    def output(index):
        own_len, model = third_src.shape[1:]
        rows = pl.ds(pl.multiple_of(index * own_len, own_len), own_len)

        def column(c, carry):
            cols = pl.ds(pl.multiple_of(c * 512, 512), 512)
            third_src[index, :, cols] = dot_nn(gated_in[rows, :], weight_in[:, cols]).astype(BF16)
            return carry

        lax.fori_loop(0, model // 512, column, 0)

    def outputs():
        for load in loads:
            load.wait()

        def leave(j, carry):
            output(third.index(j, 1))
            third.across(j, 1).start()
            return carry

        def stay(j, carry):
            output(third.index(j, 0))
            return carry

        lax.fori_loop(0, seq.lines, leave, 0)
        lax.fori_loop(0, seq.lines, stay, 0)

    plan[0].append(outputs)
    for j in third.order():
        plan[min(ticks - 1, 5 + 2 * j)].append(functools.partial(third.middle, j))

    def add_base(at, total):
        third_out[at, :] = (total + base_ref[at, :].astype(F32)).astype(BF16)

    plan[min(ticks - 1, 13)].append(functools.partial(third.finish, add_base))

    def part_of_step(h, carry):
        lax.fori_loop(h * (groups // 2), (h + 1) * (groups // 2), group, 0)
        for tick in range(ticks - 1):
            if plan[tick]:

                @pl.when(step * 2 + h == tick)
                def _():
                    for event in plan[tick]:
                        event()

        return carry

    lax.fori_loop(0, 2, part_of_step, 0)
    g_rate = from_planes(grate_pl) * (1.0 / LOG2E)
    through = from_planes(thr_pl)
    pre = pre_ref[...]
    rate = softplus(pre)
    act = act_ref[...].astype(F32)
    gy = gy_ref[...]
    g_dtpre = ((g_rate + act * through) * sigmoid(pre)).astype(BF16)
    gact_ref[...] = gy * skip_ref[...] + rate * through
    dtb_ref[...] += jnp.sum(g_dtpre.astype(F32), axis=0, keepdims=True)
    sgrad_ref[...] += jnp.sum(gy * act, axis=0, keepdims=True)
    dtp_ref[...] += dot_nn(low_ref[...], g_dtpre)
    rows = 2 * width
    ones = jnp.ones((LANES, LANES), F32)
    sums = jnp.dot(part[...], ones, preferred_element_type=F32)
    sums = sums.reshape(count, rows, LANES)
    pick = lax.broadcasted_iota(jnp.int32, (1, rows, LANES), 1) == lax.broadcasted_iota(
        jnp.int32, (1, rows, LANES), 2
    )
    g_bc = jnp.sum(jnp.where(pick, sums, 0.0), axis=1)
    tokens_at = pl.ds(pl.multiple_of((steps - 1 - step) * count, count), count)
    mix_s[pl.ds(0, low_rank), tokens_at] = dot_nt(wdt_ref[...], g_dtpre)
    mix_s[pl.ds(low_rank, rows), tokens_at] = g_bc.T[:rows]

    @pl.when(step == steps - 1)
    def _():
        start_ref[...] = carry_s[...]
        sum_over_seq(seq, mix_s, mix_ref, *scratch[28:])
        for event in plan[ticks - 1]:
            event()
        first.finish(into(first_out))
        second.finish(into(second_out))
        for scatter in (first, second, third):
            scatter.drain()


def forward_scan(
    shape, low, w_dt, bias, act, bc, a2, skip, init, weight, cot, tok, gate_one, gate_part, block
):
    lines, fast, seq_lines = shape
    length, features = act.shape
    width, planes, _ = a2.shape
    low_rank = w_dt.shape[0]
    steps = length // block
    rows = pl.BlockSpec((block, features), lambda i: (i, 0))
    one = pl.Buffered(1)

    def whole(*dims):
        return pl.BlockSpec(dims, lambda i: (0,) * len(dims), pipeline_mode=one)

    plane = pltpu.VMEM((block // UNROLL, planes * UNROLL, LANES), F32)
    return pl.pallas_call(
        functools.partial(forward_kernel, shape, steps),
        grid=(steps,),
        in_specs=[
            pl.BlockSpec((low_rank, block), lambda i: (0, i)),
            whole(low_rank, features), whole(1, features), rows,
            pl.BlockSpec((block, 2 * width), lambda i: (i, 0), memory_space=pltpu.SMEM),
            whole(width, planes, LANES), whole(1, features), whole(width, planes, LANES),
            whole(*weight.shape), whole(*cot.shape), whole(*tok.shape), ANY, ANY,
        ],
        out_specs=[
            whole(length, features), rows,
            pl.BlockSpec((block // UNROLL, width, planes, LANES), lambda i: (i, 0, 0, 0)),
            whole(width, planes, LANES), whole(length, features), whole(length, features),
            ANY, ANY, ANY,
        ],
        out_shape=[
            jax.ShapeDtypeStruct((length, features), F32),
            jax.ShapeDtypeStruct((length, features), F32),
            jax.ShapeDtypeStruct((length // UNROLL, width, planes, LANES), F32),
            jax.ShapeDtypeStruct((width, planes, LANES), F32),
            jax.ShapeDtypeStruct((length, features), F32),
            jax.ShapeDtypeStruct((length, features), BF16),
            jax.ShapeDtypeStruct((lines * fast,) + weight.shape, BF16),
            jax.ShapeDtypeStruct((seq_lines * 2,) + cot.shape, BF16),
            jax.ShapeDtypeStruct(gate_one.shape, BF16),
        ],
        scratch_shapes=[
            pltpu.VMEM((width, planes, LANES), F32), plane, plane, plane,
            pltpu.VMEM(gate_one.shape, BF16), pltpu.VMEM(gate_one.shape, BF16),
            pltpu.SemaphoreType.DMA((4,)),
            *Gather.semaphores(lines, fast), *Gather.semaphores(lines, fast),
            *Gather.semaphores(seq_lines, 2),
        ],
        compiler_params=comm_params(5),
        cost_estimate=pl.CostEstimate(
            flops=8 * length * features * width,
            bytes_accessed=24 * length * features,
            transcendentals=length * features * width,
        ),
        name="scan_forward",
    )(low, w_dt, bias, act, bc, a2, skip, init, weight, cot, tok, gate_one, gate_part)


def backward_scan(
    shape, pre, act, gy, bc, a2, skip, checks, w_dt, dt_low, base, first, second, gated, weight,
    block,
):
    lines, fast, seq_lines = shape
    length, features = pre.shape
    width, planes, _ = a2.shape
    low_rank = w_dt.shape[0]
    steps = length // block
    rows = pl.BlockSpec((block, features), lambda i: (steps - 1 - i, 0))
    whole = pl.BlockSpec((width, planes, LANES), lambda i: (0, 0, 0))

    def all_of(rows, columns):
        return pl.BlockSpec((rows, columns), lambda i: (0, 0))

    line = all_of(1, features)
    plane = pltpu.VMEM((block // UNROLL, planes * UNROLL, LANES), F32)
    mixed = (low_rank + 2 * width, length)
    return pl.pallas_call(
        functools.partial(backward_kernel, shape, steps),
        grid=(steps,),
        in_specs=[
            rows, rows, rows,
            pl.BlockSpec(
                (block, 2 * width), lambda i: (steps - 1 - i, 0), memory_space=pltpu.SMEM
            ),
            whole, line,
            pl.BlockSpec(
                (block // UNROLL, width, planes, LANES), lambda i: (steps - 1 - i, 0, 0, 0)
            ),
            all_of(low_rank, features),
            pl.BlockSpec((low_rank, block), lambda i: (0, steps - 1 - i)),
            all_of(*base.shape),
            ANY, ANY, ANY, ANY,
        ],
        out_specs=[
            rows, whole, whole, line, line, all_of(low_rank, features), all_of(*mixed),
            all_of(*first.shape[1:]), all_of(*second.shape[1:]), all_of(*base.shape),
        ],
        out_shape=[
            jax.ShapeDtypeStruct((length, features), F32),
            jax.ShapeDtypeStruct((width, planes, LANES), F32),
            jax.ShapeDtypeStruct((width, planes, LANES), F32),
            jax.ShapeDtypeStruct((1, features), F32),
            jax.ShapeDtypeStruct((1, features), F32),
            jax.ShapeDtypeStruct((low_rank, features), F32),
            jax.ShapeDtypeStruct(mixed, BF16),
            jax.ShapeDtypeStruct(first.shape[1:], BF16),
            jax.ShapeDtypeStruct(second.shape[1:], F32),
            jax.ShapeDtypeStruct(base.shape, BF16),
        ],
        scratch_shapes=[pltpu.VMEM((width, planes, LANES), F32)]
        + [plane] * 5
        + [
            pltpu.VMEM((UNROLL * 2 * width // 8, planes * 8, LANES), F32),
            pltpu.VMEM((block * 2 * width, LANES), F32),
            pltpu.VMEM(mixed, F32),
            pltpu.VMEM(gated.shape, BF16),
            pltpu.VMEM(weight.shape, BF16),
            pltpu.VMEM((2 * seq_lines,) + base.shape, BF16),
            pltpu.SemaphoreType.DMA((2,)),
            *Scatter.scratch(lines, fast, first.shape[1:]),
            *Scatter.scratch(lines, fast, second.shape[1:]),
            *Scatter.scratch(seq_lines, 2, base.shape, inside=True),
            *sum_scratch(seq_lines, *mixed),
        ],
        compiler_params=comm_params(6),
        cost_estimate=pl.CostEstimate(
            flops=20 * length * features * width,
            bytes_accessed=28 * length * features,
            transcendentals=length * features * width,
        ),
        name="scan_backward",
    )(pre, act, gy, bc, a2, skip, checks, w_dt, dt_low, base, first, second, gated, weight)


def finish_kernel(shape, taps, history, refs, scratch):
    (
        gact, x_in, act, tok, w_x, w_g, w_h, gs_gate,
        mix, w_xt, head, kern, b_conv, dtp, a_grad, dtb, sgrad, g_half, own_tok, own_cot,
        final, start,
        small_out, halves_out, input_out, ends_out,
    ) = refs
    (
        gc, xb, actb, tokb, wxb, wgb, gsg, gs_x, xg, q_src, pack, small_src, ends_src, x_half,
        in_s, own_s,
    ) = scratch[:16]
    seg, seq = grids(shape)
    length, feats = act.shape
    at = 16
    sets = []
    for inside, size in ((True, 8), (True, 8), (True, 8)):
        sets.append(scratch[at : at + size])
        at += size
    swaps_s = [scratch[at + 2 * i : at + 2 * i + 2] for i in range(3)]
    small = Scatter(seg, small_src, sets[0], inside=True)
    x_sum = Scatter(seg, xg, sets[1], inside=True)
    q_sum = Scatter(seq, q_src, sets[2], inside=True)
    loads = [
        pltpu.make_async_copy(gact, gc.at[pl.ds(0, length)], in_s.at[0]),
        pltpu.make_async_copy(x_in, xb.at[pl.ds(8, length)], in_s.at[1]),
        pltpu.make_async_copy(tok, tokb, in_s.at[2]),
        pltpu.make_async_copy(act, actb, in_s.at[3]),
        pltpu.make_async_copy(gs_gate, gsg, in_s.at[4]),
        pltpu.make_async_copy(w_g, wgb.at[0], in_s.at[5]),
        pltpu.make_async_copy(w_h, wgb.at[1], in_s.at[6]),
        pltpu.make_async_copy(w_x, wxb, in_s.at[7]),
    ]
    for load in loads:
        load.start()
    meet((seg, seq))
    own_rows = g_half.shape[0] // (seq.lines * seq.fast)

    def swap(half, src, sems):
        return Exchange(
            seq,
            lambda p: src.at[pl.ds(pl.multiple_of(p * own_rows, own_rows), own_rows)],
            lambda m: halves_out.at[half, m],
            sems,
        )

    swap_g = swap(1, g_half, swaps_s[1])
    swap_g.begin()
    xb[pl.ds(0, 8), :] = head[...]
    gc[pl.ds(length, 8), :] = jnp.zeros((8, feats), F32)
    loads[0].wait()
    big = LANES

    def add_mixed(i, carry):
        rows = pl.ds(pl.multiple_of(i * big, big), big)
        gc[rows, :] += dot_tn(mix[:, rows], w_xt[...])
        return carry

    lax.fori_loop(0, length // big, add_mixed, 0)
    loads[1].wait()
    tall = 32
    chunk = min(512, feats)
    sums_at = 8 * (taps + 1)
    pack[...] = jnp.zeros_like(pack)

    def through_conv(i, carry):
        t0 = pl.multiple_of(i * tall, tall)
        for c in range(0, feats, chunk):
            cols = pl.ds(c, chunk)
            wide = xb[pl.ds(t0, tall + 8), cols]
            rows = [wide[8 - history + k : 8 - history + k + tall] for k in range(taps)]
            conv = b_conv[:, cols]
            for k in range(taps):
                conv = conv + kern[pl.ds(k, 1), cols] * rows[k]
            sig = sigmoid(conv)
            g_conv = gc[pl.ds(t0, tall), cols] * sig * (1.0 + conv * (1.0 - sig))
            gc[pl.ds(t0, tall), cols] = g_conv
            for k in range(taps):
                term = g_conv * rows[k]
                pack[pl.ds(8 * k, 8), cols] += sum(
                    term[8 * j : 8 * j + 8] for j in range(tall // 8)
                )
            pack[pl.ds(8 * taps, 8), cols] += sum(
                g_conv[8 * j : 8 * j + 8] for j in range(tall // 8)
            )
        return carry

    lax.fori_loop(0, length // tall, through_conv, 0)
    loads[2].wait()

    def to_input(i, carry):
        t0 = pl.multiple_of(i * tall, tall)
        lines = tokb[pl.ds(t0, tall), :].astype(F32)
        rstd = lax.rsqrt(jnp.mean(lines * lines, axis=1, keepdims=True) + EPSILON)
        for c in range(0, feats, chunk):
            cols = pl.ds(c, chunk)
            wide = gc[pl.ds(t0, tall + 8), cols]
            g_x = kern[pl.ds(0, 1), cols] * wide[history : history + tall]
            for k in range(1, taps):
                g_x = g_x + kern[pl.ds(k, 1), cols] * wide[history - k : history - k + tall]
            gs_x[pl.ds(t0, tall), cols] = (rstd * g_x).astype(BF16)
        return carry

    lax.fori_loop(0, length // tall, to_input, 0)
    loads[3].wait()
    low_rank = dtp.shape[0]
    mixes = mix.shape[0]
    width = a_grad.shape[0]
    part = small_src.shape[2]
    xp = dot_nn(mix[...], actb[...])
    for g in range(small_src.shape[0]):
        cols = slice(g * part, (g + 1) * part)
        small_src[g, pl.ds(0, low_rank), :] = dtp[:, cols].astype(BF16)
        small_src[g, pl.ds(low_rank, mixes), :] = xp[:, cols].astype(BF16)
        base = low_rank + mixes
        small_src[g, pl.ds(base, width), :] = a_grad[:, cols].astype(BF16)
        lines = [
            jnp.sum(pack[pl.ds(8 * k, 8), cols], axis=0, keepdims=True) for k in range(taps + 1)
        ]
        lines += [dtb[:, cols], sgrad[:, cols]]
        lines.append(jnp.zeros((16 - len(lines), part), F32))
        small_src[g, pl.ds(base + width, 16), :] = jnp.concatenate(lines, axis=0).astype(BF16)
    small.begin()

    block_rows = xg.shape[1]

    def partial(index):
        cols = pl.ds(pl.multiple_of(index * block_rows, block_rows), block_rows)
        xg[index] = dot_tn(tokb[:, cols], gs_x[...]).astype(BF16)

    by_block = block_rows % LANES == 0
    if not by_block:
        for index in range(xg.shape[0]):
            cols = slice(index * block_rows, (index + 1) * block_rows)
            xg[index] = dot_tn(tokb[:, cols], gs_x[...]).astype(BF16)

    def leave(j, carry):
        for e in range(1, seg.fast):
            if by_block:
                partial(x_sum.index(j, e))
            x_sum.across(j, e).start()
        return carry

    lax.fori_loop(0, seg.lines, leave, 0)
    def stay(j, carry):
        if by_block:
            partial(x_sum.index(j, 0))
        return carry

    lax.fori_loop(0, seg.lines, stay, 0)
    ends_in = jnp.concatenate(
        [
            final[...],
            xb[pl.ds(length, 8), :][8 - history :],
            start[...],
            sum_head(gc, kern, history, taps),
            jnp.zeros((ends_src.shape[1] - 2 * (width + history), feats), F32),
        ],
        axis=0,
    )
    piece = ends_src.shape[2]
    for p in range(ends_src.shape[0]):
        ends_src[p] = ends_in[:, p * piece : (p + 1) * piece]
    end_swap = Exchange(seq, lambda p: ends_src.at[p], lambda m: ends_out.at[m], swaps_s[2])
    end_swap.begin()
    loads[4].wait()
    loads[5].wait()
    loads[6].wait()
    loads[7].wait()
    own_len = own_tok.shape[0]
    model = own_tok.shape[1]
    wide = 512
    half = feats // 2

    def normed(index):
        rows = pl.ds(pl.multiple_of(index * own_len, own_len), own_len)

        def column(c, carry):
            cols = pl.ds(pl.multiple_of(c * wide, wide), wide)
            q_src[index, :, cols] = (
                dot_nt(gsg[rows, pl.ds(0, half)], wgb[0, cols, :])
                + dot_nt(gsg[rows, pl.ds(half, half)], wgb[1, cols, :])
                + dot_nt(gs_x[rows, :], wxb[cols, :])
            ).astype(BF16)
            return carry

        lax.fori_loop(0, model // wide, column, 0)

    def leave_q(j, carry):
        normed(q_sum.index(j, 1))
        q_sum.across(j, 1).start()
        return carry

    def stay_q(j, carry):
        normed(q_sum.index(j, 0))
        return carry

    lax.fori_loop(0, seq.lines, leave_q, 0)
    lax.fori_loop(0, seq.lines, stay_q, 0)
    for k in small.order():
        small.middle(k)
    for j, k in enumerate(x_sum.order()):
        x_sum.middle(k)
        if j == seg.lines - 2:
            for m in q_sum.order():
                q_sum.middle(m)

    def input_grad(at, total):
        own = own_tok[at, :].astype(F32)
        square = 1.0 / (jnp.mean(own * own, axis=1, keepdims=True) + EPSILON)
        input_out[at, :] = (
            own_cot[at, :].astype(F32)
            + total
            - own * (square * jnp.mean(total * own, axis=1, keepdims=True))
        ).astype(BF16)

    q_sum.finish(input_grad)
    small.finish(into(small_out))
    x_sum.finish(into(x_half))
    swap_x = swap(0, x_half, swaps_s[0])
    swap_x.begin()
    own = pl.ds(pl.multiple_of(seq.here * own_rows, own_rows), own_rows)
    keeps = [
        pltpu.make_async_copy(x_half.at[own], halves_out.at[0, seq.here], own_s.at[0]),
        pltpu.make_async_copy(g_half.at[own], halves_out.at[1, seq.here], own_s.at[1]),
        pltpu.make_async_copy(ends_src.at[seq.here], ends_out.at[seq.here], own_s.at[2]),
    ]
    for keep in keeps:
        keep.start()
    for scatter in (small, x_sum, q_sum):
        scatter.drain()
    for exchange in (swap_g, end_swap, swap_x):
        exchange.arrived()
        exchange.drain()
    for keep in keeps:
        keep.wait()


def sum_head(gc, kern, history, taps):
    top = gc[pl.ds(0, 8), :]
    rows = []
    for j in range(history):
        rows.append(
            sum(kern[pl.ds(k, 1), :] * top[j - k : j - k + 1] for k in range(min(j + 1, taps)))
        )
    return jnp.concatenate(rows, axis=0)


def finish_all(shape, taps, history, big, small):
    lines, fast, seq_lines = shape
    segs, seqs = lines * fast, seq_lines * 2
    gact, x_in, act, tok, w_x, w_g, w_h, gs_gate = big
    mix, w_xt, head, kern, b_conv, dtp, a_grad, dtb, sgrad, g_half, own_tok, own_cot = small[:12]
    length, feats = act.shape
    own_len, model = own_tok.shape
    width = a_grad.shape[0]
    rows = dtp.shape[0] + mix.shape[0] + width + 16
    block_rows = model // segs
    own_rows = g_half.shape[0] // seqs
    ends = (seqs, 2 * (width + history) + (-2 * (width + history)) % 8, feats // seqs)
    dma = pltpu.SemaphoreType.DMA
    scratch = [
        pltpu.VMEM((length + 8, feats), F32),
        pltpu.VMEM((length + 8, feats), F32),
        pltpu.VMEM((length, feats), BF16),
        pltpu.VMEM((length, model), BF16),
        pltpu.VMEM((model, feats), BF16),
        pltpu.VMEM((2, model, feats // 2), BF16),
        pltpu.VMEM((length, feats), BF16),
        pltpu.VMEM((length, feats), BF16),
        pltpu.VMEM((segs, block_rows, feats), BF16),
        pltpu.VMEM((seqs, own_len, model), BF16),
        pltpu.VMEM((8 * (taps + 1), feats), F32),
        pltpu.VMEM((segs, rows, feats // segs), BF16),
        pltpu.VMEM(ends, F32),
        pltpu.VMEM((block_rows, feats), BF16),
        dma((8,)), dma((3,)),
        *Scatter.scratch(lines, fast, (rows, feats // segs), inside=True),
        *Scatter.scratch(lines, fast, (block_rows, feats), inside=True),
        *Scatter.scratch(seq_lines, 2, (own_len, model), inside=True),
        *Exchange.semaphores(seqs), *Exchange.semaphores(seqs), *Exchange.semaphores(seqs),
    ]

    def kernel(*refs):
        finish_kernel(shape, taps, history, refs[:26], refs[26:])

    return pl.pallas_call(
        kernel,
        in_specs=[ANY] * 8 + [INSIDE] * 14,
        out_specs=[INSIDE] * 4,
        out_shape=[
            jax.ShapeDtypeStruct((rows, feats // segs), F32),
            jax.ShapeDtypeStruct((2, seqs, own_rows, feats), BF16),
            jax.ShapeDtypeStruct((own_len, model), BF16),
            jax.ShapeDtypeStruct(ends, F32),
        ],
        scratch_shapes=scratch,
        compiler_params=comm_params(4),
        name="finish",
    )(*big, *small)


def gather_kernel(
    shape, scaled_x, scaled_g, small, tokens, w_x, small_all, tok, g_part, x_part, tok_in, g_own,
    local_s, small_sems, tok_sems, swap_x, swap_g, x_sems,
):
    seg, seq = grids(shape)
    size = seq.lines * seq.fast
    load_tok = pltpu.make_async_copy(tokens, tok_in, local_s.at[0])
    load_own = pltpu.make_async_copy(scaled_x.at[seq.here], x_part.at[seq.here], local_s.at[1])
    load_gate = pltpu.make_async_copy(scaled_g.at[seq.here], g_own, local_s.at[3])
    load_tok.start()
    load_own.start()
    load_gate.start()
    meet((seg, seq))
    swap_x = Exchange(seq, lambda p: scaled_x.at[p], lambda m: x_part.at[m], swap_x)
    swap_g = Exchange(seq, lambda p: scaled_g.at[p], lambda m: g_part.at[m], swap_g)
    swap_x.begin()
    pieces = []
    for k in range(size):
        place = lax.rem(seq.here - k + size, size)
        pieces.append(Gather(seg, x_part.at[place], w_x, x_sems[6 * k : 6 * k + 6], place))
    smalls = Gather(seg, small, small_all, small_sems)
    load_own.wait()
    pieces[0].begin()
    smalls.begin()
    load_tok.wait()
    toks = Gather(seq, tok_in, tok, tok_sems)
    for k in range(1, size):
        swap_x.one(k).wait_recv()
        pieces[k].begin()
    toks.begin()
    swap_g.begin()
    load_gate.wait()
    keeps = [
        pltpu.make_async_copy(tok_in, tok.at[seq.here], local_s.at[0]),
        pltpu.make_async_copy(x_part, w_x.at[seg.here], local_s.at[1]),
        pltpu.make_async_copy(small, small_all.at[seg.here], local_s.at[2]),
        pltpu.make_async_copy(g_own, g_part.at[seq.here], local_s.at[3]),
    ]
    for keep in keeps:
        keep.start()
    for k in range(1, max(seg.lines, seq.lines)):
        if k < seg.lines:
            pieces[0].step(k)
            smalls.step(k)
            for piece in pieces[1:]:
                piece.step(k)
        if k < seq.lines:
            toks.step(k)
    toks.finish()
    smalls.finish()
    for piece in pieces:
        piece.finish()
    swap_g.arrived()
    swap_x.drain()
    swap_g.drain()
    for keep in keeps:
        keep.wait()


def gather_start(shape, scaled_x, scaled_g, small, tokens):
    lines, fast, seq_lines = shape
    segs, seqs = lines * fast, seq_lines * 2
    rows, feats = scaled_x.shape[1:]
    sems = Gather.semaphores

    def kernel(*refs):
        ins, rest = refs[:11], refs[11:]
        gather_kernel(
            shape, *ins, rest[0], rest[1:7], rest[7:13], rest[13:15], rest[15:17], rest[17:]
        )

    w_x, small_all, tok, g_part = pl.pallas_call(
        kernel,
        in_specs=[ANY, ANY, INSIDE, ANY],
        out_specs=[ANY] * 4,
        out_shape=[
            jax.ShapeDtypeStruct((segs, seqs, rows, feats), BF16),
            jax.ShapeDtypeStruct((segs,) + small.shape, BF16),
            jax.ShapeDtypeStruct((seqs,) + tokens.shape, BF16),
            jax.ShapeDtypeStruct((seqs,) + scaled_g.shape[1:], BF16),
        ],
        scratch_shapes=[
            pltpu.VMEM((seqs, rows, feats), BF16),
            pltpu.VMEM(tokens.shape, BF16),
            pltpu.VMEM(scaled_g.shape[1:], BF16),
            pltpu.SemaphoreType.DMA((4,)),
            *sems(lines, fast), *sems(seq_lines, 2),
            *Exchange.semaphores(seqs), *Exchange.semaphores(seqs),
            *(sems(lines, fast) * seqs),
        ],
        compiler_params=comm_params(1),
        name="gather_start",
    )(scaled_x, scaled_g, small, tokens)
    return w_x.reshape(-1, feats), small_all, tok.reshape(-1, tokens.shape[1]), g_part


def front_kernel(
    shape, steps, taps, history, width,
    tok_ref, wx_ref, small_ref, head_ref, gate_src,
    x_ref, act_ref, rstd_ref, wdt_ref, wxt_ref, par_ref, a2_ref, low_ref, bc_ref, gate_out,
    xb, mix_s, mix, local_s, *scratch,
):
    seg, seq = grids(shape)
    step = pl.program_id(0)
    gates = Gather(seg, gate_src.at[:, 0], gate_out, scratch[:6])
    count = tok_ref.shape[0]
    low_rank = wdt_ref.shape[0]
    mixes = wxt_ref.shape[0]
    feats = wx_ref.shape[1]
    part = small_ref.shape[2]

    @pl.when(step == 0)
    def _():
        meet((seg, seq))
        gates.begin()
        xb[pl.ds(0, 8), :] = head_ref[...]
        for g in range(small_ref.shape[0]):
            cols = slice(g * part, (g + 1) * part)
            wdt_ref[:, cols] = small_ref[g, pl.ds(0, low_rank), :]
            wxt_ref[:, cols] = small_ref[g, pl.ds(low_rank, mixes), :]
            rest = small_ref[g, pl.ds(low_rank + mixes, width + 16), :].astype(F32)
            par_ref[:, cols] = rest
        a_mat = -jnp.exp(par_ref[pl.ds(0, width), :])
        par_ref[pl.ds(0, width), :] = a_mat
        for s in range(feats // LANES):
            a2_ref[:, s, :] = a_mat[:, s * LANES : (s + 1) * LANES] * LOG2E

    kern = par_ref[pl.ds(width, 8), :]
    rows = tok_ref[...].astype(F32)
    rstd = lax.rsqrt(jnp.mean(rows * rows, axis=1, keepdims=True) + EPSILON)
    rstd_ref[...] = jnp.broadcast_to(rstd, rstd_ref.shape)
    x_in = rstd * dot_nn(tok_ref[...], wx_ref[...])
    x_ref[...] = x_in
    xb[pl.ds(8, count), :] = x_in
    tall = 32
    chunk = min(512, feats)

    def through_conv(i, carry):
        t0 = pl.multiple_of(i * tall, tall)
        for c in range(0, feats, chunk):
            cols = slice(c, c + chunk)
            wide = xb[pl.ds(t0, tall + 8), pl.ds(c, chunk)]
            conv = kern[taps : taps + 1, cols]
            for k in range(taps):
                conv = conv + kern[k : k + 1, cols] * wide[8 - history + k : 8 - history + k + tall]
            act_ref[pl.ds(t0, tall), pl.ds(c, chunk)] = (conv * sigmoid(conv)).astype(BF16)
        return carry

    lax.fori_loop(0, count // tall, through_conv, 0)
    xb[pl.ds(0, 8), :] = xb[pl.ds(count, 8), :]
    mix_s[:, pl.ds(pl.multiple_of(step * count, count), count)] = dot_nt(wxt_ref[...], act_ref[...])
    for k in range(1, seg.lines - 1):

        @pl.when(step == min(steps - 1, 2 * k - 1))
        def _():
            gates.step(k)

    @pl.when(step == steps - 1)
    def _():
        sum_over_seq(seq, mix_s, mix, *scratch[6:])
        low_ref[...] = mix[pl.ds(0, low_rank), :]
        bc_ref[...] = mix[pl.ds(low_rank, 2 * width), :].astype(F32).T
        gates.step(seg.lines - 1)
        keep = pltpu.make_async_copy(gate_src.at[:, 0], gate_out.at[seg.here], local_s)
        keep.start()
        gates.finish()
        keep.wait()


def front(shape, taps, history, width, tok, w_x, small_all, head, gate_part, block):
    lines, fast, seq_lines = shape
    segs, seqs = lines * fast, seq_lines * 2
    length, model = tok.shape
    feats = w_x.shape[1]
    low_rank = LANES
    mixes = low_rank + 2 * width
    steps = length // block

    def whole(*dims):
        return pl.BlockSpec(dims, lambda i: (0,) * len(dims))

    def rows(columns):
        return pl.BlockSpec((block, columns), lambda i: (i, 0))

    one = pl.Buffered(1)
    return pl.pallas_call(
        functools.partial(front_kernel, shape, steps, taps, history, width),
        grid=(steps,),
        in_specs=[
            rows(model),
            pl.BlockSpec((model, feats), lambda i: (0, 0), pipeline_mode=one),
            whole(*small_all.shape), whole(*head.shape), ANY,
        ],
        out_specs=[
            rows(feats), rows(feats), rows(LANES), whole(low_rank, feats), whole(mixes, feats),
            whole(width + 16, feats), whole(width, feats // LANES, LANES),
            whole(low_rank, length), whole(length, 2 * width), ANY,
        ],
        out_shape=[
            jax.ShapeDtypeStruct((length, feats), F32),
            jax.ShapeDtypeStruct((length, feats), BF16),
            jax.ShapeDtypeStruct((length, LANES), F32),
            jax.ShapeDtypeStruct((low_rank, feats), BF16),
            jax.ShapeDtypeStruct((mixes, feats), BF16),
            jax.ShapeDtypeStruct((width + 16, feats), F32),
            jax.ShapeDtypeStruct((width, feats // LANES, LANES), F32),
            jax.ShapeDtypeStruct((low_rank, length), BF16),
            jax.ShapeDtypeStruct((length, 2 * width), F32),
            jax.ShapeDtypeStruct((segs, seqs) + gate_part.shape[2:], BF16),
        ],
        scratch_shapes=[
            pltpu.VMEM((block + 8, feats), F32),
            pltpu.VMEM((mixes, length), F32),
            pltpu.VMEM((mixes, length), BF16),
            pltpu.SemaphoreType.DMA,
            *Gather.semaphores(lines, fast),
            *sum_scratch(seq_lines, mixes, length),
        ],
        compiler_params=comm_params(2),
        name="front",
    )(tok, w_x, small_all, head, gate_part)


def sum_scratch(seq_lines, rows, width):
    part = pltpu.VMEM((rows, width // 2), BF16)
    dma = pltpu.SemaphoreType.DMA
    return [
        part, part, part,
        pltpu.VMEM((max(seq_lines - 1, 1), rows, width // 2), BF16),
        pltpu.VMEM((2, rows, width // 2), BF16),
        dma, dma, dma((seq_lines,)), dma((seq_lines,)), dma, dma,
    ]


def unpack_kernel(
    seqs, taps, history, low_rank, width,
    small, halves, ends, mixed, input_grad, out_grad, weight, gain,
    mixed_o, final_o, final_c, input_o, start_o, start_c, gain_o, in_o, cw_o, cb_o, xp_o, dtp_o,
    dtb_o, a_o, skip_o, out_o,
):
    mixed_o[0] = mixed[...]
    input_o[0] = input_grad[...]
    out_o[...] = out_grad[...]
    part = small.shape[1]
    columns = xp_o.shape[1]
    dtp_o[...] = small[pl.ds(0, low_rank), :]
    turned = small[pl.ds(low_rank, low_rank), :].T
    xp_o[:, pl.ds(0, low_rank)] = turned
    xp_o[:, pl.ds(low_rank, columns - low_rank)] = small[
        pl.ds(2 * low_rank, columns - low_rank), :
    ].T
    at = low_rank + columns
    a_o[...] = small[pl.ds(at, width), :]
    lines = small[pl.ds(at + width, 16), :]
    cw_o[...] = lines[:taps]
    cb_o[...] = lines[taps]
    dtb_o[...] = lines[taps + 1]
    skip_o[...] = lines[taps + 2]
    each = final_o.shape[2] // part // seqs
    for s in range(seqs):
        rows = ends[s]
        for g in range(each):
            got = rows[:, g * part : (g + 1) * part]
            cols = pl.ds((g * seqs + s) * part, part)
            final_o[0, :, cols] = got[:width]
            final_c[0, :, cols] = got[width : width + history]
            start_o[0, :, cols] = got[width + history : 2 * width + history]
            start_c[0, :, cols] = got[2 * width + history : 2 * (width + history)]
    scale = gain[...]
    total = jnp.zeros((in_o.shape[0], part), F32)
    groups = halves.shape[3] // part
    for half in range(2):
        for s in range(seqs):
            for g in range(groups):
                raw = halves[half, s, :, g * part : (g + 1) * part].astype(F32)
                cols = pl.ds(((half * groups + g) * seqs + s) * part, part)
                in_o[:, cols] = raw * scale
                total = total + raw * weight[:, cols].astype(F32)
    gain_o[...] = jnp.sum(total.T, axis=0)


def unpack(taps, history, low_rank, width, small, halves, ends, mixed, input_grad, out_grad,
           weight, gain):
    seqs, own_rows, feats = halves.shape[1:]
    part = small.shape[1]
    model = mixed.shape[1]
    kept = ends.shape[2] * seqs
    f32 = lambda *dims: jax.ShapeDtypeStruct(dims, F32)
    args = (small, halves, ends, mixed, input_grad, out_grad, weight, gain)
    outs = [
        jax.ShapeDtypeStruct((1,) + mixed.shape, BF16),
        f32(1, width, kept), f32(1, history, kept),
        jax.ShapeDtypeStruct((1,) + input_grad.shape, BF16),
        f32(1, width, kept), f32(1, history, kept),
        f32(own_rows), f32(*weight.shape),
        f32(taps, part), f32(part), f32(part, low_rank + 2 * width), f32(low_rank, part),
        f32(part), f32(width, part), f32(part), f32(part, model),
    ]

    def whole(a):
        return pl.BlockSpec(
            a.shape, lambda i: (0,) * len(a.shape), pipeline_mode=pl.Buffered(1)
        )

    return pl.pallas_call(
        functools.partial(unpack_kernel, seqs, taps, history, low_rank, width),
        grid=(1,),
        in_specs=[whole(a) for a in args],
        out_specs=[whole(a) for a in outs],
        out_shape=outs,
        name="unpack",
    )(*args)


def body(
    tokens, norm_gain, in_proj, conv_weight, conv_bias, x_proj, dt_proj, dt_bias,
    a_log, d_skip, out_proj, init_state, init_conv, cotangent,
):
    segs, seqs = lax.axis_size("seg"), lax.axis_size("seq")
    place = lax.axis_index("seq")
    own_rows, both = in_proj.shape
    part = conv_bias.shape[0]
    feats = segs * part
    taps = conv_weight.shape[0]
    width = a_log.shape[0]
    low_rank = dt_proj.shape[0]
    planes = feats // LANES
    own_len, model = tokens.shape[1:]
    length = own_len * seqs
    block = 64
    seq_lines = seqs // 2
    shape = (segs // seq_lines, seq_lines, seq_lines)

    def mine(rows):
        shaped = rows.reshape(rows.shape[0], segs, seqs, part)
        return lax.dynamic_index_in_dim(shaped, place, 2, keepdims=False).reshape(
            rows.shape[0], feats
        )

    gain_col = norm_gain.astype(F32)[:, None]
    own_weight = in_proj.astype(F32)
    scaled = (own_weight * gain_col).astype(BF16)
    scaled = scaled.reshape(own_rows, 2, segs, seqs, part)
    scaled_x = scaled[:, 0].transpose(2, 0, 1, 3).reshape(seqs, own_rows, feats)
    scaled_g = scaled[:, 1].reshape(own_rows, 2, segs // 2, seqs, part).transpose(3, 1, 0, 2, 4)
    scaled_g = scaled_g.reshape(seqs, 2, own_rows, feats // 2)
    small = jnp.concatenate(
        [
            dt_proj, x_proj.T, a_log, conv_weight, conv_bias[None], dt_bias[None], d_skip[None],
        ],
        axis=0,
    )
    small = jnp.pad(small, ((0, -small.shape[0] % 16), (0, 0)))
    w_x_half, small_all, tok, g_part = gather_start(shape, scaled_x, scaled_g, small, tokens[0])
    history = init_conv.shape[1]
    head = jnp.pad(mine(init_conv[0]), ((8 - history, 0), (0, 0)))
    x_in, act, rstd, w_dt, w_xt, params, a2, dt_low, bc, w_g_one = front(
        shape, taps, history, width, tok, w_x_half, small_all, head, g_part, 4 * block
    )
    rstd = rstd[:, :1]
    init = mine(init_state[0]).reshape(width, planes, LANES)
    a_mat = params[:width]
    kernel = params[width : width + 8]
    b_conv, b_dt, skip = (params[width + taps + i][None] for i in range(3))
    y_val, pre, checks, final, gate, gated, w_out, cot, w_g_two = forward_scan(
        shape, dt_low, w_dt, b_dt, act, bc, a2, skip, init, out_proj, cotangent[0], tok,
        w_g_one, g_part, 2 * block,
    )
    w_out = w_out.reshape(feats, model)
    cot = cot.reshape(length, model)
    w_g_one = w_g_one.reshape(model, feats // 2)
    w_g_two = w_g_two.reshape(model, feats // 2)
    g_gated = dot_nt(cot, w_out)
    sig_gate = jax.nn.sigmoid(gate)
    gy = g_gated * gate * sig_gate
    gs_gate = (
        rstd * g_gated * y_val * sig_gate * (1.0 + gate * (1.0 - sig_gate))
    ).astype(BF16)
    out_grad = dot_tn(gated, cot).astype(BF16)
    gate_grad = dot_tn(tok, gs_gate).astype(BF16)
    g_actp, a_sum, start, dtb_grad, skip_grad, dtp_grad, g_mixed, g_half, out_grad, mixed_out = (
        backward_scan(
            shape, pre, act, gy, bc, a2, skip, checks, w_dt, dt_low, tokens[0],
            gate_grad.reshape(segs, seqs * own_rows, feats),
            out_grad.reshape(segs, part, model),
            gated, w_out, 2 * block,
        )
    )
    grads, halves, input_grad, ends = finish_all(
        shape, taps, history,
        (g_actp, x_in, act, tok, w_x_half, w_g_one, w_g_two, gs_gate),
        (
            g_mixed, w_xt, head, kernel, b_conv, dtp_grad, a_sum.reshape(width, feats) * a_mat, dtb_grad, skip_grad, g_half,
            tokens[0], cotangent[0],
            final.reshape(width, feats), start.reshape(width, feats),
        ),
    )
    if part % LANES == 0:
        return unpack(
            taps, history, low_rank, width, grads, halves, ends, mixed_out, input_grad, out_grad,
            in_proj, gain_col,
        )
    ends = (
        ends.reshape(seqs, ends.shape[1], segs // seqs, part)
        .transpose(1, 2, 0, 3)
        .reshape(ends.shape[1], feats)
    )
    raw_grad = (
        halves.reshape(2, seqs, own_rows, segs, part)
        .transpose(2, 0, 3, 1, 4)
        .reshape(own_rows, both)
        .astype(F32)
    )
    in_grad = raw_grad * gain_col
    gain_grad = jnp.sum(raw_grad * own_weight, axis=1)

    at = width + history
    xp_at = low_rank + x_proj.shape[1]
    return (
        mixed_out[None],
        ends[None, :width],
        ends[None, width:at],
        input_grad[None],
        ends[None, at : at + width],
        ends[None, at + width : at + width + history],
        gain_grad,
        in_grad,
        grads[xp_at + width : xp_at + width + taps],
        grads[xp_at + width + taps],
        grads[low_rank:xp_at].T,
        grads[:low_rank],
        grads[xp_at + width + taps + 1],
        grads[xp_at : xp_at + width],
        grads[xp_at + width + taps + 2],
        out_grad,
    )


def solution(mesh):
    spread = ("seg", "seq")
    placed = (
        P("seg", "seq", None),
        P(spread),
        P(spread, None),
        P(None, spread),
        P(spread),
        P(spread, None),
        P(None, spread),
        P(spread),
        P(None, spread),
        P(spread),
        P(spread, None),
        P("seg", None, None),
        P("seg", None, None),
        P("seg", "seq", None),
    )
    return jax.shard_map(
        body,
        mesh=mesh,
        in_specs=placed,
        out_specs=(
            P("seg", "seq", None),
            P("seg", None, "seq"),
            P("seg", None, "seq"),
            P("seg", "seq", None),
            P("seg", None, "seq"),
            P("seg", None, "seq"),
            P(spread),
            P(spread, None),
            P(None, spread),
            P(spread),
            P(spread, None),
            P(None, spread),
            P(spread),
            P(None, spread),
            P(spread),
            P(spread, None),
        ),
        check_vma=False,
    )
```

```python
import functools

import jax
import jax.numpy as jnp
from jax import lax
from jax.experimental import pallas as pl
from jax.experimental.pallas import tpu as pltpu
from jax.sharding import PartitionSpec as P

EPSILON = 1e-05
LOG2E = 1.4426950408889634
LANES = 128
UNROLL = 8
F32 = jnp.float32
BF16 = jnp.bfloat16


def dot_nn(a, b):
    return jnp.dot(a, b, preferred_element_type=F32)


def dot_tn(a, b):
    return lax.dot_general(a, b, (((0,), (0,)), ((), ())), preferred_element_type=F32)


def dot_nt(a, b):
    return lax.dot_general(a, b, (((1,), (1,)), ((), ())), preferred_element_type=F32)


def sigmoid(v):
    return 1.0 / (1.0 + jnp.exp(-v))


def softplus(v):
    return jnp.maximum(v, 0.0) + jnp.log1p(jnp.exp(-jnp.abs(v)))


def to_planes(planes_ref, rows):
    groups = planes_ref.shape[0]
    for s in range(rows.shape[1] // LANES):
        tile = rows[:, s * LANES : (s + 1) * LANES].reshape(groups, UNROLL, LANES)
        planes_ref[:, pl.ds(s * UNROLL, UNROLL), :] = tile


def from_planes(planes_ref):
    groups, rows, _ = planes_ref.shape
    return jnp.concatenate(
        [
            planes_ref[:, pl.ds(s * UNROLL, UNROLL), :].reshape(groups * UNROLL, LANES)
            for s in range(rows // UNROLL)
        ],
        axis=1,
    )


def token_of(planes, i):
    return pl.ds(i, planes, stride=UNROLL)


MESH_ID = pl.DeviceIdType.MESH
VMEM_MOST = 67_043_328


class Grid:
    def __init__(self, axis, lines, fast):
        self.axis, self.lines, self.fast = axis, lines, fast
        self.here = lax.axis_index(axis)
        self.line = self.here // fast
        self.lane = self.here - self.line * fast

    def at(self, line, lane):
        return line * self.fast + lane

    def line_peer(self, k):
        return lax.rem(self.line + k, self.lines)

    def lane_peer(self, e):
        return lax.rem(self.lane + e, self.fast)

    def copy(self, src, dst, sent, got, index):
        return pltpu.make_async_remote_copy(
            src_ref=src, dst_ref=dst, send_sem=sent, recv_sem=got,
            device_id={self.axis: index}, device_id_type=MESH_ID,
        )


def meet(groups):
    barrier = pltpu.get_barrier_semaphore()
    total = 0
    for grid in groups:
        size = grid.lines * grid.fast
        for k in range(1, size):
            pl.semaphore_signal(
                barrier, inc=1, device_id={grid.axis: lax.rem(grid.here + k, size)},
                device_id_type=MESH_ID,
            )
        total += size - 1
    pl.semaphore_wait(barrier, total)


class Gather:
    def __init__(self, grid, own, out, sems, piece=None):
        self.grid, self.own, self.out, self.piece = grid, own, out, piece
        self.up_s, self.up_r, self.dn_s, self.dn_r, self.x_s, self.x_r = sems

    @staticmethod
    def semaphores(lines, fast):
        hops = pltpu.SemaphoreType.DMA((lines,))
        across = pltpu.SemaphoreType.DMA((lines, fast))
        return [hops, hops, hops, hops, across, across]

    def block(self, line, lane=None):
        grid = self.grid
        index = grid.at(line, grid.lane if lane is None else lane)
        return self.out.at[index] if self.piece is None else self.out.at[index, self.piece]

    def up(self, k):
        grid = self.grid
        block = self.block(jnp.maximum(grid.line - k, 0))
        return grid.copy(
            self.own if k == 0 else block, block, self.up_s.at[k], self.up_r.at[k],
            grid.at(jnp.minimum(grid.line + 1, grid.lines - 1), grid.lane),
        )

    def down(self, k):
        grid = self.grid
        block = self.block(jnp.minimum(grid.line + k, grid.lines - 1))
        return grid.copy(
            self.own if k == 0 else block, block, self.dn_s.at[k], self.dn_r.at[k],
            grid.at(jnp.maximum(grid.line - 1, 0), grid.lane),
        )

    def sends_up(self, k):
        return jnp.logical_and(self.grid.line + 1 < self.grid.lines, self.grid.line >= k)

    def sends_down(self, k):
        return jnp.logical_and(self.grid.line > 0, self.grid.line + k < self.grid.lines)

    def across(self, line, slot, e, own=False):
        grid = self.grid
        block = self.block(line)
        return grid.copy(
            self.own if own else block, block, self.x_s.at[slot, e], self.x_r.at[slot, e],
            grid.at(grid.line, grid.lane_peer(e)),
        )

    def slots(self):
        return range(self.grid.lines)

    def begin(self):
        grid = self.grid
        for when, copy in ((self.sends_up(0), self.up(0)), (self.sends_down(0), self.down(0))):
            pl.when(when)(copy.start)
        for e in range(1, grid.fast):
            self.across(grid.line, 0, e, own=True).start()

    def step(self, k):
        grid = self.grid

        def arrived(copy, line, slot, forward, onward):
            copy.wait_recv()
            if k < grid.lines - 1:
                pl.when(forward(k))(onward(k).start)
            for e in range(1, grid.fast):
                self.across(line, slot, e).start()

        below, above = grid.line - k, grid.line + k

        @pl.when(below >= 0)
        def _():
            arrived(self.up(k - 1), below, grid.lines - k, self.sends_up, self.up)

        @pl.when(above < grid.lines)
        def _():
            arrived(self.down(k - 1), above, k, self.sends_down, self.down)

    def finish(self):
        grid = self.grid
        for k in range(grid.lines - 1):
            pl.when(self.sends_up(k))(self.up(k).wait_send)
            pl.when(self.sends_down(k))(self.down(k).wait_send)
        for slot in self.slots():
            for e in range(1, grid.fast):
                copy = self.across(grid.line_peer(slot), slot, e, own=slot == 0)
                copy.wait_send()
                copy.wait_recv()


class Scatter:
    def __init__(self, grid, src, scratch, inside=False):
        self.grid, self.src, self.inside = grid, src, inside
        if not inside:
            self.own, self.o_s = scratch[:2]
            scratch = scratch[2:]
        self.xbuf, self.stage, self.zbuf, self.acc = scratch[:4]
        self.x_s, self.x_r, self.z_s, self.z_r = scratch[4:]
        self.last = grid.lines - 1

    @staticmethod
    def scratch(lines, fast, shape, inside=False):
        dma = pltpu.SemaphoreType.DMA
        shape = tuple(shape)
        loads = [] if inside else [pltpu.VMEM((lines,) + shape, BF16), dma((lines,))]
        return loads + [
            pltpu.VMEM((lines, fast - 1) + shape, BF16),
            pltpu.VMEM((lines - 1,) + shape, BF16),
            pltpu.VMEM((lines + 1,) + shape, BF16),
            pltpu.VMEM(shape, F32),
            dma((lines, fast)), dma((lines, fast)), dma((lines,)), dma((lines + 1,)),
        ]

    def dest(self, j):
        line, last = self.grid.line, self.last
        above, below = last - line, line
        low = jnp.where(j < above, last - j, j - above)
        high = jnp.where(j < below, j, last - (j - below))
        other = jnp.where(2 * line <= last, low, high)
        return jnp.where(j == last, line, other)

    def index(self, j, e):
        return self.grid.at(self.dest(j), self.grid.lane_peer(e))

    def across(self, j, e):
        grid = self.grid
        return grid.copy(
            self.src.at[self.index(j, e)], self.xbuf.at[j, e - 1],
            self.x_s.at[j, e], self.x_r.at[j, e], grid.at(grid.line, grid.lane_peer(e)),
        )

    def local(self, j):
        return pltpu.make_async_copy(
            self.src.at[self.index(j, 0)], self.own.at[j], self.o_s.at[j]
        )

    def along(self, j):
        grid = self.grid
        dest = self.dest(j)
        up = dest > grid.line
        to = jnp.clip(jnp.where(up, grid.line + 1, grid.line - 1), 0, self.last)
        slot = jnp.where(jnp.logical_and(jnp.logical_not(up), dest == to), grid.lines, dest)
        return grid.copy(
            self.stage.at[j], self.zbuf.at[slot], self.z_s.at[j], self.z_r.at[slot],
            grid.at(to, grid.lane),
        )

    def arrival(self, slot):
        grid = self.grid
        return grid.copy(
            self.stage.at[0], self.zbuf.at[slot], self.z_s.at[0], self.z_r.at[slot],
            grid.at(lax.rem(grid.line + 1, grid.lines), grid.lane),
        )

    def order(self):
        return list(range(self.grid.lines))

    def begin(self):
        for j in self.order():
            for e in range(1, self.grid.fast):
                self.across(j, e).start()
            if not self.inside:
                self.local(j).start()

    def rows(self, step):
        count = self.acc.shape[0]
        size = 16 if count % 16 == 0 else 8

        def run(i, carry):
            step(pl.ds(pl.multiple_of(i * size, size), size))
            return carry

        lax.fori_loop(0, count // size, run, 0)

    def middle(self, j):
        grid = self.grid
        for e in range(1, grid.fast):
            self.across(j, e).wait_recv()
        if self.inside:
            own = self.src.at[self.index(j, 0)]
        else:
            self.local(j).wait()
            own = self.own.at[j]

        def partial(at):
            total = own[at, :].astype(F32)
            for e in range(grid.fast - 1):
                total = total + self.xbuf[j, e, at, :].astype(F32)
            return total

        if j == self.last:

            def keep(at):
                self.acc[at, :] = partial(at)

            self.rows(keep)
            return
        dest = self.dest(j)
        carried = jnp.where(dest > grid.line, grid.line > 0, grid.line < self.last)

        @pl.when(carried)
        def _():
            self.arrival(dest).wait_recv()

            def add(at):
                total = partial(at) + self.zbuf[dest, at, :].astype(F32)
                self.stage[j, at, :] = total.astype(BF16)

            self.rows(add)

        @pl.when(jnp.logical_not(carried))
        def _():
            def add(at):
                self.stage[j, at, :] = partial(at).astype(BF16)

            self.rows(add)

        self.along(j).start()

    def finish(self, write):
        line, last = self.grid.line, self.last
        from_below, from_above = line > 0, line < last

        @pl.when(from_below)
        def _():
            self.arrival(line).wait_recv()

        @pl.when(from_above)
        def _():
            self.arrival(self.grid.lines).wait_recv()

        def total(at, below, above):
            result = self.acc[at, :]
            if below:
                result = result + self.zbuf[line, at, :].astype(F32)
            if above:
                result = result + self.zbuf[last + 1, at, :].astype(F32)
            write(at, result)

        for when, below, above in (
            (jnp.logical_and(from_below, from_above), True, True),
            (jnp.logical_not(from_below), False, True),
            (jnp.logical_not(from_above), True, False),
        ):

            @pl.when(when)
            def _():
                self.rows(lambda at: total(at, below, above))

    def drain(self):
        for j in self.order():
            for e in range(1, self.grid.fast):
                self.across(j, e).wait_send()
            if j < self.last:
                self.along(j).wait_send()


def into(ref):
    def write(at, total):
        ref[at, :] = total.astype(ref.dtype)

    return write


class Exchange:
    def __init__(self, grid, src, dst, sems):
        self.grid, self.src, self.dst = grid, src, dst
        self.sent, self.got = sems
        self.size = grid.lines * grid.fast

    @staticmethod
    def semaphores(size):
        return [pltpu.SemaphoreType.DMA((size,)), pltpu.SemaphoreType.DMA((size,))]

    def one(self, k):
        grid = self.grid
        peer = lax.rem(grid.here + k, self.size)
        return grid.copy(
            self.src(peer), self.dst(grid.here), self.sent.at[k], self.got.at[k], peer
        )

    def begin(self):
        for k in range(1, self.size):
            self.one(k).start()

    def arrived(self):
        for k in range(1, self.size):
            self.one(k).wait_recv()

    def drain(self):
        for k in range(1, self.size):
            self.one(k).wait_send()


ANY = pl.BlockSpec(memory_space=pl.ANY)
INSIDE = pl.BlockSpec(memory_space=pltpu.VMEM)


def comm_params(collective_id):
    return pltpu.CompilerParams(
        collective_id=collective_id, has_side_effects=True, vmem_limit_bytes=VMEM_MOST
    )


def grids(shape):
    lines, fast, seq_lines = shape
    return Grid("seg", lines, fast), Grid("seq", seq_lines, 2)


def sum_over_seq(seq, x_ref, out_ref, half, got, mine, others, whole, *sems):
    lane_s, lane_r, line_s, line_r, back_s, back_r = sems
    width = x_ref.shape[1] // 2
    lines = seq.lines
    other = 1 - seq.lane
    left = pl.ds(0, width)
    right = pl.ds(width, width)

    @pl.when(seq.lane == 0)
    def _():
        half[...] = x_ref[:, right].astype(BF16)

    @pl.when(seq.lane == 1)
    def _():
        half[...] = x_ref[:, left].astype(BF16)

    swap = seq.copy(half, got, lane_s, lane_r, seq.at(seq.line, other))
    swap.start()
    swap.wait()

    @pl.when(seq.lane == 0)
    def _():
        mine[...] = (x_ref[:, left] + got[...].astype(F32)).astype(BF16)

    @pl.when(seq.lane == 1)
    def _():
        mine[...] = (x_ref[:, right] + got[...].astype(F32)).astype(BF16)

    copies = [
        seq.copy(
            mine, others.at[k - 1], line_s.at[k], line_r.at[k], seq.at(seq.line_peer(k), seq.lane)
        )
        for k in range(1, lines)
    ]
    for copy in copies:
        copy.start()
    for copy in copies:
        copy.wait()
    total = mine[...].astype(F32)
    for k in range(lines - 1):
        total = total + others[k].astype(F32)
    whole[seq.lane] = total.astype(BF16)
    back = seq.copy(
        whole.at[seq.lane], whole.at[seq.lane], back_s, back_r, seq.at(seq.line, other)
    )
    back.start()
    back.wait()
    out_ref[:, left] = whole[0]
    out_ref[:, right] = whole[1]


def forward_kernel(
    shape, steps, taps,
    low_ref, wdt_ref, params_ref, act_ref, bc_ref, a_ref, init_ref, weight_ref, cot_ref,
    tok_ref, gate_one, gate_src,
    y_ref, pre_ref, check_ref, final_ref, gate_ref, gated_ref, weights_ref, cots_ref, gate_two,
    state, rate_pl, drive_pl, y_pl, w_one, w_two, local_s, *sems,
):
    count = pre_ref.shape[0]
    width, planes, _ = a_ref.shape
    seg, seq = grids(shape)
    gates = Gather(seg, gate_src.at[:, 1], gate_two, sems[:6])
    weights = Gather(seg, weight_ref, weights_ref, sems[6:12])
    cots = Gather(seq, cot_ref, cots_ref, sems[12:])
    step = pl.program_id(0)
    keeps = [
        pltpu.make_async_copy(weight_ref, weights_ref.at[seg.here], local_s.at[0]),
        pltpu.make_async_copy(cot_ref, cots_ref.at[seq.here], local_s.at[1]),
        pltpu.make_async_copy(gate_src.at[:, 1], gate_two.at[seg.here], local_s.at[2]),
    ]
    load_one = pltpu.make_async_copy(gate_one, w_one, local_s.at[3])

    @pl.when(step == 0)
    def _():
        meet((seg, seq))
        gates.begin()
        weights.begin()
        cots.begin()
        for keep in keeps:
            keep.start()
        load_one.start()
        state[...] = init_ref[...]

    lines = params_ref[pl.ds(width, 8), :]
    bias, skip = lines[taps + 1 : taps + 2], lines[taps + 2 : taps + 3]
    pre = dot_tn(low_ref[...], wdt_ref[...]) + bias
    pre_ref[...] = pre
    rate = softplus(pre)
    act = act_ref[...].astype(F32)
    to_planes(rate_pl, rate)
    to_planes(drive_pl, rate * act)
    groups = count // UNROLL

    def group(k, carry):
        at = k * UNROLL
        rates = [rate_pl[k, token_of(planes, i), :] for i in range(UNROLL)]
        drives = [drive_pl[k, token_of(planes, i), :] for i in range(UNROLL)]
        sums = [None] * UNROLL
        for n in range(width):
            a = a_ref[n]
            h = state[n]
            check_ref[k, n] = h
            for i in range(UNROLL):
                h = jnp.exp2(rates[i] * a) * h + bc_ref[at + i, n] * drives[i]
                term = bc_ref[at + i, width + n] * h
                sums[i] = term if n == 0 else sums[i] + term
            state[n] = h
        for i in range(UNROLL):
            y_pl[k, token_of(planes, i), :] = sums[i]
        return carry

    ticks = 2 * steps
    plan = [[] for _ in range(ticks)]
    late = []
    for k in range(1, seg.lines):
        for gather, share in ((gates, 4 * k), (weights, 9 * k)):
            tick = ticks * share // 16
            (plan[tick - 1] if tick < ticks else late).append(functools.partial(gather.step, k))
        if k < seq.lines:
            plan[ticks - 1].append(functools.partial(cots.step, k))

    def part_of_step(h, carry):
        lax.fori_loop(h * (groups // 2), (h + 1) * (groups // 2), group, 0)
        for tick in range(ticks):
            if plan[tick]:

                @pl.when(step * 2 + h == tick)
                def _():
                    for event in plan[tick]:
                        event()

        return carry

    lax.fori_loop(0, 2, part_of_step, 0)
    y_ref[pl.ds(pl.multiple_of(step * count, count), count), :] = (
        from_planes(y_pl) + skip * act_ref[...].astype(F32)
    )

    @pl.when(step == steps - 1)
    def _():
        final_ref[...] = state[...]
        for event in late[:-1]:
            event()
        gates.finish()
        keeps[2].wait()
        load_one.wait()
        load_two = pltpu.make_async_copy(gate_two, w_two, local_s.at[3])
        load_two.start()
        load_two.wait()
        model = tok_ref.shape[1]
        half = w_one.shape[3]
        block = 256

        def gating(i, carry):
            rows = pl.ds(pl.multiple_of(i * block, block), block)
            lines = tok_ref[rows, :].astype(F32)
            rstd = lax.rsqrt(jnp.mean(lines * lines, axis=1, keepdims=True) + EPSILON)
            for j, w in enumerate((w_one, w_two)):
                cols = pl.ds(j * half, half)
                gate = rstd * dot_nn(tok_ref[rows, :], w[...].reshape(model, half))
                sig = sigmoid(gate)
                y_val = y_ref[rows, cols]
                gate_ref[rows, cols] = gate * sig
                gated_ref[rows, cols] = (y_val * gate * sig).astype(BF16)
                y_ref[rows, cols] = rstd * y_val * sig * (1.0 + gate * (1.0 - sig))
            return carry

        blocks = y_ref.shape[0] // block
        lax.fori_loop(0, blocks // 2, gating, 0)
        late[-1]()
        lax.fori_loop(blocks // 2, blocks, gating, 0)
        weights.finish()
        cots.finish()
        for keep in keeps[:2]:
            keep.wait()


def backward_kernel(
    shape, steps, taps,
    pre_ref, act_ref, gy_ref, bc_ref, a_ref, params_ref, check_ref, wdt_ref, low_ref, base_ref,
    first_src, second_src, gated_src, weight_src,
    gact_ref, agrad_ref, start_ref, dtb_ref, sgrad_ref, dtp_ref, mix_ref,
    first_out, second_out, third_out,
    carry_s, rate_pl, drive_pl, gy_pl, grate_pl, thr_pl, prod, part, mix_s,
    gated_in, weight_in, third_src, load_s, *scratch,
):
    count = pre_ref.shape[0]
    width, planes, _ = a_ref.shape
    low_rank = wdt_ref.shape[0]
    seg, seq = grids(shape)
    first = Scatter(seg, first_src, scratch[:10])
    second = Scatter(seg, second_src, scratch[10:20])
    third = Scatter(seq, third_src, scratch[20:28], inside=True)
    loads = [
        pltpu.make_async_copy(gated_src, gated_in, load_s.at[0]),
        pltpu.make_async_copy(weight_src, weight_in, load_s.at[1]),
    ]
    step = pl.program_id(0)

    @pl.when(step == 0)
    def _():
        meet((seg, seq))
        first.begin()
        second.begin()
        for load in loads:
            load.start()
        carry_s[...] = jnp.zeros_like(carry_s)
        agrad_ref[...] = jnp.zeros_like(agrad_ref)
        dtb_ref[...] = jnp.zeros_like(dtb_ref)
        sgrad_ref[...] = jnp.zeros_like(sgrad_ref)
        dtp_ref[...] = jnp.zeros_like(dtp_ref)

    pre = pre_ref[...]
    rate = softplus(pre)
    act = act_ref[...].astype(F32)
    to_planes(rate_pl, rate)
    to_planes(drive_pl, rate * act)
    to_planes(gy_pl, gy_ref[...])
    groups = count // UNROLL

    def group(j, carry):
        k = groups - 1 - j
        at = k * UNROLL
        rates = [rate_pl[k, token_of(planes, i), :] for i in range(UNROLL)]
        drives = [drive_pl[k, token_of(planes, i), :] for i in range(UNROLL)]
        gys = [gy_pl[k, token_of(planes, i), :] for i in range(UNROLL)]
        g_rate = [None] * UNROLL
        through = [None] * UNROLL
        for n in range(width):
            a = a_ref[n]
            states = [check_ref[k, n]]
            decays = []
            for i in range(UNROLL):
                decays.append(jnp.exp2(rates[i] * a))
                states.append(decays[i] * states[i] + bc_ref[at + i, n] * drives[i])
            lam = carry_s[n]
            acc = agrad_ref[n]
            for i in reversed(range(UNROLL)):
                lam = lam + bc_ref[at + i, width + n] * gys[i]
                b_term = bc_ref[at + i, n] * lam
                region = (i * 2 * width + n) // 8
                prod[region, token_of(planes, n % 8), :] = lam * drives[i]
                prod[region + width // 8, token_of(planes, n % 8), :] = states[i + 1] * gys[i]
                lam = decays[i] * lam
                weighted = lam * states[i]
                acc = acc + weighted * rates[i]
                a_term = weighted * a
                g_rate[i] = a_term if n == 0 else g_rate[i] + a_term
                through[i] = b_term if n == 0 else through[i] + b_term
            carry_s[n] = lam
            agrad_ref[n] = acc
        for i in range(UNROLL):
            grate_pl[k, token_of(planes, i), :] = g_rate[i]
            thr_pl[k, token_of(planes, i), :] = through[i]
            for q in range(2 * width // 8):
                region = i * 2 * width // 8 + q
                total = prod[region, pl.ds(0, 8), :]
                for s in range(1, planes):
                    total = total + prod[region, pl.ds(s * 8, 8), :]
                row = pl.multiple_of((at + i) * 2 * width + q * 8, 8)
                part[pl.ds(row, 8), :] = total
        return carry

    events = [functools.partial(s.middle, k) for s in (first, second) for k in s.order()]
    ticks = 2 * steps
    plan = [[] for _ in range(ticks)]
    for j, event in enumerate(events):
        plan[min(ticks - 1, ticks * (j + 1) // len(events))].append(event)

    def output(index):
        own_len, model = third_src.shape[1:]
        rows = pl.ds(pl.multiple_of(index * own_len, own_len), own_len)

        def column(c, carry):
            cols = pl.ds(pl.multiple_of(c * 512, 512), 512)
            third_src[index, :, cols] = dot_nn(gated_in[rows, :], weight_in[:, cols]).astype(BF16)
            return carry

        lax.fori_loop(0, model // 512, column, 0)

    def outputs():
        for load in loads:
            load.wait()

        def leave(j, carry):
            output(third.index(j, 1))
            third.across(j, 1).start()
            return carry

        def stay(j, carry):
            output(third.index(j, 0))
            return carry

        lax.fori_loop(0, seq.lines, leave, 0)
        lax.fori_loop(0, seq.lines, stay, 0)

    plan[0].append(outputs)
    for j in third.order():
        plan[min(ticks - 1, 5 + 2 * j)].append(functools.partial(third.middle, j))

    def add_base(at, total):
        third_out[at, :] = (total + base_ref[at, :].astype(F32)).astype(BF16)

    plan[min(ticks - 1, 13)].append(functools.partial(third.finish, add_base))

    def part_of_step(h, carry):
        lax.fori_loop(h * (groups // 2), (h + 1) * (groups // 2), group, 0)
        for tick in range(ticks - 1):
            if plan[tick]:

                @pl.when(step * 2 + h == tick)
                def _():
                    for event in plan[tick]:
                        event()

        return carry

    lax.fori_loop(0, 2, part_of_step, 0)
    g_rate = from_planes(grate_pl) * (1.0 / LOG2E)
    through = from_planes(thr_pl)
    pre = pre_ref[...]
    rate = softplus(pre)
    act = act_ref[...].astype(F32)
    gy = gy_ref[...]
    g_dtpre = ((g_rate + act * through) * sigmoid(pre)).astype(BF16)
    skip = params_ref[pl.ds(width, 8), :][taps + 2 : taps + 3]
    gact_ref[...] = gy * skip + rate * through
    dtb_ref[...] += jnp.sum(g_dtpre.astype(F32), axis=0, keepdims=True)
    sgrad_ref[...] += jnp.sum(gy * act, axis=0, keepdims=True)
    dtp_ref[...] += dot_nn(low_ref[...], g_dtpre)
    rows = 2 * width
    ones = jnp.ones((LANES, LANES), F32)
    sums = jnp.dot(part[...], ones, preferred_element_type=F32)
    sums = sums.reshape(count, rows, LANES)
    pick = lax.broadcasted_iota(jnp.int32, (1, rows, LANES), 1) == lax.broadcasted_iota(
        jnp.int32, (1, rows, LANES), 2
    )
    g_bc = jnp.sum(jnp.where(pick, sums, 0.0), axis=1)
    tokens_at = pl.ds(pl.multiple_of((steps - 1 - step) * count, count), count)
    mix_s[pl.ds(0, low_rank), tokens_at] = dot_nt(wdt_ref[...], g_dtpre)
    mix_s[pl.ds(low_rank, rows), tokens_at] = g_bc.T[:rows]

    @pl.when(step == steps - 1)
    def _():
        start_ref[...] = carry_s[...]
        sum_over_seq(seq, mix_s, mix_ref, *scratch[28:])
        for event in plan[ticks - 1]:
            event()
        first.finish(into(first_out))
        second.finish(into(second_out))
        for scatter in (first, second, third):
            scatter.drain()


def forward_scan(
    shape, taps, low, w_dt, params, act, bc, a2, init, weight, cot, tok, gate_one, gate_part, block
):
    lines, fast, seq_lines = shape
    length, features = act.shape
    width, planes, _ = a2.shape
    low_rank = w_dt.shape[0]
    steps = length // block
    rows = pl.BlockSpec((block, features), lambda i: (i, 0))
    one = pl.Buffered(1)

    def whole(*dims):
        return pl.BlockSpec(dims, lambda i: (0,) * len(dims), pipeline_mode=one)

    plane = pltpu.VMEM((block // UNROLL, planes * UNROLL, LANES), F32)
    return pl.pallas_call(
        functools.partial(forward_kernel, shape, steps, taps),
        grid=(steps,),
        in_specs=[
            pl.BlockSpec((low_rank, block), lambda i: (0, i)),
            whole(low_rank, features), whole(*params.shape), rows,
            pl.BlockSpec((block, 2 * width), lambda i: (i, 0), memory_space=pltpu.SMEM),
            whole(width, planes, LANES), whole(width, planes, LANES),
            whole(*weight.shape), whole(*cot.shape), whole(*tok.shape), ANY, ANY,
        ],
        out_specs=[
            whole(length, features), rows,
            pl.BlockSpec((block // UNROLL, width, planes, LANES), lambda i: (i, 0, 0, 0)),
            whole(width, planes, LANES), whole(length, features), whole(length, features),
            ANY, ANY, ANY,
        ],
        out_shape=[
            jax.ShapeDtypeStruct((length, features), F32),
            jax.ShapeDtypeStruct((length, features), F32),
            jax.ShapeDtypeStruct((length // UNROLL, width, planes, LANES), F32),
            jax.ShapeDtypeStruct((width, planes, LANES), F32),
            jax.ShapeDtypeStruct((length, features), F32),
            jax.ShapeDtypeStruct((length, features), BF16),
            jax.ShapeDtypeStruct((lines * fast,) + weight.shape, BF16),
            jax.ShapeDtypeStruct((seq_lines * 2,) + cot.shape, BF16),
            jax.ShapeDtypeStruct(gate_one.shape, BF16),
        ],
        scratch_shapes=[
            pltpu.VMEM((width, planes, LANES), F32), plane, plane, plane,
            pltpu.VMEM(gate_one.shape, BF16), pltpu.VMEM(gate_one.shape, BF16),
            pltpu.SemaphoreType.DMA((4,)),
            *Gather.semaphores(lines, fast), *Gather.semaphores(lines, fast),
            *Gather.semaphores(seq_lines, 2),
        ],
        compiler_params=comm_params(5),
        cost_estimate=pl.CostEstimate(
            flops=8 * length * features * width,
            bytes_accessed=24 * length * features,
            transcendentals=length * features * width,
        ),
        name="scan_forward",
    )(low, w_dt, params, act, bc, a2, init, weight, cot, tok, gate_one, gate_part)


def backward_scan(
    shape, taps, pre, act, gy, bc, a2, params, checks, w_dt, dt_low, base, first, second, gated, weight,
    block,
):
    lines, fast, seq_lines = shape
    length, features = pre.shape
    width, planes, _ = a2.shape
    low_rank = w_dt.shape[0]
    steps = length // block
    rows = pl.BlockSpec((block, features), lambda i: (steps - 1 - i, 0))
    whole = pl.BlockSpec((width, planes, LANES), lambda i: (0, 0, 0))

    def all_of(rows, columns):
        return pl.BlockSpec((rows, columns), lambda i: (0, 0))

    line = all_of(1, features)
    plane = pltpu.VMEM((block // UNROLL, planes * UNROLL, LANES), F32)
    mixed = (low_rank + 2 * width, length)
    return pl.pallas_call(
        functools.partial(backward_kernel, shape, steps, taps),
        grid=(steps,),
        in_specs=[
            rows, rows, rows,
            pl.BlockSpec(
                (block, 2 * width), lambda i: (steps - 1 - i, 0), memory_space=pltpu.SMEM
            ),
            whole, all_of(*params.shape),
            pl.BlockSpec(
                (block // UNROLL, width, planes, LANES), lambda i: (steps - 1 - i, 0, 0, 0)
            ),
            all_of(low_rank, features),
            pl.BlockSpec((low_rank, block), lambda i: (0, steps - 1 - i)),
            all_of(*base.shape),
            ANY, ANY, ANY, ANY,
        ],
        out_specs=[
            rows, whole, whole, line, line, all_of(low_rank, features), all_of(*mixed),
            all_of(*first.shape[1:]), all_of(*second.shape[1:]), all_of(*base.shape),
        ],
        out_shape=[
            jax.ShapeDtypeStruct((length, features), F32),
            jax.ShapeDtypeStruct((width, planes, LANES), F32),
            jax.ShapeDtypeStruct((width, planes, LANES), F32),
            jax.ShapeDtypeStruct((1, features), F32),
            jax.ShapeDtypeStruct((1, features), F32),
            jax.ShapeDtypeStruct((low_rank, features), F32),
            jax.ShapeDtypeStruct(mixed, BF16),
            jax.ShapeDtypeStruct(first.shape[1:], BF16),
            jax.ShapeDtypeStruct(second.shape[1:], F32),
            jax.ShapeDtypeStruct(base.shape, BF16),
        ],
        scratch_shapes=[pltpu.VMEM((width, planes, LANES), F32)]
        + [plane] * 5
        + [
            pltpu.VMEM((UNROLL * 2 * width // 8, planes * 8, LANES), F32),
            pltpu.VMEM((block * 2 * width, LANES), F32),
            pltpu.VMEM(mixed, F32),
            pltpu.VMEM(gated.shape, BF16),
            pltpu.VMEM(weight.shape, BF16),
            pltpu.VMEM((2 * seq_lines,) + base.shape, BF16),
            pltpu.SemaphoreType.DMA((2,)),
            *Scatter.scratch(lines, fast, first.shape[1:]),
            *Scatter.scratch(lines, fast, second.shape[1:]),
            *Scatter.scratch(seq_lines, 2, base.shape, inside=True),
            *sum_scratch(seq_lines, *mixed),
        ],
        compiler_params=comm_params(6),
        cost_estimate=pl.CostEstimate(
            flops=20 * length * features * width,
            bytes_accessed=28 * length * features,
            transcendentals=length * features * width,
        ),
        name="scan_backward",
    )(pre, act, gy, bc, a2, params, checks, w_dt, dt_low, base, first, second, gated, weight)


def finish_kernel(shape, taps, history, refs, scratch):
    (
        gact, x_in, act, tok, w_x, w_g, w_h, gs_gate,
        mix, w_xt, head, params, dtp, a_sum, dtb, sgrad, g_half, own_tok, own_cot,
        final, start,
        small_out, halves_out, input_out, ends_out,
    ) = refs
    (
        gc, xb, actb, tokb, wxb, wgb, gsg, gs_x, xg, q_src, pack, small_src, ends_src, x_half,
        in_s, own_s,
    ) = scratch[:16]
    seg, seq = grids(shape)
    length, feats = act.shape
    width = a_sum.shape[0]
    kern = params.at[pl.ds(width, 8)]
    b_conv = params.at[pl.ds(width + taps, 1)]
    at = 16
    sets = []
    for inside, size in ((True, 8), (True, 8), (True, 8)):
        sets.append(scratch[at : at + size])
        at += size
    swaps_s = [scratch[at + 2 * i : at + 2 * i + 2] for i in range(3)]
    small = Scatter(seg, small_src, sets[0], inside=True)
    x_sum = Scatter(seg, xg, sets[1], inside=True)
    q_sum = Scatter(seq, q_src, sets[2], inside=True)
    loads = [
        pltpu.make_async_copy(gact, gc.at[pl.ds(0, length)], in_s.at[0]),
        pltpu.make_async_copy(x_in, xb.at[pl.ds(8, length)], in_s.at[1]),
        pltpu.make_async_copy(tok, tokb, in_s.at[2]),
        pltpu.make_async_copy(act, actb, in_s.at[3]),
        pltpu.make_async_copy(gs_gate, gsg, in_s.at[4]),
        pltpu.make_async_copy(w_g, wgb.at[0], in_s.at[5]),
        pltpu.make_async_copy(w_h, wgb.at[1], in_s.at[6]),
        pltpu.make_async_copy(w_x, wxb, in_s.at[7]),
    ]
    for load in loads:
        load.start()
    meet((seg, seq))
    own_rows = g_half.shape[0] // (seq.lines * seq.fast)

    def swap(half, src, sems):
        return Exchange(
            seq,
            lambda p: src.at[pl.ds(pl.multiple_of(p * own_rows, own_rows), own_rows)],
            lambda m: halves_out.at[half, m],
            sems,
        )

    swap_g = swap(1, g_half, swaps_s[1])
    swap_g.begin()
    xb[pl.ds(0, 8), :] = head[...]
    gc[pl.ds(length, 8), :] = jnp.zeros((8, feats), F32)
    loads[0].wait()
    big = LANES

    def add_mixed(i, carry):
        rows = pl.ds(pl.multiple_of(i * big, big), big)
        gc[rows, :] += dot_tn(mix[:, rows], w_xt[...])
        return carry

    lax.fori_loop(0, length // big, add_mixed, 0)
    loads[1].wait()
    tall = 32
    chunk = min(512, feats)
    sums_at = 8 * (taps + 1)
    pack[...] = jnp.zeros_like(pack)

    def through_conv(i, carry):
        t0 = pl.multiple_of(i * tall, tall)
        for c in range(0, feats, chunk):
            cols = pl.ds(c, chunk)
            wide = xb[pl.ds(t0, tall + 8), cols]
            rows = [wide[8 - history + k : 8 - history + k + tall] for k in range(taps)]
            conv = b_conv[:, cols]
            for k in range(taps):
                conv = conv + kern[pl.ds(k, 1), cols] * rows[k]
            sig = sigmoid(conv)
            g_conv = gc[pl.ds(t0, tall), cols] * sig * (1.0 + conv * (1.0 - sig))
            gc[pl.ds(t0, tall), cols] = g_conv
            for k in range(taps):
                term = g_conv * rows[k]
                pack[pl.ds(8 * k, 8), cols] += sum(
                    term[8 * j : 8 * j + 8] for j in range(tall // 8)
                )
            pack[pl.ds(8 * taps, 8), cols] += sum(
                g_conv[8 * j : 8 * j + 8] for j in range(tall // 8)
            )
        return carry

    lax.fori_loop(0, length // tall, through_conv, 0)
    loads[2].wait()

    def to_input(i, carry):
        t0 = pl.multiple_of(i * tall, tall)
        lines = tokb[pl.ds(t0, tall), :].astype(F32)
        rstd = lax.rsqrt(jnp.mean(lines * lines, axis=1, keepdims=True) + EPSILON)
        for c in range(0, feats, chunk):
            cols = pl.ds(c, chunk)
            wide = gc[pl.ds(t0, tall + 8), cols]
            g_x = kern[pl.ds(0, 1), cols] * wide[history : history + tall]
            for k in range(1, taps):
                g_x = g_x + kern[pl.ds(k, 1), cols] * wide[history - k : history - k + tall]
            gs_x[pl.ds(t0, tall), cols] = (rstd * g_x).astype(BF16)
        return carry

    lax.fori_loop(0, length // tall, to_input, 0)
    loads[3].wait()
    low_rank = dtp.shape[0]
    mixes = mix.shape[0]
    part = small_src.shape[2]
    a_grad = from_states(a_sum) * params[pl.ds(0, width), :]
    xp = dot_nn(mix[...], actb[...])
    for g in range(small_src.shape[0]):
        cols = slice(g * part, (g + 1) * part)
        small_src[g, pl.ds(0, low_rank), :] = dtp[:, cols].astype(BF16)
        small_src[g, pl.ds(low_rank, mixes), :] = xp[:, cols].astype(BF16)
        base = low_rank + mixes
        small_src[g, pl.ds(base, width), :] = a_grad[:, cols].astype(BF16)
        lines = [
            jnp.sum(pack[pl.ds(8 * k, 8), cols], axis=0, keepdims=True) for k in range(taps + 1)
        ]
        lines += [dtb[:, cols], sgrad[:, cols]]
        lines.append(jnp.zeros((16 - len(lines), part), F32))
        small_src[g, pl.ds(base + width, 16), :] = jnp.concatenate(lines, axis=0).astype(BF16)
    small.begin()

    block_rows = xg.shape[1]

    def partial(index):
        cols = pl.ds(pl.multiple_of(index * block_rows, block_rows), block_rows)
        xg[index] = dot_tn(tokb[:, cols], gs_x[...]).astype(BF16)

    by_block = block_rows % LANES == 0
    if not by_block:
        for index in range(xg.shape[0]):
            cols = slice(index * block_rows, (index + 1) * block_rows)
            xg[index] = dot_tn(tokb[:, cols], gs_x[...]).astype(BF16)

    def leave(j, carry):
        for e in range(1, seg.fast):
            if by_block:
                partial(x_sum.index(j, e))
            x_sum.across(j, e).start()
        return carry

    lax.fori_loop(0, seg.lines, leave, 0)
    def stay(j, carry):
        if by_block:
            partial(x_sum.index(j, 0))
        return carry

    lax.fori_loop(0, seg.lines, stay, 0)
    ends_in = jnp.concatenate(
        [
            from_states(final),
            xb[pl.ds(length, 8), :][8 - history :],
            from_states(start),
            sum_head(gc, kern, history, taps),
            jnp.zeros((ends_src.shape[1] - 2 * (width + history), feats), F32),
        ],
        axis=0,
    )
    piece = ends_src.shape[2]
    for p in range(ends_src.shape[0]):
        ends_src[p] = ends_in[:, p * piece : (p + 1) * piece]
    end_swap = Exchange(seq, lambda p: ends_src.at[p], lambda m: ends_out.at[m], swaps_s[2])
    end_swap.begin()
    loads[4].wait()
    loads[5].wait()
    loads[6].wait()
    loads[7].wait()
    own_len = own_tok.shape[0]
    model = own_tok.shape[1]
    wide = 512
    half = feats // 2

    def normed(index):
        rows = pl.ds(pl.multiple_of(index * own_len, own_len), own_len)

        def column(c, carry):
            cols = pl.ds(pl.multiple_of(c * wide, wide), wide)
            q_src[index, :, cols] = (
                dot_nt(gsg[rows, pl.ds(0, half)], wgb[0, cols, :])
                + dot_nt(gsg[rows, pl.ds(half, half)], wgb[1, cols, :])
                + dot_nt(gs_x[rows, :], wxb[cols, :])
            ).astype(BF16)
            return carry

        lax.fori_loop(0, model // wide, column, 0)

    def leave_q(j, carry):
        normed(q_sum.index(j, 1))
        q_sum.across(j, 1).start()
        return carry

    def stay_q(j, carry):
        normed(q_sum.index(j, 0))
        return carry

    lax.fori_loop(0, seq.lines, leave_q, 0)
    lax.fori_loop(0, seq.lines, stay_q, 0)
    for k in small.order():
        small.middle(k)
    for j, k in enumerate(x_sum.order()):
        x_sum.middle(k)
        if j == seg.lines - 2:
            for m in q_sum.order():
                q_sum.middle(m)

    def input_grad(at, total):
        own = own_tok[at, :].astype(F32)
        square = 1.0 / (jnp.mean(own * own, axis=1, keepdims=True) + EPSILON)
        input_out[at, :] = (
            own_cot[at, :].astype(F32)
            + total
            - own * (square * jnp.mean(total * own, axis=1, keepdims=True))
        ).astype(BF16)

    q_sum.finish(input_grad)
    small.finish(into(small_out))
    x_sum.finish(into(x_half))
    swap_x = swap(0, x_half, swaps_s[0])
    swap_x.begin()
    own = pl.ds(pl.multiple_of(seq.here * own_rows, own_rows), own_rows)
    keeps = [
        pltpu.make_async_copy(x_half.at[own], halves_out.at[0, seq.here], own_s.at[0]),
        pltpu.make_async_copy(g_half.at[own], halves_out.at[1, seq.here], own_s.at[1]),
        pltpu.make_async_copy(ends_src.at[seq.here], ends_out.at[seq.here], own_s.at[2]),
    ]
    for keep in keeps:
        keep.start()
    for scatter in (small, x_sum, q_sum):
        scatter.drain()
    for exchange in (swap_g, end_swap, swap_x):
        exchange.arrived()
        exchange.drain()
    for keep in keeps:
        keep.wait()


def from_states(ref):
    return jnp.concatenate([ref[:, s, :] for s in range(ref.shape[1])], axis=1)


def sum_head(gc, kern, history, taps):
    top = gc[pl.ds(0, 8), :]
    rows = []
    for j in range(history):
        rows.append(
            sum(kern[pl.ds(k, 1), :] * top[j - k : j - k + 1] for k in range(min(j + 1, taps)))
        )
    return jnp.concatenate(rows, axis=0)


def finish_all(shape, taps, history, big, small):
    lines, fast, seq_lines = shape
    segs, seqs = lines * fast, seq_lines * 2
    gact, x_in, act, tok, w_x, w_g, w_h, gs_gate = big
    mix, w_xt, head, params, dtp, a_sum, dtb, sgrad, g_half, own_tok, own_cot = small[:11]
    length, feats = act.shape
    own_len, model = own_tok.shape
    width = a_sum.shape[0]
    rows = dtp.shape[0] + mix.shape[0] + width + 16
    block_rows = model // segs
    own_rows = g_half.shape[0] // seqs
    ends = (seqs, 2 * (width + history) + (-2 * (width + history)) % 8, feats // seqs)
    dma = pltpu.SemaphoreType.DMA
    scratch = [
        pltpu.VMEM((length + 8, feats), F32),
        pltpu.VMEM((length + 8, feats), F32),
        pltpu.VMEM((length, feats), BF16),
        pltpu.VMEM((length, model), BF16),
        pltpu.VMEM((model, feats), BF16),
        pltpu.VMEM((2, model, feats // 2), BF16),
        pltpu.VMEM((length, feats), BF16),
        pltpu.VMEM((length, feats), BF16),
        pltpu.VMEM((segs, block_rows, feats), BF16),
        pltpu.VMEM((seqs, own_len, model), BF16),
        pltpu.VMEM((8 * (taps + 1), feats), F32),
        pltpu.VMEM((segs, rows, feats // segs), BF16),
        pltpu.VMEM(ends, F32),
        pltpu.VMEM((block_rows, feats), BF16),
        dma((8,)), dma((3,)),
        *Scatter.scratch(lines, fast, (rows, feats // segs), inside=True),
        *Scatter.scratch(lines, fast, (block_rows, feats), inside=True),
        *Scatter.scratch(seq_lines, 2, (own_len, model), inside=True),
        *Exchange.semaphores(seqs), *Exchange.semaphores(seqs), *Exchange.semaphores(seqs),
    ]

    def kernel(*refs):
        finish_kernel(shape, taps, history, refs[:25], refs[25:])

    return pl.pallas_call(
        kernel,
        in_specs=[ANY] * 8 + [INSIDE] * 13,
        out_specs=[INSIDE] * 4,
        out_shape=[
            jax.ShapeDtypeStruct((rows, feats // segs), F32),
            jax.ShapeDtypeStruct((2, seqs, own_rows, feats), BF16),
            jax.ShapeDtypeStruct((own_len, model), BF16),
            jax.ShapeDtypeStruct(ends, F32),
        ],
        scratch_shapes=scratch,
        compiler_params=comm_params(4),
        name="finish",
    )(*big, *small)


def gather_kernel(
    shape, scaled_x, scaled_g, small, tokens, w_x, small_all, tok, g_part, x_part, tok_in, g_own,
    local_s, small_sems, tok_sems, swap_x, swap_g, x_sems,
):
    seg, seq = grids(shape)
    size = seq.lines * seq.fast
    load_tok = pltpu.make_async_copy(tokens, tok_in, local_s.at[0])
    load_own = pltpu.make_async_copy(scaled_x.at[seq.here], x_part.at[seq.here], local_s.at[1])
    load_gate = pltpu.make_async_copy(scaled_g.at[seq.here], g_own, local_s.at[3])
    load_tok.start()
    load_own.start()
    load_gate.start()
    meet((seg, seq))
    swap_x = Exchange(seq, lambda p: scaled_x.at[p], lambda m: x_part.at[m], swap_x)
    swap_g = Exchange(seq, lambda p: scaled_g.at[p], lambda m: g_part.at[m], swap_g)
    swap_x.begin()
    pieces = []
    for k in range(size):
        place = lax.rem(seq.here - k + size, size)
        pieces.append(Gather(seg, x_part.at[place], w_x, x_sems[6 * k : 6 * k + 6], place))
    smalls = Gather(seg, small, small_all, small_sems)
    load_own.wait()
    pieces[0].begin()
    smalls.begin()
    load_tok.wait()
    toks = Gather(seq, tok_in, tok, tok_sems)
    for k in range(1, size):
        swap_x.one(k).wait_recv()
        pieces[k].begin()
    toks.begin()
    swap_g.begin()
    load_gate.wait()
    keeps = [
        pltpu.make_async_copy(tok_in, tok.at[seq.here], local_s.at[0]),
        pltpu.make_async_copy(x_part, w_x.at[seg.here], local_s.at[1]),
        pltpu.make_async_copy(small, small_all.at[seg.here], local_s.at[2]),
        pltpu.make_async_copy(g_own, g_part.at[seq.here], local_s.at[3]),
    ]
    for keep in keeps:
        keep.start()
    for k in range(1, max(seg.lines, seq.lines)):
        if k < seg.lines:
            pieces[0].step(k)
            smalls.step(k)
            for piece in pieces[1:]:
                piece.step(k)
        if k < seq.lines:
            toks.step(k)
    toks.finish()
    smalls.finish()
    for piece in pieces:
        piece.finish()
    swap_g.arrived()
    swap_x.drain()
    swap_g.drain()
    for keep in keeps:
        keep.wait()


def gather_start(shape, scaled_x, scaled_g, small, tokens):
    lines, fast, seq_lines = shape
    segs, seqs = lines * fast, seq_lines * 2
    rows, feats = scaled_x.shape[1:]
    sems = Gather.semaphores

    def kernel(*refs):
        ins, rest = refs[:11], refs[11:]
        gather_kernel(
            shape, *ins, rest[0], rest[1:7], rest[7:13], rest[13:15], rest[15:17], rest[17:]
        )

    w_x, small_all, tok, g_part = pl.pallas_call(
        kernel,
        in_specs=[ANY, ANY, INSIDE, ANY],
        out_specs=[ANY] * 4,
        out_shape=[
            jax.ShapeDtypeStruct((segs, seqs, rows, feats), BF16),
            jax.ShapeDtypeStruct((segs,) + small.shape, BF16),
            jax.ShapeDtypeStruct((seqs,) + tokens.shape, BF16),
            jax.ShapeDtypeStruct((seqs,) + scaled_g.shape[1:], BF16),
        ],
        scratch_shapes=[
            pltpu.VMEM((seqs, rows, feats), BF16),
            pltpu.VMEM(tokens.shape, BF16),
            pltpu.VMEM(scaled_g.shape[1:], BF16),
            pltpu.SemaphoreType.DMA((4,)),
            *sems(lines, fast), *sems(seq_lines, 2),
            *Exchange.semaphores(seqs), *Exchange.semaphores(seqs),
            *(sems(lines, fast) * seqs),
        ],
        compiler_params=comm_params(1),
        name="gather_start",
    )(scaled_x, scaled_g, small, tokens)
    return w_x.reshape(-1, feats), small_all, tok.reshape(-1, tokens.shape[1]), g_part


def front_kernel(
    shape, steps, taps, history, width,
    tok_ref, wx_ref, small_ref, head_ref, gate_src,
    x_ref, act_ref, wdt_ref, wxt_ref, par_ref, a2_ref, low_ref, bc_ref, gate_out,
    xb, mix_s, mix, local_s, *scratch,
):
    seg, seq = grids(shape)
    step = pl.program_id(0)
    gates = Gather(seg, gate_src.at[:, 0], gate_out, scratch[:6])
    count = tok_ref.shape[0]
    low_rank = wdt_ref.shape[0]
    mixes = wxt_ref.shape[0]
    feats = wx_ref.shape[1]
    part = small_ref.shape[2]

    @pl.when(step == 0)
    def _():
        meet((seg, seq))
        gates.begin()
        xb[pl.ds(0, 8), :] = head_ref[...]
        for g in range(small_ref.shape[0]):
            cols = slice(g * part, (g + 1) * part)
            wdt_ref[:, cols] = small_ref[g, pl.ds(0, low_rank), :]
            wxt_ref[:, cols] = small_ref[g, pl.ds(low_rank, mixes), :]
            rest = small_ref[g, pl.ds(low_rank + mixes, width + 16), :].astype(F32)
            par_ref[:, cols] = rest
        a_mat = -jnp.exp(par_ref[pl.ds(0, width), :])
        par_ref[pl.ds(0, width), :] = a_mat
        for s in range(feats // LANES):
            a2_ref[:, s, :] = a_mat[:, s * LANES : (s + 1) * LANES] * LOG2E

    kern = par_ref[pl.ds(width, 8), :]
    rows = tok_ref[...].astype(F32)
    rstd = lax.rsqrt(jnp.mean(rows * rows, axis=1, keepdims=True) + EPSILON)
    x_in = rstd * dot_nn(tok_ref[...], wx_ref[...])
    x_ref[...] = x_in
    xb[pl.ds(8, count), :] = x_in
    tall = 32
    chunk = min(512, feats)

    def through_conv(i, carry):
        t0 = pl.multiple_of(i * tall, tall)
        for c in range(0, feats, chunk):
            cols = slice(c, c + chunk)
            wide = xb[pl.ds(t0, tall + 8), pl.ds(c, chunk)]
            conv = kern[taps : taps + 1, cols]
            for k in range(taps):
                conv = conv + kern[k : k + 1, cols] * wide[8 - history + k : 8 - history + k + tall]
            act_ref[pl.ds(t0, tall), pl.ds(c, chunk)] = (conv * sigmoid(conv)).astype(BF16)
        return carry

    lax.fori_loop(0, count // tall, through_conv, 0)
    xb[pl.ds(0, 8), :] = xb[pl.ds(count, 8), :]
    mix_s[:, pl.ds(pl.multiple_of(step * count, count), count)] = dot_nt(wxt_ref[...], act_ref[...])
    for k in range(1, seg.lines - 1):

        @pl.when(step == min(steps - 1, 2 * k - 1))
        def _():
            gates.step(k)

    @pl.when(step == steps - 1)
    def _():
        sum_over_seq(seq, mix_s, mix, *scratch[6:])
        low_ref[...] = mix[pl.ds(0, low_rank), :]
        bc_ref[...] = mix[pl.ds(low_rank, 2 * width), :].astype(F32).T
        gates.step(seg.lines - 1)
        keep = pltpu.make_async_copy(gate_src.at[:, 0], gate_out.at[seg.here], local_s)
        keep.start()
        gates.finish()
        keep.wait()


def front(shape, taps, history, width, tok, w_x, small_all, head, gate_part, block):
    lines, fast, seq_lines = shape
    segs, seqs = lines * fast, seq_lines * 2
    length, model = tok.shape
    feats = w_x.shape[1]
    low_rank = LANES
    mixes = low_rank + 2 * width
    steps = length // block

    def whole(*dims):
        return pl.BlockSpec(dims, lambda i: (0,) * len(dims))

    def rows(columns):
        return pl.BlockSpec((block, columns), lambda i: (i, 0))

    one = pl.Buffered(1)
    return pl.pallas_call(
        functools.partial(front_kernel, shape, steps, taps, history, width),
        grid=(steps,),
        in_specs=[
            rows(model),
            pl.BlockSpec((model, feats), lambda i: (0, 0), pipeline_mode=one),
            whole(*small_all.shape), whole(*head.shape), ANY,
        ],
        out_specs=[
            rows(feats), rows(feats), whole(low_rank, feats), whole(mixes, feats),
            whole(width + 16, feats), whole(width, feats // LANES, LANES),
            whole(low_rank, length), whole(length, 2 * width), ANY,
        ],
        out_shape=[
            jax.ShapeDtypeStruct((length, feats), F32),
            jax.ShapeDtypeStruct((length, feats), BF16),
            jax.ShapeDtypeStruct((low_rank, feats), BF16),
            jax.ShapeDtypeStruct((mixes, feats), BF16),
            jax.ShapeDtypeStruct((width + 16, feats), F32),
            jax.ShapeDtypeStruct((width, feats // LANES, LANES), F32),
            jax.ShapeDtypeStruct((low_rank, length), BF16),
            jax.ShapeDtypeStruct((length, 2 * width), F32),
            jax.ShapeDtypeStruct((segs, seqs) + gate_part.shape[2:], BF16),
        ],
        scratch_shapes=[
            pltpu.VMEM((block + 8, feats), F32),
            pltpu.VMEM((mixes, length), F32),
            pltpu.VMEM((mixes, length), BF16),
            pltpu.SemaphoreType.DMA,
            *Gather.semaphores(lines, fast),
            *sum_scratch(seq_lines, mixes, length),
        ],
        compiler_params=comm_params(2),
        name="front",
    )(tok, w_x, small_all, head, gate_part)


def sum_scratch(seq_lines, rows, width):
    part = pltpu.VMEM((rows, width // 2), BF16)
    dma = pltpu.SemaphoreType.DMA
    return [
        part, part, part,
        pltpu.VMEM((max(seq_lines - 1, 1), rows, width // 2), BF16),
        pltpu.VMEM((2, rows, width // 2), BF16),
        dma, dma, dma((seq_lines,)), dma((seq_lines,)), dma, dma,
    ]


def unpack_kernel(
    seqs, taps, history, low_rank, width,
    small, halves, ends, mixed, input_grad, out_grad, weight, gain,
    mixed_o, final_o, final_c, input_o, start_o, start_c, gain_o, in_o, cw_o, cb_o, xp_o, dtp_o,
    dtb_o, a_o, skip_o, out_o,
):
    mixed_o[0] = mixed[...]
    input_o[0] = input_grad[...]
    out_o[...] = out_grad[...]
    part = small.shape[1]
    columns = xp_o.shape[0]
    dtp_o[...] = small[pl.ds(0, low_rank), :]
    xp_o[...] = small[pl.ds(low_rank, columns), :]
    at = low_rank + columns
    a_o[...] = small[pl.ds(at, width), :]
    lines = small[pl.ds(at + width, 16), :]
    cw_o[...] = lines[:taps]
    cb_o[...] = lines[taps]
    dtb_o[...] = lines[taps + 1]
    skip_o[...] = lines[taps + 2]
    each = final_o.shape[2] // part // seqs
    for s in range(seqs):
        rows = ends[s]
        for g in range(each):
            got = rows[:, g * part : (g + 1) * part]
            cols = pl.ds((g * seqs + s) * part, part)
            final_o[0, :, cols] = got[:width]
            start_o[0, :, cols] = got[width + history : 2 * width + history]
            for r in range(history):
                final_c[r, :, cols] = got[width + r : width + r + 1]
                at = 2 * width + history + r
                start_c[r, :, cols] = got[at : at + 1]
    scale = gain[...]
    total = jnp.zeros((in_o.shape[0], part), F32)
    groups = halves.shape[3] // part
    for half in range(2):
        for s in range(seqs):
            for g in range(groups):
                raw = halves[half, s, :, g * part : (g + 1) * part].astype(F32)
                cols = pl.ds(((half * groups + g) * seqs + s) * part, part)
                in_o[:, cols] = raw * scale
                total = total + raw * weight[:, cols].astype(F32)
    gain_o[...] = jnp.sum(total.T, axis=0)


def unpack(taps, history, low_rank, width, small, halves, ends, mixed, input_grad, out_grad,
           weight, gain):
    seqs, own_rows, feats = halves.shape[1:]
    part = small.shape[1]
    model = mixed.shape[1]
    kept = ends.shape[2] * seqs
    f32 = lambda *dims: jax.ShapeDtypeStruct(dims, F32)
    args = (small, halves, ends, mixed, input_grad, out_grad, weight, gain)
    outs = [
        jax.ShapeDtypeStruct((1,) + mixed.shape, BF16),
        f32(1, width, kept), f32(history, 1, kept),
        jax.ShapeDtypeStruct((1,) + input_grad.shape, BF16),
        f32(1, width, kept), f32(history, 1, kept),
        f32(own_rows), f32(*weight.shape),
        f32(taps, part), f32(part), f32(low_rank + 2 * width, part), f32(low_rank, part),
        f32(part), f32(width, part), f32(part), f32(part, model),
    ]

    def whole(a):
        return pl.BlockSpec(
            a.shape, lambda i: (0,) * len(a.shape), pipeline_mode=pl.Buffered(1)
        )

    return pl.pallas_call(
        functools.partial(unpack_kernel, seqs, taps, history, low_rank, width),
        grid=(1,),
        in_specs=[whole(a) for a in args],
        out_specs=[whole(a) for a in outs],
        out_shape=outs,
        name="unpack",
    )(*args)


def body(
    tokens, norm_gain, in_proj, conv_weight, conv_bias, x_proj, dt_proj, dt_bias,
    a_log, d_skip, out_proj, init_state, init_conv, cotangent,
):
    segs, seqs = lax.axis_size("seg"), lax.axis_size("seq")
    place = lax.axis_index("seq")
    own_rows, both = in_proj.shape
    part = conv_bias.shape[0]
    feats = segs * part
    taps = conv_weight.shape[0]
    width = a_log.shape[0]
    low_rank = dt_proj.shape[0]
    planes = feats // LANES
    own_len, model = tokens.shape[1:]
    length = own_len * seqs
    block = 64
    seq_lines = seqs // 2
    shape = (segs // seq_lines, seq_lines, seq_lines)

    def mine(rows):
        shaped = rows.reshape(rows.shape[0], segs, seqs, part)
        return lax.dynamic_index_in_dim(shaped, place, 2, keepdims=False).reshape(
            rows.shape[0], feats
        )

    gain_col = norm_gain.astype(F32)[:, None]
    own_weight = in_proj.astype(F32)
    scaled = (own_weight * gain_col).astype(BF16)
    scaled = scaled.reshape(own_rows, 2, segs, seqs, part)
    scaled_x = scaled[:, 0].transpose(2, 0, 1, 3).reshape(seqs, own_rows, feats)
    scaled_g = scaled[:, 1].reshape(own_rows, 2, segs // 2, seqs, part).transpose(3, 1, 0, 2, 4)
    scaled_g = scaled_g.reshape(seqs, 2, own_rows, feats // 2)
    small = jnp.concatenate(
        [
            dt_proj, x_proj.T, a_log, conv_weight, conv_bias[None], dt_bias[None], d_skip[None],
        ],
        axis=0,
    )
    small = jnp.pad(small, ((0, -small.shape[0] % 16), (0, 0)))
    w_x_half, small_all, tok, g_part = gather_start(shape, scaled_x, scaled_g, small, tokens[0])
    history = init_conv.shape[1]
    head = jnp.pad(mine(init_conv[0]), ((8 - history, 0), (0, 0)))
    x_in, act, w_dt, w_xt, params, a2, dt_low, bc, w_g_one = front(
        shape, taps, history, width, tok, w_x_half, small_all, head, g_part, 4 * block
    )
    init = mine(init_state[0]).reshape(width, planes, LANES)
    slope, pre, checks, final, gate_act, gated, w_out, cot, w_g_two = forward_scan(
        shape, taps, dt_low, w_dt, params, act, bc, a2, init, out_proj, cotangent[0], tok,
        w_g_one, g_part, 2 * block,
    )
    w_out = w_out.reshape(feats, model)
    cot = cot.reshape(length, model)
    w_g_one = w_g_one.reshape(model, feats // 2)
    w_g_two = w_g_two.reshape(model, feats // 2)
    g_gated = dot_nt(cot, w_out)
    gy = g_gated * gate_act
    gs_gate = (g_gated * slope).astype(BF16)
    out_grad = dot_tn(gated, cot).astype(BF16)
    gate_grad = dot_tn(tok, gs_gate).astype(BF16)
    g_actp, a_sum, start, dtb_grad, skip_grad, dtp_grad, g_mixed, g_half, out_grad, mixed_out = (
        backward_scan(
            shape, taps, pre, act, gy, bc, a2, params, checks, w_dt, dt_low, tokens[0],
            gate_grad.reshape(segs, seqs * own_rows, feats),
            out_grad.reshape(segs, part, model),
            gated, w_out, 2 * block,
        )
    )
    grads, halves, input_grad, ends = finish_all(
        shape, taps, history,
        (g_actp, x_in, act, tok, w_x_half, w_g_one, w_g_two, gs_gate),
        (
            g_mixed, w_xt, head, params, dtp_grad, a_sum, dtb_grad, skip_grad, g_half,
            tokens[0], cotangent[0], final, start,
        ),
    )
    if part % LANES == 0:
        outs = list(
            unpack(
                taps, history, low_rank, width, grads, halves, ends, mixed_out, input_grad,
                out_grad, in_proj, gain_col,
            )
        )
        outs[2], outs[5], outs[10] = (
            outs[2].transpose(1, 0, 2), outs[5].transpose(1, 0, 2), outs[10].T
        )
        return tuple(outs)
    ends = (
        ends.reshape(seqs, ends.shape[1], segs // seqs, part)
        .transpose(1, 2, 0, 3)
        .reshape(ends.shape[1], feats)
    )
    raw_grad = (
        halves.reshape(2, seqs, own_rows, segs, part)
        .transpose(2, 0, 3, 1, 4)
        .reshape(own_rows, both)
        .astype(F32)
    )
    in_grad = raw_grad * gain_col
    gain_grad = jnp.sum(raw_grad * own_weight, axis=1)

    at = width + history
    xp_at = low_rank + x_proj.shape[1]
    return (
        mixed_out[None],
        ends[None, :width],
        ends[None, width:at],
        input_grad[None],
        ends[None, at : at + width],
        ends[None, at + width : at + width + history],
        gain_grad,
        in_grad,
        grads[xp_at + width : xp_at + width + taps],
        grads[xp_at + width + taps],
        grads[low_rank:xp_at].T,
        grads[:low_rank],
        grads[xp_at + width + taps + 1],
        grads[xp_at : xp_at + width],
        grads[xp_at + width + taps + 2],
        out_grad,
    )


def solution(mesh):
    spread = ("seg", "seq")
    placed = (
        P("seg", "seq", None),
        P(spread),
        P(spread, None),
        P(None, spread),
        P(spread),
        P(spread, None),
        P(None, spread),
        P(spread),
        P(None, spread),
        P(spread),
        P(spread, None),
        P("seg", None, None),
        P("seg", None, None),
        P("seg", "seq", None),
    )
    return jax.shard_map(
        body,
        mesh=mesh,
        in_specs=placed,
        out_specs=(
            P("seg", "seq", None),
            P("seg", None, "seq"),
            P("seg", None, "seq"),
            P("seg", "seq", None),
            P("seg", None, "seq"),
            P("seg", None, "seq"),
            P(spread),
            P(spread, None),
            P(None, spread),
            P(spread),
            P(spread, None),
            P(None, spread),
            P(spread),
            P(None, spread),
            P(spread),
            P(spread, None),
        ),
        check_vma=False,
    )
```

```python
import functools

import jax
import jax.numpy as jnp
from jax import lax
from jax.experimental import pallas as pl
from jax.experimental.pallas import tpu as pltpu
from jax.sharding import PartitionSpec as P

EPSILON = 1e-05
LOG2E = 1.4426950408889634
LANES = 128
UNROLL = 8
F32 = jnp.float32
BF16 = jnp.bfloat16


def dot_nn(a, b):
    return jnp.dot(a, b, preferred_element_type=F32)


def dot_tn(a, b):
    return lax.dot_general(a, b, (((0,), (0,)), ((), ())), preferred_element_type=F32)


def dot_nt(a, b):
    return lax.dot_general(a, b, (((1,), (1,)), ((), ())), preferred_element_type=F32)


def sigmoid(v):
    return 1.0 / (1.0 + jnp.exp(-v))


def softplus(v):
    return jnp.maximum(v, 0.0) + jnp.log1p(jnp.exp(-jnp.abs(v)))


def to_planes(planes_ref, rows):
    groups = planes_ref.shape[0]
    for s in range(rows.shape[1] // LANES):
        tile = rows[:, s * LANES : (s + 1) * LANES].reshape(groups, UNROLL, LANES)
        planes_ref[:, pl.ds(s * UNROLL, UNROLL), :] = tile


def from_planes(planes_ref):
    groups, rows, _ = planes_ref.shape
    return jnp.concatenate(
        [
            planes_ref[:, pl.ds(s * UNROLL, UNROLL), :].reshape(groups * UNROLL, LANES)
            for s in range(rows // UNROLL)
        ],
        axis=1,
    )


def token_of(planes, i):
    return pl.ds(i, planes, stride=UNROLL)


MESH_ID = pl.DeviceIdType.MESH
VMEM_MOST = 67_043_328


class Grid:
    def __init__(self, axis, lines, fast):
        self.axis, self.lines, self.fast = axis, lines, fast
        self.here = lax.axis_index(axis)
        self.line = self.here // fast
        self.lane = self.here - self.line * fast

    def at(self, line, lane):
        return line * self.fast + lane

    def line_peer(self, k):
        return lax.rem(self.line + k, self.lines)

    def lane_peer(self, e):
        return lax.rem(self.lane + e, self.fast)

    def copy(self, src, dst, sent, got, index):
        return pltpu.make_async_remote_copy(
            src_ref=src, dst_ref=dst, send_sem=sent, recv_sem=got,
            device_id={self.axis: index}, device_id_type=MESH_ID,
        )


def meet(groups):
    barrier = pltpu.get_barrier_semaphore()
    total = 0
    for grid in groups:
        size = grid.lines * grid.fast
        for k in range(1, size):
            pl.semaphore_signal(
                barrier, inc=1, device_id={grid.axis: lax.rem(grid.here + k, size)},
                device_id_type=MESH_ID,
            )
        total += size - 1
    pl.semaphore_wait(barrier, total)


class Gather:
    def __init__(self, grid, own, out, sems, piece=None):
        self.grid, self.own, self.out, self.piece = grid, own, out, piece
        self.up_s, self.up_r, self.dn_s, self.dn_r, self.x_s, self.x_r = sems

    @staticmethod
    def semaphores(lines, fast):
        hops = pltpu.SemaphoreType.DMA((lines,))
        across = pltpu.SemaphoreType.DMA((lines, fast))
        return [hops, hops, hops, hops, across, across]

    def block(self, line, lane=None):
        grid = self.grid
        index = grid.at(line, grid.lane if lane is None else lane)
        return self.out.at[index] if self.piece is None else self.out.at[index, self.piece]

    def up(self, k):
        grid = self.grid
        block = self.block(jnp.maximum(grid.line - k, 0))
        return grid.copy(
            self.own if k == 0 else block, block, self.up_s.at[k], self.up_r.at[k],
            grid.at(jnp.minimum(grid.line + 1, grid.lines - 1), grid.lane),
        )

    def down(self, k):
        grid = self.grid
        block = self.block(jnp.minimum(grid.line + k, grid.lines - 1))
        return grid.copy(
            self.own if k == 0 else block, block, self.dn_s.at[k], self.dn_r.at[k],
            grid.at(jnp.maximum(grid.line - 1, 0), grid.lane),
        )

    def sends_up(self, k):
        return jnp.logical_and(self.grid.line + 1 < self.grid.lines, self.grid.line >= k)

    def sends_down(self, k):
        return jnp.logical_and(self.grid.line > 0, self.grid.line + k < self.grid.lines)

    def across(self, line, slot, e, own=False):
        grid = self.grid
        block = self.block(line)
        return grid.copy(
            self.own if own else block, block, self.x_s.at[slot, e], self.x_r.at[slot, e],
            grid.at(grid.line, grid.lane_peer(e)),
        )

    def slots(self):
        return range(self.grid.lines)

    def begin(self):
        grid = self.grid
        for when, copy in ((self.sends_up(0), self.up(0)), (self.sends_down(0), self.down(0))):
            pl.when(when)(copy.start)
        for e in range(1, grid.fast):
            self.across(grid.line, 0, e, own=True).start()

    def step(self, k):
        grid = self.grid

        def arrived(copy, line, slot, forward, onward):
            copy.wait_recv()
            if k < grid.lines - 1:
                pl.when(forward(k))(onward(k).start)
            for e in range(1, grid.fast):
                self.across(line, slot, e).start()

        below, above = grid.line - k, grid.line + k

        @pl.when(below >= 0)
        def _():
            arrived(self.up(k - 1), below, grid.lines - k, self.sends_up, self.up)

        @pl.when(above < grid.lines)
        def _():
            arrived(self.down(k - 1), above, k, self.sends_down, self.down)

    def finish(self):
        grid = self.grid
        for k in range(grid.lines - 1):
            pl.when(self.sends_up(k))(self.up(k).wait_send)
            pl.when(self.sends_down(k))(self.down(k).wait_send)
        for slot in self.slots():
            for e in range(1, grid.fast):
                copy = self.across(grid.line_peer(slot), slot, e, own=slot == 0)
                copy.wait_send()
                copy.wait_recv()


class Scatter:
    def __init__(self, grid, src, scratch, inside=False):
        self.grid, self.src, self.inside = grid, src, inside
        if not inside:
            self.own, self.o_s = scratch[:2]
            scratch = scratch[2:]
        self.xbuf, self.stage, self.zbuf, self.acc = scratch[:4]
        self.x_s, self.x_r, self.z_s, self.z_r = scratch[4:]
        self.last = grid.lines - 1

    @staticmethod
    def scratch(lines, fast, shape, inside=False):
        dma = pltpu.SemaphoreType.DMA
        shape = tuple(shape)
        loads = [] if inside else [pltpu.VMEM((lines,) + shape, BF16), dma((lines,))]
        return loads + [
            pltpu.VMEM((lines, fast - 1) + shape, BF16),
            pltpu.VMEM((lines - 1,) + shape, BF16),
            pltpu.VMEM((lines + 1,) + shape, BF16),
            pltpu.VMEM(shape, F32),
            dma((lines, fast)), dma((lines, fast)), dma((lines,)), dma((lines + 1,)),
        ]

    def dest(self, j):
        line, last = self.grid.line, self.last
        above, below = last - line, line
        low = jnp.where(j < above, last - j, j - above)
        high = jnp.where(j < below, j, last - (j - below))
        other = jnp.where(2 * line <= last, low, high)
        return jnp.where(j == last, line, other)

    def index(self, j, e):
        return self.grid.at(self.dest(j), self.grid.lane_peer(e))

    def across(self, j, e):
        grid = self.grid
        return grid.copy(
            self.src.at[self.index(j, e)], self.xbuf.at[j, e - 1],
            self.x_s.at[j, e], self.x_r.at[j, e], grid.at(grid.line, grid.lane_peer(e)),
        )

    def local(self, j):
        return pltpu.make_async_copy(
            self.src.at[self.index(j, 0)], self.own.at[j], self.o_s.at[j]
        )

    def along(self, j):
        grid = self.grid
        dest = self.dest(j)
        up = dest > grid.line
        to = jnp.clip(jnp.where(up, grid.line + 1, grid.line - 1), 0, self.last)
        slot = jnp.where(jnp.logical_and(jnp.logical_not(up), dest == to), grid.lines, dest)
        return grid.copy(
            self.stage.at[j], self.zbuf.at[slot], self.z_s.at[j], self.z_r.at[slot],
            grid.at(to, grid.lane),
        )

    def arrival(self, slot):
        grid = self.grid
        return grid.copy(
            self.stage.at[0], self.zbuf.at[slot], self.z_s.at[0], self.z_r.at[slot],
            grid.at(lax.rem(grid.line + 1, grid.lines), grid.lane),
        )

    def order(self):
        return list(range(self.grid.lines))

    def begin(self):
        for j in self.order():
            for e in range(1, self.grid.fast):
                self.across(j, e).start()
            if not self.inside:
                self.local(j).start()

    def rows(self, step):
        count = self.acc.shape[0]
        size = 16 if count % 16 == 0 else 8

        def run(i, carry):
            step(pl.ds(pl.multiple_of(i * size, size), size))
            return carry

        lax.fori_loop(0, count // size, run, 0)

    def middle(self, j):
        grid = self.grid
        for e in range(1, grid.fast):
            self.across(j, e).wait_recv()
        if self.inside:
            own = self.src.at[self.index(j, 0)]
        else:
            self.local(j).wait()
            own = self.own.at[j]

        def partial(at):
            total = own[at, :].astype(F32)
            for e in range(grid.fast - 1):
                total = total + self.xbuf[j, e, at, :].astype(F32)
            return total

        if j == self.last:

            def keep(at):
                self.acc[at, :] = partial(at)

            self.rows(keep)
            return
        dest = self.dest(j)
        carried = jnp.where(dest > grid.line, grid.line > 0, grid.line < self.last)

        @pl.when(carried)
        def _():
            self.arrival(dest).wait_recv()

            def add(at):
                total = partial(at) + self.zbuf[dest, at, :].astype(F32)
                self.stage[j, at, :] = total.astype(BF16)

            self.rows(add)

        @pl.when(jnp.logical_not(carried))
        def _():
            def add(at):
                self.stage[j, at, :] = partial(at).astype(BF16)

            self.rows(add)

        self.along(j).start()

    def finish(self, write):
        line, last = self.grid.line, self.last
        from_below, from_above = line > 0, line < last

        @pl.when(from_below)
        def _():
            self.arrival(line).wait_recv()

        @pl.when(from_above)
        def _():
            self.arrival(self.grid.lines).wait_recv()

        def total(at, below, above):
            result = self.acc[at, :]
            if below:
                result = result + self.zbuf[line, at, :].astype(F32)
            if above:
                result = result + self.zbuf[last + 1, at, :].astype(F32)
            write(at, result)

        for when, below, above in (
            (jnp.logical_and(from_below, from_above), True, True),
            (jnp.logical_not(from_below), False, True),
            (jnp.logical_not(from_above), True, False),
        ):

            @pl.when(when)
            def _():
                self.rows(lambda at: total(at, below, above))

    def drain(self):
        for j in self.order():
            for e in range(1, self.grid.fast):
                self.across(j, e).wait_send()
            if j < self.last:
                self.along(j).wait_send()


def into(ref):
    def write(at, total):
        ref[at, :] = total.astype(ref.dtype)

    return write


class Exchange:
    def __init__(self, grid, src, dst, sems):
        self.grid, self.src, self.dst = grid, src, dst
        self.sent, self.got = sems
        self.size = grid.lines * grid.fast

    @staticmethod
    def semaphores(size):
        return [pltpu.SemaphoreType.DMA((size,)), pltpu.SemaphoreType.DMA((size,))]

    def one(self, k):
        grid = self.grid
        peer = lax.rem(grid.here + k, self.size)
        return grid.copy(
            self.src(peer), self.dst(grid.here), self.sent.at[k], self.got.at[k], peer
        )

    def begin(self):
        for k in range(1, self.size):
            self.one(k).start()

    def arrived(self):
        for k in range(1, self.size):
            self.one(k).wait_recv()

    def drain(self):
        for k in range(1, self.size):
            self.one(k).wait_send()


ANY = pl.BlockSpec(memory_space=pl.ANY)
INSIDE = pl.BlockSpec(memory_space=pltpu.VMEM)


def comm_params(collective_id):
    return pltpu.CompilerParams(
        collective_id=collective_id, has_side_effects=True, vmem_limit_bytes=VMEM_MOST
    )


def grids(shape):
    lines, fast, seq_lines = shape
    return Grid("seg", lines, fast), Grid("seq", seq_lines, 2)


def sum_over_seq(seq, x_ref, out_ref, half, got, mine, others, whole, *sems):
    lane_s, lane_r, line_s, line_r, back_s, back_r = sems
    width = x_ref.shape[1] // 2
    lines = seq.lines
    other = 1 - seq.lane
    left = pl.ds(0, width)
    right = pl.ds(width, width)

    @pl.when(seq.lane == 0)
    def _():
        half[...] = x_ref[:, right].astype(BF16)

    @pl.when(seq.lane == 1)
    def _():
        half[...] = x_ref[:, left].astype(BF16)

    swap = seq.copy(half, got, lane_s, lane_r, seq.at(seq.line, other))
    swap.start()
    swap.wait()

    @pl.when(seq.lane == 0)
    def _():
        mine[...] = (x_ref[:, left] + got[...].astype(F32)).astype(BF16)

    @pl.when(seq.lane == 1)
    def _():
        mine[...] = (x_ref[:, right] + got[...].astype(F32)).astype(BF16)

    copies = [
        seq.copy(
            mine, others.at[k - 1], line_s.at[k], line_r.at[k], seq.at(seq.line_peer(k), seq.lane)
        )
        for k in range(1, lines)
    ]
    for copy in copies:
        copy.start()
    for copy in copies:
        copy.wait()
    total = mine[...].astype(F32)
    for k in range(lines - 1):
        total = total + others[k].astype(F32)
    whole[seq.lane] = total.astype(BF16)
    back = seq.copy(
        whole.at[seq.lane], whole.at[seq.lane], back_s, back_r, seq.at(seq.line, other)
    )
    back.start()
    back.wait()
    out_ref[:, left] = whole[0]
    out_ref[:, right] = whole[1]


def forward_kernel(
    shape, steps, taps,
    low_ref, wdt_ref, params_ref, act_ref, bc_ref, a_ref, init_ref, weight_ref, cot_ref,
    tok_ref, gate_one, gate_src,
    y_ref, pre_ref, check_ref, final_ref, gate_ref, gated_ref, weights_ref, cots_ref, gate_two,
    state, rate_pl, drive_pl, y_pl, w_one, w_two, local_s, *sems,
):
    count = pre_ref.shape[0]
    width, planes, _ = a_ref.shape
    seg, seq = grids(shape)
    gates = Gather(seg, gate_src.at[:, 1], gate_two, sems[:6])
    weights = Gather(seg, weight_ref, weights_ref, sems[6:12])
    cots = Gather(seq, cot_ref, cots_ref, sems[12:])
    step = pl.program_id(0)
    keeps = [
        pltpu.make_async_copy(weight_ref, weights_ref.at[seg.here], local_s.at[0]),
        pltpu.make_async_copy(cot_ref, cots_ref.at[seq.here], local_s.at[1]),
        pltpu.make_async_copy(gate_src.at[:, 1], gate_two.at[seg.here], local_s.at[2]),
    ]
    load_one = pltpu.make_async_copy(gate_one, w_one, local_s.at[3])

    @pl.when(step == 0)
    def _():
        meet((seg, seq))
        gates.begin()
        weights.begin()
        cots.begin()
        for keep in keeps:
            keep.start()
        load_one.start()
        state[...] = init_ref[...]

    lines = params_ref[pl.ds(width, 8), :]
    bias, skip = lines[taps + 1 : taps + 2], lines[taps + 2 : taps + 3]
    pre = dot_tn(low_ref[...], wdt_ref[...]) + bias
    pre_ref[...] = pre
    rate = softplus(pre)
    act = act_ref[...].astype(F32)
    to_planes(rate_pl, rate)
    to_planes(drive_pl, rate * act)
    groups = count // UNROLL

    def group(k, carry):
        at = k * UNROLL
        rates = [rate_pl[k, token_of(planes, i), :] for i in range(UNROLL)]
        drives = [drive_pl[k, token_of(planes, i), :] for i in range(UNROLL)]
        sums = [None] * UNROLL
        for n in range(width):
            a = a_ref[n]
            h = state[n]
            check_ref[k, n] = h
            for i in range(UNROLL):
                h = jnp.exp2(rates[i] * a) * h + bc_ref[at + i, n] * drives[i]
                term = bc_ref[at + i, width + n] * h
                sums[i] = term if n == 0 else sums[i] + term
            state[n] = h
        for i in range(UNROLL):
            y_pl[k, token_of(planes, i), :] = sums[i]
        return carry

    ticks = 2 * steps
    plan = [[] for _ in range(ticks)]
    late = []
    for k in range(1, seg.lines):
        for gather, share in ((gates, 4 * k), (weights, 9 * k)):
            tick = ticks * share // 16
            (plan[tick - 1] if tick < ticks else late).append(functools.partial(gather.step, k))
        if k < seq.lines:
            plan[ticks - 1].append(functools.partial(cots.step, k))

    def part_of_step(h, carry):
        lax.fori_loop(h * (groups // 2), (h + 1) * (groups // 2), group, 0)
        for tick in range(ticks):
            if plan[tick]:

                @pl.when(step * 2 + h == tick)
                def _():
                    for event in plan[tick]:
                        event()

        return carry

    lax.fori_loop(0, 2, part_of_step, 0)
    y_ref[pl.ds(pl.multiple_of(step * count, count), count), :] = (
        from_planes(y_pl) + skip * act_ref[...].astype(F32)
    )

    @pl.when(step == steps - 1)
    def _():
        final_ref[...] = state[...]
        for event in late[:-1]:
            event()
        gates.finish()
        keeps[2].wait()
        load_one.wait()
        load_two = pltpu.make_async_copy(gate_two, w_two, local_s.at[3])
        load_two.start()
        load_two.wait()
        model = tok_ref.shape[1]
        half = w_one.shape[3]
        block = 256

        def gating(i, carry):
            rows = pl.ds(pl.multiple_of(i * block, block), block)
            lines = tok_ref[rows, :].astype(F32)
            rstd = lax.rsqrt(jnp.mean(lines * lines, axis=1, keepdims=True) + EPSILON)
            for j, w in enumerate((w_one, w_two)):
                cols = pl.ds(j * half, half)
                gate = rstd * dot_nn(tok_ref[rows, :], w[...].reshape(model, half))
                sig = sigmoid(gate)
                y_val = y_ref[rows, cols]
                gate_ref[rows, cols] = gate * sig
                gated_ref[rows, cols] = (y_val * gate * sig).astype(BF16)
                y_ref[rows, cols] = rstd * y_val * sig * (1.0 + gate * (1.0 - sig))
            return carry

        blocks = y_ref.shape[0] // block
        lax.fori_loop(0, blocks // 2, gating, 0)
        late[-1]()
        lax.fori_loop(blocks // 2, blocks, gating, 0)
        weights.finish()
        cots.finish()
        for keep in keeps[:2]:
            keep.wait()


def backward_kernel(
    shape, steps, taps,
    pre_ref, act_ref, gy_ref, bc_ref, a_ref, params_ref, check_ref, wdt_ref, low_ref, base_ref,
    first_src, second_src, gated_src, weight_src,
    gact_ref, agrad_ref, start_ref, dtb_ref, sgrad_ref, dtp_ref, mix_ref,
    first_out, second_out, third_out,
    carry_s, rate_pl, drive_pl, gy_pl, grate_pl, thr_pl, prod, part, mix_s,
    gated_in, weight_in, third_src, load_s, *scratch,
):
    count = pre_ref.shape[0]
    width, planes, _ = a_ref.shape
    low_rank = wdt_ref.shape[0]
    seg, seq = grids(shape)
    first = Scatter(seg, first_src, scratch[:10])
    second = Scatter(seg, second_src, scratch[10:20])
    third = Scatter(seq, third_src, scratch[20:28], inside=True)
    loads = [
        pltpu.make_async_copy(gated_src, gated_in, load_s.at[0]),
        pltpu.make_async_copy(weight_src, weight_in, load_s.at[1]),
    ]
    step = pl.program_id(0)

    @pl.when(step == 0)
    def _():
        meet((seg, seq))
        first.begin()
        second.begin()
        for load in loads:
            load.start()
        carry_s[...] = jnp.zeros_like(carry_s)
        agrad_ref[...] = jnp.zeros_like(agrad_ref)
        dtb_ref[...] = jnp.zeros_like(dtb_ref)
        sgrad_ref[...] = jnp.zeros_like(sgrad_ref)
        dtp_ref[...] = jnp.zeros_like(dtp_ref)

    pre = pre_ref[...]
    rate = softplus(pre)
    act = act_ref[...].astype(F32)
    to_planes(rate_pl, rate)
    to_planes(drive_pl, rate * act)
    to_planes(gy_pl, gy_ref[...])
    groups = count // UNROLL

    def group(j, carry):
        k = groups - 1 - j
        at = k * UNROLL
        rates = [rate_pl[k, token_of(planes, i), :] for i in range(UNROLL)]
        drives = [drive_pl[k, token_of(planes, i), :] for i in range(UNROLL)]
        gys = [gy_pl[k, token_of(planes, i), :] for i in range(UNROLL)]
        g_rate = [None] * UNROLL
        through = [None] * UNROLL
        for n in range(width):
            a = a_ref[n]
            states = [check_ref[k, n]]
            decays = []
            for i in range(UNROLL):
                decays.append(jnp.exp2(rates[i] * a))
                states.append(decays[i] * states[i] + bc_ref[at + i, n] * drives[i])
            lam = carry_s[n]
            acc = agrad_ref[n]
            for i in reversed(range(UNROLL)):
                lam = lam + bc_ref[at + i, width + n] * gys[i]
                b_term = bc_ref[at + i, n] * lam
                region = (i * 2 * width + n) // 8
                prod[region, token_of(planes, n % 8), :] = lam * drives[i]
                prod[region + width // 8, token_of(planes, n % 8), :] = states[i + 1] * gys[i]
                lam = decays[i] * lam
                weighted = lam * states[i]
                acc = acc + weighted * rates[i]
                a_term = weighted * a
                g_rate[i] = a_term if n == 0 else g_rate[i] + a_term
                through[i] = b_term if n == 0 else through[i] + b_term
            carry_s[n] = lam
            agrad_ref[n] = acc
        for i in range(UNROLL):
            grate_pl[k, token_of(planes, i), :] = g_rate[i]
            thr_pl[k, token_of(planes, i), :] = through[i]
            for q in range(2 * width // 8):
                region = i * 2 * width // 8 + q
                total = prod[region, pl.ds(0, 8), :]
                for s in range(1, planes):
                    total = total + prod[region, pl.ds(s * 8, 8), :]
                row = pl.multiple_of((at + i) * 2 * width + q * 8, 8)
                part[pl.ds(row, 8), :] = total
        return carry

    events = [functools.partial(s.middle, k) for s in (first, second) for k in s.order()]
    ticks = 2 * steps
    plan = [[] for _ in range(ticks)]
    for j, event in enumerate(events):
        plan[min(ticks - 1, ticks * (j + 1) // len(events))].append(event)

    def output(index):
        own_len, model = third_src.shape[1:]
        rows = pl.ds(pl.multiple_of(index * own_len, own_len), own_len)

        def column(c, carry):
            cols = pl.ds(pl.multiple_of(c * 512, 512), 512)
            third_src[index, :, cols] = dot_nn(gated_in[rows, :], weight_in[:, cols]).astype(BF16)
            return carry

        lax.fori_loop(0, model // 512, column, 0)

    def outputs():
        for load in loads:
            load.wait()

        def leave(j, carry):
            output(third.index(j, 1))
            third.across(j, 1).start()
            return carry

        def stay(j, carry):
            output(third.index(j, 0))
            return carry

        lax.fori_loop(0, seq.lines, leave, 0)
        lax.fori_loop(0, seq.lines, stay, 0)

    plan[0].append(outputs)
    for j in third.order():
        plan[min(ticks - 1, 5 + 2 * j)].append(functools.partial(third.middle, j))

    def add_base(at, total):
        third_out[at, :] = (total + base_ref[at, :].astype(F32)).astype(BF16)

    plan[min(ticks - 1, 13)].append(functools.partial(third.finish, add_base))

    def part_of_step(h, carry):
        lax.fori_loop(h * (groups // 2), (h + 1) * (groups // 2), group, 0)
        for tick in range(ticks - 1):
            if plan[tick]:

                @pl.when(step * 2 + h == tick)
                def _():
                    for event in plan[tick]:
                        event()

        return carry

    lax.fori_loop(0, 2, part_of_step, 0)
    g_rate = from_planes(grate_pl) * (1.0 / LOG2E)
    through = from_planes(thr_pl)
    pre = pre_ref[...]
    rate = softplus(pre)
    act = act_ref[...].astype(F32)
    gy = gy_ref[...]
    g_dtpre = ((g_rate + act * through) * sigmoid(pre)).astype(BF16)
    skip = params_ref[pl.ds(width, 8), :][taps + 2 : taps + 3]
    gact_ref[...] = gy * skip + rate * through
    dtb_ref[...] += jnp.sum(g_dtpre.astype(F32), axis=0, keepdims=True)
    sgrad_ref[...] += jnp.sum(gy * act, axis=0, keepdims=True)
    dtp_ref[...] += dot_nn(low_ref[...], g_dtpre)
    rows = 2 * width
    ones = jnp.ones((LANES, LANES), F32)
    sums = jnp.dot(part[...], ones, preferred_element_type=F32)
    sums = sums.reshape(count, rows, LANES)
    pick = lax.broadcasted_iota(jnp.int32, (1, rows, LANES), 1) == lax.broadcasted_iota(
        jnp.int32, (1, rows, LANES), 2
    )
    g_bc = jnp.sum(jnp.where(pick, sums, 0.0), axis=1)
    tokens_at = pl.ds(pl.multiple_of((steps - 1 - step) * count, count), count)
    mix_s[pl.ds(0, low_rank), tokens_at] = dot_nt(wdt_ref[...], g_dtpre)
    mix_s[pl.ds(low_rank, rows), tokens_at] = g_bc.T[:rows]

    @pl.when(step == steps - 1)
    def _():
        start_ref[...] = carry_s[...]
        sum_over_seq(seq, mix_s, mix_ref, *scratch[28:])
        for event in plan[ticks - 1]:
            event()
        first.finish(into(first_out))
        second.finish(into(second_out))
        for scatter in (first, second, third):
            scatter.drain()


def forward_scan(
    shape, taps, low, w_dt, params, act, bc, a2, init, weight, cot, tok, gate_one, gate_part, block
):
    lines, fast, seq_lines = shape
    length, features = act.shape
    width, planes, _ = a2.shape
    low_rank = w_dt.shape[0]
    steps = length // block
    rows = pl.BlockSpec((block, features), lambda i: (i, 0))
    one = pl.Buffered(1)

    def whole(*dims):
        return pl.BlockSpec(dims, lambda i: (0,) * len(dims), pipeline_mode=one)

    plane = pltpu.VMEM((block // UNROLL, planes * UNROLL, LANES), F32)
    return pl.pallas_call(
        functools.partial(forward_kernel, shape, steps, taps),
        grid=(steps,),
        in_specs=[
            pl.BlockSpec((low_rank, block), lambda i: (0, i)),
            whole(low_rank, features), whole(*params.shape), rows,
            pl.BlockSpec((block, 2 * width), lambda i: (i, 0), memory_space=pltpu.SMEM),
            whole(width, planes, LANES), whole(width, planes, LANES),
            whole(*weight.shape), whole(*cot.shape), whole(*tok.shape), ANY, ANY,
        ],
        out_specs=[
            whole(length, features), rows,
            pl.BlockSpec((block // UNROLL, width, planes, LANES), lambda i: (i, 0, 0, 0)),
            whole(width, planes, LANES), whole(length, features), whole(length, features),
            ANY, ANY, ANY,
        ],
        out_shape=[
            jax.ShapeDtypeStruct((length, features), F32),
            jax.ShapeDtypeStruct((length, features), F32),
            jax.ShapeDtypeStruct((length // UNROLL, width, planes, LANES), F32),
            jax.ShapeDtypeStruct((width, planes, LANES), F32),
            jax.ShapeDtypeStruct((length, features), F32),
            jax.ShapeDtypeStruct((length, features), BF16),
            jax.ShapeDtypeStruct((lines * fast,) + weight.shape, BF16),
            jax.ShapeDtypeStruct((seq_lines * 2,) + cot.shape, BF16),
            jax.ShapeDtypeStruct(gate_one.shape, BF16),
        ],
        scratch_shapes=[
            pltpu.VMEM((width, planes, LANES), F32), plane, plane, plane,
            pltpu.VMEM(gate_one.shape, BF16), pltpu.VMEM(gate_one.shape, BF16),
            pltpu.SemaphoreType.DMA((4,)),
            *Gather.semaphores(lines, fast), *Gather.semaphores(lines, fast),
            *Gather.semaphores(seq_lines, 2),
        ],
        compiler_params=comm_params(5),
        cost_estimate=pl.CostEstimate(
            flops=8 * length * features * width,
            bytes_accessed=24 * length * features,
            transcendentals=length * features * width,
        ),
        name="scan_forward",
    )(low, w_dt, params, act, bc, a2, init, weight, cot, tok, gate_one, gate_part)


def backward_scan(
    shape, taps, pre, act, gy, bc, a2, params, checks, w_dt, dt_low, base, first, second, gated, weight,
    block,
):
    lines, fast, seq_lines = shape
    length, features = pre.shape
    width, planes, _ = a2.shape
    low_rank = w_dt.shape[0]
    steps = length // block
    rows = pl.BlockSpec((block, features), lambda i: (steps - 1 - i, 0))
    whole = pl.BlockSpec((width, planes, LANES), lambda i: (0, 0, 0))

    def all_of(rows, columns):
        return pl.BlockSpec((rows, columns), lambda i: (0, 0))

    line = all_of(1, features)
    plane = pltpu.VMEM((block // UNROLL, planes * UNROLL, LANES), F32)
    mixed = (low_rank + 2 * width, length)
    return pl.pallas_call(
        functools.partial(backward_kernel, shape, steps, taps),
        grid=(steps,),
        in_specs=[
            rows, rows, rows,
            pl.BlockSpec(
                (block, 2 * width), lambda i: (steps - 1 - i, 0), memory_space=pltpu.SMEM
            ),
            whole, all_of(*params.shape),
            pl.BlockSpec(
                (block // UNROLL, width, planes, LANES), lambda i: (steps - 1 - i, 0, 0, 0)
            ),
            all_of(low_rank, features),
            pl.BlockSpec((low_rank, block), lambda i: (0, steps - 1 - i)),
            all_of(*base.shape),
            ANY, ANY, ANY, ANY,
        ],
        out_specs=[
            rows, whole, whole, line, line, all_of(low_rank, features), all_of(*mixed),
            all_of(*first.shape[1:]), all_of(*second.shape[1:]), all_of(*base.shape),
        ],
        out_shape=[
            jax.ShapeDtypeStruct((length, features), F32),
            jax.ShapeDtypeStruct((width, planes, LANES), F32),
            jax.ShapeDtypeStruct((width, planes, LANES), F32),
            jax.ShapeDtypeStruct((1, features), F32),
            jax.ShapeDtypeStruct((1, features), F32),
            jax.ShapeDtypeStruct((low_rank, features), F32),
            jax.ShapeDtypeStruct(mixed, BF16),
            jax.ShapeDtypeStruct(first.shape[1:], BF16),
            jax.ShapeDtypeStruct(second.shape[1:], F32),
            jax.ShapeDtypeStruct(base.shape, BF16),
        ],
        scratch_shapes=[pltpu.VMEM((width, planes, LANES), F32)]
        + [plane] * 5
        + [
            pltpu.VMEM((UNROLL * 2 * width // 8, planes * 8, LANES), F32),
            pltpu.VMEM((block * 2 * width, LANES), F32),
            pltpu.VMEM(mixed, F32),
            pltpu.VMEM(gated.shape, BF16),
            pltpu.VMEM(weight.shape, BF16),
            pltpu.VMEM((2 * seq_lines,) + base.shape, BF16),
            pltpu.SemaphoreType.DMA((2,)),
            *Scatter.scratch(lines, fast, first.shape[1:]),
            *Scatter.scratch(lines, fast, second.shape[1:]),
            *Scatter.scratch(seq_lines, 2, base.shape, inside=True),
            *sum_scratch(seq_lines, *mixed),
        ],
        compiler_params=comm_params(6),
        cost_estimate=pl.CostEstimate(
            flops=20 * length * features * width,
            bytes_accessed=28 * length * features,
            transcendentals=length * features * width,
        ),
        name="scan_backward",
    )(pre, act, gy, bc, a2, params, checks, w_dt, dt_low, base, first, second, gated, weight)


def finish_kernel(shape, taps, history, refs, scratch):
    (
        gact, x_in, act, tok, w_x, w_g, w_h, gs_gate,
        mix, w_xt, head, params, dtp, a_sum, dtb, sgrad, g_half, own_tok, own_cot,
        final, start,
        small_out, halves_out, input_out, ends_out,
    ) = refs
    (
        gc, xb, actb, tokb, wxb, wgb, gsg, gs_x, xg, xh, q_src, pack, small_src, ends_src, x_half,
        in_s, own_s,
    ) = scratch[:17]
    seg, seq = grids(shape)
    length, feats = act.shape
    width = a_sum.shape[0]
    kern = params.at[pl.ds(width, 8)]
    b_conv = params.at[pl.ds(width + taps, 1)]
    at = 17
    sets = []
    for size in (8, 8, 8, 8):
        sets.append(scratch[at : at + size])
        at += size
    swaps_s = [scratch[at + 2 * i : at + 2 * i + 2] for i in range(3)]
    small = Scatter(seg, small_src, sets[0], inside=True)
    x_sums = [
        Scatter(seg, xg, sets[1], inside=True), Scatter(seg, xh, sets[2], inside=True)
    ]
    q_sum = Scatter(seq, q_src, sets[3], inside=True)
    loads = [
        pltpu.make_async_copy(gact, gc.at[pl.ds(0, length)], in_s.at[0]),
        pltpu.make_async_copy(x_in, xb.at[pl.ds(8, length)], in_s.at[1]),
        pltpu.make_async_copy(tok, tokb, in_s.at[2]),
        pltpu.make_async_copy(act, actb, in_s.at[3]),
        pltpu.make_async_copy(gs_gate, gsg, in_s.at[4]),
        pltpu.make_async_copy(w_g, wgb.at[0], in_s.at[5]),
        pltpu.make_async_copy(w_h, wgb.at[1], in_s.at[6]),
        pltpu.make_async_copy(w_x, wxb, in_s.at[7]),
    ]
    for load in loads:
        load.start()
    meet((seg, seq))
    own_rows = g_half.shape[0] // (seq.lines * seq.fast)

    def swap(half, src, sems):
        return Exchange(
            seq,
            lambda p: src.at[pl.ds(pl.multiple_of(p * own_rows, own_rows), own_rows)],
            lambda m: halves_out.at[half, m],
            sems,
        )

    swap_g = swap(1, g_half, swaps_s[1])
    swap_g.begin()
    xb[pl.ds(0, 8), :] = head[...]
    gc[pl.ds(length, 8), :] = jnp.zeros((8, feats), F32)
    loads[0].wait()
    big = LANES

    def add_mixed(i, carry):
        rows = pl.ds(pl.multiple_of(i * big, big), big)
        gc[rows, :] += dot_tn(mix[:, rows], w_xt[...])
        return carry

    lax.fori_loop(0, length // big, add_mixed, 0)
    loads[1].wait()
    tall = 32
    chunk = feats // 2
    sums_at = 8 * (taps + 1)
    pack[...] = jnp.zeros_like(pack)

    def through_conv(side, i, carry):
        t0 = pl.multiple_of(i * tall, tall)
        for c in (side * chunk,):
            cols = pl.ds(c, chunk)
            wide = xb[pl.ds(t0, tall + 8), cols]
            rows = [wide[8 - history + k : 8 - history + k + tall] for k in range(taps)]
            conv = b_conv[:, cols]
            for k in range(taps):
                conv = conv + kern[pl.ds(k, 1), cols] * rows[k]
            sig = sigmoid(conv)
            g_conv = gc[pl.ds(t0, tall), cols] * sig * (1.0 + conv * (1.0 - sig))
            gc[pl.ds(t0, tall), cols] = g_conv
            for k in range(taps):
                term = g_conv * rows[k]
                pack[pl.ds(8 * k, 8), cols] += sum(
                    term[8 * j : 8 * j + 8] for j in range(tall // 8)
                )
            pack[pl.ds(8 * taps, 8), cols] += sum(
                g_conv[8 * j : 8 * j + 8] for j in range(tall // 8)
            )
        return carry

    loads[2].wait()

    def to_input(side, i, carry):
        t0 = pl.multiple_of(i * tall, tall)
        lines = tokb[pl.ds(t0, tall), :].astype(F32)
        rstd = lax.rsqrt(jnp.mean(lines * lines, axis=1, keepdims=True) + EPSILON)
        for c in (side * chunk,):
            cols = pl.ds(c, chunk)
            wide = gc[pl.ds(t0, tall + 8), cols]
            g_x = kern[pl.ds(0, 1), cols] * wide[history : history + tall]
            for k in range(1, taps):
                g_x = g_x + kern[pl.ds(k, 1), cols] * wide[history - k : history - k + tall]
            gs_x[pl.ds(t0, tall), cols] = (rstd * g_x).astype(BF16)
        return carry

    block_rows = xg.shape[1]
    by_block = block_rows % LANES == 0

    def partial(side, index):
        cols = pl.ds(pl.multiple_of(index * block_rows, block_rows), block_rows)
        x_sums[side].src[index] = dot_tn(
            tokb[:, cols], gs_x[:, pl.ds(side * chunk, chunk)]
        ).astype(BF16)

    def one_side(side):
        lax.fori_loop(0, length // tall, functools.partial(through_conv, side), 0)
        lax.fori_loop(0, length // tall, functools.partial(to_input, side), 0)
        if not by_block:

            def several(i, carry):
                cols = pl.ds(pl.multiple_of(i * LANES, LANES), LANES)
                got = dot_tn(tokb[:, cols], gs_x[:, pl.ds(side * chunk, chunk)])
                each = LANES // block_rows
                for p in range(each):
                    rows = slice(p * block_rows, (p + 1) * block_rows)
                    x_sums[side].src[i * each + p] = got[rows].astype(BF16)
                return carry

            lax.fori_loop(0, tokb.shape[1] // LANES, several, 0)

        def leave(j, carry):
            for e in range(1, seg.fast):
                if by_block:
                    partial(side, x_sums[side].index(j, e))
                x_sums[side].across(j, e).start()
            return carry

        lax.fori_loop(0, seg.lines, leave, 0)

    def stay(side, j, carry):
        if by_block:
            partial(side, x_sums[side].index(j, 0))
        return carry

    one_side(0)
    one_side(1)
    loads[3].wait()
    low_rank = dtp.shape[0]
    mixes = mix.shape[0]
    part = small_src.shape[2]
    a_grad = from_states(a_sum) * params[pl.ds(0, width), :]
    xp = dot_nn(mix[...], actb[...])
    for g in range(small_src.shape[0]):
        cols = slice(g * part, (g + 1) * part)
        small_src[g, pl.ds(0, low_rank), :] = dtp[:, cols].astype(BF16)
        small_src[g, pl.ds(low_rank, mixes), :] = xp[:, cols].astype(BF16)
        base = low_rank + mixes
        small_src[g, pl.ds(base, width), :] = a_grad[:, cols].astype(BF16)
        lines = [
            jnp.sum(pack[pl.ds(8 * k, 8), cols], axis=0, keepdims=True) for k in range(taps + 1)
        ]
        lines += [dtb[:, cols], sgrad[:, cols]]
        lines.append(jnp.zeros((16 - len(lines), part), F32))
        small_src[g, pl.ds(base + width, 16), :] = jnp.concatenate(lines, axis=0).astype(BF16)
    small.begin()

    lax.fori_loop(0, seg.lines, functools.partial(stay, 0), 0)
    ends_in = jnp.concatenate(
        [
            from_states(final),
            xb[pl.ds(length, 8), :][8 - history :],
            from_states(start),
            sum_head(gc, kern, history, taps),
            jnp.zeros((ends_src.shape[1] - 2 * (width + history), feats), F32),
        ],
        axis=0,
    )
    piece = ends_src.shape[2]
    for p in range(ends_src.shape[0]):
        ends_src[p] = ends_in[:, p * piece : (p + 1) * piece]
    end_swap = Exchange(seq, lambda p: ends_src.at[p], lambda m: ends_out.at[m], swaps_s[2])
    end_swap.begin()
    loads[4].wait()
    loads[5].wait()
    loads[6].wait()
    loads[7].wait()
    own_len = own_tok.shape[0]
    model = own_tok.shape[1]
    wide = 512
    half = feats // 2

    def normed(index):
        rows = pl.ds(pl.multiple_of(index * own_len, own_len), own_len)

        def column(c, carry):
            cols = pl.ds(pl.multiple_of(c * wide, wide), wide)
            q_src[index, :, cols] = (
                dot_nt(gsg[rows, pl.ds(0, half)], wgb[0, cols, :])
                + dot_nt(gsg[rows, pl.ds(half, half)], wgb[1, cols, :])
                + dot_nt(gs_x[rows, :], wxb[cols, :])
            ).astype(BF16)
            return carry

        lax.fori_loop(0, model // wide, column, 0)

    def leave_q(j):
        normed(q_sum.index(j, 1))
        q_sum.across(j, 1).start()

    rest = [functools.partial(leave_q, j) for j in q_sum.order()]
    rest += [lambda j=j: normed(q_sum.index(j, 0)) for j in q_sum.order()]
    turns = x_sums[0].order()
    for j in turns:
        x_sums[0].middle(j)
        for work in rest[j * len(rest) // len(turns) : (j + 1) * len(rest) // len(turns)]:
            work()
        if j == 0:
            lax.fori_loop(0, seg.lines, functools.partial(stay, 1), 0)
    for j in q_sum.order():
        q_sum.middle(j)
    for j in x_sums[1].order():
        x_sums[1].middle(j)
    for j in small.order():
        small.middle(j)

    def input_grad(at, total):
        own = own_tok[at, :].astype(F32)
        square = 1.0 / (jnp.mean(own * own, axis=1, keepdims=True) + EPSILON)
        input_out[at, :] = (
            own_cot[at, :].astype(F32)
            + total
            - own * (square * jnp.mean(total * own, axis=1, keepdims=True))
        ).astype(BF16)

    for side in (0, 1):

        def put(at, total):
            x_half[at, pl.ds(side * chunk, chunk)] = total.astype(BF16)

        x_sums[side].finish(put)
    swap_x = swap(0, x_half, swaps_s[0])
    swap_x.begin()
    q_sum.finish(input_grad)
    small.finish(into(small_out))
    own = pl.ds(pl.multiple_of(seq.here * own_rows, own_rows), own_rows)
    keeps = [
        pltpu.make_async_copy(x_half.at[own], halves_out.at[0, seq.here], own_s.at[0]),
        pltpu.make_async_copy(g_half.at[own], halves_out.at[1, seq.here], own_s.at[1]),
        pltpu.make_async_copy(ends_src.at[seq.here], ends_out.at[seq.here], own_s.at[2]),
    ]
    for keep in keeps:
        keep.start()
    for scatter in (small, *x_sums, q_sum):
        scatter.drain()
    for exchange in (swap_g, end_swap, swap_x):
        exchange.arrived()
        exchange.drain()
    for keep in keeps:
        keep.wait()


def from_states(ref):
    return jnp.concatenate([ref[:, s, :] for s in range(ref.shape[1])], axis=1)


def sum_head(gc, kern, history, taps):
    top = gc[pl.ds(0, 8), :]
    rows = []
    for j in range(history):
        rows.append(
            sum(kern[pl.ds(k, 1), :] * top[j - k : j - k + 1] for k in range(min(j + 1, taps)))
        )
    return jnp.concatenate(rows, axis=0)


def finish_all(shape, taps, history, big, small):
    lines, fast, seq_lines = shape
    segs, seqs = lines * fast, seq_lines * 2
    gact, x_in, act, tok, w_x, w_g, w_h, gs_gate = big
    mix, w_xt, head, params, dtp, a_sum, dtb, sgrad, g_half, own_tok, own_cot = small[:11]
    length, feats = act.shape
    own_len, model = own_tok.shape
    width = a_sum.shape[0]
    rows = dtp.shape[0] + mix.shape[0] + width + 16
    block_rows = model // segs
    own_rows = g_half.shape[0] // seqs
    ends = (seqs, 2 * (width + history) + (-2 * (width + history)) % 8, feats // seqs)
    dma = pltpu.SemaphoreType.DMA
    scratch = [
        pltpu.VMEM((length + 8, feats), F32),
        pltpu.VMEM((length + 8, feats), F32),
        pltpu.VMEM((length, feats), BF16),
        pltpu.VMEM((length, model), BF16),
        pltpu.VMEM((model, feats), BF16),
        pltpu.VMEM((2, model, feats // 2), BF16),
        pltpu.VMEM((length, feats), BF16),
        pltpu.VMEM((length, feats), BF16),
        pltpu.VMEM((segs, block_rows, feats // 2), BF16),
        pltpu.VMEM((segs, block_rows, feats // 2), BF16),
        pltpu.VMEM((seqs, own_len, model), BF16),
        pltpu.VMEM((8 * (taps + 1), feats), F32),
        pltpu.VMEM((segs, rows, feats // segs), BF16),
        pltpu.VMEM(ends, F32),
        pltpu.VMEM((block_rows, feats), BF16),
        dma((8,)), dma((3,)),
        *Scatter.scratch(lines, fast, (rows, feats // segs), inside=True),
        *Scatter.scratch(lines, fast, (block_rows, feats // 2), inside=True),
        *Scatter.scratch(lines, fast, (block_rows, feats // 2), inside=True),
        *Scatter.scratch(seq_lines, 2, (own_len, model), inside=True),
        *Exchange.semaphores(seqs), *Exchange.semaphores(seqs), *Exchange.semaphores(seqs),
    ]

    def kernel(*refs):
        finish_kernel(shape, taps, history, refs[:25], refs[25:])

    return pl.pallas_call(
        kernel,
        in_specs=[ANY] * 8 + [INSIDE] * 13,
        out_specs=[INSIDE] * 4,
        out_shape=[
            jax.ShapeDtypeStruct((rows, feats // segs), F32),
            jax.ShapeDtypeStruct((2, seqs, own_rows, feats), BF16),
            jax.ShapeDtypeStruct((own_len, model), BF16),
            jax.ShapeDtypeStruct(ends, F32),
        ],
        scratch_shapes=scratch,
        compiler_params=comm_params(4),
        name="finish",
    )(*big, *small)


def gather_kernel(
    shape, scaled_x, scaled_g, small, tokens, w_x, small_all, tok, g_part, x_part, tok_in, g_own,
    local_s, small_sems, tok_sems, swap_x, swap_g, x_sems,
):
    seg, seq = grids(shape)
    size = seq.lines * seq.fast
    load_tok = pltpu.make_async_copy(tokens, tok_in, local_s.at[0])
    load_own = pltpu.make_async_copy(scaled_x.at[seq.here], x_part.at[seq.here], local_s.at[1])
    load_gate = pltpu.make_async_copy(scaled_g.at[seq.here], g_own, local_s.at[3])
    load_tok.start()
    load_own.start()
    load_gate.start()
    meet((seg, seq))
    swap_x = Exchange(seq, lambda p: scaled_x.at[p], lambda m: x_part.at[m], swap_x)
    swap_g = Exchange(seq, lambda p: scaled_g.at[p], lambda m: g_part.at[m], swap_g)
    swap_x.begin()
    pieces = []
    for k in range(size):
        place = lax.rem(seq.here - k + size, size)
        pieces.append(Gather(seg, x_part.at[place], w_x, x_sems[6 * k : 6 * k + 6], place))
    smalls = Gather(seg, small, small_all, small_sems)
    load_own.wait()
    pieces[0].begin()
    smalls.begin()
    load_tok.wait()
    toks = Gather(seq, tok_in, tok, tok_sems)
    for k in range(1, size):
        swap_x.one(k).wait_recv()
        pieces[k].begin()
    toks.begin()
    swap_g.begin()
    load_gate.wait()
    keeps = [
        pltpu.make_async_copy(tok_in, tok.at[seq.here], local_s.at[0]),
        pltpu.make_async_copy(x_part, w_x.at[seg.here], local_s.at[1]),
        pltpu.make_async_copy(small, small_all.at[seg.here], local_s.at[2]),
        pltpu.make_async_copy(g_own, g_part.at[seq.here], local_s.at[3]),
    ]
    for keep in keeps:
        keep.start()
    for k in range(1, max(seg.lines, seq.lines)):
        if k < seg.lines:
            pieces[0].step(k)
            smalls.step(k)
            for piece in pieces[1:]:
                piece.step(k)
        if k < seq.lines:
            toks.step(k)
    toks.finish()
    smalls.finish()
    for piece in pieces:
        piece.finish()
    swap_g.arrived()
    swap_x.drain()
    swap_g.drain()
    for keep in keeps:
        keep.wait()


def gather_start(shape, scaled_x, scaled_g, small, tokens):
    lines, fast, seq_lines = shape
    segs, seqs = lines * fast, seq_lines * 2
    rows, feats = scaled_x.shape[1:]
    sems = Gather.semaphores

    def kernel(*refs):
        ins, rest = refs[:11], refs[11:]
        gather_kernel(
            shape, *ins, rest[0], rest[1:7], rest[7:13], rest[13:15], rest[15:17], rest[17:]
        )

    w_x, small_all, tok, g_part = pl.pallas_call(
        kernel,
        in_specs=[ANY, ANY, INSIDE, ANY],
        out_specs=[ANY] * 4,
        out_shape=[
            jax.ShapeDtypeStruct((segs, seqs, rows, feats), BF16),
            jax.ShapeDtypeStruct((segs,) + small.shape, BF16),
            jax.ShapeDtypeStruct((seqs,) + tokens.shape, BF16),
            jax.ShapeDtypeStruct((seqs,) + scaled_g.shape[1:], BF16),
        ],
        scratch_shapes=[
            pltpu.VMEM((seqs, rows, feats), BF16),
            pltpu.VMEM(tokens.shape, BF16),
            pltpu.VMEM(scaled_g.shape[1:], BF16),
            pltpu.SemaphoreType.DMA((4,)),
            *sems(lines, fast), *sems(seq_lines, 2),
            *Exchange.semaphores(seqs), *Exchange.semaphores(seqs),
            *(sems(lines, fast) * seqs),
        ],
        compiler_params=comm_params(1),
        name="gather_start",
    )(scaled_x, scaled_g, small, tokens)
    return w_x.reshape(-1, feats), small_all, tok.reshape(-1, tokens.shape[1]), g_part


def front_kernel(
    shape, steps, taps, history, width,
    tok_ref, wx_ref, small_ref, head_ref, gate_src,
    x_ref, act_ref, wdt_ref, wxt_ref, par_ref, a2_ref, low_ref, bc_ref, gate_out,
    xb, mix_s, mix, local_s, *scratch,
):
    seg, seq = grids(shape)
    step = pl.program_id(0)
    gates = Gather(seg, gate_src.at[:, 0], gate_out, scratch[:6])
    count = tok_ref.shape[0]
    low_rank = wdt_ref.shape[0]
    mixes = wxt_ref.shape[0]
    feats = wx_ref.shape[1]
    part = small_ref.shape[2]

    @pl.when(step == 0)
    def _():
        meet((seg, seq))
        gates.begin()
        xb[pl.ds(0, 8), :] = head_ref[...]
        for g in range(small_ref.shape[0]):
            cols = slice(g * part, (g + 1) * part)
            wdt_ref[:, cols] = small_ref[g, pl.ds(0, low_rank), :]
            wxt_ref[:, cols] = small_ref[g, pl.ds(low_rank, mixes), :]
            rest = small_ref[g, pl.ds(low_rank + mixes, width + 16), :].astype(F32)
            par_ref[:, cols] = rest
        a_mat = -jnp.exp(par_ref[pl.ds(0, width), :])
        par_ref[pl.ds(0, width), :] = a_mat
        for s in range(feats // LANES):
            a2_ref[:, s, :] = a_mat[:, s * LANES : (s + 1) * LANES] * LOG2E

    kern = par_ref[pl.ds(width, 8), :]
    rows = tok_ref[...].astype(F32)
    rstd = lax.rsqrt(jnp.mean(rows * rows, axis=1, keepdims=True) + EPSILON)
    x_in = rstd * dot_nn(tok_ref[...], wx_ref[...])
    x_ref[...] = x_in
    xb[pl.ds(8, count), :] = x_in
    tall = 32
    chunk = min(512, feats)

    def through_conv(i, carry):
        t0 = pl.multiple_of(i * tall, tall)
        for c in range(0, feats, chunk):
            cols = slice(c, c + chunk)
            wide = xb[pl.ds(t0, tall + 8), pl.ds(c, chunk)]
            conv = kern[taps : taps + 1, cols]
            for k in range(taps):
                conv = conv + kern[k : k + 1, cols] * wide[8 - history + k : 8 - history + k + tall]
            act_ref[pl.ds(t0, tall), pl.ds(c, chunk)] = (conv * sigmoid(conv)).astype(BF16)
        return carry

    lax.fori_loop(0, count // tall, through_conv, 0)
    xb[pl.ds(0, 8), :] = xb[pl.ds(count, 8), :]
    mix_s[:, pl.ds(pl.multiple_of(step * count, count), count)] = dot_nt(wxt_ref[...], act_ref[...])
    for k in range(1, seg.lines - 1):

        @pl.when(step == min(steps - 1, 2 * k - 1))
        def _():
            gates.step(k)

    @pl.when(step == steps - 1)
    def _():
        sum_over_seq(seq, mix_s, mix, *scratch[6:])
        low_ref[...] = mix[pl.ds(0, low_rank), :]
        bc_ref[...] = mix[pl.ds(low_rank, 2 * width), :].astype(F32).T
        gates.step(seg.lines - 1)
        keep = pltpu.make_async_copy(gate_src.at[:, 0], gate_out.at[seg.here], local_s)
        keep.start()
        gates.finish()
        keep.wait()


def front(shape, taps, history, width, tok, w_x, small_all, head, gate_part, block):
    lines, fast, seq_lines = shape
    segs, seqs = lines * fast, seq_lines * 2
    length, model = tok.shape
    feats = w_x.shape[1]
    low_rank = LANES
    mixes = low_rank + 2 * width
    steps = length // block

    def whole(*dims):
        return pl.BlockSpec(dims, lambda i: (0,) * len(dims))

    def rows(columns):
        return pl.BlockSpec((block, columns), lambda i: (i, 0))

    one = pl.Buffered(1)
    return pl.pallas_call(
        functools.partial(front_kernel, shape, steps, taps, history, width),
        grid=(steps,),
        in_specs=[
            rows(model),
            pl.BlockSpec((model, feats), lambda i: (0, 0), pipeline_mode=one),
            whole(*small_all.shape), whole(*head.shape), ANY,
        ],
        out_specs=[
            rows(feats), rows(feats), whole(low_rank, feats), whole(mixes, feats),
            whole(width + 16, feats), whole(width, feats // LANES, LANES),
            whole(low_rank, length), whole(length, 2 * width), ANY,
        ],
        out_shape=[
            jax.ShapeDtypeStruct((length, feats), F32),
            jax.ShapeDtypeStruct((length, feats), BF16),
            jax.ShapeDtypeStruct((low_rank, feats), BF16),
            jax.ShapeDtypeStruct((mixes, feats), BF16),
            jax.ShapeDtypeStruct((width + 16, feats), F32),
            jax.ShapeDtypeStruct((width, feats // LANES, LANES), F32),
            jax.ShapeDtypeStruct((low_rank, length), BF16),
            jax.ShapeDtypeStruct((length, 2 * width), F32),
            jax.ShapeDtypeStruct((segs, seqs) + gate_part.shape[2:], BF16),
        ],
        scratch_shapes=[
            pltpu.VMEM((block + 8, feats), F32),
            pltpu.VMEM((mixes, length), F32),
            pltpu.VMEM((mixes, length), BF16),
            pltpu.SemaphoreType.DMA,
            *Gather.semaphores(lines, fast),
            *sum_scratch(seq_lines, mixes, length),
        ],
        compiler_params=comm_params(2),
        name="front",
    )(tok, w_x, small_all, head, gate_part)


def sum_scratch(seq_lines, rows, width):
    part = pltpu.VMEM((rows, width // 2), BF16)
    dma = pltpu.SemaphoreType.DMA
    return [
        part, part, part,
        pltpu.VMEM((max(seq_lines - 1, 1), rows, width // 2), BF16),
        pltpu.VMEM((2, rows, width // 2), BF16),
        dma, dma, dma((seq_lines,)), dma((seq_lines,)), dma, dma,
    ]


def unpack_kernel(
    seqs, taps, history, low_rank, width,
    small, halves, ends, mixed, input_grad, out_grad, weight, gain,
    mixed_o, final_o, final_c, input_o, start_o, start_c, gain_o, in_o, cw_o, cb_o, xp_o, dtp_o,
    dtb_o, a_o, skip_o, out_o,
):
    mixed_o[0] = mixed[...]
    input_o[0] = input_grad[...]
    out_o[...] = out_grad[...]
    part = small.shape[1]
    columns = xp_o.shape[0]
    dtp_o[...] = small[pl.ds(0, low_rank), :]
    xp_o[...] = small[pl.ds(low_rank, columns), :]
    at = low_rank + columns
    a_o[...] = small[pl.ds(at, width), :]
    lines = small[pl.ds(at + width, 16), :]
    cw_o[...] = lines[:taps]
    cb_o[...] = lines[taps]
    dtb_o[...] = lines[taps + 1]
    skip_o[...] = lines[taps + 2]
    each = final_o.shape[2] // part // seqs
    for s in range(seqs):
        rows = ends[s]
        for g in range(each):
            got = rows[:, g * part : (g + 1) * part]
            cols = pl.ds((g * seqs + s) * part, part)
            final_o[0, :, cols] = got[:width]
            start_o[0, :, cols] = got[width + history : 2 * width + history]
            for r in range(history):
                final_c[r, :, cols] = got[width + r : width + r + 1]
                at = 2 * width + history + r
                start_c[r, :, cols] = got[at : at + 1]
    scale = gain[...]
    total = jnp.zeros((in_o.shape[0], part), F32)
    groups = halves.shape[3] // part
    for half in range(2):
        for s in range(seqs):
            for g in range(groups):
                raw = halves[half, s, :, g * part : (g + 1) * part].astype(F32)
                cols = pl.ds(((half * groups + g) * seqs + s) * part, part)
                in_o[:, cols] = raw * scale
                total = total + raw * weight[:, cols].astype(F32)
    gain_o[...] = jnp.sum(total.T, axis=0)


def unpack(taps, history, low_rank, width, small, halves, ends, mixed, input_grad, out_grad,
           weight, gain):
    seqs, own_rows, feats = halves.shape[1:]
    part = small.shape[1]
    model = mixed.shape[1]
    kept = ends.shape[2] * seqs
    f32 = lambda *dims: jax.ShapeDtypeStruct(dims, F32)
    args = (small, halves, ends, mixed, input_grad, out_grad, weight, gain)
    outs = [
        jax.ShapeDtypeStruct((1,) + mixed.shape, BF16),
        f32(1, width, kept), f32(history, 1, kept),
        jax.ShapeDtypeStruct((1,) + input_grad.shape, BF16),
        f32(1, width, kept), f32(history, 1, kept),
        f32(own_rows), f32(*weight.shape),
        f32(taps, part), f32(part), f32(low_rank + 2 * width, part), f32(low_rank, part),
        f32(part), f32(width, part), f32(part), f32(part, model),
    ]

    def whole(a):
        return pl.BlockSpec(
            a.shape, lambda i: (0,) * len(a.shape), pipeline_mode=pl.Buffered(1)
        )

    return pl.pallas_call(
        functools.partial(unpack_kernel, seqs, taps, history, low_rank, width),
        grid=(1,),
        in_specs=[whole(a) for a in args],
        out_specs=[whole(a) for a in outs],
        out_shape=outs,
        name="unpack",
    )(*args)


def body(
    tokens, norm_gain, in_proj, conv_weight, conv_bias, x_proj, dt_proj, dt_bias,
    a_log, d_skip, out_proj, init_state, init_conv, cotangent,
):
    segs, seqs = lax.axis_size("seg"), lax.axis_size("seq")
    place = lax.axis_index("seq")
    own_rows, both = in_proj.shape
    part = conv_bias.shape[0]
    feats = segs * part
    taps = conv_weight.shape[0]
    width = a_log.shape[0]
    low_rank = dt_proj.shape[0]
    planes = feats // LANES
    own_len, model = tokens.shape[1:]
    length = own_len * seqs
    block = 64
    seq_lines = seqs // 2
    shape = (segs // seq_lines, seq_lines, seq_lines)

    def mine(rows):
        shaped = rows.reshape(rows.shape[0], segs, seqs, part)
        return lax.dynamic_index_in_dim(shaped, place, 2, keepdims=False).reshape(
            rows.shape[0], feats
        )

    gain_col = norm_gain.astype(F32)[:, None]
    own_weight = in_proj.astype(F32)
    scaled = (own_weight * gain_col).astype(BF16)
    scaled = scaled.reshape(own_rows, 2, segs, seqs, part)
    scaled_x = scaled[:, 0].transpose(2, 0, 1, 3).reshape(seqs, own_rows, feats)
    scaled_g = scaled[:, 1].reshape(own_rows, 2, segs // 2, seqs, part).transpose(3, 1, 0, 2, 4)
    scaled_g = scaled_g.reshape(seqs, 2, own_rows, feats // 2)
    small = jnp.concatenate(
        [
            dt_proj, x_proj.T, a_log, conv_weight, conv_bias[None], dt_bias[None], d_skip[None],
        ],
        axis=0,
    )
    small = jnp.pad(small, ((0, -small.shape[0] % 16), (0, 0)))
    w_x_half, small_all, tok, g_part = gather_start(shape, scaled_x, scaled_g, small, tokens[0])
    history = init_conv.shape[1]
    head = jnp.pad(mine(init_conv[0]), ((8 - history, 0), (0, 0)))
    x_in, act, w_dt, w_xt, params, a2, dt_low, bc, w_g_one = front(
        shape, taps, history, width, tok, w_x_half, small_all, head, g_part, 4 * block
    )
    init = mine(init_state[0]).reshape(width, planes, LANES)
    slope, pre, checks, final, gate_act, gated, w_out, cot, w_g_two = forward_scan(
        shape, taps, dt_low, w_dt, params, act, bc, a2, init, out_proj, cotangent[0], tok,
        w_g_one, g_part, 2 * block,
    )
    w_out = w_out.reshape(feats, model)
    cot = cot.reshape(length, model)
    w_g_one = w_g_one.reshape(model, feats // 2)
    w_g_two = w_g_two.reshape(model, feats // 2)
    g_gated = dot_nt(cot, w_out)
    gy = g_gated * gate_act
    gs_gate = (g_gated * slope).astype(BF16)
    out_grad = dot_tn(gated, cot).astype(BF16)
    gate_grad = dot_tn(tok, gs_gate).astype(BF16)
    g_actp, a_sum, start, dtb_grad, skip_grad, dtp_grad, g_mixed, g_half, out_grad, mixed_out = (
        backward_scan(
            shape, taps, pre, act, gy, bc, a2, params, checks, w_dt, dt_low, tokens[0],
            gate_grad.reshape(segs, seqs * own_rows, feats),
            out_grad.reshape(segs, part, model),
            gated, w_out, 2 * block,
        )
    )
    grads, halves, input_grad, ends = finish_all(
        shape, taps, history,
        (g_actp, x_in, act, tok, w_x_half, w_g_one, w_g_two, gs_gate),
        (
            g_mixed, w_xt, head, params, dtp_grad, a_sum, dtb_grad, skip_grad, g_half,
            tokens[0], cotangent[0], final, start,
        ),
    )
    if part % LANES == 0:
        outs = list(
            unpack(
                taps, history, low_rank, width, grads, halves, ends, mixed_out, input_grad,
                out_grad, in_proj, gain_col,
            )
        )
        outs[2], outs[5], outs[10] = (
            outs[2].transpose(1, 0, 2), outs[5].transpose(1, 0, 2), outs[10].T
        )
        return tuple(outs)
    ends = (
        ends.reshape(seqs, ends.shape[1], segs // seqs, part)
        .transpose(1, 2, 0, 3)
        .reshape(ends.shape[1], feats)
    )
    raw_grad = (
        halves.reshape(2, seqs, own_rows, segs, part)
        .transpose(2, 0, 3, 1, 4)
        .reshape(own_rows, both)
        .astype(F32)
    )
    in_grad = raw_grad * gain_col
    gain_grad = jnp.sum(raw_grad * own_weight, axis=1)

    at = width + history
    xp_at = low_rank + x_proj.shape[1]
    return (
        mixed_out[None],
        ends[None, :width],
        ends[None, width:at],
        input_grad[None],
        ends[None, at : at + width],
        ends[None, at + width : at + width + history],
        gain_grad,
        in_grad,
        grads[xp_at + width : xp_at + width + taps],
        grads[xp_at + width + taps],
        grads[low_rank:xp_at].T,
        grads[:low_rank],
        grads[xp_at + width + taps + 1],
        grads[xp_at : xp_at + width],
        grads[xp_at + width + taps + 2],
        out_grad,
    )


def solution(mesh):
    spread = ("seg", "seq")
    placed = (
        P("seg", "seq", None),
        P(spread),
        P(spread, None),
        P(None, spread),
        P(spread),
        P(spread, None),
        P(None, spread),
        P(spread),
        P(None, spread),
        P(spread),
        P(spread, None),
        P("seg", None, None),
        P("seg", None, None),
        P("seg", "seq", None),
    )
    return jax.shard_map(
        body,
        mesh=mesh,
        in_specs=placed,
        out_specs=(
            P("seg", "seq", None),
            P("seg", None, "seq"),
            P("seg", None, "seq"),
            P("seg", "seq", None),
            P("seg", None, "seq"),
            P("seg", None, "seq"),
            P(spread),
            P(spread, None),
            P(None, spread),
            P(spread),
            P(spread, None),
            P(None, spread),
            P(spread),
            P(None, spread),
            P(spread),
            P(spread, None),
        ),
        check_vma=False,
    )
```

```python
import functools

import jax
import jax.numpy as jnp
from jax import lax
from jax.experimental import pallas as pl
from jax.experimental.pallas import tpu as pltpu
from jax.sharding import PartitionSpec as P

EPSILON = 1e-05
LOG2E = 1.4426950408889634
LANES = 128
UNROLL = 8
F32 = jnp.float32
BF16 = jnp.bfloat16


def dot_nn(a, b):
    return jnp.dot(a, b, preferred_element_type=F32)


def dot_tn(a, b):
    return lax.dot_general(a, b, (((0,), (0,)), ((), ())), preferred_element_type=F32)


def dot_nt(a, b):
    return lax.dot_general(a, b, (((1,), (1,)), ((), ())), preferred_element_type=F32)


def sigmoid(v):
    return 1.0 / (1.0 + jnp.exp(-v))


def softplus(v):
    return jnp.maximum(v, 0.0) + jnp.log1p(jnp.exp(-jnp.abs(v)))


def to_planes(planes_ref, rows):
    groups = planes_ref.shape[0]
    for s in range(rows.shape[1] // LANES):
        tile = rows[:, s * LANES : (s + 1) * LANES].reshape(groups, UNROLL, LANES)
        planes_ref[:, pl.ds(s * UNROLL, UNROLL), :] = tile


def from_planes(planes_ref):
    groups, rows, _ = planes_ref.shape
    return jnp.concatenate(
        [
            planes_ref[:, pl.ds(s * UNROLL, UNROLL), :].reshape(groups * UNROLL, LANES)
            for s in range(rows // UNROLL)
        ],
        axis=1,
    )


def token_of(planes, i):
    return pl.ds(i, planes, stride=UNROLL)


MESH_ID = pl.DeviceIdType.MESH
VMEM_MOST = 67_043_328


class Grid:
    def __init__(self, axis, lines, fast):
        self.axis, self.lines, self.fast = axis, lines, fast
        self.here = lax.axis_index(axis)
        self.line = self.here // fast
        self.lane = self.here - self.line * fast

    def at(self, line, lane):
        return line * self.fast + lane

    def line_peer(self, k):
        return lax.rem(self.line + k, self.lines)

    def lane_peer(self, e):
        return lax.rem(self.lane + e, self.fast)

    def copy(self, src, dst, sent, got, index):
        return pltpu.make_async_remote_copy(
            src_ref=src, dst_ref=dst, send_sem=sent, recv_sem=got,
            device_id={self.axis: index}, device_id_type=MESH_ID,
        )


def meet(groups):
    barrier = pltpu.get_barrier_semaphore()
    total = 0
    for grid in groups:
        size = grid.lines * grid.fast
        for k in range(1, size):
            pl.semaphore_signal(
                barrier, inc=1, device_id={grid.axis: lax.rem(grid.here + k, size)},
                device_id_type=MESH_ID,
            )
        total += size - 1
    pl.semaphore_wait(barrier, total)


class Gather:
    def __init__(self, grid, own, out, sems, piece=None):
        self.grid, self.own, self.out, self.piece = grid, own, out, piece
        self.up_s, self.up_r, self.dn_s, self.dn_r, self.x_s, self.x_r = sems

    @staticmethod
    def semaphores(lines, fast):
        hops = pltpu.SemaphoreType.DMA((lines,))
        across = pltpu.SemaphoreType.DMA((lines, fast))
        return [hops, hops, hops, hops, across, across]

    def block(self, line, lane=None):
        grid = self.grid
        index = grid.at(line, grid.lane if lane is None else lane)
        return self.out.at[index] if self.piece is None else self.out.at[index, self.piece]

    def up(self, k):
        grid = self.grid
        block = self.block(jnp.maximum(grid.line - k, 0))
        return grid.copy(
            self.own if k == 0 else block, block, self.up_s.at[k], self.up_r.at[k],
            grid.at(jnp.minimum(grid.line + 1, grid.lines - 1), grid.lane),
        )

    def down(self, k):
        grid = self.grid
        block = self.block(jnp.minimum(grid.line + k, grid.lines - 1))
        return grid.copy(
            self.own if k == 0 else block, block, self.dn_s.at[k], self.dn_r.at[k],
            grid.at(jnp.maximum(grid.line - 1, 0), grid.lane),
        )

    def sends_up(self, k):
        return jnp.logical_and(self.grid.line + 1 < self.grid.lines, self.grid.line >= k)

    def sends_down(self, k):
        return jnp.logical_and(self.grid.line > 0, self.grid.line + k < self.grid.lines)

    def across(self, line, slot, e, own=False):
        grid = self.grid
        block = self.block(line)
        return grid.copy(
            self.own if own else block, block, self.x_s.at[slot, e], self.x_r.at[slot, e],
            grid.at(grid.line, grid.lane_peer(e)),
        )

    def slots(self):
        return range(self.grid.lines)

    def begin(self):
        grid = self.grid
        for when, copy in ((self.sends_up(0), self.up(0)), (self.sends_down(0), self.down(0))):
            pl.when(when)(copy.start)
        for e in range(1, grid.fast):
            self.across(grid.line, 0, e, own=True).start()

    def step(self, k):
        grid = self.grid

        def arrived(copy, line, slot, forward, onward):
            copy.wait_recv()
            if k < grid.lines - 1:
                pl.when(forward(k))(onward(k).start)
            for e in range(1, grid.fast):
                self.across(line, slot, e).start()

        below, above = grid.line - k, grid.line + k

        @pl.when(below >= 0)
        def _():
            arrived(self.up(k - 1), below, grid.lines - k, self.sends_up, self.up)

        @pl.when(above < grid.lines)
        def _():
            arrived(self.down(k - 1), above, k, self.sends_down, self.down)

    def finish(self):
        grid = self.grid
        for k in range(grid.lines - 1):
            pl.when(self.sends_up(k))(self.up(k).wait_send)
            pl.when(self.sends_down(k))(self.down(k).wait_send)
        for slot in self.slots():
            for e in range(1, grid.fast):
                copy = self.across(grid.line_peer(slot), slot, e, own=slot == 0)
                copy.wait_send()
                copy.wait_recv()


class Scatter:
    def __init__(self, grid, src, scratch, inside=False):
        self.grid, self.src, self.inside = grid, src, inside
        if not inside:
            self.own, self.o_s = scratch[:2]
            scratch = scratch[2:]
        self.xbuf, self.stage, self.zbuf, self.acc = scratch[:4]
        self.x_s, self.x_r, self.z_s, self.z_r = scratch[4:]
        self.last = grid.lines - 1

    @staticmethod
    def scratch(lines, fast, shape, inside=False):
        dma = pltpu.SemaphoreType.DMA
        shape = tuple(shape)
        loads = [] if inside else [pltpu.VMEM((lines,) + shape, BF16), dma((lines,))]
        return loads + [
            pltpu.VMEM((lines, fast - 1) + shape, BF16),
            pltpu.VMEM((lines - 1,) + shape, BF16),
            pltpu.VMEM((lines + 1,) + shape, BF16),
            pltpu.VMEM(shape, F32),
            dma((lines, fast)), dma((lines, fast)), dma((lines,)), dma((lines + 1,)),
        ]

    def dest(self, j):
        line, last = self.grid.line, self.last
        above, below = last - line, line
        low = jnp.where(j < above, last - j, j - above)
        high = jnp.where(j < below, j, last - (j - below))
        other = jnp.where(2 * line <= last, low, high)
        return jnp.where(j == last, line, other)

    def index(self, j, e):
        return self.grid.at(self.dest(j), self.grid.lane_peer(e))

    def across(self, j, e):
        grid = self.grid
        return grid.copy(
            self.src.at[self.index(j, e)], self.xbuf.at[j, e - 1],
            self.x_s.at[j, e], self.x_r.at[j, e], grid.at(grid.line, grid.lane_peer(e)),
        )

    def local(self, j):
        return pltpu.make_async_copy(
            self.src.at[self.index(j, 0)], self.own.at[j], self.o_s.at[j]
        )

    def along(self, j):
        grid = self.grid
        dest = self.dest(j)
        up = dest > grid.line
        to = jnp.clip(jnp.where(up, grid.line + 1, grid.line - 1), 0, self.last)
        slot = jnp.where(jnp.logical_and(jnp.logical_not(up), dest == to), grid.lines, dest)
        return grid.copy(
            self.stage.at[j], self.zbuf.at[slot], self.z_s.at[j], self.z_r.at[slot],
            grid.at(to, grid.lane),
        )

    def arrival(self, slot):
        grid = self.grid
        return grid.copy(
            self.stage.at[0], self.zbuf.at[slot], self.z_s.at[0], self.z_r.at[slot],
            grid.at(lax.rem(grid.line + 1, grid.lines), grid.lane),
        )

    def order(self):
        return list(range(self.grid.lines))

    def begin(self):
        for j in self.order():
            for e in range(1, self.grid.fast):
                self.across(j, e).start()
            if not self.inside:
                self.local(j).start()

    def rows(self, step):
        count = self.acc.shape[0]
        size = 16 if count % 16 == 0 else 8

        def run(i, carry):
            step(pl.ds(pl.multiple_of(i * size, size), size))
            return carry

        lax.fori_loop(0, count // size, run, 0)

    def middle(self, j):
        grid = self.grid
        for e in range(1, grid.fast):
            self.across(j, e).wait_recv()
        if self.inside:
            own = self.src.at[self.index(j, 0)]
        else:
            self.local(j).wait()
            own = self.own.at[j]

        def partial(at):
            total = own[at, :].astype(F32)
            for e in range(grid.fast - 1):
                total = total + self.xbuf[j, e, at, :].astype(F32)
            return total

        if j == self.last:

            def keep(at):
                self.acc[at, :] = partial(at)

            self.rows(keep)
            return
        dest = self.dest(j)
        carried = jnp.where(dest > grid.line, grid.line > 0, grid.line < self.last)

        @pl.when(carried)
        def _():
            self.arrival(dest).wait_recv()

            def add(at):
                total = partial(at) + self.zbuf[dest, at, :].astype(F32)
                self.stage[j, at, :] = total.astype(BF16)

            self.rows(add)

        @pl.when(jnp.logical_not(carried))
        def _():
            def add(at):
                self.stage[j, at, :] = partial(at).astype(BF16)

            self.rows(add)

        self.along(j).start()

    def finish(self, write):
        line, last = self.grid.line, self.last
        from_below, from_above = line > 0, line < last

        @pl.when(from_below)
        def _():
            self.arrival(line).wait_recv()

        @pl.when(from_above)
        def _():
            self.arrival(self.grid.lines).wait_recv()

        def total(at, below, above):
            result = self.acc[at, :]
            if below:
                result = result + self.zbuf[line, at, :].astype(F32)
            if above:
                result = result + self.zbuf[last + 1, at, :].astype(F32)
            write(at, result)

        for when, below, above in (
            (jnp.logical_and(from_below, from_above), True, True),
            (jnp.logical_not(from_below), False, True),
            (jnp.logical_not(from_above), True, False),
        ):

            @pl.when(when)
            def _():
                self.rows(lambda at: total(at, below, above))

    def drain(self):
        for j in self.order():
            for e in range(1, self.grid.fast):
                self.across(j, e).wait_send()
            if j < self.last:
                self.along(j).wait_send()


def into(ref):
    def write(at, total):
        ref[at, :] = total.astype(ref.dtype)

    return write


class Exchange:
    def __init__(self, grid, src, dst, sems):
        self.grid, self.src, self.dst = grid, src, dst
        self.sent, self.got = sems
        self.size = grid.lines * grid.fast

    @staticmethod
    def semaphores(size):
        return [pltpu.SemaphoreType.DMA((size,)), pltpu.SemaphoreType.DMA((size,))]

    def one(self, k):
        grid = self.grid
        peer = lax.rem(grid.here + k, self.size)
        return grid.copy(
            self.src(peer), self.dst(grid.here), self.sent.at[k], self.got.at[k], peer
        )

    def begin(self):
        for k in range(1, self.size):
            self.one(k).start()

    def arrived(self):
        for k in range(1, self.size):
            self.one(k).wait_recv()

    def drain(self):
        for k in range(1, self.size):
            self.one(k).wait_send()


ANY = pl.BlockSpec(memory_space=pl.ANY)
INSIDE = pl.BlockSpec(memory_space=pltpu.VMEM)


def comm_params(collective_id):
    return pltpu.CompilerParams(
        collective_id=collective_id, has_side_effects=True, vmem_limit_bytes=VMEM_MOST
    )


def grids(shape):
    lines, fast, seq_lines = shape
    return Grid("seg", lines, fast), Grid("seq", seq_lines, 2)


def sum_over_seq(seq, x_ref, out_ref, half, got, mine, others, whole, *sems):
    lane_s, lane_r, line_s, line_r, back_s, back_r = sems
    width = x_ref.shape[1] // 2
    lines = seq.lines
    other = 1 - seq.lane
    left = pl.ds(0, width)
    right = pl.ds(width, width)

    @pl.when(seq.lane == 0)
    def _():
        half[...] = x_ref[:, right].astype(BF16)

    @pl.when(seq.lane == 1)
    def _():
        half[...] = x_ref[:, left].astype(BF16)

    swap = seq.copy(half, got, lane_s, lane_r, seq.at(seq.line, other))
    swap.start()
    swap.wait()

    @pl.when(seq.lane == 0)
    def _():
        mine[...] = (x_ref[:, left] + got[...].astype(F32)).astype(BF16)

    @pl.when(seq.lane == 1)
    def _():
        mine[...] = (x_ref[:, right] + got[...].astype(F32)).astype(BF16)

    copies = [
        seq.copy(
            mine, others.at[k - 1], line_s.at[k], line_r.at[k], seq.at(seq.line_peer(k), seq.lane)
        )
        for k in range(1, lines)
    ]
    for copy in copies:
        copy.start()
    for copy in copies:
        copy.wait()
    total = mine[...].astype(F32)
    for k in range(lines - 1):
        total = total + others[k].astype(F32)
    whole[seq.lane] = total.astype(BF16)
    back = seq.copy(
        whole.at[seq.lane], whole.at[seq.lane], back_s, back_r, seq.at(seq.line, other)
    )
    back.start()
    back.wait()
    out_ref[:, left] = whole[0]
    out_ref[:, right] = whole[1]


def forward_kernel(
    shape, steps, taps,
    low_ref, wdt_ref, params_ref, act_ref, bc_ref, a_ref, init_ref, weight_ref, cot_ref,
    tok_ref, gate_one, gate_src,
    y_out, pre_ref, check_ref, final_ref, gate_out, gated_out, weights_ref, cots_ref, gate_two,
    y_ref, gate_ref, gated_ref, state, rate_pl, drive_pl, y_pl, w_one, w_two, local_s, *sems,
):
    count = pre_ref.shape[0]
    width, planes, _ = a_ref.shape
    seg, seq = grids(shape)
    gates = Gather(seg, gate_src.at[:, 1], gate_two, sems[:6])
    weights = Gather(seg, weight_ref, weights_ref, sems[6:12])
    cots = Gather(seq, cot_ref, cots_ref, sems[12:])
    step = pl.program_id(0)
    keeps = [
        pltpu.make_async_copy(weight_ref, weights_ref.at[seg.here], local_s.at[0]),
        pltpu.make_async_copy(cot_ref, cots_ref.at[seq.here], local_s.at[1]),
        pltpu.make_async_copy(gate_src.at[:, 1], gate_two.at[seg.here], local_s.at[2]),
    ]
    load_one = pltpu.make_async_copy(gate_one, w_one, local_s.at[3])

    @pl.when(step == 0)
    def _():
        meet((seg, seq))
        gates.begin()
        weights.begin()
        cots.begin()
        for keep in keeps:
            keep.start()
        load_one.start()
        state[...] = init_ref[...]

    lines = params_ref[pl.ds(width, 8), :]
    bias, skip = lines[taps + 1 : taps + 2], lines[taps + 2 : taps + 3]
    pre = dot_tn(low_ref[...], wdt_ref[...]) + bias
    pre_ref[...] = pre
    rate = softplus(pre)
    act = act_ref[...].astype(F32)
    to_planes(rate_pl, rate)
    to_planes(drive_pl, rate * act)
    groups = count // UNROLL

    def group(k, carry):
        at = k * UNROLL
        rates = [rate_pl[k, token_of(planes, i), :] for i in range(UNROLL)]
        drives = [drive_pl[k, token_of(planes, i), :] for i in range(UNROLL)]
        sums = [None] * UNROLL
        for n in range(width):
            a = a_ref[n]
            h = state[n]
            check_ref[k, n] = h
            for i in range(UNROLL):
                h = jnp.exp2(rates[i] * a) * h + bc_ref[at + i, n] * drives[i]
                term = bc_ref[at + i, width + n] * h
                sums[i] = term if n == 0 else sums[i] + term
            state[n] = h
        for i in range(UNROLL):
            y_pl[k, token_of(planes, i), :] = sums[i]
        return carry

    ticks = 2 * steps
    plan = [[] for _ in range(ticks)]
    late = []
    for k in range(1, seg.lines):
        for gather, share in ((gates, 4 * k), (weights, 9 * k)):
            tick = ticks * share // 16
            (plan[tick - 1] if tick < ticks else late).append(functools.partial(gather.step, k))
        if k < seq.lines:
            plan[ticks - 1].append(functools.partial(cots.step, k))

    def part_of_step(h, carry):
        lax.fori_loop(h * (groups // 2), (h + 1) * (groups // 2), group, 0)
        for tick in range(ticks):
            if plan[tick]:

                @pl.when(step * 2 + h == tick)
                def _():
                    for event in plan[tick]:
                        event()

        return carry

    lax.fori_loop(0, 2, part_of_step, 0)
    y_ref[pl.ds(pl.multiple_of(step * count, count), count), :] = (
        from_planes(y_pl) + skip * act_ref[...].astype(F32)
    )

    @pl.when(step == steps - 1)
    def _():
        final_ref[...] = state[...]
        for event in late[:-1]:
            event()
        gates.finish()
        keeps[2].wait()
        load_one.wait()
        load_two = pltpu.make_async_copy(gate_two, w_two, local_s.at[3])
        load_two.start()
        load_two.wait()
        model = tok_ref.shape[1]
        half = w_one.shape[3]
        block = 256

        def gating(i, carry):
            rows = pl.ds(pl.multiple_of(i * block, block), block)
            lines = tok_ref[rows, :].astype(F32)
            rstd = lax.rsqrt(jnp.mean(lines * lines, axis=1, keepdims=True) + EPSILON)
            for j, w in enumerate((w_one, w_two)):
                cols = pl.ds(j * half, half)
                gate = rstd * dot_nn(tok_ref[rows, :], w[...].reshape(model, half))
                sig = sigmoid(gate)
                y_val = y_ref[rows, cols]
                gate_ref[rows, cols] = gate * sig
                gated_ref[rows, cols] = (y_val * gate * sig).astype(BF16)
                y_ref[rows, cols] = rstd * y_val * sig * (1.0 + gate * (1.0 - sig))
            return carry

        blocks = y_ref.shape[0] // block
        lax.fori_loop(0, blocks // 2, gating, 0)
        late[-1]()
        lax.fori_loop(blocks // 2, blocks, gating, 0)
        leaving = [
            pltpu.make_async_copy(y_ref, y_out, local_s.at[4]),
            pltpu.make_async_copy(gate_ref, gate_out, local_s.at[5]),
            pltpu.make_async_copy(gated_ref, gated_out, local_s.at[6]),
        ]
        for leave in leaving:
            leave.start()
        weights.finish()
        cots.finish()
        for keep in keeps[:2]:
            keep.wait()
        for leave in leaving:
            leave.wait()


def backward_kernel(
    shape, steps, taps,
    pre_ref, act_ref, gy_ref, bc_ref, a_ref, params_ref, check_ref, wdt_ref, low_ref, base_ref,
    first_src, second_src, gated_src, weight_src,
    gact_ref, agrad_ref, start_ref, dtb_ref, sgrad_ref, dtp_ref, mix_ref,
    first_out, second_out, third_out,
    carry_s, rate_pl, drive_pl, gy_pl, grate_pl, thr_pl, prod, part, mix_s,
    gated_in, weight_in, third_src, load_s, *scratch,
):
    count = pre_ref.shape[0]
    width, planes, _ = a_ref.shape
    low_rank = wdt_ref.shape[0]
    seg, seq = grids(shape)
    first = Scatter(seg, first_src, scratch[:10])
    second = Scatter(seg, second_src, scratch[10:20])
    third = Scatter(seq, third_src, scratch[20:28], inside=True)
    loads = [
        pltpu.make_async_copy(gated_src, gated_in, load_s.at[0]),
        pltpu.make_async_copy(weight_src, weight_in, load_s.at[1]),
    ]
    step = pl.program_id(0)

    @pl.when(step == 0)
    def _():
        meet((seg, seq))
        first.begin()
        second.begin()
        for load in loads:
            load.start()
        carry_s[...] = jnp.zeros_like(carry_s)
        agrad_ref[...] = jnp.zeros_like(agrad_ref)
        dtb_ref[...] = jnp.zeros_like(dtb_ref)
        sgrad_ref[...] = jnp.zeros_like(sgrad_ref)
        dtp_ref[...] = jnp.zeros_like(dtp_ref)

    pre = pre_ref[...]
    rate = softplus(pre)
    act = act_ref[...].astype(F32)
    to_planes(rate_pl, rate)
    to_planes(drive_pl, rate * act)
    to_planes(gy_pl, gy_ref[...])
    groups = count // UNROLL

    def group(j, carry):
        k = groups - 1 - j
        at = k * UNROLL
        rates = [rate_pl[k, token_of(planes, i), :] for i in range(UNROLL)]
        drives = [drive_pl[k, token_of(planes, i), :] for i in range(UNROLL)]
        gys = [gy_pl[k, token_of(planes, i), :] for i in range(UNROLL)]
        g_rate = [None] * UNROLL
        through = [None] * UNROLL
        for n in range(width):
            a = a_ref[n]
            states = [check_ref[k, n]]
            decays = []
            for i in range(UNROLL):
                decays.append(jnp.exp2(rates[i] * a))
                states.append(decays[i] * states[i] + bc_ref[at + i, n] * drives[i])
            lam = carry_s[n]
            acc = agrad_ref[n]
            for i in reversed(range(UNROLL)):
                lam = lam + bc_ref[at + i, width + n] * gys[i]
                b_term = bc_ref[at + i, n] * lam
                region = (i * 2 * width + n) // 8
                prod[region, token_of(planes, n % 8), :] = lam * drives[i]
                prod[region + width // 8, token_of(planes, n % 8), :] = states[i + 1] * gys[i]
                lam = decays[i] * lam
                weighted = lam * states[i]
                acc = acc + weighted * rates[i]
                a_term = weighted * a
                g_rate[i] = a_term if n == 0 else g_rate[i] + a_term
                through[i] = b_term if n == 0 else through[i] + b_term
            carry_s[n] = lam
            agrad_ref[n] = acc
        for i in range(UNROLL):
            grate_pl[k, token_of(planes, i), :] = g_rate[i]
            thr_pl[k, token_of(planes, i), :] = through[i]
            for q in range(2 * width // 8):
                region = i * 2 * width // 8 + q
                total = prod[region, pl.ds(0, 8), :]
                for s in range(1, planes):
                    total = total + prod[region, pl.ds(s * 8, 8), :]
                row = pl.multiple_of((at + i) * 2 * width + q * 8, 8)
                part[pl.ds(row, 8), :] = total
        return carry

    events = [functools.partial(s.middle, k) for s in (first, second) for k in s.order()]
    ticks = 2 * steps
    plan = [[] for _ in range(ticks)]
    for j, event in enumerate(events):
        plan[min(ticks - 1, 1 + 5 * ticks * (j + 1) // (4 * len(events)))].append(event)

    def output(index):
        own_len, model = third_src.shape[1:]
        rows = pl.ds(pl.multiple_of(index * own_len, own_len), own_len)

        def column(c, carry):
            cols = pl.ds(pl.multiple_of(c * 512, 512), 512)
            third_src[index, :, cols] = dot_nn(gated_in[rows, :], weight_in[:, cols]).astype(BF16)
            return carry

        lax.fori_loop(0, model // 512, column, 0)

    def outputs():
        for load in loads:
            load.wait()

        def leave(j, carry):
            output(third.index(j, 1))
            third.across(j, 1).start()
            return carry

        def stay(j, carry):
            output(third.index(j, 0))
            return carry

        lax.fori_loop(0, seq.lines, leave, 0)
        lax.fori_loop(0, seq.lines, stay, 0)

    plan[0].append(outputs)
    for j in third.order():
        plan[min(ticks - 1, 5 + 2 * j)].append(functools.partial(third.middle, j))

    def add_base(at, total):
        third_out[at, :] = (total + base_ref[at, :].astype(F32)).astype(BF16)

    plan[min(ticks - 1, 13)].append(functools.partial(third.finish, add_base))

    def part_of_step(h, carry):
        lax.fori_loop(h * (groups // 2), (h + 1) * (groups // 2), group, 0)
        for tick in range(ticks - 1):
            if plan[tick]:

                @pl.when(step * 2 + h == tick)
                def _():
                    for event in plan[tick]:
                        event()

        return carry

    lax.fori_loop(0, 2, part_of_step, 0)
    g_rate = from_planes(grate_pl) * (1.0 / LOG2E)
    through = from_planes(thr_pl)
    pre = pre_ref[...]
    rate = softplus(pre)
    act = act_ref[...].astype(F32)
    gy = gy_ref[...]
    g_dtpre = ((g_rate + act * through) * sigmoid(pre)).astype(BF16)
    skip = params_ref[pl.ds(width, 8), :][taps + 2 : taps + 3]
    gact_ref[...] = gy * skip + rate * through
    dtb_ref[...] += jnp.sum(g_dtpre.astype(F32), axis=0, keepdims=True)
    sgrad_ref[...] += jnp.sum(gy * act, axis=0, keepdims=True)
    dtp_ref[...] += dot_nn(low_ref[...], g_dtpre)
    rows = 2 * width
    ones = jnp.ones((LANES, LANES), F32)
    sums = jnp.dot(part[...], ones, preferred_element_type=F32)
    sums = sums.reshape(count, rows, LANES)
    pick = lax.broadcasted_iota(jnp.int32, (1, rows, LANES), 1) == lax.broadcasted_iota(
        jnp.int32, (1, rows, LANES), 2
    )
    g_bc = jnp.sum(jnp.where(pick, sums, 0.0), axis=1)
    tokens_at = pl.ds(pl.multiple_of((steps - 1 - step) * count, count), count)
    mix_s[pl.ds(0, low_rank), tokens_at] = dot_nt(wdt_ref[...], g_dtpre)
    mix_s[pl.ds(low_rank, rows), tokens_at] = g_bc.T[:rows]

    @pl.when(step == steps - 1)
    def _():
        start_ref[...] = carry_s[...]
        for event in plan[ticks - 1][:-1]:
            event()
        sum_over_seq(seq, mix_s, mix_ref, *scratch[28:])
        plan[ticks - 1][-1]()
        first.finish(into(first_out))
        second.finish(into(second_out))
        for scatter in (first, second, third):
            scatter.drain()


def forward_scan(
    shape, taps, low, w_dt, params, act, bc, a2, init, weight, cot, tok, gate_one, gate_part, block
):
    lines, fast, seq_lines = shape
    length, features = act.shape
    width, planes, _ = a2.shape
    low_rank = w_dt.shape[0]
    steps = length // block
    rows = pl.BlockSpec((block, features), lambda i: (i, 0))
    one = pl.Buffered(1)

    def whole(*dims):
        return pl.BlockSpec(dims, lambda i: (0,) * len(dims), pipeline_mode=one)

    plane = pltpu.VMEM((block // UNROLL, planes * UNROLL, LANES), F32)
    return pl.pallas_call(
        functools.partial(forward_kernel, shape, steps, taps),
        grid=(steps,),
        in_specs=[
            pl.BlockSpec((low_rank, block), lambda i: (0, i)),
            whole(low_rank, features), whole(*params.shape), rows,
            pl.BlockSpec((block, 2 * width), lambda i: (i, 0), memory_space=pltpu.SMEM),
            whole(width, planes, LANES), whole(width, planes, LANES),
            whole(*weight.shape), whole(*cot.shape), whole(*tok.shape), ANY, ANY,
        ],
        out_specs=[
            ANY, rows,
            pl.BlockSpec((block // UNROLL, width, planes, LANES), lambda i: (i, 0, 0, 0)),
            whole(width, planes, LANES), ANY, ANY, ANY, ANY, ANY,
        ],
        out_shape=[
            jax.ShapeDtypeStruct((length, features), F32),
            jax.ShapeDtypeStruct((length, features), F32),
            jax.ShapeDtypeStruct((length // UNROLL, width, planes, LANES), F32),
            jax.ShapeDtypeStruct((width, planes, LANES), F32),
            jax.ShapeDtypeStruct((length, features), F32),
            jax.ShapeDtypeStruct((length, features), BF16),
            jax.ShapeDtypeStruct((lines * fast,) + weight.shape, BF16),
            jax.ShapeDtypeStruct((seq_lines * 2,) + cot.shape, BF16),
            jax.ShapeDtypeStruct(gate_one.shape, BF16),
        ],
        scratch_shapes=[
            pltpu.VMEM((length, features), F32), pltpu.VMEM((length, features), F32),
            pltpu.VMEM((length, features), BF16),
            pltpu.VMEM((width, planes, LANES), F32), plane, plane, plane,
            pltpu.VMEM(gate_one.shape, BF16), pltpu.VMEM(gate_one.shape, BF16),
            pltpu.SemaphoreType.DMA((7,)),
            *Gather.semaphores(lines, fast), *Gather.semaphores(lines, fast),
            *Gather.semaphores(seq_lines, 2),
        ],
        compiler_params=comm_params(5),
        cost_estimate=pl.CostEstimate(
            flops=8 * length * features * width,
            bytes_accessed=24 * length * features,
            transcendentals=length * features * width,
        ),
        name="scan_forward",
    )(low, w_dt, params, act, bc, a2, init, weight, cot, tok, gate_one, gate_part)


def backward_scan(
    shape, taps, pre, act, gy, bc, a2, params, checks, w_dt, dt_low, base, first, second, gated, weight,
    block,
):
    lines, fast, seq_lines = shape
    length, features = pre.shape
    width, planes, _ = a2.shape
    low_rank = w_dt.shape[0]
    steps = length // block
    rows = pl.BlockSpec((block, features), lambda i: (steps - 1 - i, 0))
    whole = pl.BlockSpec((width, planes, LANES), lambda i: (0, 0, 0))

    def all_of(rows, columns):
        return pl.BlockSpec((rows, columns), lambda i: (0, 0))

    line = all_of(1, features)
    plane = pltpu.VMEM((block // UNROLL, planes * UNROLL, LANES), F32)
    mixed = (low_rank + 2 * width, length)
    return pl.pallas_call(
        functools.partial(backward_kernel, shape, steps, taps),
        grid=(steps,),
        in_specs=[
            rows, rows, rows,
            pl.BlockSpec(
                (block, 2 * width), lambda i: (steps - 1 - i, 0), memory_space=pltpu.SMEM
            ),
            whole, all_of(*params.shape),
            pl.BlockSpec(
                (block // UNROLL, width, planes, LANES), lambda i: (steps - 1 - i, 0, 0, 0)
            ),
            all_of(low_rank, features),
            pl.BlockSpec((low_rank, block), lambda i: (0, steps - 1 - i)),
            all_of(*base.shape),
            ANY, ANY, ANY, ANY,
        ],
        out_specs=[
            rows, whole, whole, line, line, all_of(low_rank, features), all_of(*mixed),
            all_of(*first.shape[1:]), all_of(*second.shape[1:]), all_of(*base.shape),
        ],
        out_shape=[
            jax.ShapeDtypeStruct((length, features), F32),
            jax.ShapeDtypeStruct((width, planes, LANES), F32),
            jax.ShapeDtypeStruct((width, planes, LANES), F32),
            jax.ShapeDtypeStruct((1, features), F32),
            jax.ShapeDtypeStruct((1, features), F32),
            jax.ShapeDtypeStruct((low_rank, features), F32),
            jax.ShapeDtypeStruct(mixed, BF16),
            jax.ShapeDtypeStruct(first.shape[1:], BF16),
            jax.ShapeDtypeStruct(second.shape[1:], F32),
            jax.ShapeDtypeStruct(base.shape, BF16),
        ],
        scratch_shapes=[pltpu.VMEM((width, planes, LANES), F32)]
        + [plane] * 5
        + [
            pltpu.VMEM((UNROLL * 2 * width // 8, planes * 8, LANES), F32),
            pltpu.VMEM((block * 2 * width, LANES), F32),
            pltpu.VMEM(mixed, F32),
            pltpu.VMEM(gated.shape, BF16),
            pltpu.VMEM(weight.shape, BF16),
            pltpu.VMEM((2 * seq_lines,) + base.shape, BF16),
            pltpu.SemaphoreType.DMA((2,)),
            *Scatter.scratch(lines, fast, first.shape[1:]),
            *Scatter.scratch(lines, fast, second.shape[1:]),
            *Scatter.scratch(seq_lines, 2, base.shape, inside=True),
            *sum_scratch(seq_lines, *mixed),
        ],
        compiler_params=comm_params(6),
        cost_estimate=pl.CostEstimate(
            flops=20 * length * features * width,
            bytes_accessed=28 * length * features,
            transcendentals=length * features * width,
        ),
        name="scan_backward",
    )(pre, act, gy, bc, a2, params, checks, w_dt, dt_low, base, first, second, gated, weight)


def finish_kernel(shape, taps, history, refs, scratch):
    (
        gact, x_in, act, tok, w_x, w_g, w_h, gs_gate,
        mix, w_xt, head, params, dtp, a_sum, dtb, sgrad, g_half, own_tok, own_cot,
        final, start,
        small_out, halves_out, input_out, ends_out,
    ) = refs
    (
        gc, xb, actb, tokb, wxb, wgb, gsg, gs_x, xg, xh, q_src, pack, small_src, ends_src, x_half,
        in_s, own_s,
    ) = scratch[:17]
    seg, seq = grids(shape)
    length, feats = act.shape
    width = a_sum.shape[0]
    kern = params.at[pl.ds(width, 8)]
    b_conv = params.at[pl.ds(width + taps, 1)]
    at = 17
    sets = []
    for size in (8, 8, 8, 8):
        sets.append(scratch[at : at + size])
        at += size
    swaps_s = [scratch[at + 2 * i : at + 2 * i + 2] for i in range(3)]
    small = Scatter(seg, small_src, sets[0], inside=True)
    x_sums = [
        Scatter(seg, xg, sets[1], inside=True), Scatter(seg, xh, sets[2], inside=True)
    ]
    q_sum = Scatter(seq, q_src, sets[3], inside=True)
    loads = [
        pltpu.make_async_copy(gact, gc.at[pl.ds(0, length)], in_s.at[0]),
        pltpu.make_async_copy(x_in, xb.at[pl.ds(8, length)], in_s.at[1]),
        pltpu.make_async_copy(tok, tokb, in_s.at[2]),
        pltpu.make_async_copy(act, actb, in_s.at[3]),
        pltpu.make_async_copy(gs_gate, gsg, in_s.at[4]),
        pltpu.make_async_copy(w_g, wgb.at[0], in_s.at[5]),
        pltpu.make_async_copy(w_h, wgb.at[1], in_s.at[6]),
        pltpu.make_async_copy(w_x, wxb, in_s.at[7]),
    ]
    for load in loads:
        load.start()
    meet((seg, seq))
    own_rows = g_half.shape[0] // (seq.lines * seq.fast)

    def swap(half, src, sems):
        return Exchange(
            seq,
            lambda p: src.at[pl.ds(pl.multiple_of(p * own_rows, own_rows), own_rows)],
            lambda m: halves_out.at[half, m],
            sems,
        )

    swap_g = swap(1, g_half, swaps_s[1])
    swap_g.begin()
    xb[pl.ds(0, 8), :] = head[...]
    gc[pl.ds(length, 8), :] = jnp.zeros((8, feats), F32)
    loads[0].wait()
    big = LANES

    def add_mixed(i, carry):
        rows = pl.ds(pl.multiple_of(i * big, big), big)
        gc[rows, :] += dot_tn(mix[:, rows], w_xt[...])
        return carry

    lax.fori_loop(0, length // big, add_mixed, 0)
    loads[1].wait()
    tall = 32
    chunk = feats // 2
    sums_at = 8 * (taps + 1)
    pack[...] = jnp.zeros_like(pack)

    def through_conv(side, i, carry):
        t0 = pl.multiple_of(i * tall, tall)
        for c in (side * chunk,):
            cols = pl.ds(c, chunk)
            wide = xb[pl.ds(t0, tall + 8), cols]
            rows = [wide[8 - history + k : 8 - history + k + tall] for k in range(taps)]
            conv = b_conv[:, cols]
            for k in range(taps):
                conv = conv + kern[pl.ds(k, 1), cols] * rows[k]
            sig = sigmoid(conv)
            g_conv = gc[pl.ds(t0, tall), cols] * sig * (1.0 + conv * (1.0 - sig))
            gc[pl.ds(t0, tall), cols] = g_conv
            for k in range(taps):
                term = g_conv * rows[k]
                pack[pl.ds(8 * k, 8), cols] += sum(
                    term[8 * j : 8 * j + 8] for j in range(tall // 8)
                )
            pack[pl.ds(8 * taps, 8), cols] += sum(
                g_conv[8 * j : 8 * j + 8] for j in range(tall // 8)
            )
        return carry

    loads[2].wait()

    def to_input(side, i, carry):
        t0 = pl.multiple_of(i * tall, tall)
        lines = tokb[pl.ds(t0, tall), :].astype(F32)
        rstd = lax.rsqrt(jnp.mean(lines * lines, axis=1, keepdims=True) + EPSILON)
        for c in (side * chunk,):
            cols = pl.ds(c, chunk)
            wide = gc[pl.ds(t0, tall + 8), cols]
            g_x = kern[pl.ds(0, 1), cols] * wide[history : history + tall]
            for k in range(1, taps):
                g_x = g_x + kern[pl.ds(k, 1), cols] * wide[history - k : history - k + tall]
            gs_x[pl.ds(t0, tall), cols] = (rstd * g_x).astype(BF16)
        return carry

    block_rows = xg.shape[1]
    by_block = block_rows % LANES == 0

    def partial(side, index):
        cols = pl.ds(pl.multiple_of(index * block_rows, block_rows), block_rows)
        x_sums[side].src[index] = dot_tn(
            tokb[:, cols], gs_x[:, pl.ds(side * chunk, chunk)]
        ).astype(BF16)

    def one_side(side):
        lax.fori_loop(0, length // tall, functools.partial(through_conv, side), 0)
        lax.fori_loop(0, length // tall, functools.partial(to_input, side), 0)
        if not by_block:

            def several(i, carry):
                cols = pl.ds(pl.multiple_of(i * LANES, LANES), LANES)
                got = dot_tn(tokb[:, cols], gs_x[:, pl.ds(side * chunk, chunk)])
                each = LANES // block_rows
                for p in range(each):
                    rows = slice(p * block_rows, (p + 1) * block_rows)
                    x_sums[side].src[i * each + p] = got[rows].astype(BF16)
                return carry

            lax.fori_loop(0, tokb.shape[1] // LANES, several, 0)

        def leave(j, carry):
            for e in range(1, seg.fast):
                if by_block:
                    partial(side, x_sums[side].index(j, e))
                x_sums[side].across(j, e).start()
            return carry

        lax.fori_loop(0, seg.lines, leave, 0)

    def stay(side, j, carry):
        if by_block:
            partial(side, x_sums[side].index(j, 0))
        return carry

    one_side(0)
    one_side(1)
    loads[3].wait()
    low_rank = dtp.shape[0]
    mixes = mix.shape[0]
    part = small_src.shape[2]
    a_grad = from_states(a_sum) * params[pl.ds(0, width), :]
    xp = dot_nn(mix[...], actb[...])
    for g in range(small_src.shape[0]):
        cols = slice(g * part, (g + 1) * part)
        small_src[g, pl.ds(0, low_rank), :] = dtp[:, cols].astype(BF16)
        small_src[g, pl.ds(low_rank, mixes), :] = xp[:, cols].astype(BF16)
        base = low_rank + mixes
        small_src[g, pl.ds(base, width), :] = a_grad[:, cols].astype(BF16)
        lines = [
            jnp.sum(pack[pl.ds(8 * k, 8), cols], axis=0, keepdims=True) for k in range(taps + 1)
        ]
        lines += [dtb[:, cols], sgrad[:, cols]]
        lines.append(jnp.zeros((16 - len(lines), part), F32))
        small_src[g, pl.ds(base + width, 16), :] = jnp.concatenate(lines, axis=0).astype(BF16)
    small.begin()

    lax.fori_loop(0, seg.lines, functools.partial(stay, 0), 0)
    ends_in = jnp.concatenate(
        [
            from_states(final),
            xb[pl.ds(length, 8), :][8 - history :],
            from_states(start),
            sum_head(gc, kern, history, taps),
            jnp.zeros((ends_src.shape[1] - 2 * (width + history), feats), F32),
        ],
        axis=0,
    )
    piece = ends_src.shape[2]
    for p in range(ends_src.shape[0]):
        ends_src[p] = ends_in[:, p * piece : (p + 1) * piece]
    end_swap = Exchange(seq, lambda p: ends_src.at[p], lambda m: ends_out.at[m], swaps_s[2])
    end_swap.begin()
    loads[4].wait()
    loads[5].wait()
    loads[6].wait()
    loads[7].wait()
    own_len = own_tok.shape[0]
    model = own_tok.shape[1]
    wide = 512
    half = feats // 2

    def normed(index):
        rows = pl.ds(pl.multiple_of(index * own_len, own_len), own_len)

        def column(c, carry):
            cols = pl.ds(pl.multiple_of(c * wide, wide), wide)
            q_src[index, :, cols] = (
                dot_nt(gsg[rows, pl.ds(0, half)], wgb[0, cols, :])
                + dot_nt(gsg[rows, pl.ds(half, half)], wgb[1, cols, :])
                + dot_nt(gs_x[rows, :], wxb[cols, :])
            ).astype(BF16)
            return carry

        lax.fori_loop(0, model // wide, column, 0)

    def leave_q(j):
        normed(q_sum.index(j, 1))
        q_sum.across(j, 1).start()

    rest = [functools.partial(leave_q, j) for j in q_sum.order()]
    rest += [lambda j=j: normed(q_sum.index(j, 0)) for j in q_sum.order()]
    turns = x_sums[0].order()
    for j in turns:
        x_sums[0].middle(j)
        for work in rest[j * len(rest) // len(turns) : (j + 1) * len(rest) // len(turns)]:
            work()
        if j == 0:
            lax.fori_loop(0, seg.lines, functools.partial(stay, 1), 0)
    for j in q_sum.order():
        q_sum.middle(j)
    for j in x_sums[1].order():
        x_sums[1].middle(j)
    for j in small.order():
        small.middle(j)

    def input_grad(at, total):
        own = own_tok[at, :].astype(F32)
        square = 1.0 / (jnp.mean(own * own, axis=1, keepdims=True) + EPSILON)
        input_out[at, :] = (
            own_cot[at, :].astype(F32)
            + total
            - own * (square * jnp.mean(total * own, axis=1, keepdims=True))
        ).astype(BF16)

    for side in (0, 1):

        def put(at, total):
            x_half[at, pl.ds(side * chunk, chunk)] = total.astype(BF16)

        x_sums[side].finish(put)
    swap_x = swap(0, x_half, swaps_s[0])
    swap_x.begin()
    q_sum.finish(input_grad)
    small.finish(into(small_out))
    own = pl.ds(pl.multiple_of(seq.here * own_rows, own_rows), own_rows)
    keeps = [
        pltpu.make_async_copy(x_half.at[own], halves_out.at[0, seq.here], own_s.at[0]),
        pltpu.make_async_copy(g_half.at[own], halves_out.at[1, seq.here], own_s.at[1]),
        pltpu.make_async_copy(ends_src.at[seq.here], ends_out.at[seq.here], own_s.at[2]),
    ]
    for keep in keeps:
        keep.start()
    for scatter in (small, *x_sums, q_sum):
        scatter.drain()
    for exchange in (swap_g, end_swap, swap_x):
        exchange.arrived()
        exchange.drain()
    for keep in keeps:
        keep.wait()


def from_states(ref):
    return jnp.concatenate([ref[:, s, :] for s in range(ref.shape[1])], axis=1)


def sum_head(gc, kern, history, taps):
    top = gc[pl.ds(0, 8), :]
    rows = []
    for j in range(history):
        rows.append(
            sum(kern[pl.ds(k, 1), :] * top[j - k : j - k + 1] for k in range(min(j + 1, taps)))
        )
    return jnp.concatenate(rows, axis=0)


def finish_all(shape, taps, history, big, small):
    lines, fast, seq_lines = shape
    segs, seqs = lines * fast, seq_lines * 2
    gact, x_in, act, tok, w_x, w_g, w_h, gs_gate = big
    mix, w_xt, head, params, dtp, a_sum, dtb, sgrad, g_half, own_tok, own_cot = small[:11]
    length, feats = act.shape
    own_len, model = own_tok.shape
    width = a_sum.shape[0]
    rows = dtp.shape[0] + mix.shape[0] + width + 16
    block_rows = model // segs
    own_rows = g_half.shape[0] // seqs
    ends = (seqs, 2 * (width + history) + (-2 * (width + history)) % 8, feats // seqs)
    dma = pltpu.SemaphoreType.DMA
    scratch = [
        pltpu.VMEM((length + 8, feats), F32),
        pltpu.VMEM((length + 8, feats), F32),
        pltpu.VMEM((length, feats), BF16),
        pltpu.VMEM((length, model), BF16),
        pltpu.VMEM((model, feats), BF16),
        pltpu.VMEM((2, model, feats // 2), BF16),
        pltpu.VMEM((length, feats), BF16),
        pltpu.VMEM((length, feats), BF16),
        pltpu.VMEM((segs, block_rows, feats // 2), BF16),
        pltpu.VMEM((segs, block_rows, feats // 2), BF16),
        pltpu.VMEM((seqs, own_len, model), BF16),
        pltpu.VMEM((8 * (taps + 1), feats), F32),
        pltpu.VMEM((segs, rows, feats // segs), BF16),
        pltpu.VMEM(ends, F32),
        pltpu.VMEM((block_rows, feats), BF16),
        dma((8,)), dma((3,)),
        *Scatter.scratch(lines, fast, (rows, feats // segs), inside=True),
        *Scatter.scratch(lines, fast, (block_rows, feats // 2), inside=True),
        *Scatter.scratch(lines, fast, (block_rows, feats // 2), inside=True),
        *Scatter.scratch(seq_lines, 2, (own_len, model), inside=True),
        *Exchange.semaphores(seqs), *Exchange.semaphores(seqs), *Exchange.semaphores(seqs),
    ]

    def kernel(*refs):
        finish_kernel(shape, taps, history, refs[:25], refs[25:])

    return pl.pallas_call(
        kernel,
        in_specs=[ANY] * 8 + [INSIDE] * 13,
        out_specs=[INSIDE] * 4,
        out_shape=[
            jax.ShapeDtypeStruct((rows, feats // segs), F32),
            jax.ShapeDtypeStruct((2, seqs, own_rows, feats), BF16),
            jax.ShapeDtypeStruct((own_len, model), BF16),
            jax.ShapeDtypeStruct(ends, F32),
        ],
        scratch_shapes=scratch,
        compiler_params=comm_params(4),
        name="finish",
    )(*big, *small)


def gather_kernel(
    shape, scaled_x, scaled_g, small, tokens, w_x, small_all, tok, g_part, x_part, tok_in, g_own,
    local_s, small_sems, tok_sems, swap_x, swap_g, x_sems,
):
    seg, seq = grids(shape)
    size = seq.lines * seq.fast
    load_tok = pltpu.make_async_copy(tokens, tok_in, local_s.at[0])
    load_own = pltpu.make_async_copy(scaled_x.at[seq.here], x_part.at[seq.here], local_s.at[1])
    load_gate = pltpu.make_async_copy(scaled_g.at[seq.here], g_own, local_s.at[3])
    load_tok.start()
    load_own.start()
    load_gate.start()
    meet((seg, seq))
    swap_x = Exchange(seq, lambda p: scaled_x.at[p], lambda m: x_part.at[m], swap_x)
    swap_g = Exchange(seq, lambda p: scaled_g.at[p], lambda m: g_part.at[m], swap_g)
    swap_x.begin()
    pieces = []
    for k in range(size):
        place = lax.rem(seq.here - k + size, size)
        pieces.append(Gather(seg, x_part.at[place], w_x, x_sems[6 * k : 6 * k + 6], place))
    smalls = Gather(seg, small, small_all, small_sems)
    load_own.wait()
    pieces[0].begin()
    smalls.begin()
    load_tok.wait()
    toks = Gather(seq, tok_in, tok, tok_sems)
    for k in range(1, size):
        swap_x.one(k).wait_recv()
        pieces[k].begin()
    toks.begin()
    swap_g.begin()
    load_gate.wait()
    keeps = [
        pltpu.make_async_copy(tok_in, tok.at[seq.here], local_s.at[0]),
        pltpu.make_async_copy(x_part, w_x.at[seg.here], local_s.at[1]),
        pltpu.make_async_copy(small, small_all.at[seg.here], local_s.at[2]),
        pltpu.make_async_copy(g_own, g_part.at[seq.here], local_s.at[3]),
    ]
    for keep in keeps:
        keep.start()
    for k in range(1, max(seg.lines, seq.lines)):
        if k < seg.lines:
            pieces[0].step(k)
            smalls.step(k)
            for piece in pieces[1:]:
                piece.step(k)
        if k < seq.lines:
            toks.step(k)
    toks.finish()
    smalls.finish()
    for piece in pieces:
        piece.finish()
    swap_g.arrived()
    swap_x.drain()
    swap_g.drain()
    for keep in keeps:
        keep.wait()


def gather_start(shape, scaled_x, scaled_g, small, tokens):
    lines, fast, seq_lines = shape
    segs, seqs = lines * fast, seq_lines * 2
    rows, feats = scaled_x.shape[1:]
    sems = Gather.semaphores

    def kernel(*refs):
        ins, rest = refs[:11], refs[11:]
        gather_kernel(
            shape, *ins, rest[0], rest[1:7], rest[7:13], rest[13:15], rest[15:17], rest[17:]
        )

    w_x, small_all, tok, g_part = pl.pallas_call(
        kernel,
        in_specs=[ANY, ANY, INSIDE, ANY],
        out_specs=[ANY] * 4,
        out_shape=[
            jax.ShapeDtypeStruct((segs, seqs, rows, feats), BF16),
            jax.ShapeDtypeStruct((segs,) + small.shape, BF16),
            jax.ShapeDtypeStruct((seqs,) + tokens.shape, BF16),
            jax.ShapeDtypeStruct((seqs,) + scaled_g.shape[1:], BF16),
        ],
        scratch_shapes=[
            pltpu.VMEM((seqs, rows, feats), BF16),
            pltpu.VMEM(tokens.shape, BF16),
            pltpu.VMEM(scaled_g.shape[1:], BF16),
            pltpu.SemaphoreType.DMA((4,)),
            *sems(lines, fast), *sems(seq_lines, 2),
            *Exchange.semaphores(seqs), *Exchange.semaphores(seqs),
            *(sems(lines, fast) * seqs),
        ],
        compiler_params=comm_params(1),
        name="gather_start",
    )(scaled_x, scaled_g, small, tokens)
    return w_x.reshape(-1, feats), small_all, tok.reshape(-1, tokens.shape[1]), g_part


def front_kernel(
    shape, steps, taps, history, width,
    tok_ref, wx_ref, small_ref, head_ref, gate_src,
    x_ref, act_ref, wdt_ref, wxt_ref, par_ref, a2_ref, low_ref, bc_ref, gate_out,
    xb, mix_s, mix, local_s, *scratch,
):
    seg, seq = grids(shape)
    step = pl.program_id(0)
    gates = Gather(seg, gate_src.at[:, 0], gate_out, scratch[:6])
    count = tok_ref.shape[0]
    low_rank = wdt_ref.shape[0]
    mixes = wxt_ref.shape[0]
    feats = wx_ref.shape[1]
    part = small_ref.shape[2]

    @pl.when(step == 0)
    def _():
        meet((seg, seq))
        gates.begin()
        xb[pl.ds(0, 8), :] = head_ref[...]
        for g in range(small_ref.shape[0]):
            cols = slice(g * part, (g + 1) * part)
            wdt_ref[:, cols] = small_ref[g, pl.ds(0, low_rank), :]
            wxt_ref[:, cols] = small_ref[g, pl.ds(low_rank, mixes), :]
            rest = small_ref[g, pl.ds(low_rank + mixes, width + 16), :].astype(F32)
            par_ref[:, cols] = rest
        a_mat = -jnp.exp(par_ref[pl.ds(0, width), :])
        par_ref[pl.ds(0, width), :] = a_mat
        for s in range(feats // LANES):
            a2_ref[:, s, :] = a_mat[:, s * LANES : (s + 1) * LANES] * LOG2E

    kern = par_ref[pl.ds(width, 8), :]
    rows = tok_ref[...].astype(F32)
    rstd = lax.rsqrt(jnp.mean(rows * rows, axis=1, keepdims=True) + EPSILON)
    x_in = rstd * dot_nn(tok_ref[...], wx_ref[...])
    x_ref[...] = x_in
    xb[pl.ds(8, count), :] = x_in
    tall = 32
    chunk = min(512, feats)

    def through_conv(i, carry):
        t0 = pl.multiple_of(i * tall, tall)
        for c in range(0, feats, chunk):
            cols = slice(c, c + chunk)
            wide = xb[pl.ds(t0, tall + 8), pl.ds(c, chunk)]
            conv = kern[taps : taps + 1, cols]
            for k in range(taps):
                conv = conv + kern[k : k + 1, cols] * wide[8 - history + k : 8 - history + k + tall]
            act_ref[pl.ds(t0, tall), pl.ds(c, chunk)] = (conv * sigmoid(conv)).astype(BF16)
        return carry

    lax.fori_loop(0, count // tall, through_conv, 0)
    xb[pl.ds(0, 8), :] = xb[pl.ds(count, 8), :]
    mix_s[:, pl.ds(pl.multiple_of(step * count, count), count)] = dot_nt(wxt_ref[...], act_ref[...])
    for k in range(1, seg.lines - 1):

        @pl.when(step == min(steps - 1, 2 * k - 1))
        def _():
            gates.step(k)

    @pl.when(step == steps - 1)
    def _():
        sum_over_seq(seq, mix_s, mix, *scratch[6:])
        low_ref[...] = mix[pl.ds(0, low_rank), :]
        bc_ref[...] = mix[pl.ds(low_rank, 2 * width), :].astype(F32).T
        gates.step(seg.lines - 1)
        keep = pltpu.make_async_copy(gate_src.at[:, 0], gate_out.at[seg.here], local_s)
        keep.start()
        gates.finish()
        keep.wait()


def front(shape, taps, history, width, tok, w_x, small_all, head, gate_part, block):
    lines, fast, seq_lines = shape
    segs, seqs = lines * fast, seq_lines * 2
    length, model = tok.shape
    feats = w_x.shape[1]
    low_rank = LANES
    mixes = low_rank + 2 * width
    steps = length // block

    def whole(*dims):
        return pl.BlockSpec(dims, lambda i: (0,) * len(dims))

    def rows(columns):
        return pl.BlockSpec((block, columns), lambda i: (i, 0))

    one = pl.Buffered(1)
    return pl.pallas_call(
        functools.partial(front_kernel, shape, steps, taps, history, width),
        grid=(steps,),
        in_specs=[
            rows(model),
            pl.BlockSpec((model, feats), lambda i: (0, 0), pipeline_mode=one),
            whole(*small_all.shape), whole(*head.shape), ANY,
        ],
        out_specs=[
            rows(feats), rows(feats), whole(low_rank, feats), whole(mixes, feats),
            whole(width + 16, feats), whole(width, feats // LANES, LANES),
            whole(low_rank, length), whole(length, 2 * width), ANY,
        ],
        out_shape=[
            jax.ShapeDtypeStruct((length, feats), F32),
            jax.ShapeDtypeStruct((length, feats), BF16),
            jax.ShapeDtypeStruct((low_rank, feats), BF16),
            jax.ShapeDtypeStruct((mixes, feats), BF16),
            jax.ShapeDtypeStruct((width + 16, feats), F32),
            jax.ShapeDtypeStruct((width, feats // LANES, LANES), F32),
            jax.ShapeDtypeStruct((low_rank, length), BF16),
            jax.ShapeDtypeStruct((length, 2 * width), F32),
            jax.ShapeDtypeStruct((segs, seqs) + gate_part.shape[2:], BF16),
        ],
        scratch_shapes=[
            pltpu.VMEM((block + 8, feats), F32),
            pltpu.VMEM((mixes, length), F32),
            pltpu.VMEM((mixes, length), BF16),
            pltpu.SemaphoreType.DMA,
            *Gather.semaphores(lines, fast),
            *sum_scratch(seq_lines, mixes, length),
        ],
        compiler_params=comm_params(2),
        name="front",
    )(tok, w_x, small_all, head, gate_part)


def sum_scratch(seq_lines, rows, width):
    part = pltpu.VMEM((rows, width // 2), BF16)
    dma = pltpu.SemaphoreType.DMA
    return [
        part, part, part,
        pltpu.VMEM((max(seq_lines - 1, 1), rows, width // 2), BF16),
        pltpu.VMEM((2, rows, width // 2), BF16),
        dma, dma, dma((seq_lines,)), dma((seq_lines,)), dma, dma,
    ]


def unpack_kernel(
    seqs, taps, history, low_rank, width,
    small, halves, ends, mixed, input_grad, out_grad, weight, gain,
    mixed_o, final_o, final_c, input_o, start_o, start_c, gain_o, in_o, cw_o, cb_o, xp_o, dtp_o,
    dtb_o, a_o, skip_o, out_o,
):
    mixed_o[0] = mixed[...]
    input_o[0] = input_grad[...]
    out_o[...] = out_grad[...]
    part = small.shape[1]
    columns = xp_o.shape[0]
    dtp_o[...] = small[pl.ds(0, low_rank), :]
    xp_o[...] = small[pl.ds(low_rank, columns), :]
    at = low_rank + columns
    a_o[...] = small[pl.ds(at, width), :]
    lines = small[pl.ds(at + width, 16), :]
    cw_o[...] = lines[:taps]
    cb_o[...] = lines[taps]
    dtb_o[...] = lines[taps + 1]
    skip_o[...] = lines[taps + 2]
    each = final_o.shape[2] // part // seqs
    for s in range(seqs):
        rows = ends[s]
        for g in range(each):
            got = rows[:, g * part : (g + 1) * part]
            cols = pl.ds((g * seqs + s) * part, part)
            final_o[0, :, cols] = got[:width]
            start_o[0, :, cols] = got[width + history : 2 * width + history]
            for r in range(history):
                final_c[r, :, cols] = got[width + r : width + r + 1]
                at = 2 * width + history + r
                start_c[r, :, cols] = got[at : at + 1]
    scale = gain[...]
    total = jnp.zeros((in_o.shape[0], part), F32)
    groups = halves.shape[3] // part
    for half in range(2):
        for s in range(seqs):
            for g in range(groups):
                raw = halves[half, s, :, g * part : (g + 1) * part].astype(F32)
                cols = pl.ds(((half * groups + g) * seqs + s) * part, part)
                in_o[:, cols] = raw * scale
                total = total + raw * weight[:, cols].astype(F32)
    gain_o[...] = jnp.sum(total.T, axis=0)


def unpack(taps, history, low_rank, width, small, halves, ends, mixed, input_grad, out_grad,
           weight, gain):
    seqs, own_rows, feats = halves.shape[1:]
    part = small.shape[1]
    model = mixed.shape[1]
    kept = ends.shape[2] * seqs
    f32 = lambda *dims: jax.ShapeDtypeStruct(dims, F32)
    args = (small, halves, ends, mixed, input_grad, out_grad, weight, gain)
    outs = [
        jax.ShapeDtypeStruct((1,) + mixed.shape, BF16),
        f32(1, width, kept), f32(history, 1, kept),
        jax.ShapeDtypeStruct((1,) + input_grad.shape, BF16),
        f32(1, width, kept), f32(history, 1, kept),
        f32(own_rows), f32(*weight.shape),
        f32(taps, part), f32(part), f32(low_rank + 2 * width, part), f32(low_rank, part),
        f32(part), f32(width, part), f32(part), f32(part, model),
    ]

    def whole(a):
        return pl.BlockSpec(
            a.shape, lambda i: (0,) * len(a.shape), pipeline_mode=pl.Buffered(1)
        )

    return pl.pallas_call(
        functools.partial(unpack_kernel, seqs, taps, history, low_rank, width),
        grid=(1,),
        in_specs=[whole(a) for a in args],
        out_specs=[whole(a) for a in outs],
        out_shape=outs,
        name="unpack",
    )(*args)


def body(
    tokens, norm_gain, in_proj, conv_weight, conv_bias, x_proj, dt_proj, dt_bias,
    a_log, d_skip, out_proj, init_state, init_conv, cotangent,
):
    segs, seqs = lax.axis_size("seg"), lax.axis_size("seq")
    place = lax.axis_index("seq")
    own_rows, both = in_proj.shape
    part = conv_bias.shape[0]
    feats = segs * part
    taps = conv_weight.shape[0]
    width = a_log.shape[0]
    low_rank = dt_proj.shape[0]
    planes = feats // LANES
    own_len, model = tokens.shape[1:]
    length = own_len * seqs
    block = 64
    seq_lines = seqs // 2
    shape = (segs // seq_lines, seq_lines, seq_lines)

    def mine(rows):
        shaped = rows.reshape(rows.shape[0], segs, seqs, part)
        return lax.dynamic_index_in_dim(shaped, place, 2, keepdims=False).reshape(
            rows.shape[0], feats
        )

    gain_col = norm_gain.astype(F32)[:, None]
    own_weight = in_proj.astype(F32)
    scaled = (own_weight * gain_col).astype(BF16)
    scaled = scaled.reshape(own_rows, 2, segs, seqs, part)
    scaled_x = scaled[:, 0].transpose(2, 0, 1, 3).reshape(seqs, own_rows, feats)
    scaled_g = scaled[:, 1].reshape(own_rows, 2, segs // 2, seqs, part).transpose(3, 1, 0, 2, 4)
    scaled_g = scaled_g.reshape(seqs, 2, own_rows, feats // 2)
    small = jnp.concatenate(
        [
            dt_proj, x_proj.T, a_log, conv_weight, conv_bias[None], dt_bias[None], d_skip[None],
        ],
        axis=0,
    )
    small = jnp.pad(small, ((0, -small.shape[0] % 16), (0, 0)))
    w_x_half, small_all, tok, g_part = gather_start(shape, scaled_x, scaled_g, small, tokens[0])
    history = init_conv.shape[1]
    head = jnp.pad(mine(init_conv[0]), ((8 - history, 0), (0, 0)))
    x_in, act, w_dt, w_xt, params, a2, dt_low, bc, w_g_one = front(
        shape, taps, history, width, tok, w_x_half, small_all, head, g_part, 4 * block
    )
    init = mine(init_state[0]).reshape(width, planes, LANES)
    slope, pre, checks, final, gate_act, gated, w_out, cot, w_g_two = forward_scan(
        shape, taps, dt_low, w_dt, params, act, bc, a2, init, out_proj, cotangent[0], tok,
        w_g_one, g_part, 2 * block,
    )
    w_out = w_out.reshape(feats, model)
    cot = cot.reshape(length, model)
    w_g_one = w_g_one.reshape(model, feats // 2)
    w_g_two = w_g_two.reshape(model, feats // 2)
    g_gated = dot_nt(cot, w_out)
    gy = g_gated * gate_act
    gs_gate = (g_gated * slope).astype(BF16)
    out_grad = dot_tn(gated, cot).astype(BF16)
    gate_grad = dot_tn(tok, gs_gate).astype(BF16)
    g_actp, a_sum, start, dtb_grad, skip_grad, dtp_grad, g_mixed, g_half, out_grad, mixed_out = (
        backward_scan(
            shape, taps, pre, act, gy, bc, a2, params, checks, w_dt, dt_low, tokens[0],
            gate_grad.reshape(segs, seqs * own_rows, feats),
            out_grad.reshape(segs, part, model),
            gated, w_out, 2 * block,
        )
    )
    grads, halves, input_grad, ends = finish_all(
        shape, taps, history,
        (g_actp, x_in, act, tok, w_x_half, w_g_one, w_g_two, gs_gate),
        (
            g_mixed, w_xt, head, params, dtp_grad, a_sum, dtb_grad, skip_grad, g_half,
            tokens[0], cotangent[0], final, start,
        ),
    )
    if part % LANES == 0:
        outs = list(
            unpack(
                taps, history, low_rank, width, grads, halves, ends, mixed_out, input_grad,
                out_grad, in_proj, gain_col,
            )
        )
        outs[2], outs[5], outs[10] = (
            outs[2].transpose(1, 0, 2), outs[5].transpose(1, 0, 2), outs[10].T
        )
        return tuple(outs)
    ends = (
        ends.reshape(seqs, ends.shape[1], segs // seqs, part)
        .transpose(1, 2, 0, 3)
        .reshape(ends.shape[1], feats)
    )
    raw_grad = (
        halves.reshape(2, seqs, own_rows, segs, part)
        .transpose(2, 0, 3, 1, 4)
        .reshape(own_rows, both)
        .astype(F32)
    )
    in_grad = raw_grad * gain_col
    gain_grad = jnp.sum(raw_grad * own_weight, axis=1)

    at = width + history
    xp_at = low_rank + x_proj.shape[1]
    return (
        mixed_out[None],
        ends[None, :width],
        ends[None, width:at],
        input_grad[None],
        ends[None, at : at + width],
        ends[None, at + width : at + width + history],
        gain_grad,
        in_grad,
        grads[xp_at + width : xp_at + width + taps],
        grads[xp_at + width + taps],
        grads[low_rank:xp_at].T,
        grads[:low_rank],
        grads[xp_at + width + taps + 1],
        grads[xp_at : xp_at + width],
        grads[xp_at + width + taps + 2],
        out_grad,
    )


def solution(mesh):
    spread = ("seg", "seq")
    placed = (
        P("seg", "seq", None),
        P(spread),
        P(spread, None),
        P(None, spread),
        P(spread),
        P(spread, None),
        P(None, spread),
        P(spread),
        P(None, spread),
        P(spread),
        P(spread, None),
        P("seg", None, None),
        P("seg", None, None),
        P("seg", "seq", None),
    )
    return jax.shard_map(
        body,
        mesh=mesh,
        in_specs=placed,
        out_specs=(
            P("seg", "seq", None),
            P("seg", None, "seq"),
            P("seg", None, "seq"),
            P("seg", "seq", None),
            P("seg", None, "seq"),
            P("seg", None, "seq"),
            P(spread),
            P(spread, None),
            P(None, spread),
            P(spread),
            P(spread, None),
            P(None, spread),
            P(spread),
            P(None, spread),
            P(spread),
            P(spread, None),
        ),
        check_vma=False,
    )
```
